32 devices in a mesh: ctx: 8 (over y, x, core), fsdp: 4 (over z).
Axes of the slice: x: 2, y: 2, z: 4, core: 2. Of those that a mesh axis runs over, the one named last changes fastest.
Arguments:
- tokens: bfloat16 [4, 2048, 960], P('fsdp', 'ctx'), may hold values from -6 to 6
- w_query: bfloat16 [960, 960], P('fsdp'), may hold values from -0.1875 to 0.1875
- w_key: bfloat16 [960, 320], P('fsdp'), may hold values from -0.1875 to 0.1875
- w_value: bfloat16 [960, 320], P('fsdp'), may hold values from -0.1875 to 0.1875
- w_out: bfloat16 [960, 960], P('fsdp'), may hold values from -2 to 2
- w_gate: bfloat16 [2560, 960], P('fsdp'), may hold values from -0.1875 to 0.1875
- w_up: bfloat16 [2560, 960], P('fsdp'), may hold values from -0.1875 to 0.1875
- w_down: bfloat16 [2560, 960], P('fsdp'), may hold values from -0.125 to 0.125
- gain_attn: bfloat16 [960], P('fsdp'), may hold values from 0.25 to 1.75
- gain_ffn: bfloat16 [960], P('fsdp'), may hold values from 0.25 to 1.75
- router: bfloat16 [960], P('fsdp'), may hold values from -0.125 to 0.125
- cotangent: bfloat16 [4, 2048, 960], P('fsdp', 'ctx'), may hold values from -6 to 6
- positions: int32 [4, 2048], P('fsdp', 'ctx'), may hold values from 0 to 2047, as said below
- lengths: int32 [4], P('fsdp'), may hold values from 1025 to 2048, as said below
- chosen: int32 [4, 2048], P('fsdp', 'ctx'), may hold values 0 or 1
Outputs:
- block_out: bfloat16 [4, 2048, 960], P('fsdp', 'ctx')
- grad_tokens: bfloat16 [4, 2048, 960], P('fsdp', 'ctx')
- grad_query: float32 [960, 960], P('fsdp')
- grad_key: float32 [960, 320], P('fsdp')
- grad_value: float32 [960, 320], P('fsdp')
- grad_out: float32 [960, 960], P('fsdp')
- grad_gate: float32 [2560, 960], P('fsdp')
- grad_up: float32 [2560, 960], P('fsdp')
- grad_down: float32 [2560, 960], P('fsdp')
- grad_gain_attn: float32 [960], P('fsdp')
- grad_gain_ffn: float32 [960], P('fsdp')
- grad_router: float32 [960], P('fsdp')
The draws below stay inside these ranges and needn't reach their ends.
Inputs may be any that keep to these rules, and one draw needn't show every extreme that they name: In each sequence every position from 0 to 2047 stands in exactly one slot. The 256 slots of each device along ctx hold, in order, the 128 positions of some block b and then those of block 15 - b, a block being a run of 128 positions; b differs between the devices of a sequence. `lengths`: one sequence of every draw is full.
All inputs are finite; a program needn't handle non-finite values. No bound on the sum of `chosen` on one device may be relied on, other than what follows from the above.
Results may differ from the reference program's by a relative error of at most 0.024.
Values may be sent and summed in bfloat16 or wider, within the bound.
A program may use at most 384 MiB of HBM per device.

```python
import jax
import jax.numpy as jnp
from jax import lax

D = 960
HEADS = 15
KV_HEADS = 5
HEAD = 64
FF = 2560
QD = 960
KVD = 320
SLOTS = 2048
SEQS = 4
BLK = 128
BLOCKS = 16


def draw_positions(key, part):
    dev_count = BLOCKS // 2

    def dealt(sequence):
        shuffle = jax.random.permutation(jax.random.fold_in(key, sequence), dev_count)
        inside = jnp.arange(BLK)[None, :]
        first_block = shuffle[:, None] * BLK + inside
        second_block = (BLOCKS - 1 - shuffle)[:, None] * BLK + inside
        return jnp.concatenate([first_block, second_block], 1).reshape(dev_count * 2 * BLK)
    return jax.vmap(dealt)(jnp.arange(SEQS)).astype(jnp.int32)


def draw_lengths(key, part):
    drawn = jax.random.randint(jax.random.fold_in(key, 11), (SEQS,), SLOTS // 2 + 1, SLOTS + 1)
    full_at = jax.random.randint(jax.random.fold_in(key, 12), (), 0, SEQS)
    return jnp.where(jnp.arange(SEQS) == full_at, SLOTS, drawn).astype(jnp.int32)


def with_ends(values, rng, smallest, high):
    dims = values.shape
    index_at = [jax.random.randint(jax.random.fold_in(rng, axis), (), 0, dims[axis]) for axis in range(len(dims))]
    values = values.at[tuple(index_at)].set(smallest)
    longest = dims.index(max(dims))
    index_at[longest] = (index_at[longest] + 1) % dims[longest]
    return values.at[tuple(index_at)].set(high)


def levels(stream_key, dims, shards, low, high):
    factor_of, own = 1.0, jax.random.fold_in(stream_key, 6)
    for dim, blocks in shards:
        steps = jnp.exp(jax.random.uniform(jax.random.fold_in(own, dim), (blocks,), jnp.float32, low / len(shards), high / len(shards)))
        factor_of = factor_of * jnp.repeat(steps, dims[dim] // blocks).reshape([-1 if axis == dim else 1 for axis in range(len(dims))])
    return factor_of


def noise(own_key, extent, deviation, limit, cuts=(), held_as=jnp.bfloat16):
    level = levels(own_key, extent, cuts, -0.22, 0.18) if cuts else 1.0
    values = jax.random.normal(own_key, extent, jnp.float32) * deviation * level
    return jnp.minimum(jnp.maximum(values, -limit), limit).astype(held_as)


def setup_inputs(seed: int = 0) -> dict:
    splits = jax.random.split(jax.random.key(seed), 16)
    return {
        "tokens": noise(splits[0], (SEQS, SLOTS, D), 1.0, 6.0, ((0, 4), (1, 8))),
        "w_query": noise(splits[1], (D, QD), D ** -0.5, 0.1875, ((0, 4),)),
        "w_key": noise(splits[2], (D, KVD), D ** -0.5, 0.1875, ((0, 4),)),
        "w_value": noise(splits[3], (D, KVD), D ** -0.5, 0.1875, ((0, 4),)),
        "w_out": noise(splits[4], (QD, D), (max(1, D * 16 // SLOTS)) ** -0.5, 2.0, ((0, 4),)),
        "w_gate": noise(splits[5], (FF, D), D ** -0.5, 0.1875, ((0, 4),)),
        "w_up": noise(splits[6], (FF, D), D ** -0.5, 0.1875, ((0, 4),)),
        "w_down": noise(splits[7], (FF, D), FF ** -0.5, 0.125, ((0, 4),)),
        "gain_attn": jnp.clip(1.0 + 0.15 * jax.random.normal(splits[8], (D,), jnp.float32), 0.25, 1.75).astype(jnp.bfloat16),
        "gain_ffn": jnp.clip(1.0 + 0.15 * jax.random.normal(splits[9], (D,), jnp.float32), 0.25, 1.75).astype(jnp.bfloat16),
        "router": noise(splits[10], (D,), (2 * D) ** -0.5, 0.125, ((0, 4),)),
        "cotangent": noise(splits[11], (SEQS, SLOTS, D), 1.0, 6.0, ((0, 4), (1, 8))),
        "positions": draw_positions(jax.random.fold_in(splits[15], 71), 0),
        "lengths": draw_lengths(jax.random.fold_in(splits[15], 71), 0),
        "chosen": with_ends((jax.random.randint(splits[14], (SEQS, SLOTS), 0, 3) < 2).astype(jnp.int32), jax.random.fold_in(splits[14], 1), 0, 1),
    }


@jax.custom_vjp
def low(v):
    return lax.optimization_barrier(v.astype(jnp.bfloat16)).astype(jnp.float32)

@jax.custom_vjp
def low_back(v):
    return v

def low_keep(v):
    return (low(v), None)

def low_pass(kept, grad):
    return (grad,)

def back_keep(v):
    return (v, None)

def back_low(kept, grad):
    return (low(grad),)
low.defvjp(low_keep, low_pass)
low_back.defvjp(back_keep, back_low)
epsilon = 1e-05
negative = -1e+30
highest = lax.Precision.HIGHEST

def rope_tables(positions):
    half_dim = HEAD // 2
    frequency = 10000.0 ** (-2.0 * jnp.arange(half_dim, dtype=jnp.float32) / HEAD)
    angles = positions.astype(jnp.float32)[:, None] * frequency[None, :]
    cos_tab = jnp.cos(angles)
    sin_tab = jnp.sin(angles)
    return (jnp.concatenate([cos_tab, cos_tab], -1), jnp.concatenate([sin_tab, sin_tab], -1))

def rotate(values, cos_tab, sin_tab):
    half_dim = values.shape[-1] // 2
    turned = jnp.concatenate([-values[..., half_dim:], values[..., :half_dim]], -1)
    return values * cos_tab[:, None, :] + turned * sin_tab[:, None, :]

def sequence_forward(hidden, positions, live_mask, selected, params):
    w_query, w_key, w_value, w_out, w_gate, w_up, w_down, gain_attn, gain_ffn, router = params
    row_count = hidden.shape[0]
    groups = HEADS // KV_HEADS
    cos_tab, sin_tab = rope_tables(positions)
    inv_one = lax.rsqrt(lax.optimization_barrier(jnp.mean(hidden * hidden, -1, keepdims=True)) + epsilon)
    normed_one = low(hidden * inv_one * gain_attn)
    query_raw = low_back(jnp.dot(normed_one, w_query, precision=highest))
    queries = low(rotate(query_raw.reshape(row_count, HEADS, HEAD), cos_tab, sin_tab))
    key_raw = low_back(jnp.dot(normed_one, w_key, precision=highest))
    key_rot = low(rotate(key_raw.reshape(row_count, KV_HEADS, HEAD), cos_tab, sin_tab))
    value_proj = low(low_back(jnp.dot(normed_one, w_value, precision=highest))).reshape(row_count, KV_HEADS, HEAD)
    block_rows = min(512, row_count)
    query_blocks = queries.reshape(row_count // block_rows, block_rows, KV_HEADS, groups, HEAD)
    position_blocks = positions.reshape(row_count // block_rows, block_rows)

    def attend(inputs):
        query_block, position_block = inputs
        scores = low_back(jnp.einsum('qngd,knd->qngk', query_block, key_rot, precision=highest) * 0.125)
        earlier = positions[None, :] <= position_block[:, None]
        usable = selected[None, :] | (positions[None, :] == position_block[:, None])
        allowed = (earlier & usable)[:, None, None, :]
        masked = jnp.where(allowed, scores, negative)
        row_max = lax.optimization_barrier(jnp.max(masked, -1, keepdims=True))
        weights = jnp.where(allowed, jnp.exp(masked - row_max), 0.0)
        weights = low(weights / lax.optimization_barrier(jnp.sum(weights, -1, keepdims=True)))
        return jnp.einsum('qngk,knd->qngd', weights, value_proj, precision=highest)
    attended = low_back(lax.map(jax.checkpoint(attend), (query_blocks, position_blocks)).reshape(row_count, HEADS * HEAD))
    outcome = low(attended)
    branch = low_back(jnp.dot(outcome, w_out, precision=highest))
    middle = hidden + branch
    inv_two = lax.rsqrt(lax.optimization_barrier(jnp.mean(middle * middle, -1, keepdims=True)) + epsilon)
    normed_two = low(middle * inv_two * gain_ffn)
    gate_proj = low_back(jnp.dot(normed_two, w_gate.T, precision=highest))
    up_proj = low_back(jnp.dot(normed_two, w_up.T, precision=highest))
    inner_act = low(jax.nn.silu(gate_proj) * up_proj)
    ffn_out = low_back(jnp.dot(inner_act, w_down, precision=highest))
    gating = jax.nn.sigmoid(lax.optimization_barrier(jnp.sum(hidden * router, -1, keepdims=True)))
    chosen_mask = selected.astype(jnp.float32)[:, None]
    return live_mask[:, None] * (hidden + chosen_mask * gating * (branch + ffn_out))

def reference(tokens, w_query, w_key, w_value, w_out, w_gate, w_up, w_down, gain_attn, gain_ffn, router, cotangent, positions, lengths, chosen):
    live = positions < lengths[:, None]
    selected = live & (chosen == 1)
    live_mask = live.astype(jnp.float32)
    params = (w_query.astype(jnp.float32), w_key.astype(jnp.float32), w_value.astype(jnp.float32), w_out.astype(jnp.float32), w_gate.astype(jnp.float32), w_up.astype(jnp.float32), w_down.astype(jnp.float32), gain_attn.astype(jnp.float32), gain_ffn.astype(jnp.float32), router.astype(jnp.float32))

    def forward(hidden, weights_all):
        outputs = [sequence_forward(hidden[sequence], positions[sequence], live_mask[sequence], selected[sequence], weights_all) for sequence in range(SEQS)]
        return jnp.stack(outputs)
    result, pullback = jax.vjp(forward, tokens.astype(jnp.float32), params)
    grad_hidden, grads = pullback(cotangent.astype(jnp.float32))
    return (result.astype(jnp.bfloat16), grad_hidden.astype(jnp.bfloat16), grads[0], grads[1], grads[2], grads[3], grads[4], grads[5], grads[6], grads[7], grads[8], grads[9])
```

```python
import jax
import jax.numpy as jnp
from jax import lax
from jax.sharding import PartitionSpec as P

HEADS = 15
KV_HEADS = 5
HEAD = 64


epsilon = 1e-05
negative = -1e30
across_rows = (((0,), (0,)), ((), ()))
across_cols = (((1,), (1,)), ((), ()))


def rope_tables(positions):
    half_dim = HEAD // 2
    frequency = 10000.0 ** (-2.0 * jnp.arange(half_dim, dtype=jnp.float32) / HEAD)
    angles = positions.astype(jnp.float32)[:, None] * frequency[None, :]
    cos_tab = jnp.cos(angles)
    sin_tab = jnp.sin(angles)
    return (jnp.concatenate([cos_tab, cos_tab], -1), jnp.concatenate([sin_tab, sin_tab], -1))


def rotate(values, cos_tab, sin_tab):
    half_dim = values.shape[-1] // 2
    turned = jnp.concatenate([-values[..., half_dim:], values[..., :half_dim]], -1)
    return values * cos_tab[:, None, :] + turned * sin_tab[:, None, :]


def norm_forward(values, gain_vec):
    inv_rms = lax.rsqrt(jnp.mean(values * values, -1, keepdims=True) + epsilon)
    return (values * inv_rms * gain_vec, inv_rms)


def norm_backward(values, inv_rms, gain_vec, grad_normed):
    weighted = gain_vec * grad_normed
    grad_gain = jnp.sum(grad_normed * values * inv_rms, 0)
    cubed = inv_rms * inv_rms * inv_rms
    grad_values = inv_rms * weighted - values * cubed * jnp.mean(
        weighted * values, -1, keepdims=True
    )
    return (grad_values, grad_gain)


def allowed_mask(query_pos, key_tags):
    key_pos = jnp.where(key_tags >= 0, key_tags, -key_tags - 1)
    earlier = key_pos[None, :] <= query_pos[:, None]
    usable = (key_tags[None, :] >= 0) | (key_pos[None, :] == query_pos[:, None])
    return (earlier & usable)[:, None, None, :]


def forward_step(carried, portion, query_heads, query_pos):
    acc_out, running_max, summed = carried
    key_piece, value_piece, key_tags = portion
    piece_rows = key_piece.shape[0]
    key_heads = key_piece.reshape(piece_rows, KV_HEADS, HEAD)
    value_heads = value_piece.reshape(piece_rows, KV_HEADS, HEAD)
    scores = (
        jnp.einsum("qngd,knd->qngk", query_heads, key_heads, preferred_element_type=jnp.float32)
        * 0.125
    )
    allowed = allowed_mask(query_pos, key_tags)
    new_max = jnp.maximum(running_max, jnp.max(jnp.where(allowed, scores, negative), -1))
    weights = jnp.exp(jnp.where(allowed, scores - new_max[..., None], negative))
    summed = jnp.sum(weights, -1)
    weights_low = weights.astype(jnp.bfloat16)
    acc_out = jnp.einsum(
        "qngk,knd->qngd", weights_low, value_heads, preferred_element_type=jnp.float32
    )
    return (acc_out, new_max, summed)


def backward_step(portion, query_heads, query_pos, grad_heads, log_total, row_delta):
    key_piece, value_piece, key_tags = portion
    piece_rows = key_piece.shape[0]
    key_heads = key_piece.reshape(piece_rows, KV_HEADS, HEAD)
    value_heads = value_piece.reshape(piece_rows, KV_HEADS, HEAD)
    scores = (
        jnp.einsum("qngd,knd->qngk", query_heads, key_heads, preferred_element_type=jnp.float32)
        * 0.125
    )
    allowed = allowed_mask(query_pos, key_tags)
    softmax_w = jnp.exp(jnp.where(allowed, scores - log_total[..., None], negative))
    grad_probs = jnp.einsum(
        "qngd,knd->qngk", grad_heads, value_heads, preferred_element_type=jnp.float32
    )
    grad_scores = (softmax_w * (grad_probs - row_delta[..., None])).astype(jnp.bfloat16)
    probs_low = softmax_w.astype(jnp.bfloat16)
    grad_qrot = 0.125 * jnp.einsum(
        "qngk,knd->qngd", grad_scores, key_heads, preferred_element_type=jnp.float32
    )
    key_part = 0.125 * jnp.einsum(
        "qngk,qngd->knd", grad_scores, query_heads, preferred_element_type=jnp.float32
    )
    value_part = jnp.einsum(
        "qngk,qngd->knd", probs_low, grad_heads, preferred_element_type=jnp.float32
    )
    key_part = key_part.reshape(piece_rows, KV_HEADS * HEAD)
    value_part = value_part.reshape(piece_rows, KV_HEADS * HEAD)
    return (grad_qrot, key_part, value_part)


def ffn_both(normed, grad_mixed, gate_rows, up_rows, down_rows):
    gate_proj = lax.dot_general(normed, gate_rows, across_cols, preferred_element_type=jnp.float32)
    up_proj = lax.dot_general(normed, up_rows, across_cols, preferred_element_type=jnp.float32)
    sigma = jax.nn.sigmoid(gate_proj)
    activated = gate_proj * sigma
    inner_act = (activated * up_proj).astype(jnp.bfloat16)
    grad_inner = lax.dot_general(
        grad_mixed, down_rows, across_cols, preferred_element_type=jnp.float32
    )
    grad_gate_act = (grad_inner * up_proj * sigma * (1.0 + gate_proj * (1.0 - sigma))).astype(
        jnp.bfloat16
    )
    grad_up_act = (grad_inner * activated).astype(jnp.bfloat16)
    grad_normed = jnp.dot(grad_gate_act, gate_rows, preferred_element_type=jnp.float32) + jnp.dot(
        grad_up_act, up_rows, preferred_element_type=jnp.float32
    )
    return (inner_act, grad_gate_act, grad_up_act, grad_normed.astype(jnp.bfloat16))


def on_device(
    tokens,
    w_query,
    w_key,
    w_value,
    w_out,
    w_gate,
    w_up,
    w_down,
    gain_attn,
    gain_ffn,
    router,
    cotangent,
    positions,
    lengths,
    chosen,
):
    hidden = tokens[0].astype(jnp.float32)
    row_count, width = hidden.shape
    groups = HEADS // KV_HEADS
    qdim = HEADS * HEAD
    kdim = KV_HEADS * HEAD
    query_pos = positions[0]
    live = query_pos < lengths[0]
    selected = live & (chosen[0] == 1)
    live_mask = live.astype(jnp.float32)[:, None]
    chosen_mask = selected.astype(jnp.float32)[:, None]
    cos_tab, sin_tab = rope_tables(query_pos)
    key_tags = jnp.where(selected, query_pos, -query_pos - 1)
    tags_all = lax.all_gather(key_tags, "ctx", axis=0, tiled=True)
    vectors = lax.all_gather(jnp.stack([gain_attn, gain_ffn, router]), "fsdp", axis=1, tiled=True)
    gain_one = vectors[0].astype(jnp.float32)
    gain_two = vectors[1].astype(jnp.float32)
    router_vec = vectors[2].astype(jnp.float32)
    w_qkv = lax.all_gather(
        jnp.concatenate([w_query, w_key, w_value], 1), "fsdp", axis=0, tiled=True
    )
    w_out_full = lax.all_gather(w_out, "fsdp", axis=0, tiled=True)
    gating = jax.nn.sigmoid(jnp.sum(hidden * router_vec, -1, keepdims=True))
    grad_y = cotangent[0].astype(jnp.float32) * live_mask
    grad_inc = grad_y * chosen_mask * gating
    grad_ffn = grad_inc.astype(jnp.bfloat16)
    grad_ffn_all = lax.all_gather(grad_ffn, "fsdp", axis=0, tiled=True)

    normed_one, inv_one = norm_forward(hidden, gain_one)
    normed_one = normed_one.astype(jnp.bfloat16)
    qkv_raw = jnp.dot(normed_one, w_qkv, preferred_element_type=jnp.float32)
    rotated = rotate(
        qkv_raw[:, : qdim + kdim].reshape(row_count, HEADS + KV_HEADS, HEAD), cos_tab, sin_tab
    ).astype(jnp.bfloat16)
    query_heads = rotated[:, :HEADS].reshape(row_count, KV_HEADS, groups, HEAD)
    key_rot = rotated[:, HEADS:].reshape(row_count, kdim)
    value_proj = qkv_raw[:, qdim + kdim :].astype(jnp.bfloat16)
    kv_all = lax.all_gather(
        jnp.concatenate([key_rot, value_proj], 1), "ctx", axis=0, tiled=True
    )
    portion = (kv_all[:, :kdim], kv_all[:, kdim:], tags_all)
    start_state = (None, jnp.full((row_count, KV_HEADS, groups), negative, jnp.float32), None)
    acc_out, running_max, summed = forward_step(start_state, portion, query_heads, query_pos)
    attended = acc_out / summed[..., None]
    log_total = running_max + jnp.log(summed)
    outcome = attended.reshape(row_count, qdim).astype(jnp.bfloat16)
    branch = jnp.dot(outcome, w_out_full, preferred_element_type=jnp.float32)
    middle = hidden + branch
    normed_two, inv_two = norm_forward(middle, gain_two)
    normed_two = normed_two.astype(jnp.bfloat16)
    normed_all = lax.all_gather(normed_two, "fsdp", axis=0, tiled=True)
    inner_act, grad_gate_act, grad_up_act, grad_normed_part = ffn_both(
        normed_all, grad_ffn_all, w_gate, w_up, w_down
    )
    grad_normed_two = lax.psum_scatter(
        grad_normed_part, "fsdp", scatter_dimension=0, tiled=True
    ).astype(jnp.float32)
    ffn_part = jnp.dot(inner_act, w_down, preferred_element_type=jnp.float32).astype(jnp.bfloat16)
    grad_wgate = lax.dot_general(
        grad_gate_act, normed_all, across_rows, preferred_element_type=jnp.float32
    )
    grad_wup = lax.dot_general(
        grad_up_act, normed_all, across_rows, preferred_element_type=jnp.float32
    )
    grad_wdown = lax.dot_general(
        inner_act, grad_ffn_all, across_rows, preferred_element_type=jnp.float32
    )
    low = jnp.bfloat16
    totals = tuple(
        lax.psum(grad.astype(low), "ctx") for grad in (grad_wgate, grad_wup, grad_wdown)
    )
    grad_middle, grad_gain_two = norm_backward(middle, inv_two, gain_two, grad_normed_two)
    ffn_part, grad_middle = lax.optimization_barrier((ffn_part, grad_middle))
    ffn_out = lax.psum_scatter(ffn_part, "fsdp", scatter_dimension=0, tiled=True).astype(
        jnp.float32
    )
    grad_branch = (grad_inc + grad_middle).astype(jnp.bfloat16)
    grad_attended = lax.dot_general(
        grad_branch, w_out_full, across_cols, preferred_element_type=jnp.float32
    ).astype(jnp.bfloat16)
    grad_wout = lax.dot_general(
        outcome, grad_branch, across_rows, preferred_element_type=jnp.float32
    )
    grad_heads = grad_attended.reshape(row_count, KV_HEADS, groups, HEAD)
    row_delta = jnp.sum(grad_heads.astype(jnp.float32) * attended, -1)
    grad_qrot, grad_keys_all, grad_values_all = backward_step(
        portion, query_heads, query_pos, grad_heads, log_total, row_delta
    )
    grad_kv = lax.psum_scatter(
        jnp.concatenate([grad_keys_all, grad_values_all], 1).astype(jnp.bfloat16),
        "ctx",
        scatter_dimension=0,
        tiled=True,
    ).astype(jnp.float32)
    increment = branch + ffn_out
    block_out = live_mask * (hidden + chosen_mask * gating * increment)
    grad_logit = (
        jnp.sum(grad_y * chosen_mask * increment, -1, keepdims=True) * gating * (1.0 - gating)
    )
    grad_router = jnp.sum(hidden * grad_logit, 0)
    grad_rotated = jnp.concatenate(
        [
            grad_qrot.reshape(row_count, HEADS, HEAD),
            grad_kv[:, :kdim].reshape(row_count, KV_HEADS, HEAD),
        ],
        1,
    )
    grad_qkv = jnp.concatenate(
        [
            rotate(grad_rotated, cos_tab, -sin_tab).reshape(row_count, qdim + kdim),
            grad_kv[:, kdim:],
        ],
        1,
    ).astype(jnp.bfloat16)
    grad_normed_one = lax.dot_general(
        grad_qkv, w_qkv, across_cols, preferred_element_type=jnp.float32
    )
    grad_wqkv = lax.dot_general(
        normed_one, grad_qkv, across_rows, preferred_element_type=jnp.float32
    )
    grad_hidden_one, grad_gain_one = norm_backward(hidden, inv_one, gain_one, grad_normed_one)
    grad_tokens = (grad_y + grad_logit * router_vec + grad_middle + grad_hidden_one).astype(
        jnp.bfloat16
    )
    own_out = lax.psum_scatter(grad_wout.astype(low), "fsdp", scatter_dimension=0, tiled=True)
    own_qkv = lax.psum_scatter(grad_wqkv.astype(low), "fsdp", scatter_dimension=0, tiled=True)
    own_out, own_qkv, *totals = lax.optimization_barrier((own_out, own_qkv, *totals))
    total_gate, total_up, total_down = (total.astype(jnp.float32) for total in totals)
    total_out = lax.psum(own_out, "ctx").astype(jnp.float32)
    total_qkv = lax.psum(own_qkv, "ctx").astype(jnp.float32)
    small = lax.psum(
        jnp.stack([grad_gain_one, grad_gain_two, grad_router]), ("ctx", "fsdp")
    )
    mine = lax.dynamic_slice_in_dim(
        small, lax.axis_index("fsdp") * gain_attn.shape[0], gain_attn.shape[0], 1
    )
    return (
        block_out.astype(jnp.bfloat16)[None],
        grad_tokens[None],
        total_qkv[:, :qdim],
        total_qkv[:, qdim : qdim + kdim],
        total_qkv[:, qdim + kdim :],
        total_out,
        total_gate,
        total_up,
        total_down,
        mine[0],
        mine[1],
        mine[2],
    )


def solution(mesh):
    in_specs = (
        P("fsdp", "ctx", None),
        P("fsdp", None),
        P("fsdp", None),
        P("fsdp", None),
        P("fsdp", None),
        P("fsdp", None),
        P("fsdp", None),
        P("fsdp", None),
        P("fsdp"),
        P("fsdp"),
        P("fsdp"),
        P("fsdp", "ctx", None),
        P("fsdp", "ctx"),
        P("fsdp"),
        P("fsdp", "ctx"),
    )
    out_specs = (
        P("fsdp", "ctx", None),
        P("fsdp", "ctx", None),
        P("fsdp", None),
        P("fsdp", None),
        P("fsdp", None),
        P("fsdp", None),
        P("fsdp", None),
        P("fsdp", None),
        P("fsdp", None),
        P("fsdp"),
        P("fsdp"),
        P("fsdp"),
    )
    return jax.shard_map(
        on_device, mesh=mesh, in_specs=in_specs, out_specs=out_specs, check_vma=False
    )
```

```python
import functools

import jax
import jax.numpy as jnp
from jax import lax
from jax.experimental import pallas as pl
from jax.experimental.pallas import tpu as pltpu
from jax.sharding import PartitionSpec as P

HEADS = 15
KV_HEADS = 5
HEAD = 64


epsilon = 1e-05
negative = -1e30
across_rows = (((0,), (0,)), ((), ()))
across_cols = (((1,), (1,)), ((), ()))


def rope_tables(positions):
    half_dim = HEAD // 2
    frequency = 10000.0 ** (-2.0 * jnp.arange(half_dim, dtype=jnp.float32) / HEAD)
    angles = positions.astype(jnp.float32)[:, None] * frequency[None, :]
    cos_tab = jnp.cos(angles)
    sin_tab = jnp.sin(angles)
    return (jnp.concatenate([cos_tab, cos_tab], -1), jnp.concatenate([sin_tab, sin_tab], -1))


def rotate(values, cos_tab, sin_tab):
    half_dim = values.shape[-1] // 2
    turned = jnp.concatenate([-values[..., half_dim:], values[..., :half_dim]], -1)
    return values * cos_tab[:, None, :] + turned * sin_tab[:, None, :]


def norm_forward(values, gain_vec):
    inv_rms = lax.rsqrt(jnp.mean(values * values, -1, keepdims=True) + epsilon)
    return (values * inv_rms * gain_vec, inv_rms)


def norm_backward(values, inv_rms, gain_vec, grad_normed):
    weighted = gain_vec * grad_normed
    grad_gain = jnp.sum(grad_normed * values * inv_rms, 0)
    cubed = inv_rms * inv_rms * inv_rms
    grad_values = inv_rms * weighted - values * cubed * jnp.mean(
        weighted * values, -1, keepdims=True
    )
    return (grad_values, grad_gain)


def allowed_mask(query_pos, key_tags):
    key_pos = jnp.where(key_tags >= 0, key_tags, -key_tags - 1)
    earlier = key_pos[None, :] <= query_pos[:, None]
    usable = (key_tags[None, :] >= 0) | (key_pos[None, :] == query_pos[:, None])
    return (earlier & usable)[:, None, None, :]


def forward_step(carried, portion, query_heads, query_pos):
    acc_out, running_max, summed = carried
    key_piece, value_piece, key_tags = portion
    piece_rows = key_piece.shape[0]
    key_heads = key_piece.reshape(piece_rows, KV_HEADS, HEAD)
    value_heads = value_piece.reshape(piece_rows, KV_HEADS, HEAD)
    scores = (
        jnp.einsum("qngd,knd->qngk", query_heads, key_heads, preferred_element_type=jnp.float32)
        * 0.125
    )
    allowed = allowed_mask(query_pos, key_tags)
    new_max = jnp.maximum(running_max, jnp.max(jnp.where(allowed, scores, negative), -1))
    weights = jnp.exp(jnp.where(allowed, scores - new_max[..., None], negative))
    summed = jnp.sum(weights, -1)
    weights_low = weights.astype(jnp.bfloat16)
    acc_out = jnp.einsum(
        "qngk,knd->qngd", weights_low, value_heads, preferred_element_type=jnp.float32
    )
    return (acc_out, new_max, summed)


def backward_step(portion, query_heads, query_pos, grad_heads, log_total, row_delta):
    key_piece, value_piece, key_tags = portion
    piece_rows = key_piece.shape[0]
    key_heads = key_piece.reshape(piece_rows, KV_HEADS, HEAD)
    value_heads = value_piece.reshape(piece_rows, KV_HEADS, HEAD)
    scores = (
        jnp.einsum("qngd,knd->qngk", query_heads, key_heads, preferred_element_type=jnp.float32)
        * 0.125
    )
    allowed = allowed_mask(query_pos, key_tags)
    softmax_w = jnp.exp(jnp.where(allowed, scores - log_total[..., None], negative))
    grad_probs = jnp.einsum(
        "qngd,knd->qngk", grad_heads, value_heads, preferred_element_type=jnp.float32
    )
    grad_scores = (softmax_w * (grad_probs - row_delta[..., None])).astype(jnp.bfloat16)
    probs_low = softmax_w.astype(jnp.bfloat16)
    grad_qrot = 0.125 * jnp.einsum(
        "qngk,knd->qngd", grad_scores, key_heads, preferred_element_type=jnp.float32
    )
    key_part = 0.125 * jnp.einsum(
        "qngk,qngd->knd", grad_scores, query_heads, preferred_element_type=jnp.float32
    )
    value_part = jnp.einsum(
        "qngk,qngd->knd", probs_low, grad_heads, preferred_element_type=jnp.float32
    )
    key_part = key_part.reshape(piece_rows, KV_HEADS * HEAD)
    value_part = value_part.reshape(piece_rows, KV_HEADS * HEAD)
    return (grad_qrot, key_part, value_part)


def padded_to(values, row_dim):
    pads = [(0, 0)] * values.ndim
    pads[row_dim] = (0, -values.shape[row_dim] % 128)
    pads[-1] = (0, -values.shape[-1] % 128)
    return jnp.pad(values, pads)


def ffn_both(normed, grad_mixed, gate_rows, up_rows, down_rows):
    gate_proj = lax.dot_general(normed, gate_rows, across_cols, preferred_element_type=jnp.float32)
    up_proj = lax.dot_general(normed, up_rows, across_cols, preferred_element_type=jnp.float32)
    sigma = jax.nn.sigmoid(gate_proj)
    activated = gate_proj * sigma
    inner_act = (activated * up_proj).astype(jnp.bfloat16)
    grad_inner = lax.dot_general(
        grad_mixed, down_rows, across_cols, preferred_element_type=jnp.float32
    )
    grad_gate_act = (grad_inner * up_proj * sigma * (1.0 + gate_proj * (1.0 - sigma))).astype(
        jnp.bfloat16
    )
    grad_up_act = (grad_inner * activated).astype(jnp.bfloat16)
    grad_normed = jnp.dot(grad_gate_act, gate_rows, preferred_element_type=jnp.float32) + jnp.dot(
        grad_up_act, up_rows, preferred_element_type=jnp.float32
    )
    return (inner_act, grad_gate_act, grad_up_act, grad_normed.astype(jnp.bfloat16))


CHIPS = 4
SPAN = 2 * CHIPS
VMEM_BYTES = 60 * 1024 * 1024
MESH = pl.DeviceIdType.MESH


def plane_of():
    me = lax.axis_index("ctx")
    core = lax.rem(me, 2)
    chip = me // 2
    return me, core, chip, me + 1 - 2 * core


def chip_at(chip, core, step):
    return 2 * lax.rem(chip + step + CHIPS, CHIPS) + core


def greet(devices):
    barrier = pltpu.get_barrier_semaphore()
    for device in devices:
        pl.semaphore_signal(barrier, inc=1, device_id=device, device_id_type=MESH)
    pl.semaphore_wait(barrier, len(devices))


def send(src, dst, send_sem, recv_sem, device):
    copy = pltpu.make_async_remote_copy(
        src_ref=src,
        dst_ref=dst,
        send_sem=send_sem,
        recv_sem=recv_sem,
        device_id=device,
        device_id_type=MESH,
    )
    copy.start()
    return copy


def comm_params(number):
    return pltpu.CompilerParams(
        collective_id=number, has_side_effects=True, vmem_limit_bytes=VMEM_BYTES
    )


def comm_cost(moved):
    return pl.CostEstimate(flops=0, bytes_accessed=moved * 30, transcendentals=0)


def in_vmem(count):
    return [pl.BlockSpec(memory_space=pltpu.VMEM)] * count


def gather_rows_kernel(depth, own_ref, out_ref, z_sems, p_sems, f_sems):
    me, core, chip, partner = plane_of()
    layer = lax.axis_index("fsdp")
    layers = [lax.rem(layer + d, depth) for d in range(1, depth)]
    peers = [chip_at(chip, core, j) for j in range(1, CHIPS)]
    greet([(me, other) for other in layers] + [(peer, layer) for peer in peers + [partner]])
    first = [
        send(own_ref.at[me], out_ref.at[layer, me], z_sems.at[0, d], z_sems.at[1, d], (me, other))
        for d, other in enumerate(layers)
    ]
    for piece in range(SPAN):
        out_ref[layer, piece] = own_ref[piece]
    spread = []
    for d, copy in enumerate(first):
        copy.wait_recv()
        source = lax.rem(layer + depth - d - 1, depth)
        for j, peer in enumerate(peers):
            block = out_ref.at[source, me]
            spread.append(
                send(block, block, p_sems.at[0, d, j], p_sems.at[1, d, j], (peer, layer))
            )
        block = out_ref.at[source, me]
        first[d] = (
            copy,
            send(block, block, f_sems.at[0, d, 3], f_sems.at[1, d, 3], (partner, layer)),
        )
    passed = []
    for d in range(depth - 1):
        source = lax.rem(layer + depth - d - 1, depth)
        for j in range(CHIPS - 1):
            spread[d * (CHIPS - 1) + j].wait_recv()
            block = out_ref.at[source, chip_at(chip, core, -j - 1)]
            passed.append(
                send(block, block, f_sems.at[0, d, j], f_sems.at[1, d, j], (partner, layer))
            )
    for copy, handed in first:
        copy.wait_send()
        handed.wait()
    for copy in spread:
        copy.wait_send()
    for copy in passed:
        copy.wait()


def gather_rows(own, depth):
    if lax.axis_size("ctx") != SPAN:
        return lax.all_gather(own, "fsdp", axis=0)
    rows, columns = own.shape
    piece = rows // SPAN
    return pl.pallas_call(
        functools.partial(gather_rows_kernel, depth),
        out_shape=jax.ShapeDtypeStruct((depth, SPAN, piece, columns), own.dtype),
        in_specs=in_vmem(1),
        out_specs=in_vmem(1)[0],
        scratch_shapes=[
            pltpu.SemaphoreType.DMA((2, depth - 1)),
            pltpu.SemaphoreType.DMA((2, depth - 1, CHIPS - 1)),
            pltpu.SemaphoreType.DMA((2, depth - 1, CHIPS)),
        ],
        compiler_params=comm_params(1),
        cost_estimate=comm_cost(own.size * 2 * depth),
    )(own.reshape(SPAN, piece, columns)).reshape(depth, rows, columns)


def gather_plane_kernel(kv_ref, tag_ref, kv_out, tag_out, p_sems, f_sems):
    me, core, chip, partner = plane_of()
    layer = lax.axis_index("fsdp")
    peers = [chip_at(chip, core, j) for j in range(1, CHIPS)]
    greet([(peer, layer) for peer in peers + [partner]])
    pairs = ((kv_ref, kv_out), (tag_ref, tag_out))
    spread, passed = [], []
    for j, peer in enumerate(peers):
        for a, (own, out) in enumerate(pairs):
            spread.append(
                send(own, out.at[me], p_sems.at[0, a, j], p_sems.at[1, a, j], (peer, layer))
            )
    for a, (own, out) in enumerate(pairs):
        passed.append(
            send(own, out.at[me], f_sems.at[0, a, 3], f_sems.at[1, a, 3], (partner, layer))
        )
    kv_out[me] = kv_ref[...]
    tag_out[me] = tag_ref[...]
    for j in range(CHIPS - 1):
        for a, (own, out) in enumerate(pairs):
            spread[2 * j + a].wait_recv()
            block = out.at[chip_at(chip, core, -j - 1)]
            passed.append(
                send(block, block, f_sems.at[0, a, j], f_sems.at[1, a, j], (partner, layer))
            )
    for copy in spread:
        copy.wait_send()
    for copy in passed:
        copy.wait()


def gather_plane(kv, tags):
    if lax.axis_size("ctx") != SPAN:
        return tuple(lax.all_gather(part, "ctx", axis=0, tiled=True) for part in (kv, tags))
    rows, columns = kv.shape
    kv_all, tags_all = pl.pallas_call(
        gather_plane_kernel,
        out_shape=(
            jax.ShapeDtypeStruct((SPAN, rows, columns), kv.dtype),
            jax.ShapeDtypeStruct((SPAN, 1, rows), tags.dtype),
        ),
        in_specs=in_vmem(2),
        out_specs=tuple(in_vmem(2)),
        scratch_shapes=[
            pltpu.SemaphoreType.DMA((2, 2, CHIPS - 1)),
            pltpu.SemaphoreType.DMA((2, 2, CHIPS)),
        ],
        compiler_params=comm_params(2),
        cost_estimate=comm_cost(kv.size * 2 * SPAN),
    )(kv, tags[None])
    return kv_all.reshape(SPAN * rows, columns), tags_all.reshape(SPAN * rows)


def added(*parts):
    total = parts[0].astype(jnp.float32)
    for part in parts[1:]:
        total = total + part.astype(jnp.float32)
    return total


def reduce_plane(x_ref, axis, halves, sums, arrived, h_sems, p_sems, layer):
    me, core, chip, partner = plane_of()
    slabs = x_ref.shape[1 - axis]

    def piece_of(index):
        return x_ref.at[index] if axis == 0 else x_ref.at[:, index]

    handed, spread = [], []
    for j in range(CHIPS):
        slot = (j + 1) % CHIPS
        handed.append(
            send(
                piece_of(chip_at(chip, 1 - core, slot)),
                halves.at[slot],
                h_sems.at[0, slot],
                h_sems.at[1, slot],
                (partner, layer),
            )
        )
    for j in range(CHIPS):
        slot = (j + 1) % CHIPS
        handed[j].wait_recv()
        mine = chip_at(chip, core, slot)

        def add_half(slab, carry, slot=slot, mine=mine):
            sums[slot, slab] = added(piece_of(mine)[slab], halves[slot, slab]).astype(sums.dtype)
            return carry

        lax.fori_loop(0, slabs, add_half, 0)
        if slot:
            spread.append(
                send(
                    sums.at[slot],
                    arrived.at[slot - 1],
                    p_sems.at[0, slot - 1],
                    p_sems.at[1, slot - 1],
                    (mine, layer),
                )
            )
    for copy in spread:
        copy.wait_recv()
    return handed + spread


def reduce_plane_kernel(x_ref, out_ref, halves, sums, arrived, h_sems, p_sems):
    me, core, chip, partner = plane_of()
    layer = lax.axis_index("fsdp")
    greet([(chip_at(chip, core, j), layer) for j in range(1, CHIPS)] + [(partner, layer)])
    copies = reduce_plane(x_ref, 0, halves, sums, arrived, h_sems, p_sems, layer)

    def add_slab(slab, carry):
        out_ref[slab] = added(
            sums[0, slab], arrived[0, slab], arrived[1, slab], arrived[2, slab]
        )
        return carry

    lax.fori_loop(0, x_ref.shape[1], add_slab, 0)
    for copy in copies:
        copy.wait_send()


def plane_scratch(block, dtype):
    return [
        pltpu.VMEM((CHIPS, *block), dtype),
        pltpu.VMEM((CHIPS, *block), dtype),
        pltpu.VMEM((CHIPS - 1, *block), dtype),
        pltpu.SemaphoreType.DMA((2, CHIPS)),
        pltpu.SemaphoreType.DMA((2, CHIPS - 1)),
    ]


def scatter_plane(values):
    if lax.axis_size("ctx") != SPAN:
        own = lax.psum_scatter(values, "ctx", scatter_dimension=0, tiled=True)
        return own.astype(jnp.float32)
    rows, columns = values.shape
    slabs = 8
    block = (slabs, rows // SPAN // slabs, columns)
    return pl.pallas_call(
        reduce_plane_kernel,
        out_shape=jax.ShapeDtypeStruct(block, jnp.float32),
        in_specs=in_vmem(1),
        out_specs=in_vmem(1)[0],
        scratch_shapes=plane_scratch(block, values.dtype),
        compiler_params=comm_params(3),
        cost_estimate=comm_cost(values.size * 2),
    )(values.reshape(SPAN, *block)).reshape(rows // SPAN, columns)


def reduce_rows_kernel(
    depth, x_ref, out_ref, halves, sums, arrived, across, h_sems, p_sems, z_sems, g_sems, f_sems
):
    me, core, chip, partner = plane_of()
    layer = lax.axis_index("fsdp")
    layers = [lax.rem(layer + d, depth) for d in range(1, depth)]
    peers = [chip_at(chip, core, j) for j in range(1, CHIPS)]
    greet([(me, other) for other in layers] + [(peer, layer) for peer in peers + [partner]])
    copies = reduce_plane(x_ref, 1, halves, sums, arrived, h_sems, p_sems, layer)
    for d in list(range(1, depth)) + [0]:
        target = lax.rem(layer + d, depth)
        across[0, d] = added(
            sums[0, target], arrived[0, target], arrived[1, target], arrived[2, target]
        ).astype(across.dtype)
        if d:
            copies.append(
                send(
                    across.at[0, d],
                    across.at[1, d],
                    z_sems.at[0, d - 1],
                    z_sems.at[1, d - 1],
                    (me, target),
                )
            )
    for copy in copies[-(depth - 1) :]:
        copy.wait_recv()
    parts = [across[0, 0]] + [across[1, d] for d in range(1, depth)]
    out_ref[me] = added(*parts).astype(out_ref.dtype)
    spread, passed = [], []
    mine = out_ref.at[me]
    for j, peer in enumerate(peers):
        spread.append(send(mine, mine, g_sems.at[0, j], g_sems.at[1, j], (peer, layer)))
    passed.append(send(mine, mine, f_sems.at[0, 3], f_sems.at[1, 3], (partner, layer)))
    for j in range(CHIPS - 1):
        spread[j].wait_recv()
        block = out_ref.at[chip_at(chip, core, -j - 1)]
        passed.append(send(block, block, f_sems.at[0, j], f_sems.at[1, j], (partner, layer)))
    for copy in copies + spread:
        copy.wait_send()
    for copy in passed:
        copy.wait()


def reduce_rows(values, depth, number):
    if lax.axis_size("ctx") != SPAN:
        return lax.psum(lax.psum_scatter(values, "fsdp", scatter_dimension=0), "ctx")
    _, rows, columns = values.shape
    piece = rows // SPAN
    block = (depth, piece, columns)
    pieces = values.reshape(depth, SPAN, piece, columns)
    return pl.pallas_call(
        functools.partial(reduce_rows_kernel, depth),
        out_shape=jax.ShapeDtypeStruct((SPAN, piece, columns), values.dtype),
        in_specs=in_vmem(1),
        out_specs=in_vmem(1)[0],
        scratch_shapes=plane_scratch(block, values.dtype)[:3]
        + [pltpu.VMEM((2, depth, piece, columns), values.dtype)]
        + plane_scratch(block, values.dtype)[3:]
        + [
            pltpu.SemaphoreType.DMA((2, depth - 1)),
            pltpu.SemaphoreType.DMA((2, CHIPS - 1)),
            pltpu.SemaphoreType.DMA((2, CHIPS)),
        ],
        compiler_params=comm_params(number),
        cost_estimate=comm_cost(values.size * 2),
    )(pieces).reshape(rows, columns)


def on_device(
    tokens,
    w_query,
    w_key,
    w_value,
    w_out,
    w_gate,
    w_up,
    w_down,
    gain_attn,
    gain_ffn,
    router,
    cotangent,
    positions,
    lengths,
    chosen,
):
    hidden = tokens[0].astype(jnp.float32)
    row_count, width = hidden.shape
    groups = HEADS // KV_HEADS
    qdim = HEADS * HEAD
    kdim = KV_HEADS * HEAD
    query_pos = positions[0]
    live = query_pos < lengths[0]
    selected = live & (chosen[0] == 1)
    live_mask = live.astype(jnp.float32)[:, None]
    chosen_mask = selected.astype(jnp.float32)[:, None]
    cos_tab, sin_tab = rope_tables(query_pos)
    key_tags = jnp.where(selected, query_pos, -query_pos - 1)
    depth = lax.axis_size("fsdp")
    own_rows = w_query.shape[0]
    w_out_full = lax.all_gather(w_out, "fsdp", axis=0, tiled=True)
    vectors = jnp.stack([gain_attn, gain_ffn, router], 1)
    own_attn = padded_to(jnp.concatenate([w_query, w_key, w_value, vectors], 1), 0)
    gathered = gather_rows(own_attn, depth)[:, :own_rows]
    w_qkv = gathered[..., : qdim + 2 * kdim].reshape(width, qdim + 2 * kdim)
    vectors = gathered[..., qdim + 2 * kdim : qdim + 2 * kdim + 3].reshape(width, 3)
    gain_one, gain_two, router_vec = vectors.T.astype(jnp.float32)
    gating = jax.nn.sigmoid(jnp.sum(hidden * router_vec, -1, keepdims=True))
    grad_y = cotangent[0].astype(jnp.float32) * live_mask
    grad_inc = grad_y * chosen_mask * gating
    grad_ffn = grad_inc.astype(jnp.bfloat16)
    grad_ffn_all = lax.all_gather(grad_ffn, "fsdp", axis=0, tiled=True)

    normed_one, inv_one = norm_forward(hidden, gain_one)
    normed_one = normed_one.astype(jnp.bfloat16)
    qkv_raw = jnp.dot(normed_one, w_qkv, preferred_element_type=jnp.float32)
    rotated = rotate(
        qkv_raw[:, : qdim + kdim].reshape(row_count, HEADS + KV_HEADS, HEAD), cos_tab, sin_tab
    ).astype(jnp.bfloat16)
    query_heads = rotated[:, :HEADS].reshape(row_count, KV_HEADS, groups, HEAD)
    key_rot = rotated[:, HEADS:].reshape(row_count, kdim)
    value_proj = qkv_raw[:, qdim + kdim :].astype(jnp.bfloat16)
    kv_all, tags_all = gather_plane(jnp.concatenate([key_rot, value_proj], 1), key_tags)
    portion = (kv_all[:, :kdim], kv_all[:, kdim:], tags_all)
    start_state = (None, jnp.full((row_count, KV_HEADS, groups), negative, jnp.float32), None)
    acc_out, running_max, summed = forward_step(start_state, portion, query_heads, query_pos)
    attended = acc_out / summed[..., None]
    log_total = running_max + jnp.log(summed)
    attended, grad_ffn_all, w_out_full = lax.optimization_barrier(
        (attended, grad_ffn_all, w_out_full)
    )
    outcome = attended.reshape(row_count, qdim).astype(jnp.bfloat16)
    branch = jnp.dot(outcome, w_out_full, preferred_element_type=jnp.float32)
    middle = hidden + branch
    normed_two, inv_two = norm_forward(middle, gain_two)
    normed_two = normed_two.astype(jnp.bfloat16)
    normed_all = lax.all_gather(normed_two, "fsdp", axis=0, tiled=True)
    inner_act, grad_gate_act, grad_up_act, grad_normed_part = ffn_both(
        normed_all, grad_ffn_all, w_gate, w_up, w_down
    )
    grad_normed_two = lax.psum_scatter(
        grad_normed_part, "fsdp", scatter_dimension=0, tiled=True
    ).astype(jnp.float32)
    ffn_part = jnp.dot(inner_act, w_down, preferred_element_type=jnp.float32).astype(jnp.bfloat16)
    grad_wgate = lax.dot_general(
        grad_gate_act, normed_all, across_rows, preferred_element_type=jnp.float32
    )
    grad_wup = lax.dot_general(
        grad_up_act, normed_all, across_rows, preferred_element_type=jnp.float32
    )
    grad_wdown = lax.dot_general(
        inner_act, grad_ffn_all, across_rows, preferred_element_type=jnp.float32
    )
    low = jnp.bfloat16
    grad_normed_two, ffn_part, *grads = lax.optimization_barrier(
        (grad_normed_two, ffn_part, *(g.astype(low) for g in (grad_wgate, grad_wup, grad_wdown)))
    )
    ffn_out = lax.psum_scatter(ffn_part, "fsdp", scatter_dimension=0, tiled=True).astype(
        jnp.float32
    )
    totals = tuple(lax.psum(grad, "ctx") for grad in grads)
    grad_middle, grad_gain_two = norm_backward(middle, inv_two, gain_two, grad_normed_two)
    grad_branch = (grad_inc + grad_middle).astype(jnp.bfloat16)
    grad_attended = lax.dot_general(
        grad_branch, w_out_full, across_cols, preferred_element_type=jnp.float32
    ).astype(jnp.bfloat16)
    grad_wout = lax.dot_general(
        outcome, grad_branch, across_rows, preferred_element_type=jnp.float32
    )
    grad_heads = grad_attended.reshape(row_count, KV_HEADS, groups, HEAD)
    row_delta = jnp.sum(grad_heads.astype(jnp.float32) * attended, -1)
    grad_qrot, grad_keys_all, grad_values_all = backward_step(
        portion, query_heads, query_pos, grad_heads, log_total, row_delta
    )
    grad_kv = scatter_plane(
        jnp.concatenate([grad_keys_all, grad_values_all], 1).astype(jnp.bfloat16)
    )
    increment = branch + ffn_out
    block_out = live_mask * (hidden + chosen_mask * gating * increment)
    grad_logit = (
        jnp.sum(grad_y * chosen_mask * increment, -1, keepdims=True) * gating * (1.0 - gating)
    )
    grad_router = jnp.sum(hidden * grad_logit, 0)
    grad_rotated = jnp.concatenate(
        [
            grad_qrot.reshape(row_count, HEADS, HEAD),
            grad_kv[:, :kdim].reshape(row_count, KV_HEADS, HEAD),
        ],
        1,
    )
    grad_qkv = jnp.concatenate(
        [
            rotate(grad_rotated, cos_tab, -sin_tab).reshape(row_count, qdim + kdim),
            grad_kv[:, kdim:],
        ],
        1,
    ).astype(jnp.bfloat16)
    grad_normed_one = lax.dot_general(
        grad_qkv, w_qkv, across_cols, preferred_element_type=jnp.float32
    )
    grad_wqkv = lax.dot_general(
        normed_one, grad_qkv, across_rows, preferred_element_type=jnp.float32
    )
    grad_hidden_one, grad_gain_one = norm_backward(hidden, inv_one, gain_one, grad_normed_one)
    grad_tokens = (grad_y + grad_logit * router_vec + grad_middle + grad_hidden_one).astype(
        jnp.bfloat16
    )
    vectors = jnp.stack([grad_gain_one, grad_gain_two, grad_router], 1)
    grads = jnp.concatenate([grad_wqkv.astype(low), grad_wout.astype(low), vectors.astype(low)], 1)
    grads = grads.reshape(depth, own_rows, grads.shape[-1])
    owned = reduce_rows(padded_to(grads, 1), depth, 4)[:own_rows].astype(jnp.float32)
    total_gate, total_up, total_down = (total.astype(jnp.float32) for total in totals)
    ends = (0, qdim, qdim + kdim, qdim + 2 * kdim, qdim + 2 * kdim + width)
    total_q, total_k, total_v, total_out = (owned[:, a:b] for a, b in zip(ends, ends[1:]))
    mine = owned[:, ends[-1] : ends[-1] + 3].T
    return (
        block_out.astype(jnp.bfloat16)[None],
        grad_tokens[None],
        total_q,
        total_k,
        total_v,
        total_out,
        total_gate,
        total_up,
        total_down,
        mine[0],
        mine[1],
        mine[2],
    )


def solution(mesh):
    in_specs = (
        P("fsdp", "ctx", None),
        P("fsdp", None),
        P("fsdp", None),
        P("fsdp", None),
        P("fsdp", None),
        P("fsdp", None),
        P("fsdp", None),
        P("fsdp", None),
        P("fsdp"),
        P("fsdp"),
        P("fsdp"),
        P("fsdp", "ctx", None),
        P("fsdp", "ctx"),
        P("fsdp"),
        P("fsdp", "ctx"),
    )
    out_specs = (
        P("fsdp", "ctx", None),
        P("fsdp", "ctx", None),
        P("fsdp", None),
        P("fsdp", None),
        P("fsdp", None),
        P("fsdp", None),
        P("fsdp", None),
        P("fsdp", None),
        P("fsdp", None),
        P("fsdp"),
        P("fsdp"),
        P("fsdp"),
    )
    return jax.shard_map(
        on_device, mesh=mesh, in_specs=in_specs, out_specs=out_specs, check_vma=False
    )
```

```python
import functools

import jax
import jax.numpy as jnp
from jax import lax
from jax.experimental import pallas as pl
from jax.experimental.pallas import tpu as pltpu
from jax.sharding import PartitionSpec as P

HEADS = 15
KV_HEADS = 5
HEAD = 64


epsilon = 1e-05
negative = -1e30
across_rows = (((0,), (0,)), ((), ()))
across_cols = (((1,), (1,)), ((), ()))


def rope_tables(positions):
    half_dim = HEAD // 2
    frequency = 10000.0 ** (-2.0 * jnp.arange(half_dim, dtype=jnp.float32) / HEAD)
    angles = positions.astype(jnp.float32)[:, None] * frequency[None, :]
    return (jnp.cos(angles), jnp.sin(angles))


def rotate(values, cos_tab, sin_tab):
    slots, width = values.shape
    low, high = jnp.split(values.reshape(slots, width // HEAD, HEAD), 2, -1)
    cos_tab, sin_tab = cos_tab[:, None], sin_tab[:, None]
    turned = [low * cos_tab - high * sin_tab, high * cos_tab + low * sin_tab]
    return jnp.concatenate(turned, -1).reshape(slots, width)


def rotate_columns(values, cos_tab, sin_tab):
    width, slots = values.shape
    low, high = jnp.split(values.reshape(width // HEAD, HEAD, slots), 2, 1)
    cos_tab, sin_tab = cos_tab.T[None], sin_tab.T[None]
    turned = [low * cos_tab - high * sin_tab, high * cos_tab + low * sin_tab]
    return jnp.concatenate(turned, 1).reshape(width, slots)


def norm_forward(values, gain_vec):
    inv_rms = lax.rsqrt(jnp.mean(values * values, -1, keepdims=True) + epsilon)
    return (values * inv_rms * gain_vec, inv_rms)


def norm_backward(values, inv_rms, gain_vec, grad_normed):
    weighted = gain_vec * grad_normed
    grad_gain = jnp.sum(grad_normed * values * inv_rms, 0)
    cubed = inv_rms * inv_rms * inv_rms
    grad_values = inv_rms * weighted - values * cubed * jnp.mean(
        weighted * values, -1, keepdims=True
    )
    return (grad_values, grad_gain)


def padded_to(values, row_dim):
    pads = [(0, 0)] * values.ndim
    pads[row_dim] = (0, -values.shape[row_dim] % 128)
    return jnp.pad(values, pads)


def padded_rows_of(values, rows):
    return jnp.pad(values, ((0, 0), (0, rows - values.shape[1]), (0, 0)))


def ffn_both(normed, grad_mixed, gate_rows, up_rows, down_rows):
    gate_proj = lax.dot_general(normed, gate_rows, across_cols, preferred_element_type=jnp.float32)
    up_proj = lax.dot_general(normed, up_rows, across_cols, preferred_element_type=jnp.float32)
    sigma = jax.nn.sigmoid(gate_proj)
    activated = gate_proj * sigma
    inner_act = (activated * up_proj).astype(jnp.bfloat16)
    grad_inner = lax.dot_general(
        grad_mixed, down_rows, across_cols, preferred_element_type=jnp.float32
    )
    grad_gate_act = (grad_inner * up_proj * sigma * (1.0 + gate_proj * (1.0 - sigma))).astype(
        jnp.bfloat16
    )
    grad_up_act = (grad_inner * activated).astype(jnp.bfloat16)
    grad_normed = jnp.dot(grad_gate_act, gate_rows, preferred_element_type=jnp.float32) + jnp.dot(
        grad_up_act, up_rows, preferred_element_type=jnp.float32
    )
    return (inner_act, grad_gate_act, grad_up_act, grad_normed.astype(jnp.bfloat16))


CHIPS = 4
SPAN = 2 * CHIPS
VMEM_BYTES = 60 * 1024 * 1024
MESH = pl.DeviceIdType.MESH


def plane_of():
    me = lax.axis_index("ctx")
    core = lax.rem(me, 2)
    chip = me // 2
    return me, core, chip, me + 1 - 2 * core


def chip_at(chip, core, step):
    return 2 * lax.rem(chip + step + CHIPS, CHIPS) + core


def greet(devices):
    barrier = pltpu.get_barrier_semaphore()
    for device in devices:
        pl.semaphore_signal(barrier, inc=1, device_id=device, device_id_type=MESH)
    pl.semaphore_wait(barrier, len(devices))


def send(src, dst, send_sem, recv_sem, device):
    copy = pltpu.make_async_remote_copy(
        src_ref=src,
        dst_ref=dst,
        send_sem=send_sem,
        recv_sem=recv_sem,
        device_id=device,
        device_id_type=MESH,
    )
    copy.start()
    return copy


def comm_params(number):
    return pltpu.CompilerParams(
        collective_id=number, has_side_effects=True, vmem_limit_bytes=VMEM_BYTES
    )


def comm_cost(moved):
    return pl.CostEstimate(flops=0, bytes_accessed=moved * 30, transcendentals=0)


def in_vmem(count):
    return [pl.BlockSpec(memory_space=pltpu.VMEM)] * count


def gather_rows_kernel(depth, own_ref, out_ref, z_sems, p_sems, f_sems):
    me, core, chip, partner = plane_of()
    layer = lax.axis_index("fsdp")
    layers = [lax.rem(layer + d, depth) for d in range(1, depth)]
    peers = [chip_at(chip, core, j) for j in range(1, CHIPS)]
    greet([(me, other) for other in layers] + [(peer, layer) for peer in peers + [partner]])
    first = [
        send(own_ref.at[me], out_ref.at[layer, me], z_sems.at[0, d], z_sems.at[1, d], (me, other))
        for d, other in enumerate(layers)
    ]
    for piece in range(SPAN):
        out_ref[layer, piece] = own_ref[piece]
    spread = []
    for d, copy in enumerate(first):
        copy.wait_recv()
        source = lax.rem(layer + depth - d - 1, depth)
        for j, peer in enumerate(peers):
            block = out_ref.at[source, me]
            spread.append(
                send(block, block, p_sems.at[0, d, j], p_sems.at[1, d, j], (peer, layer))
            )
        block = out_ref.at[source, me]
        first[d] = (
            copy,
            send(block, block, f_sems.at[0, d, 3], f_sems.at[1, d, 3], (partner, layer)),
        )
    passed = []
    for d in range(depth - 1):
        source = lax.rem(layer + depth - d - 1, depth)
        for j in range(CHIPS - 1):
            spread[d * (CHIPS - 1) + j].wait_recv()
            block = out_ref.at[source, chip_at(chip, core, -j - 1)]
            passed.append(
                send(block, block, f_sems.at[0, d, j], f_sems.at[1, d, j], (partner, layer))
            )
    for copy, handed in first:
        copy.wait_send()
        handed.wait()
    for copy in spread:
        copy.wait_send()
    for copy in passed:
        copy.wait()


def gather_rows(own, depth):
    if lax.axis_size("ctx") != SPAN:
        return lax.all_gather(own, "fsdp", axis=0)
    rows, columns = own.shape
    piece = rows // SPAN
    return pl.pallas_call(
        functools.partial(gather_rows_kernel, depth),
        out_shape=jax.ShapeDtypeStruct((depth, SPAN, piece, columns), own.dtype),
        in_specs=in_vmem(1),
        out_specs=in_vmem(1)[0],
        scratch_shapes=[
            pltpu.SemaphoreType.DMA((2, depth - 1)),
            pltpu.SemaphoreType.DMA((2, depth - 1, CHIPS - 1)),
            pltpu.SemaphoreType.DMA((2, depth - 1, CHIPS)),
        ],
        compiler_params=comm_params(1),
        cost_estimate=comm_cost(own.size * 2 * depth),
    )(own.reshape(SPAN, piece, columns)).reshape(depth, rows, columns)


def gather_plane_kernel(kv_ref, tag_ref, kv_out, tag_out, p_sems, f_sems):
    me, core, chip, partner = plane_of()
    layer = lax.axis_index("fsdp")
    peers = [chip_at(chip, core, j) for j in range(1, CHIPS)]
    greet([(peer, layer) for peer in peers + [partner]])
    pairs = ((kv_ref, kv_out), (tag_ref, tag_out))
    spread, passed = [], []
    for j, peer in enumerate(peers):
        for a, (own, out) in enumerate(pairs):
            spread.append(
                send(own, out.at[me], p_sems.at[0, a, j], p_sems.at[1, a, j], (peer, layer))
            )
    for a, (own, out) in enumerate(pairs):
        passed.append(
            send(own, out.at[me], f_sems.at[0, a, 3], f_sems.at[1, a, 3], (partner, layer))
        )
    kv_out[me] = kv_ref[...]
    tag_out[me] = tag_ref[...]
    for j in range(CHIPS - 1):
        for a, (own, out) in enumerate(pairs):
            spread[2 * j + a].wait_recv()
            block = out.at[chip_at(chip, core, -j - 1)]
            passed.append(
                send(block, block, f_sems.at[0, a, j], f_sems.at[1, a, j], (partner, layer))
            )
    for copy in spread:
        copy.wait_send()
    for copy in passed:
        copy.wait()


def gather_plane(kv, tags):
    if lax.axis_size("ctx") != SPAN:
        return tuple(lax.all_gather(part, "ctx", axis=0, tiled=True) for part in (kv, tags))
    rows, columns = kv.shape
    kv_all, tags_all = pl.pallas_call(
        gather_plane_kernel,
        out_shape=(
            jax.ShapeDtypeStruct((SPAN, rows, columns), kv.dtype),
            jax.ShapeDtypeStruct((SPAN, 1, rows), tags.dtype),
        ),
        in_specs=in_vmem(2),
        out_specs=tuple(in_vmem(2)),
        scratch_shapes=[
            pltpu.SemaphoreType.DMA((2, 2, CHIPS - 1)),
            pltpu.SemaphoreType.DMA((2, 2, CHIPS)),
        ],
        compiler_params=comm_params(2),
        cost_estimate=comm_cost(kv.size * 2 * SPAN),
    )(kv, tags[None])
    return kv_all.reshape(SPAN * rows, columns), tags_all.reshape(SPAN * rows)


def added(*parts):
    total = parts[0].astype(jnp.float32)
    for part in parts[1:]:
        total = total + part.astype(jnp.float32)
    return total


def reduce_plane(arrays, h_sems, p_sems):
    me, core, chip, partner = plane_of()
    layer = lax.axis_index("fsdp")
    handed, spread = [], []
    for a, (piece_of, halves, sums, arrived) in enumerate(arrays):
        for j in range(CHIPS):
            slot = (j + 1) % CHIPS
            handed.append(
                send(
                    piece_of(chip_at(chip, 1 - core, slot)),
                    halves.at[slot],
                    h_sems.at[0, a, slot],
                    h_sems.at[1, a, slot],
                    (partner, layer),
                )
            )
    for a, (piece_of, halves, sums, arrived) in enumerate(arrays):
        for j in range(CHIPS):
            slot = (j + 1) % CHIPS
            handed[a * CHIPS + j].wait_recv()
            mine = chip_at(chip, core, slot)

            def add_half(slab, carry, piece=piece_of(mine), halves=halves, sums=sums, slot=slot):
                sums[slot, slab] = added(piece[slab], halves[slot, slab]).astype(sums.dtype)
                return carry

            lax.fori_loop(0, sums.shape[1], add_half, 0)
            if slot:
                spread.append(
                    send(
                        sums.at[slot],
                        arrived.at[slot - 1],
                        p_sems.at[0, a, slot - 1],
                        p_sems.at[1, a, slot - 1],
                        (mine, layer),
                    )
                )
    return handed, spread


def plane_total(sums, arrived, slab):
    return added(sums[0, slab], *(arrived[j, slab] for j in range(CHIPS - 1)))


def plane_scratch(block, dtype):
    return [
        pltpu.VMEM((CHIPS, *block), dtype),
        pltpu.VMEM((CHIPS, *block), dtype),
        pltpu.VMEM((CHIPS - 1, *block), dtype),
    ]


def scatter_plane_kernel(x_ref, out_ref, halves, sums, arrived, h_sems, p_sems):
    me, core, chip, partner = plane_of()
    layer = lax.axis_index("fsdp")
    greet([(chip_at(chip, core, j), layer) for j in range(1, CHIPS)] + [(partner, layer)])
    arrays = [(lambda piece: x_ref.at[piece], halves, sums, arrived)]
    handed, spread = reduce_plane(arrays, h_sems, p_sems)
    for copy in spread:
        copy.wait_recv()

    def add_slab(slab, carry):
        out_ref[slab] = plane_total(sums, arrived, slab)
        return carry

    lax.fori_loop(0, x_ref.shape[1], add_slab, 0)
    for copy in handed + spread:
        copy.wait_send()


def scatter_plane(values):
    if lax.axis_size("ctx") != SPAN:
        own = lax.psum_scatter(values, "ctx", scatter_dimension=0, tiled=True)
        return own.astype(jnp.float32)
    rows, columns = values.shape
    slabs = 8
    block = (slabs, rows // SPAN // slabs, columns)
    return pl.pallas_call(
        scatter_plane_kernel,
        out_shape=jax.ShapeDtypeStruct(block, jnp.float32),
        in_specs=in_vmem(1),
        out_specs=in_vmem(1)[0],
        scratch_shapes=plane_scratch(block, values.dtype)
        + [pltpu.SemaphoreType.DMA((2, 1, CHIPS)), pltpu.SemaphoreType.DMA((2, 1, CHIPS - 1))],
        compiler_params=comm_params(3),
        cost_estimate=comm_cost(values.size * 2),
    )(values.reshape(SPAN, *block)).reshape(rows // SPAN, columns)


def reduce_rows_kernel(depth, count, *refs):
    inputs, outs, scratch = refs[:count], refs[count : 2 * count], refs[2 * count : 6 * count]
    h_sems, p_sems, z_sems, g_sems, f_sems = refs[6 * count :]
    me, core, chip, partner = plane_of()
    layer = lax.axis_index("fsdp")
    layers = [lax.rem(layer + d, depth) for d in range(1, depth)]
    peers = [chip_at(chip, core, j) for j in range(1, CHIPS)]
    greet([(me, other) for other in layers] + [(peer, layer) for peer in peers + [partner]])
    arrays, across = [], []
    for a, x_ref in enumerate(inputs):
        halves, sums, arrived, layers_ref = scratch[4 * a : 4 * a + 4]
        arrays.append((lambda piece, x_ref=x_ref: x_ref.at[:, piece], halves, sums, arrived))
        across.append(layers_ref)
    handed, spread = reduce_plane(arrays, h_sems, p_sems)
    moved = []
    for a, (_, _, sums, arrived) in enumerate(arrays):
        for copy in spread[a * (CHIPS - 1) : (a + 1) * (CHIPS - 1)]:
            copy.wait_recv()
        for d in list(range(1, depth)) + [0]:
            target = lax.rem(layer + d, depth)
            across[a][0, d] = plane_total(sums, arrived, target).astype(across[a].dtype)
            if d:
                moved.append(
                    send(
                        across[a].at[0, d],
                        across[a].at[1, d],
                        z_sems.at[0, a, d - 1],
                        z_sems.at[1, a, d - 1],
                        (me, target),
                    )
                )
    given, passed = [], []
    for a, out_ref in enumerate(outs):
        for copy in moved[a * (depth - 1) : (a + 1) * (depth - 1)]:
            copy.wait_recv()
        parts = [across[a][0, 0]] + [across[a][1, d] for d in range(1, depth)]
        out_ref[me] = added(*parts).astype(out_ref.dtype)
        mine = out_ref.at[me]
        for j, peer in enumerate(peers):
            given.append(send(mine, mine, g_sems.at[0, a, j], g_sems.at[1, a, j], (peer, layer)))
        passed.append(send(mine, mine, f_sems.at[0, a, 3], f_sems.at[1, a, 3], (partner, layer)))
    for a, out_ref in enumerate(outs):
        for j in range(CHIPS - 1):
            given[a * (CHIPS - 1) + j].wait_recv()
            block = out_ref.at[chip_at(chip, core, -j - 1)]
            passed.append(
                send(block, block, f_sems.at[0, a, j], f_sems.at[1, a, j], (partner, layer))
            )
    for copy in handed + spread + moved + given:
        copy.wait_send()
    for copy in passed:
        copy.wait()


def reduce_rows(arrays, number):
    if lax.axis_size("ctx") != SPAN:
        return [lax.psum(lax.psum_scatter(v, "fsdp", scatter_dimension=0), "ctx") for v in arrays]
    depth, count = arrays[0].shape[0], len(arrays)
    pieces, outs, scratch = [], [], []
    for values in arrays:
        _, rows, columns = values.shape
        piece = (rows // SPAN, columns)
        pieces.append(values.reshape(depth, SPAN, *piece))
        outs.append(jax.ShapeDtypeStruct((SPAN, *piece), values.dtype))
        scratch += plane_scratch((depth, *piece), values.dtype)
        scratch.append(pltpu.VMEM((2, depth, *piece), values.dtype))
    owned = pl.pallas_call(
        functools.partial(reduce_rows_kernel, depth, count),
        out_shape=tuple(outs),
        in_specs=in_vmem(count),
        out_specs=tuple(in_vmem(count)),
        scratch_shapes=scratch
        + [
            pltpu.SemaphoreType.DMA((2, count, CHIPS)),
            pltpu.SemaphoreType.DMA((2, count, CHIPS - 1)),
            pltpu.SemaphoreType.DMA((2, count, depth - 1)),
            pltpu.SemaphoreType.DMA((2, count, CHIPS - 1)),
            pltpu.SemaphoreType.DMA((2, count, CHIPS)),
        ],
        compiler_params=comm_params(number),
        cost_estimate=comm_cost(sum(values.size for values in arrays) * 2),
    )(*pieces)
    return [own.reshape(values.shape[1:]) for own, values in zip(owned, arrays)]


BLOCK = 128
LANES = (HEADS // KV_HEADS) * BLOCK


def dot(left, right, dims=(1, 0)):
    return lax.dot_general(
        left, right, (((dims[0],), (dims[1],)), ((), ())), preferred_element_type=jnp.float32
    )


def of_group(ref, group, at):
    first = group * (HEADS // KV_HEADS)
    heads = range(first, first + HEADS // KV_HEADS)
    return jnp.concatenate([ref[head * HEAD : (head + 1) * HEAD, at] for head in heads], 1)


def of_rows(ref, group, at):
    first = group * (HEADS // KV_HEADS)
    heads = range(first, first + HEADS // KV_HEADS)
    return jnp.concatenate([ref[head : head + 1, at] for head in heads], 1)


def columns_of(group, part):
    start = (part * KV_HEADS + group) * HEAD
    return slice(start, start + HEAD)


def mask_bias(tags, query_pos):
    key_pos = jnp.where(tags >= 0, tags, -tags - 1)
    allowed = (key_pos <= query_pos) & ((tags >= 0) | (key_pos == query_pos))
    bias = jnp.where(allowed, 0.0, negative)
    return jnp.concatenate([bias] * (HEADS // KV_HEADS), 1)


def attend_kernel(
    first_ref, q_ref, kv_ref, pos_ref, tag_ref, out_ref, log_ref, max_ref, sum_ref, acc_ref, kept
):
    blocks = kv_ref.shape[0] // BLOCK
    keep = kept.shape[0] == blocks

    def scores(group, at, rows, bias):
        keys = kv_ref[rows, columns_of(group, 0)]
        return dot(keys, of_group(q_ref, group, at)) + bias

    def query_block(qb, carry):
        at = pl.ds(pl.multiple_of(qb * BLOCK, BLOCK), BLOCK)
        max_ref[...] = jnp.full(max_ref.shape, negative, jnp.float32)
        sum_ref[...] = jnp.zeros(sum_ref.shape, jnp.float32)
        acc_ref[...] = jnp.zeros(acc_ref.shape, jnp.float32)
        limit = first_ref[blocks + qb]

        def find(kb, carry):
            @pl.when(first_ref[kb] <= limit)
            def _():
                rows = pl.ds(pl.multiple_of(kb * BLOCK, BLOCK), BLOCK)
                bias = mask_bias(tag_ref[rows, :], pos_ref[:, at])
                for group in range(KV_HEADS):
                    found = scores(group, at, rows, bias)
                    if keep:
                        kept[kb, group] = found
                    tops = jnp.max(found.reshape(BLOCK // 8, 8, LANES), 0)
                    max_ref[group] = jnp.maximum(max_ref[group], tops)

            return carry

        lax.fori_loop(0, blocks, find, 0)
        for group in range(KV_HEADS):
            top = jnp.max(max_ref[group], 0, keepdims=True)
            max_ref[group] = jnp.broadcast_to(top, max_ref.shape[1:])

        def gather(kb, carry):
            @pl.when(first_ref[kb] <= limit)
            def _():
                rows = pl.ds(pl.multiple_of(kb * BLOCK, BLOCK), BLOCK)
                bias = None if keep else mask_bias(tag_ref[rows, :], pos_ref[:, at])
                for group in range(KV_HEADS):
                    found = kept[kb, group] if keep else scores(group, at, rows, bias)
                    weights = jnp.exp(found - max_ref[group, :1])
                    sum_ref[group] += jnp.sum(weights.reshape(BLOCK // 8, 8, LANES), 0)
                    values = kv_ref[rows, columns_of(group, 1)]
                    acc_ref[group] += dot(values, weights.astype(jnp.bfloat16), (0, 0))

            return carry

        lax.fori_loop(0, blocks, gather, 0)
        for group in range(KV_HEADS):
            total = jnp.sum(sum_ref[group], 0, keepdims=True)
            attended = acc_ref[group] / total
            logs = max_ref[group, :1] + jnp.log(total)
            for j in range(HEADS // KV_HEADS):
                head = group * (HEADS // KV_HEADS) + j
                own = slice(j * BLOCK, (j + 1) * BLOCK)
                out_ref[head * HEAD : (head + 1) * HEAD, at] = attended[:, own]
                log_ref[head : head + 1, at] = logs[:, own]
        return carry

    lax.fori_loop(0, q_ref.shape[1] // BLOCK, query_block, 0)


def kernel_params():
    return pltpu.CompilerParams(vmem_limit_bytes=VMEM_BYTES)


def attend(firsts, queries, kv, query_pos, key_tags):
    blocks = kv.shape[0] // BLOCK
    slots = queries.shape[1]
    kept = blocks if blocks <= 16 else 1
    groups = (KV_HEADS, 8, LANES)
    work = 4 * kv.shape[0] * slots * HEADS * HEAD
    return pl.pallas_call(
        attend_kernel,
        out_shape=(
            jax.ShapeDtypeStruct(queries.shape, jnp.float32),
            jax.ShapeDtypeStruct((HEADS + 1, slots), jnp.float32),
        ),
        in_specs=[pl.BlockSpec(memory_space=pltpu.SMEM)] + in_vmem(4),
        out_specs=tuple(in_vmem(2)),
        scratch_shapes=[
            pltpu.VMEM(groups, jnp.float32),
            pltpu.VMEM(groups, jnp.float32),
            pltpu.VMEM((KV_HEADS, HEAD, LANES), jnp.float32),
            pltpu.VMEM((kept, KV_HEADS, BLOCK, LANES), jnp.float32),
        ],
        compiler_params=kernel_params(),
        cost_estimate=pl.CostEstimate(
            flops=work * 8, bytes_accessed=kv.size * 2, transcendentals=work // 256
        ),
    )(firsts, queries, kv, query_pos[None], key_tags[:, None])


def attend_back_kernel(
    first_ref, q_ref, kv_ref, pos_ref, tag_ref, grad_ref, log_ref, delta_ref, dq_ref, dkv_ref, acc
):
    blocks = kv_ref.shape[0] // BLOCK
    dq_ref[...] = jnp.zeros(dq_ref.shape, dq_ref.dtype)

    def key_block(kb, carry):
        rows = pl.ds(pl.multiple_of(kb * BLOCK, BLOCK), BLOCK)
        acc[...] = jnp.zeros(acc.shape, jnp.float32)

        def query_block(qb, carry):
            @pl.when(first_ref[kb] <= first_ref[blocks + qb])
            def _():
                at = pl.ds(pl.multiple_of(qb * BLOCK, BLOCK), BLOCK)
                bias = mask_bias(tag_ref[rows, :], pos_ref[:, at])
                for group in range(KV_HEADS):
                    keys = kv_ref[rows, columns_of(group, 0)]
                    values = kv_ref[rows, columns_of(group, 1)]
                    queries = of_group(q_ref, group, at)
                    grads = of_group(grad_ref, group, at)
                    found = dot(keys, queries) + bias
                    probs = jnp.exp(found - of_rows(log_ref, group, at))
                    grad_probs = dot(values, grads)
                    grad_scores = probs * (grad_probs - of_rows(delta_ref, group, at))
                    grad_scores = grad_scores.astype(jnp.bfloat16)
                    acc[group] += dot(grad_scores, queries, (1, 1))
                    acc[KV_HEADS + group] += dot(probs.astype(jnp.bfloat16), grads, (1, 1))
                    grad_q = 0.125 * dot(keys, grad_scores, (0, 0))
                    for j in range(HEADS // KV_HEADS):
                        head = group * (HEADS // KV_HEADS) + j
                        own = slice(head * HEAD, (head + 1) * HEAD)
                        dq_ref[own, at] += grad_q[:, j * BLOCK : (j + 1) * BLOCK]

            return carry

        lax.fori_loop(0, q_ref.shape[1] // BLOCK, query_block, 0)
        dkv_ref[rows, :] = jnp.concatenate(
            [acc[index] for index in range(2 * KV_HEADS)], 1
        ).astype(dkv_ref.dtype)
        return carry

    lax.fori_loop(0, blocks, key_block, 0)


def attend_back(firsts, queries, kv, query_pos, key_tags, grads, log_total, row_delta):
    slots = queries.shape[1]
    work = 10 * kv.shape[0] * slots * HEADS * HEAD
    return pl.pallas_call(
        attend_back_kernel,
        out_shape=(
            jax.ShapeDtypeStruct(queries.shape, jnp.float32),
            jax.ShapeDtypeStruct(kv.shape, jnp.bfloat16),
        ),
        in_specs=[pl.BlockSpec(memory_space=pltpu.SMEM)] + in_vmem(7),
        out_specs=tuple(in_vmem(2)),
        scratch_shapes=[pltpu.VMEM((2 * KV_HEADS, BLOCK, HEAD), jnp.float32)],
        compiler_params=kernel_params(),
        cost_estimate=pl.CostEstimate(
            flops=work * 6, bytes_accessed=kv.size * 4, transcendentals=work // 640
        ),
    )(firsts, queries, kv, query_pos[None], key_tags[:, None], grads, log_total, row_delta)


def on_device(
    tokens,
    w_query,
    w_key,
    w_value,
    w_out,
    w_gate,
    w_up,
    w_down,
    gain_attn,
    gain_ffn,
    router,
    cotangent,
    positions,
    lengths,
    chosen,
):
    hidden = tokens[0].astype(jnp.float32)
    row_count, width = hidden.shape
    qdim = HEADS * HEAD
    kdim = KV_HEADS * HEAD
    query_pos = positions[0]
    live = query_pos < lengths[0]
    selected = live & (chosen[0] == 1)
    live_mask = live.astype(jnp.float32)[:, None]
    chosen_mask = selected.astype(jnp.float32)[:, None]
    cos_tab, sin_tab = rope_tables(query_pos)
    key_tags = jnp.where(selected, query_pos, -query_pos - 1)
    depth = lax.axis_size("fsdp")
    own_rows = w_query.shape[0]
    w_out_full = lax.all_gather(w_out, "fsdp", axis=0, tiled=True)
    vectors = jnp.stack([gain_attn, gain_ffn, router], 1)
    own_attn = padded_to(jnp.concatenate([w_query, w_key, w_value, vectors], 1), 0)
    gathered = gather_rows(own_attn, depth)[:, :own_rows]
    w_qkv = gathered[..., : qdim + 2 * kdim].reshape(width, qdim + 2 * kdim)
    vectors = gathered[..., qdim + 2 * kdim : qdim + 2 * kdim + 3].reshape(width, 3)
    gain_one, gain_two, router_vec = vectors.T.astype(jnp.float32)
    gating = jax.nn.sigmoid(jnp.sum(hidden * router_vec, -1, keepdims=True))
    grad_y = cotangent[0].astype(jnp.float32) * live_mask
    grad_inc = grad_y * chosen_mask * gating
    grad_ffn = grad_inc.astype(jnp.bfloat16)
    grad_ffn_all = lax.all_gather(grad_ffn, "fsdp", axis=0, tiled=True)

    normed_one, inv_one = norm_forward(hidden, gain_one)
    normed_one = normed_one.astype(jnp.bfloat16)
    w_kv = w_qkv[:, qdim:]
    w_query = w_qkv[:, :qdim]
    query_raw = dot(w_query, normed_one, (0, 1))
    queries = rotate_columns(query_raw, cos_tab, sin_tab).astype(jnp.bfloat16) * 0.125
    kv_raw = dot(normed_one, w_kv)
    kv_own = jnp.concatenate([rotate(kv_raw[:, :kdim], cos_tab, sin_tab), kv_raw[:, kdim:]], 1)
    kv_all, tags_all = gather_plane(kv_own.astype(jnp.bfloat16), key_tags)
    first_tags = tags_all[::BLOCK]
    firsts = jnp.concatenate(
        [jnp.where(first_tags >= 0, first_tags, -first_tags - 1), query_pos[BLOCK - 1 :: BLOCK]]
    )
    attended, log_total = attend(firsts, queries, kv_all, query_pos, tags_all)
    attended, grad_ffn_all, w_out_full = lax.optimization_barrier(
        (attended, grad_ffn_all, w_out_full)
    )
    outcome = attended.astype(jnp.bfloat16)
    branch = dot(outcome, w_out_full, (0, 0))
    middle = hidden + branch
    normed_two, inv_two = norm_forward(middle, gain_two)
    normed_two = normed_two.astype(jnp.bfloat16)
    normed_all = lax.all_gather(normed_two, "fsdp", axis=0, tiled=True)
    inner_act, grad_gate_act, grad_up_act, grad_normed_part = ffn_both(
        normed_all, grad_ffn_all, w_gate, w_up, w_down
    )
    grad_normed_two = lax.psum_scatter(
        grad_normed_part, "fsdp", scatter_dimension=0, tiled=True
    ).astype(jnp.float32)
    ffn_part = jnp.dot(inner_act, w_down, preferred_element_type=jnp.float32).astype(jnp.bfloat16)
    grad_wgate = lax.dot_general(
        grad_gate_act, normed_all, across_rows, preferred_element_type=jnp.float32
    )
    grad_wup = lax.dot_general(
        grad_up_act, normed_all, across_rows, preferred_element_type=jnp.float32
    )
    grad_wdown = lax.dot_general(
        inner_act, grad_ffn_all, across_rows, preferred_element_type=jnp.float32
    )
    low = jnp.bfloat16
    grad_normed_two, ffn_part, *grads = lax.optimization_barrier(
        (grad_normed_two, ffn_part, *(g.astype(low) for g in (grad_wgate, grad_wup, grad_wdown)))
    )
    ffn_out = lax.psum_scatter(ffn_part, "fsdp", scatter_dimension=0, tiled=True).astype(
        jnp.float32
    )
    totals = tuple(lax.psum(grad, "ctx") for grad in grads)
    grad_middle, grad_gain_two = norm_backward(middle, inv_two, gain_two, grad_normed_two)
    grad_branch = (grad_inc + grad_middle).astype(jnp.bfloat16)
    grad_attended = dot(w_out_full, grad_branch, (1, 1)).astype(jnp.bfloat16)
    grad_wout = dot(outcome, grad_branch)
    row_delta = jnp.sum(
        (grad_attended.astype(jnp.float32) * attended).reshape(HEADS, HEAD, row_count), 1
    )
    row_delta = jnp.pad(row_delta, ((0, 1), (0, 0)))
    grad_qrot, grad_kv_all = attend_back(
        firsts, queries, kv_all, query_pos, tags_all, grad_attended, log_total, row_delta
    )
    grad_kv = scatter_plane(grad_kv_all)
    grad_kv, ffn_out = lax.optimization_barrier((grad_kv, ffn_out))
    increment = branch + ffn_out
    block_out = live_mask * (hidden + chosen_mask * gating * increment)
    grad_logit = (
        jnp.sum(grad_y * chosen_mask * increment, -1, keepdims=True) * gating * (1.0 - gating)
    )
    grad_router = jnp.sum(hidden * grad_logit, 0)
    grad_query_raw = rotate_columns(grad_qrot, cos_tab, -sin_tab).astype(jnp.bfloat16)
    grad_kv_raw = jnp.concatenate(
        [rotate(grad_kv[:, :kdim], cos_tab, -sin_tab), grad_kv[:, kdim:]], 1
    ).astype(jnp.bfloat16)
    grad_normed_one = dot(grad_query_raw, w_query, (0, 1)) + dot(grad_kv_raw, w_kv, (1, 1))
    spread_one = padded_to(normed_one.reshape(row_count, depth, own_rows), -1)
    spread_one = spread_one.reshape(row_count, -1)
    padded_rows = spread_one.shape[1] // depth
    grad_wq = dot(spread_one, grad_query_raw, (0, 1)).astype(low)
    grad_wkv = dot(spread_one, grad_kv_raw, (0, 0)).astype(low)
    grad_hidden_one, grad_gain_one = norm_backward(hidden, inv_one, gain_one, grad_normed_one)
    grad_tokens = (grad_y + grad_logit * router_vec + grad_middle + grad_hidden_one).astype(
        jnp.bfloat16
    )
    vectors = jnp.stack([grad_gain_one, grad_gain_two, grad_router]).reshape(3, depth, own_rows)
    vectors = jnp.pad(vectors.transpose(1, 0, 2).reshape(depth, -1), ((0, 0), (0, -3 * own_rows % 1024)))
    vectors = jnp.pad(vectors.reshape(depth, -1, 1, 128), ((0, 0), (0, 0), (0, 7), (0, 0)))
    layered = [grad.reshape(depth, padded_rows, -1) for grad in (grad_wq, grad_wkv)]
    layered.append(padded_rows_of(grad_wout.astype(low).reshape(depth, own_rows, -1), padded_rows))
    layered.append(vectors.reshape(depth, -1, 128))
    owned = reduce_rows(layered, 4)
    *owned, totals = lax.optimization_barrier((*owned, totals))
    total_q, total_kv, total_out = (own[:own_rows].astype(jnp.float32) for own in owned[:3])
    total_k, total_v = total_kv[:, :kdim], total_kv[:, kdim:]
    mine = owned[3].reshape(-1, 8, 128)[:, 0].reshape(-1)[: 3 * own_rows].reshape(3, own_rows)
    total_gate, total_up, total_down = (total.astype(jnp.float32) for total in totals)
    return (
        block_out.astype(jnp.bfloat16)[None],
        grad_tokens[None],
        total_q,
        total_k,
        total_v,
        total_out,
        total_gate,
        total_up,
        total_down,
        mine[0],
        mine[1],
        mine[2],
    )


def solution(mesh):
    in_specs = (
        P("fsdp", "ctx", None),
        P("fsdp", None),
        P("fsdp", None),
        P("fsdp", None),
        P("fsdp", None),
        P("fsdp", None),
        P("fsdp", None),
        P("fsdp", None),
        P("fsdp"),
        P("fsdp"),
        P("fsdp"),
        P("fsdp", "ctx", None),
        P("fsdp", "ctx"),
        P("fsdp"),
        P("fsdp", "ctx"),
    )
    out_specs = (
        P("fsdp", "ctx", None),
        P("fsdp", "ctx", None),
        P("fsdp", None),
        P("fsdp", None),
        P("fsdp", None),
        P("fsdp", None),
        P("fsdp", None),
        P("fsdp", None),
        P("fsdp", None),
        P("fsdp"),
        P("fsdp"),
        P("fsdp"),
    )
    return jax.shard_map(
        on_device, mesh=mesh, in_specs=in_specs, out_specs=out_specs, check_vma=False
    )
```

```python
import functools

import jax
import jax.numpy as jnp
from jax import lax
from jax.experimental import pallas as pl
from jax.experimental.pallas import tpu as pltpu
from jax.sharding import PartitionSpec as P

HEADS = 15
KV_HEADS = 5
HEAD = 64


epsilon = 1e-05
negative = -1e30
across_rows = (((0,), (0,)), ((), ()))
across_cols = (((1,), (1,)), ((), ()))


def rope_tables(positions):
    half_dim = HEAD // 2
    frequency = 10000.0 ** (-2.0 * jnp.arange(half_dim, dtype=jnp.float32) / HEAD)
    angles = positions.astype(jnp.float32)[:, None] * frequency[None, :]
    return (jnp.cos(angles), jnp.sin(angles))


def rotate(values, cos_tab, sin_tab):
    slots, width = values.shape
    low, high = jnp.split(values.reshape(slots, width // HEAD, HEAD), 2, -1)
    cos_tab, sin_tab = cos_tab[:, None], sin_tab[:, None]
    turned = [low * cos_tab - high * sin_tab, high * cos_tab + low * sin_tab]
    return jnp.concatenate(turned, -1).reshape(slots, width)


def rotate_columns(values, cos_tab, sin_tab):
    width, slots = values.shape
    low, high = jnp.split(values.reshape(width // HEAD, HEAD, slots), 2, 1)
    cos_tab, sin_tab = cos_tab.T[None], sin_tab.T[None]
    turned = [low * cos_tab - high * sin_tab, high * cos_tab + low * sin_tab]
    return jnp.concatenate(turned, 1).reshape(width, slots)


def norm_forward(values, gain_vec):
    inv_rms = lax.rsqrt(jnp.mean(values * values, -1, keepdims=True) + epsilon)
    return (values * inv_rms * gain_vec, inv_rms)


def norm_backward(values, inv_rms, gain_vec, grad_normed):
    weighted = gain_vec * grad_normed
    grad_gain = jnp.sum(grad_normed * values * inv_rms, 0)
    cubed = inv_rms * inv_rms * inv_rms
    grad_values = inv_rms * weighted - values * cubed * jnp.mean(
        weighted * values, -1, keepdims=True
    )
    return (grad_values, grad_gain)


def padded_to(values, row_dim):
    pads = [(0, 0)] * values.ndim
    pads[row_dim] = (0, -values.shape[row_dim] % 128)
    return jnp.pad(values, pads)


def ffn_both(normed, grad_mixed, gate_rows, up_rows, down_rows):
    gate_proj = lax.dot_general(normed, gate_rows, across_cols, preferred_element_type=jnp.float32)
    up_proj = lax.dot_general(normed, up_rows, across_cols, preferred_element_type=jnp.float32)
    sigma = jax.nn.sigmoid(gate_proj)
    activated = gate_proj * sigma
    inner_act = (activated * up_proj).astype(jnp.bfloat16)
    grad_inner = lax.dot_general(
        grad_mixed, down_rows, across_cols, preferred_element_type=jnp.float32
    )
    grad_gate_act = (grad_inner * up_proj * sigma * (1.0 + gate_proj * (1.0 - sigma))).astype(
        jnp.bfloat16
    )
    grad_up_act = (grad_inner * activated).astype(jnp.bfloat16)
    grad_normed = jnp.dot(grad_gate_act, gate_rows, preferred_element_type=jnp.float32) + jnp.dot(
        grad_up_act, up_rows, preferred_element_type=jnp.float32
    )
    row_dot = jnp.sum(inner_act.astype(jnp.float32) * grad_inner, -1, keepdims=True)
    grad_normed = jnp.concatenate([grad_normed, row_dot], 1).astype(jnp.bfloat16)
    return (inner_act, grad_gate_act, grad_up_act, grad_normed)


CHIPS = 4
SPAN = 2 * CHIPS
VMEM_BYTES = 60 * 1024 * 1024
MESH = pl.DeviceIdType.MESH


def plane_of():
    me = lax.axis_index("ctx")
    core = lax.rem(me, 2)
    chip = me // 2
    return me, core, chip, me + 1 - 2 * core


def chip_at(chip, core, step):
    return 2 * lax.rem(chip + step + CHIPS, CHIPS) + core


def greet(devices):
    barrier = pltpu.get_barrier_semaphore()
    for device in devices:
        pl.semaphore_signal(barrier, inc=1, device_id=device, device_id_type=MESH)
    pl.semaphore_wait(barrier, len(devices))


def send(src, dst, send_sem, recv_sem, device):
    copy = pltpu.make_async_remote_copy(
        src_ref=src,
        dst_ref=dst,
        send_sem=send_sem,
        recv_sem=recv_sem,
        device_id=device,
        device_id_type=MESH,
    )
    copy.start()
    return copy


def comm_params(number):
    return pltpu.CompilerParams(
        collective_id=number, has_side_effects=True, vmem_limit_bytes=VMEM_BYTES
    )


def comm_cost(moved):
    return pl.CostEstimate(flops=0, bytes_accessed=moved * 30, transcendentals=0)


def in_vmem(count):
    return [pl.BlockSpec(memory_space=pltpu.VMEM)] * count


def gather_rows_kernel(depth, count, *refs):
    owns, outs = refs[:count], refs[count : 2 * count]
    z_sems, p_sems, f_sems = refs[2 * count :]
    me, core, chip, partner = plane_of()
    layer = lax.axis_index("fsdp")
    layers = [lax.rem(layer + d, depth) for d in range(1, depth)]
    peers = [chip_at(chip, core, j) for j in range(1, CHIPS)]
    greet([(me, other) for other in layers] + [(peer, layer) for peer in peers + [partner]])
    first, spread, passed = [], [], []
    for a, (own, out) in enumerate(zip(owns, outs)):
        for d, other in enumerate(layers):
            first.append(
                send(
                    own.at[me],
                    out.at[layer, me],
                    z_sems.at[0, a, d],
                    z_sems.at[1, a, d],
                    (me, other),
                )
            )
    for own, out in zip(owns, outs):
        for piece in range(SPAN):
            out[layer, piece] = own[piece]
    for a, out in enumerate(outs):
        for d in range(depth - 1):
            first[a * (depth - 1) + d].wait_recv()
            block = out.at[lax.rem(layer + depth - d - 1, depth), me]
            for j, peer in enumerate(peers):
                spread.append(
                    send(block, block, p_sems.at[0, a, d, j], p_sems.at[1, a, d, j], (peer, layer))
                )
            passed.append(
                send(block, block, f_sems.at[0, a, d, 3], f_sems.at[1, a, d, 3], (partner, layer))
            )
    arrivals = iter(spread)
    for a, out in enumerate(outs):
        for d in range(depth - 1):
            source = lax.rem(layer + depth - d - 1, depth)
            for j in range(CHIPS - 1):
                next(arrivals).wait_recv()
                block = out.at[source, chip_at(chip, core, -j - 1)]
                passed.append(
                    send(
                        block,
                        block,
                        f_sems.at[0, a, d, j],
                        f_sems.at[1, a, d, j],
                        (partner, layer),
                    )
                )
    for copy in first + spread:
        copy.wait_send()
    for copy in passed:
        copy.wait()


def gather_rows(arrays, depth):
    if lax.axis_size("ctx") != SPAN:
        return [lax.all_gather(own, "fsdp", axis=0) for own in arrays]
    count, pieces, outs = len(arrays), [], []
    for own in arrays:
        piece = (own.shape[0] // SPAN, own.shape[1])
        pieces.append(own.reshape(SPAN, *piece))
        outs.append(jax.ShapeDtypeStruct((depth, SPAN, *piece), own.dtype))
    whole = pl.pallas_call(
        functools.partial(gather_rows_kernel, depth, count),
        out_shape=tuple(outs),
        in_specs=in_vmem(count),
        out_specs=tuple(in_vmem(count)),
        scratch_shapes=[
            pltpu.SemaphoreType.DMA((2, count, depth - 1)),
            pltpu.SemaphoreType.DMA((2, count, depth - 1, CHIPS - 1)),
            pltpu.SemaphoreType.DMA((2, count, depth - 1, CHIPS)),
        ],
        compiler_params=comm_params(1),
        cost_estimate=comm_cost(sum(own.size for own in arrays) * 2 * depth),
    )(*pieces)
    return [full.reshape(depth, *own.shape) for full, own in zip(whole, arrays)]


def gather_plane_kernel(kv_ref, tag_ref, kv_out, tag_out, p_sems, f_sems):
    me, core, chip, partner = plane_of()
    layer = lax.axis_index("fsdp")
    peers = [chip_at(chip, core, j) for j in range(1, CHIPS)]
    greet([(peer, layer) for peer in peers + [partner]])
    pairs = ((kv_ref, kv_out), (tag_ref, tag_out))
    spread, passed = [], []
    for j, peer in enumerate(peers):
        for a, (own, out) in enumerate(pairs):
            spread.append(
                send(own, out.at[me], p_sems.at[0, a, j], p_sems.at[1, a, j], (peer, layer))
            )
    for a, (own, out) in enumerate(pairs):
        passed.append(
            send(own, out.at[me], f_sems.at[0, a, 3], f_sems.at[1, a, 3], (partner, layer))
        )
    kv_out[me] = kv_ref[...]
    tag_out[me] = tag_ref[...]
    for j in range(CHIPS - 1):
        for a, (own, out) in enumerate(pairs):
            spread[2 * j + a].wait_recv()
            block = out.at[chip_at(chip, core, -j - 1)]
            passed.append(
                send(block, block, f_sems.at[0, a, j], f_sems.at[1, a, j], (partner, layer))
            )
    for copy in spread:
        copy.wait_send()
    for copy in passed:
        copy.wait()


def gather_plane(kv, tags):
    if lax.axis_size("ctx") != SPAN:
        return tuple(lax.all_gather(part, "ctx", axis=0, tiled=True) for part in (kv, tags))
    rows, columns = kv.shape
    kv_all, tags_all = pl.pallas_call(
        gather_plane_kernel,
        out_shape=(
            jax.ShapeDtypeStruct((SPAN, rows, columns), kv.dtype),
            jax.ShapeDtypeStruct((SPAN, 1, rows), tags.dtype),
        ),
        in_specs=in_vmem(2),
        out_specs=tuple(in_vmem(2)),
        scratch_shapes=[
            pltpu.SemaphoreType.DMA((2, 2, CHIPS - 1)),
            pltpu.SemaphoreType.DMA((2, 2, CHIPS)),
        ],
        compiler_params=comm_params(2),
        cost_estimate=comm_cost(kv.size * 2 * SPAN),
    )(kv, tags[None])
    return kv_all.reshape(SPAN * rows, columns), tags_all.reshape(SPAN * rows)


def added(*parts):
    total = parts[0].astype(jnp.float32)
    for part in parts[1:]:
        total = total + part.astype(jnp.float32)
    return total


def reduce_plane(arrays, h_sems, p_sems):
    me, core, chip, partner = plane_of()
    layer = lax.axis_index("fsdp")
    handed, spread = [], []
    for a, (piece_of, halves, sums, arrived) in enumerate(arrays):
        for j in range(CHIPS):
            slot = (j + 1) % CHIPS
            handed.append(
                send(
                    piece_of(chip_at(chip, 1 - core, slot)),
                    halves.at[slot],
                    h_sems.at[0, a, slot],
                    h_sems.at[1, a, slot],
                    (partner, layer),
                )
            )
    for a, (piece_of, halves, sums, arrived) in enumerate(arrays):
        for j in range(CHIPS):
            slot = (j + 1) % CHIPS
            handed[a * CHIPS + j].wait_recv()
            mine = chip_at(chip, core, slot)

            def add_half(slab, carry, piece=piece_of(mine), halves=halves, sums=sums, slot=slot):
                sums[slot, slab] = added(piece[slab], halves[slot, slab]).astype(sums.dtype)
                return carry

            lax.fori_loop(0, sums.shape[1], add_half, 0)
            if slot:
                spread.append(
                    send(
                        sums.at[slot],
                        arrived.at[slot - 1],
                        p_sems.at[0, a, slot - 1],
                        p_sems.at[1, a, slot - 1],
                        (mine, layer),
                    )
                )
    return handed, spread


def plane_total(sums, arrived, slab):
    return added(sums[0, slab], *(arrived[j, slab] for j in range(CHIPS - 1)))


def plane_scratch(block, dtype):
    return [
        pltpu.VMEM((CHIPS, *block), dtype),
        pltpu.VMEM((CHIPS, *block), dtype),
        pltpu.VMEM((CHIPS - 1, *block), dtype),
    ]


def scatter_plane_kernel(x_ref, out_ref, halves, sums, arrived, h_sems, p_sems):
    me, core, chip, partner = plane_of()
    layer = lax.axis_index("fsdp")
    greet([(chip_at(chip, core, j), layer) for j in range(1, CHIPS)] + [(partner, layer)])
    arrays = [(lambda piece: x_ref.at[piece], halves, sums, arrived)]
    handed, spread = reduce_plane(arrays, h_sems, p_sems)
    for copy in spread:
        copy.wait_recv()

    def add_slab(slab, carry):
        out_ref[slab] = plane_total(sums, arrived, slab)
        return carry

    lax.fori_loop(0, x_ref.shape[1], add_slab, 0)
    for copy in handed + spread:
        copy.wait_send()


def scatter_plane(values):
    if lax.axis_size("ctx") != SPAN:
        own = lax.psum_scatter(values, "ctx", scatter_dimension=0, tiled=True)
        return own.astype(jnp.float32)
    rows, columns = values.shape
    slabs = 8
    block = (slabs, rows // SPAN // slabs, columns)
    return pl.pallas_call(
        scatter_plane_kernel,
        out_shape=jax.ShapeDtypeStruct(block, jnp.float32),
        in_specs=in_vmem(1),
        out_specs=in_vmem(1)[0],
        scratch_shapes=plane_scratch(block, values.dtype)
        + [pltpu.SemaphoreType.DMA((2, 1, CHIPS)), pltpu.SemaphoreType.DMA((2, 1, CHIPS - 1))],
        compiler_params=comm_params(3),
        cost_estimate=comm_cost(values.size * 2),
    )(values.reshape(SPAN, *block)).reshape(rows // SPAN, columns)


def reduce_rows_kernel(depth, count, *refs):
    inputs, outs, scratch = refs[:count], refs[count : 2 * count], refs[2 * count : 6 * count]
    h_sems, p_sems, z_sems, g_sems, f_sems = refs[6 * count :]
    me, core, chip, partner = plane_of()
    layer = lax.axis_index("fsdp")
    layers = [lax.rem(layer + d, depth) for d in range(1, depth)]
    peers = [chip_at(chip, core, j) for j in range(1, CHIPS)]
    greet([(me, other) for other in layers] + [(peer, layer) for peer in peers + [partner]])
    arrays, across = [], []
    for a, x_ref in enumerate(inputs):
        halves, sums, arrived, layers_ref = scratch[4 * a : 4 * a + 4]
        arrays.append((lambda piece, x_ref=x_ref: x_ref.at[:, piece], halves, sums, arrived))
        across.append(layers_ref)
    handed, spread = reduce_plane(arrays, h_sems, p_sems)
    moved = []
    for a, (_, _, sums, arrived) in enumerate(arrays):
        for copy in spread[a * (CHIPS - 1) : (a + 1) * (CHIPS - 1)]:
            copy.wait_recv()
        for d in list(range(1, depth)) + [0]:
            target = lax.rem(layer + d, depth)
            across[a][0, d] = plane_total(sums, arrived, target).astype(across[a].dtype)
            if d:
                moved.append(
                    send(
                        across[a].at[0, d],
                        across[a].at[1, d],
                        z_sems.at[0, a, d - 1],
                        z_sems.at[1, a, d - 1],
                        (me, target),
                    )
                )
    given, passed = [], []
    for a, out_ref in enumerate(outs):
        for copy in moved[a * (depth - 1) : (a + 1) * (depth - 1)]:
            copy.wait_recv()
        parts = [across[a][0, 0]] + [across[a][1, d] for d in range(1, depth)]
        out_ref[me] = added(*parts).astype(out_ref.dtype)
        mine = out_ref.at[me]
        for j, peer in enumerate(peers):
            given.append(send(mine, mine, g_sems.at[0, a, j], g_sems.at[1, a, j], (peer, layer)))
        passed.append(send(mine, mine, f_sems.at[0, a, 3], f_sems.at[1, a, 3], (partner, layer)))
    for a, out_ref in enumerate(outs):
        for j in range(CHIPS - 1):
            given[a * (CHIPS - 1) + j].wait_recv()
            block = out_ref.at[chip_at(chip, core, -j - 1)]
            passed.append(
                send(block, block, f_sems.at[0, a, j], f_sems.at[1, a, j], (partner, layer))
            )
    for copy in handed + spread + moved + given:
        copy.wait_send()
    for copy in passed:
        copy.wait()


def reduce_rows(arrays, number):
    if lax.axis_size("ctx") != SPAN:
        return [lax.psum(lax.psum_scatter(v, "fsdp", scatter_dimension=0), "ctx") for v in arrays]
    depth, count = arrays[0].shape[0], len(arrays)
    pieces, outs, scratch = [], [], []
    for values in arrays:
        _, rows, columns = values.shape
        piece = (rows // SPAN, columns)
        pieces.append(values.reshape(depth, SPAN, *piece))
        outs.append(jax.ShapeDtypeStruct((SPAN, *piece), values.dtype))
        scratch += plane_scratch((depth, *piece), values.dtype)
        scratch.append(pltpu.VMEM((2, depth, *piece), values.dtype))
    owned = pl.pallas_call(
        functools.partial(reduce_rows_kernel, depth, count),
        out_shape=tuple(outs),
        in_specs=in_vmem(count),
        out_specs=tuple(in_vmem(count)),
        scratch_shapes=scratch
        + [
            pltpu.SemaphoreType.DMA((2, count, CHIPS)),
            pltpu.SemaphoreType.DMA((2, count, CHIPS - 1)),
            pltpu.SemaphoreType.DMA((2, count, depth - 1)),
            pltpu.SemaphoreType.DMA((2, count, CHIPS - 1)),
            pltpu.SemaphoreType.DMA((2, count, CHIPS)),
        ],
        compiler_params=comm_params(number),
        cost_estimate=comm_cost(sum(values.size for values in arrays) * 2),
    )(*pieces)
    return [own.reshape(values.shape[1:]) for own, values in zip(owned, arrays)]


BLOCK = 128
LANES = (HEADS // KV_HEADS) * BLOCK


def dot(left, right, dims=(1, 0)):
    return lax.dot_general(
        left, right, (((dims[0],), (dims[1],)), ((), ())), preferred_element_type=jnp.float32
    )


def of_group(ref, group, at):
    first = group * (HEADS // KV_HEADS)
    heads = range(first, first + HEADS // KV_HEADS)
    return jnp.concatenate([ref[head * HEAD : (head + 1) * HEAD, at] for head in heads], 1)


def of_rows(ref, group, at):
    first = group * (HEADS // KV_HEADS)
    heads = range(first, first + HEADS // KV_HEADS)
    return jnp.concatenate([ref[head : head + 1, at] for head in heads], 1)


def columns_of(group, part):
    start = (part * KV_HEADS + group) * HEAD
    return slice(start, start + HEAD)


def mask_bias(tags, query_pos):
    tags = jnp.broadcast_to(tags, (BLOCK, BLOCK)).T
    key_pos = jnp.where(tags >= 0, tags, -tags - 1)
    allowed = (key_pos <= query_pos) & ((tags >= 0) | (key_pos == query_pos))
    bias = jnp.where(allowed, 0.0, negative)
    return jnp.concatenate([bias] * (HEADS // KV_HEADS), 1)


def attend_kernel(
    first_ref, q_ref, kv_ref, pos_ref, tag_ref, out_ref, log_ref, max_ref, sum_ref, acc_ref, kept
):
    blocks = kv_ref.shape[0] // BLOCK
    keep = kept.shape[0] == blocks

    def scores(group, at, rows, bias):
        keys = kv_ref[rows, columns_of(group, 0)]
        return dot(keys, of_group(q_ref, group, at)) + bias

    def query_block(qb, carry):
        at = pl.ds(pl.multiple_of(qb * BLOCK, BLOCK), BLOCK)
        max_ref[...] = jnp.full(max_ref.shape, negative, jnp.float32)
        sum_ref[...] = jnp.zeros(sum_ref.shape, jnp.float32)
        acc_ref[...] = jnp.zeros(acc_ref.shape, jnp.float32)
        limit = first_ref[blocks + qb]

        def find(kb, carry):
            @pl.when(first_ref[kb] <= limit)
            def _():
                rows = pl.ds(pl.multiple_of(kb * BLOCK, BLOCK), BLOCK)
                bias = mask_bias(tag_ref[kb], pos_ref[:, at])
                for group in range(KV_HEADS):
                    found = scores(group, at, rows, bias)
                    if keep:
                        kept[kb, group] = found
                    tops = jnp.max(found.reshape(BLOCK // 8, 8, LANES), 0)
                    max_ref[group] = jnp.maximum(max_ref[group], tops)

            return carry

        lax.fori_loop(0, blocks, find, 0)
        for group in range(KV_HEADS):
            top = jnp.max(max_ref[group], 0, keepdims=True)
            max_ref[group] = jnp.broadcast_to(top, max_ref.shape[1:])

        def gather(kb, carry):
            @pl.when(first_ref[kb] <= limit)
            def _():
                rows = pl.ds(pl.multiple_of(kb * BLOCK, BLOCK), BLOCK)
                bias = None if keep else mask_bias(tag_ref[kb], pos_ref[:, at])
                for group in range(KV_HEADS):
                    found = kept[kb, group] if keep else scores(group, at, rows, bias)
                    weights = jnp.exp(found - max_ref[group, :1])
                    sum_ref[group] += jnp.sum(weights.reshape(BLOCK // 8, 8, LANES), 0)
                    values = kv_ref[rows, columns_of(group, 1)]
                    acc_ref[group] += dot(values, weights.astype(jnp.bfloat16), (0, 0))

            return carry

        lax.fori_loop(0, blocks, gather, 0)
        for group in range(KV_HEADS):
            total = jnp.sum(sum_ref[group], 0, keepdims=True)
            attended = acc_ref[group] / total
            logs = max_ref[group, :1] + jnp.log(total)
            for j in range(HEADS // KV_HEADS):
                head = group * (HEADS // KV_HEADS) + j
                own = slice(j * BLOCK, (j + 1) * BLOCK)
                out_ref[head * HEAD : (head + 1) * HEAD, at] = attended[:, own]
                log_ref[head : head + 1, at] = logs[:, own]
        return carry

    lax.fori_loop(0, q_ref.shape[1] // BLOCK, query_block, 0)


def kernel_params():
    return pltpu.CompilerParams(vmem_limit_bytes=VMEM_BYTES)


def attend(firsts, queries, kv, query_pos, key_tags):
    blocks = kv.shape[0] // BLOCK
    slots = queries.shape[1]
    kept = blocks if blocks <= 16 else 1
    groups = (KV_HEADS, 8, LANES)
    work = 4 * kv.shape[0] * slots * HEADS * HEAD
    return pl.pallas_call(
        attend_kernel,
        out_shape=(
            jax.ShapeDtypeStruct(queries.shape, jnp.float32),
            jax.ShapeDtypeStruct((HEADS + 1, slots), jnp.float32),
        ),
        in_specs=[pl.BlockSpec(memory_space=pltpu.SMEM)] + in_vmem(4),
        out_specs=tuple(in_vmem(2)),
        scratch_shapes=[
            pltpu.VMEM(groups, jnp.float32),
            pltpu.VMEM(groups, jnp.float32),
            pltpu.VMEM((KV_HEADS, HEAD, LANES), jnp.float32),
            pltpu.VMEM((kept, KV_HEADS, BLOCK, LANES), jnp.float32),
        ],
        compiler_params=kernel_params(),
        cost_estimate=pl.CostEstimate(
            flops=work * 8, bytes_accessed=kv.size * 2, transcendentals=work // 256
        ),
    )(firsts, queries, kv, query_pos[None], key_tags.reshape(-1, 1, BLOCK))


def attend_back_kernel(
    first_ref, q_ref, kv_ref, pos_ref, tag_ref, grad_ref, log_ref, delta_ref, *refs
):
    blocks = kv_ref.shape[0] // BLOCK
    cos_ref, sin_ref, out_ref, dkv_ref, acc, dq_ref = refs
    dq_ref[...] = jnp.zeros(dq_ref.shape, dq_ref.dtype)

    def key_block(kb, carry):
        rows = pl.ds(pl.multiple_of(kb * BLOCK, BLOCK), BLOCK)
        acc[...] = jnp.zeros(acc.shape, jnp.float32)

        def query_block(qb, carry):
            @pl.when(first_ref[kb] <= first_ref[blocks + qb])
            def _():
                at = pl.ds(pl.multiple_of(qb * BLOCK, BLOCK), BLOCK)
                bias = mask_bias(tag_ref[kb], pos_ref[:, at])
                for group in range(KV_HEADS):
                    keys = kv_ref[rows, columns_of(group, 0)]
                    values = kv_ref[rows, columns_of(group, 1)]
                    queries = of_group(q_ref, group, at)
                    grads = of_group(grad_ref, group, at)
                    found = dot(keys, queries) + bias
                    probs = jnp.exp(found - of_rows(log_ref, group, at))
                    grad_probs = dot(values, grads)
                    grad_scores = probs * (grad_probs - of_rows(delta_ref, group, at))
                    grad_scores = grad_scores.astype(jnp.bfloat16)
                    acc[group] += dot(grad_scores, queries, (1, 1))
                    acc[KV_HEADS + group] += dot(probs.astype(jnp.bfloat16), grads, (1, 1))
                    grad_q = 0.125 * dot(keys, grad_scores, (0, 0))
                    for j in range(HEADS // KV_HEADS):
                        head = group * (HEADS // KV_HEADS) + j
                        own = slice(head * HEAD, (head + 1) * HEAD)
                        dq_ref[own, at] += grad_q[:, j * BLOCK : (j + 1) * BLOCK]

            return carry

        lax.fori_loop(0, q_ref.shape[1] // BLOCK, query_block, 0)
        dkv_ref[rows, :] = jnp.concatenate(
            [acc[index] for index in range(2 * KV_HEADS)], 1
        ).astype(dkv_ref.dtype)
        return carry

    lax.fori_loop(0, blocks, key_block, 0)
    half_dim = HEAD // 2

    def finish(qb, carry):
        at = pl.ds(pl.multiple_of(qb * BLOCK, BLOCK), BLOCK)
        cos_tab, sin_tab = cos_ref[:, at], sin_ref[:, at]
        for head in range(0, HEADS, 2):
            pair = []
            for start in range(head * HEAD, min(head + 2, HEADS) * HEAD, HEAD):
                low = dq_ref[start : start + half_dim, at]
                high = dq_ref[start + half_dim : start + HEAD, at]
                pair += [low * cos_tab + high * sin_tab, high * cos_tab - low * sin_tab]
            turned = jnp.concatenate(pair, 0).T
            own = slice(head * HEAD, head * HEAD + turned.shape[1])
            out_ref[at, own] = turned.astype(out_ref.dtype)
        return carry

    lax.fori_loop(0, q_ref.shape[1] // BLOCK, finish, 0)


def attend_back(firsts, queries, kv, query_pos, key_tags, grads, log_total, row_delta, tables):
    slots = queries.shape[1]
    work = 10 * kv.shape[0] * slots * HEADS * HEAD
    return pl.pallas_call(
        attend_back_kernel,
        out_shape=(
            jax.ShapeDtypeStruct(queries.shape[::-1], jnp.bfloat16),
            jax.ShapeDtypeStruct(kv.shape, jnp.bfloat16),
        ),
        in_specs=[pl.BlockSpec(memory_space=pltpu.SMEM)] + in_vmem(9),
        out_specs=tuple(in_vmem(2)),
        scratch_shapes=[
            pltpu.VMEM((2 * KV_HEADS, BLOCK, HEAD), jnp.float32),
            pltpu.VMEM(queries.shape, jnp.float32),
        ],
        compiler_params=kernel_params(),
        cost_estimate=pl.CostEstimate(
            flops=work * 6, bytes_accessed=kv.size * 4, transcendentals=work // 640
        ),
    )(firsts, queries, kv, query_pos[None], key_tags.reshape(-1, 1, BLOCK), grads, log_total, row_delta, *tables)


def on_device(
    tokens,
    w_query,
    w_key,
    w_value,
    w_out,
    w_gate,
    w_up,
    w_down,
    gain_attn,
    gain_ffn,
    router,
    cotangent,
    positions,
    lengths,
    chosen,
):
    hidden = tokens[0].astype(jnp.float32)
    row_count, width = hidden.shape
    qdim = HEADS * HEAD
    kdim = KV_HEADS * HEAD
    query_pos = positions[0]
    live = query_pos < lengths[0]
    selected = live & (chosen[0] == 1)
    live_mask = live.astype(jnp.float32)[:, None]
    chosen_mask = selected.astype(jnp.float32)[:, None]
    cos_tab, sin_tab = rope_tables(query_pos)
    key_tags = jnp.where(selected, query_pos, -query_pos - 1)
    depth = lax.axis_size("fsdp")
    own_rows = w_query.shape[0]
    w_out_full = lax.all_gather(w_out, "fsdp", axis=0, tiled=True)
    vectors = jnp.stack([gain_attn, gain_ffn, router], 1)
    own_attn = [w_query, jnp.concatenate([w_key, w_value, vectors], 1)]
    gathered = gather_rows([padded_to(own, 0) for own in own_attn], depth)
    w_query, gathered = (full[:, :own_rows].reshape(width, -1) for full in gathered)
    w_kv, vectors = gathered[:, : 2 * kdim], gathered[:, 2 * kdim :]
    gain_one, gain_two, router_vec = vectors.T.astype(jnp.float32)
    gating = jax.nn.sigmoid(jnp.sum(hidden * router_vec, -1, keepdims=True))
    grad_y = cotangent[0].astype(jnp.float32) * live_mask
    grad_inc = grad_y * chosen_mask * gating
    grad_ffn = grad_inc.astype(jnp.bfloat16)
    grad_ffn_all = lax.all_gather(grad_ffn, "fsdp", axis=0, tiled=True)

    normed_one, inv_one = norm_forward(hidden, gain_one)
    normed_one = normed_one.astype(jnp.bfloat16)
    query_raw = dot(w_query, normed_one, (0, 1))
    queries = rotate_columns(query_raw, cos_tab, sin_tab).astype(jnp.bfloat16) * 0.125
    kv_raw = dot(normed_one, w_kv)
    kv_own = jnp.concatenate([rotate(kv_raw[:, :kdim], cos_tab, sin_tab), kv_raw[:, kdim:]], 1)
    kv_all, tags_all = gather_plane(kv_own.astype(jnp.bfloat16), key_tags)
    first_tags = tags_all[::BLOCK]
    firsts = jnp.concatenate(
        [jnp.where(first_tags >= 0, first_tags, -first_tags - 1), query_pos[BLOCK - 1 :: BLOCK]]
    )
    attended, log_total = attend(firsts, queries, kv_all, query_pos, tags_all)
    attended, grad_ffn_all, w_out_full = lax.optimization_barrier(
        (attended, grad_ffn_all, w_out_full)
    )
    outcome = attended.astype(jnp.bfloat16)
    branch = dot(outcome, w_out_full, (0, 0))
    middle = hidden + branch
    normed_two, inv_two = norm_forward(middle, gain_two)
    normed_two = normed_two.astype(jnp.bfloat16)
    normed_all = lax.all_gather(normed_two, "fsdp", axis=0, tiled=True)
    inner_act, grad_gate_act, grad_up_act, grad_normed_part = ffn_both(
        normed_all, grad_ffn_all, w_gate, w_up, w_down
    )
    grad_normed_two = lax.psum_scatter(
        grad_normed_part, "fsdp", scatter_dimension=0, tiled=True
    ).astype(jnp.float32)
    ffn_part = jnp.dot(inner_act, w_down, preferred_element_type=jnp.float32).astype(jnp.bfloat16)
    grad_wgate = lax.dot_general(
        grad_gate_act, normed_all, across_rows, preferred_element_type=jnp.float32
    )
    grad_wup = lax.dot_general(
        grad_up_act, normed_all, across_rows, preferred_element_type=jnp.float32
    )
    grad_wdown = lax.dot_general(
        inner_act, grad_ffn_all, across_rows, preferred_element_type=jnp.float32
    )
    low = jnp.bfloat16
    grad_normed_two, ffn_part, *grads = lax.optimization_barrier(
        (grad_normed_two, ffn_part, *(g.astype(low) for g in (grad_wgate, grad_wup, grad_wdown)))
    )
    grad_normed_two, row_dot = grad_normed_two[:, :width], grad_normed_two[:, width:]
    totals = tuple(lax.psum(grad, "ctx") for grad in grads)
    grad_middle, grad_gain_two = norm_backward(middle, inv_two, gain_two, grad_normed_two)
    grad_branch = (grad_inc + grad_middle).astype(jnp.bfloat16)
    grad_attended = dot(w_out_full, grad_branch, (1, 1)).astype(jnp.bfloat16)
    spread_out = padded_to(outcome.reshape(depth, own_rows, row_count), 1)
    grad_wout = dot(spread_out.reshape(-1, row_count), grad_branch).astype(low)
    row_delta = jnp.sum(
        (grad_attended.astype(jnp.float32) * attended).reshape(HEADS, HEAD, row_count), 1
    )
    row_delta = jnp.pad(row_delta, ((0, 1), (0, 0)))
    grad_query_raw, grad_kv_all = attend_back(
        firsts,
        queries,
        kv_all,
        query_pos,
        tags_all,
        grad_attended,
        log_total,
        row_delta,
        (cos_tab.T, sin_tab.T),
    )
    grad_kv = scatter_plane(grad_kv_all)
    grad_logit = (jnp.sum(grad_inc * branch, -1, keepdims=True) + row_dot) * (1.0 - gating)
    grad_router = jnp.sum(hidden * grad_logit, 0)
    grad_kv_raw = jnp.concatenate(
        [rotate(grad_kv[:, :kdim], cos_tab, -sin_tab), grad_kv[:, kdim:]], 1
    ).astype(jnp.bfloat16)
    grad_normed_one = dot(grad_query_raw, w_query, (1, 1)) + dot(grad_kv_raw, w_kv, (1, 1))
    spread_one = padded_to(normed_one.reshape(row_count, depth, own_rows), -1)
    spread_one = spread_one.reshape(row_count, -1)
    padded_rows = spread_one.shape[1] // depth
    grad_wq = dot(spread_one, grad_query_raw, (0, 0)).astype(low)
    grad_wkv = dot(spread_one, grad_kv_raw, (0, 0)).astype(low)
    grad_hidden_one, grad_gain_one = norm_backward(hidden, inv_one, gain_one, grad_normed_one)
    grad_tokens = (grad_y + grad_logit * router_vec + grad_middle + grad_hidden_one).astype(
        jnp.bfloat16
    )
    vectors = jnp.stack([grad_gain_one, grad_gain_two, grad_router]).reshape(3, depth, own_rows)
    vectors = jnp.pad(vectors.transpose(1, 0, 2).reshape(depth, -1), ((0, 0), (0, -3 * own_rows % 1024)))
    vectors = jnp.pad(vectors.reshape(depth, -1, 1, 128), ((0, 0), (0, 0), (0, 7), (0, 0)))
    layered = [grad.reshape(depth, padded_rows, -1) for grad in (grad_wq, grad_wkv, grad_wout)]
    layered.append(vectors.reshape(depth, -1, 128))
    owned = reduce_rows(layered, 4)
    ffn_out = lax.psum_scatter(ffn_part, "fsdp", scatter_dimension=0, tiled=True)
    *owned, totals, ffn_out = lax.optimization_barrier((*owned, totals, ffn_out))
    increment = branch + ffn_out.astype(jnp.float32)
    block_out = live_mask * (hidden + chosen_mask * gating * increment)
    total_q, total_kv, total_out = (own[:own_rows].astype(jnp.float32) for own in owned[:3])
    total_k, total_v = total_kv[:, :kdim], total_kv[:, kdim:]
    mine = owned[3].reshape(-1, 8, 128)[:, 0].reshape(-1)[: 3 * own_rows].reshape(3, own_rows)
    total_gate, total_up, total_down = (total.astype(jnp.float32) for total in totals)
    return (
        block_out.astype(jnp.bfloat16)[None],
        grad_tokens[None],
        total_q,
        total_k,
        total_v,
        total_out,
        total_gate,
        total_up,
        total_down,
        mine[0],
        mine[1],
        mine[2],
    )


def solution(mesh):
    in_specs = (
        P("fsdp", "ctx", None),
        P("fsdp", None),
        P("fsdp", None),
        P("fsdp", None),
        P("fsdp", None),
        P("fsdp", None),
        P("fsdp", None),
        P("fsdp", None),
        P("fsdp"),
        P("fsdp"),
        P("fsdp"),
        P("fsdp", "ctx", None),
        P("fsdp", "ctx"),
        P("fsdp"),
        P("fsdp", "ctx"),
    )
    out_specs = (
        P("fsdp", "ctx", None),
        P("fsdp", "ctx", None),
        P("fsdp", None),
        P("fsdp", None),
        P("fsdp", None),
        P("fsdp", None),
        P("fsdp", None),
        P("fsdp", None),
        P("fsdp", None),
        P("fsdp"),
        P("fsdp"),
        P("fsdp"),
    )
    return jax.shard_map(
        on_device, mesh=mesh, in_specs=in_specs, out_specs=out_specs, check_vma=False
    )
```

```python
import functools

import jax
import jax.numpy as jnp
from jax import lax
from jax.experimental import pallas as pl
from jax.experimental.pallas import tpu as pltpu
from jax.sharding import PartitionSpec as P

HEADS = 15
KV_HEADS = 5
HEAD = 64


epsilon = 1e-05
negative = -1e30
across_rows = (((0,), (0,)), ((), ()))
across_cols = (((1,), (1,)), ((), ()))


def rope_tables(positions):
    half_dim = HEAD // 2
    frequency = 10000.0 ** (-2.0 * jnp.arange(half_dim, dtype=jnp.float32) / HEAD)
    angles = positions.astype(jnp.float32)[:, None] * frequency[None, :]
    return (jnp.cos(angles), jnp.sin(angles))


def rotate(values, cos_tab, sin_tab):
    slots, width = values.shape
    low, high = jnp.split(values.reshape(slots, width // HEAD, HEAD), 2, -1)
    cos_tab, sin_tab = cos_tab[:, None], sin_tab[:, None]
    turned = [low * cos_tab - high * sin_tab, high * cos_tab + low * sin_tab]
    return jnp.concatenate(turned, -1).reshape(slots, width)


def rotate_columns(values, cos_tab, sin_tab):
    width, slots = values.shape
    low, high = jnp.split(values.reshape(width // HEAD, HEAD, slots), 2, 1)
    cos_tab, sin_tab = cos_tab.T[None], sin_tab.T[None]
    turned = [low * cos_tab - high * sin_tab, high * cos_tab + low * sin_tab]
    return jnp.concatenate(turned, 1).reshape(width, slots)


def norm_forward(values, gain_vec):
    inv_rms = lax.rsqrt(jnp.mean(values * values, -1, keepdims=True) + epsilon)
    return (values * inv_rms * gain_vec, inv_rms)


def norm_backward(values, inv_rms, gain_vec, grad_normed):
    weighted = gain_vec * grad_normed
    grad_gain = jnp.sum(grad_normed * values * inv_rms, 0)
    cubed = inv_rms * inv_rms * inv_rms
    grad_values = inv_rms * weighted - values * cubed * jnp.mean(
        weighted * values, -1, keepdims=True
    )
    return (grad_values, grad_gain)


def padded_to(values, row_dim):
    pads = [(0, 0)] * values.ndim
    pads[row_dim] = (0, -values.shape[row_dim] % 128)
    return jnp.pad(values, pads)


def ffn_both(normed, grad_mixed, gate_rows, up_rows, down_rows):
    gate_proj = lax.dot_general(normed, gate_rows, across_cols, preferred_element_type=jnp.float32)
    up_proj = lax.dot_general(normed, up_rows, across_cols, preferred_element_type=jnp.float32)
    sigma = jax.nn.sigmoid(gate_proj)
    activated = gate_proj * sigma
    inner_act = (activated * up_proj).astype(jnp.bfloat16)
    grad_inner = lax.dot_general(
        grad_mixed, down_rows, across_cols, preferred_element_type=jnp.float32
    )
    grad_gate_act = (grad_inner * up_proj * sigma * (1.0 + gate_proj * (1.0 - sigma))).astype(
        jnp.bfloat16
    )
    grad_up_act = (grad_inner * activated).astype(jnp.bfloat16)
    grad_normed = jnp.dot(grad_gate_act, gate_rows, preferred_element_type=jnp.float32) + jnp.dot(
        grad_up_act, up_rows, preferred_element_type=jnp.float32
    )
    row_dot = jnp.sum(inner_act.astype(jnp.float32) * grad_inner, -1, keepdims=True)
    grad_normed = jnp.concatenate([grad_normed, row_dot], 1).astype(jnp.bfloat16)
    return (inner_act, grad_gate_act, grad_up_act, grad_normed)


CHIPS = 4
SPAN = 2 * CHIPS
VMEM_BYTES = 60 * 1024 * 1024
MESH = pl.DeviceIdType.MESH


def plane_of():
    me = lax.axis_index("ctx")
    core = lax.rem(me, 2)
    chip = me // 2
    return me, core, chip, me + 1 - 2 * core


def chip_at(chip, core, step):
    return 2 * lax.rem(chip + step + CHIPS, CHIPS) + core


def greet(devices):
    barrier = pltpu.get_barrier_semaphore()
    for device in devices:
        pl.semaphore_signal(barrier, inc=1, device_id=device, device_id_type=MESH)
    pl.semaphore_wait(barrier, len(devices))


def send(src, dst, send_sem, recv_sem, device):
    copy = pltpu.make_async_remote_copy(
        src_ref=src,
        dst_ref=dst,
        send_sem=send_sem,
        recv_sem=recv_sem,
        device_id=device,
        device_id_type=MESH,
    )
    copy.start()
    return copy


def comm_params(number):
    return pltpu.CompilerParams(
        collective_id=number, has_side_effects=True, vmem_limit_bytes=VMEM_BYTES
    )


def comm_cost(moved):
    return pl.CostEstimate(flops=0, bytes_accessed=moved * 30, transcendentals=0)


def in_vmem(count):
    return [pl.BlockSpec(memory_space=pltpu.VMEM)] * count


def gather_rows_kernel(depth, count, *refs):
    owns, outs = refs[:count], refs[count : 2 * count]
    z_sems, p_sems, f_sems = refs[2 * count :]
    me, core, chip, partner = plane_of()
    layer = lax.axis_index("fsdp")
    layers = [lax.rem(layer + d, depth) for d in range(1, depth)]
    peers = [chip_at(chip, core, j) for j in range(1, CHIPS)]
    greet([(me, other) for other in layers] + [(peer, layer) for peer in peers + [partner]])
    first, spread, passed = [], [], []
    for a, (own, out) in enumerate(zip(owns, outs)):
        for d, other in enumerate(layers):
            first.append(
                send(
                    own.at[me],
                    out.at[layer, me],
                    z_sems.at[0, a, d],
                    z_sems.at[1, a, d],
                    (me, other),
                )
            )
    for own, out in zip(owns, outs):
        for piece in range(SPAN):
            out[layer, piece] = own[piece]
    for a, out in enumerate(outs):
        for d in range(depth - 1):
            first[a * (depth - 1) + d].wait_recv()
            block = out.at[lax.rem(layer + depth - d - 1, depth), me]
            for j, peer in enumerate(peers):
                spread.append(
                    send(block, block, p_sems.at[0, a, d, j], p_sems.at[1, a, d, j], (peer, layer))
                )
            passed.append(
                send(block, block, f_sems.at[0, a, d, 3], f_sems.at[1, a, d, 3], (partner, layer))
            )
    arrivals = iter(spread)
    for a, out in enumerate(outs):
        for d in range(depth - 1):
            source = lax.rem(layer + depth - d - 1, depth)
            for j in range(CHIPS - 1):
                next(arrivals).wait_recv()
                block = out.at[source, chip_at(chip, core, -j - 1)]
                passed.append(
                    send(
                        block,
                        block,
                        f_sems.at[0, a, d, j],
                        f_sems.at[1, a, d, j],
                        (partner, layer),
                    )
                )
    for copy in first + spread:
        copy.wait_send()
    for copy in passed:
        copy.wait()


def gather_rows(arrays, depth):
    if lax.axis_size("ctx") != SPAN:
        return [lax.all_gather(own, "fsdp", axis=0) for own in arrays]
    count, pieces, outs = len(arrays), [], []
    for own in arrays:
        piece = (own.shape[0] // SPAN, own.shape[1])
        pieces.append(own.reshape(SPAN, *piece))
        outs.append(jax.ShapeDtypeStruct((depth, SPAN, *piece), own.dtype))
    whole = pl.pallas_call(
        functools.partial(gather_rows_kernel, depth, count),
        out_shape=tuple(outs),
        in_specs=in_vmem(count),
        out_specs=tuple(in_vmem(count)),
        scratch_shapes=[
            pltpu.SemaphoreType.DMA((2, count, depth - 1)),
            pltpu.SemaphoreType.DMA((2, count, depth - 1, CHIPS - 1)),
            pltpu.SemaphoreType.DMA((2, count, depth - 1, CHIPS)),
        ],
        compiler_params=comm_params(1),
        cost_estimate=comm_cost(sum(own.size for own in arrays) * 2 * depth),
    )(*pieces)
    return [full.reshape(depth, *own.shape) for full, own in zip(whole, arrays)]


def gather_plane_kernel(kv_ref, tag_ref, kv_out, tag_out, p_sems, f_sems):
    me, core, chip, partner = plane_of()
    layer = lax.axis_index("fsdp")
    peers = [chip_at(chip, core, j) for j in range(1, CHIPS)]
    greet([(peer, layer) for peer in peers + [partner]])
    pairs = ((kv_ref, kv_out), (tag_ref, tag_out))
    spread, passed = [], []
    for j, peer in enumerate(peers):
        for a, (own, out) in enumerate(pairs):
            spread.append(
                send(own, out.at[me], p_sems.at[0, a, j], p_sems.at[1, a, j], (peer, layer))
            )
    for a, (own, out) in enumerate(pairs):
        passed.append(
            send(own, out.at[me], f_sems.at[0, a, 3], f_sems.at[1, a, 3], (partner, layer))
        )
    kv_out[me] = kv_ref[...]
    tag_out[me] = tag_ref[...]
    for j in range(CHIPS - 1):
        for a, (own, out) in enumerate(pairs):
            spread[2 * j + a].wait_recv()
            block = out.at[chip_at(chip, core, -j - 1)]
            passed.append(
                send(block, block, f_sems.at[0, a, j], f_sems.at[1, a, j], (partner, layer))
            )
    for copy in spread:
        copy.wait_send()
    for copy in passed:
        copy.wait()


def gather_plane(kv, tags):
    if lax.axis_size("ctx") != SPAN:
        return tuple(lax.all_gather(part, "ctx", axis=0, tiled=True) for part in (kv, tags))
    rows, columns = kv.shape
    kv_all, tags_all = pl.pallas_call(
        gather_plane_kernel,
        out_shape=(
            jax.ShapeDtypeStruct((SPAN, rows, columns), kv.dtype),
            jax.ShapeDtypeStruct((SPAN, 1, rows), tags.dtype),
        ),
        in_specs=in_vmem(2),
        out_specs=tuple(in_vmem(2)),
        scratch_shapes=[
            pltpu.SemaphoreType.DMA((2, 2, CHIPS - 1)),
            pltpu.SemaphoreType.DMA((2, 2, CHIPS)),
        ],
        compiler_params=comm_params(2),
        cost_estimate=comm_cost(kv.size * 2 * SPAN),
    )(kv, tags[None])
    return kv_all.reshape(SPAN * rows, columns), tags_all.reshape(SPAN * rows)


def added(*parts):
    total = parts[0].astype(jnp.float32)
    for part in parts[1:]:
        total = total + part.astype(jnp.float32)
    return total


def reduce_plane(arrays, h_sems, p_sems):
    me, core, chip, partner = plane_of()
    layer = lax.axis_index("fsdp")
    handed, spread = [], []
    for a, (piece_of, halves, sums, arrived) in enumerate(arrays):
        for j in range(CHIPS):
            slot = (j + 1) % CHIPS
            handed.append(
                send(
                    piece_of(chip_at(chip, 1 - core, slot)),
                    halves.at[slot],
                    h_sems.at[0, a, slot],
                    h_sems.at[1, a, slot],
                    (partner, layer),
                )
            )
    for a, (piece_of, halves, sums, arrived) in enumerate(arrays):
        for j in range(CHIPS):
            slot = (j + 1) % CHIPS
            handed[a * CHIPS + j].wait_recv()
            mine = chip_at(chip, core, slot)

            def add_half(slab, carry, piece=piece_of(mine), halves=halves, sums=sums, slot=slot):
                sums[slot, slab] = added(piece[slab], halves[slot, slab]).astype(sums.dtype)
                return carry

            lax.fori_loop(0, sums.shape[1], add_half, 0)
            if slot:
                spread.append(
                    send(
                        sums.at[slot],
                        arrived.at[slot - 1],
                        p_sems.at[0, a, slot - 1],
                        p_sems.at[1, a, slot - 1],
                        (mine, layer),
                    )
                )
    return handed, spread


def plane_total(sums, arrived, slab):
    return added(sums[0, slab], *(arrived[j, slab] for j in range(CHIPS - 1)))


def plane_scratch(block, dtype):
    return [
        pltpu.VMEM((CHIPS, *block), dtype),
        pltpu.VMEM((CHIPS, *block), dtype),
        pltpu.VMEM((CHIPS - 1, *block), dtype),
    ]


def scatter_plane_kernel(x_ref, out_ref, halves, sums, arrived, h_sems, p_sems):
    me, core, chip, partner = plane_of()
    layer = lax.axis_index("fsdp")
    greet([(chip_at(chip, core, j), layer) for j in range(1, CHIPS)] + [(partner, layer)])
    arrays = [(lambda piece: x_ref.at[piece], halves, sums, arrived)]
    handed, spread = reduce_plane(arrays, h_sems, p_sems)
    for copy in spread:
        copy.wait_recv()

    def add_slab(slab, carry):
        out_ref[slab] = plane_total(sums, arrived, slab)
        return carry

    lax.fori_loop(0, x_ref.shape[1], add_slab, 0)
    for copy in handed + spread:
        copy.wait_send()


def scatter_plane(values):
    if lax.axis_size("ctx") != SPAN:
        own = lax.psum_scatter(values, "ctx", scatter_dimension=0, tiled=True)
        return own.astype(jnp.float32)
    rows, columns = values.shape
    slabs = 8
    block = (slabs, rows // SPAN // slabs, columns)
    return pl.pallas_call(
        scatter_plane_kernel,
        out_shape=jax.ShapeDtypeStruct(block, jnp.float32),
        in_specs=in_vmem(1),
        out_specs=in_vmem(1)[0],
        scratch_shapes=plane_scratch(block, values.dtype)
        + [pltpu.SemaphoreType.DMA((2, 1, CHIPS)), pltpu.SemaphoreType.DMA((2, 1, CHIPS - 1))],
        compiler_params=comm_params(3),
        cost_estimate=comm_cost(values.size * 2),
    )(values.reshape(SPAN, *block)).reshape(rows // SPAN, columns)


def reduce_rows_kernel(depth, count, *refs):
    inputs, outs, scratch = refs[:count], refs[count : 2 * count], refs[2 * count : 6 * count]
    h_sems, p_sems, z_sems, g_sems, f_sems = refs[6 * count :]
    me, core, chip, partner = plane_of()
    layer = lax.axis_index("fsdp")
    layers = [lax.rem(layer + d, depth) for d in range(1, depth)]
    peers = [chip_at(chip, core, j) for j in range(1, CHIPS)]
    greet([(me, other) for other in layers] + [(peer, layer) for peer in peers + [partner]])
    arrays, across = [], []
    for a, x_ref in enumerate(inputs):
        halves, sums, arrived, layers_ref = scratch[4 * a : 4 * a + 4]
        arrays.append((lambda piece, x_ref=x_ref: x_ref.at[:, piece], halves, sums, arrived))
        across.append(layers_ref)
    handed, spread = reduce_plane(arrays, h_sems, p_sems)
    moved = []
    for a, (_, _, sums, arrived) in enumerate(arrays):
        for copy in spread[a * (CHIPS - 1) : (a + 1) * (CHIPS - 1)]:
            copy.wait_recv()
        for d in list(range(1, depth)) + [0]:
            target = lax.rem(layer + d, depth)
            across[a][0, d] = plane_total(sums, arrived, target).astype(across[a].dtype)
            if d:
                moved.append(
                    send(
                        across[a].at[0, d],
                        across[a].at[1, d],
                        z_sems.at[0, a, d - 1],
                        z_sems.at[1, a, d - 1],
                        (me, target),
                    )
                )
    given, passed = [], []
    for a, out_ref in enumerate(outs):
        for copy in moved[a * (depth - 1) : (a + 1) * (depth - 1)]:
            copy.wait_recv()
        parts = [across[a][0, 0]] + [across[a][1, d] for d in range(1, depth)]
        out_ref[me] = added(*parts).astype(out_ref.dtype)
        mine = out_ref.at[me]
        for j, peer in enumerate(peers):
            given.append(send(mine, mine, g_sems.at[0, a, j], g_sems.at[1, a, j], (peer, layer)))
        passed.append(send(mine, mine, f_sems.at[0, a, 3], f_sems.at[1, a, 3], (partner, layer)))
    for a, out_ref in enumerate(outs):
        for j in range(CHIPS - 1):
            given[a * (CHIPS - 1) + j].wait_recv()
            block = out_ref.at[chip_at(chip, core, -j - 1)]
            passed.append(
                send(block, block, f_sems.at[0, a, j], f_sems.at[1, a, j], (partner, layer))
            )
    for copy in handed + spread + moved + given:
        copy.wait_send()
    for copy in passed:
        copy.wait()


def reduce_rows(arrays, number):
    if lax.axis_size("ctx") != SPAN:
        return [lax.psum(lax.psum_scatter(v, "fsdp", scatter_dimension=0), "ctx") for v in arrays]
    depth, count = arrays[0].shape[0], len(arrays)
    pieces, outs, scratch = [], [], []
    for values in arrays:
        _, rows, columns = values.shape
        piece = (rows // SPAN, columns)
        pieces.append(values.reshape(depth, SPAN, *piece))
        outs.append(jax.ShapeDtypeStruct((SPAN, *piece), values.dtype))
        scratch += plane_scratch((depth, *piece), values.dtype)
        scratch.append(pltpu.VMEM((2, depth, *piece), values.dtype))
    owned = pl.pallas_call(
        functools.partial(reduce_rows_kernel, depth, count),
        out_shape=tuple(outs),
        in_specs=in_vmem(count),
        out_specs=tuple(in_vmem(count)),
        scratch_shapes=scratch
        + [
            pltpu.SemaphoreType.DMA((2, count, CHIPS)),
            pltpu.SemaphoreType.DMA((2, count, CHIPS - 1)),
            pltpu.SemaphoreType.DMA((2, count, depth - 1)),
            pltpu.SemaphoreType.DMA((2, count, CHIPS - 1)),
            pltpu.SemaphoreType.DMA((2, count, CHIPS)),
        ],
        compiler_params=comm_params(number),
        cost_estimate=comm_cost(sum(values.size for values in arrays) * 2),
    )(*pieces)
    return [own.reshape(values.shape[1:]) for own, values in zip(owned, arrays)]


BLOCK = 128
LANES = (HEADS // KV_HEADS) * BLOCK


def dot(left, right, dims=(1, 0)):
    return lax.dot_general(
        left, right, (((dims[0],), (dims[1],)), ((), ())), preferred_element_type=jnp.float32
    )


def of_group(ref, group, at):
    first = group * (HEADS // KV_HEADS)
    heads = range(first, first + HEADS // KV_HEADS)
    return jnp.concatenate([ref[head * HEAD : (head + 1) * HEAD, at] for head in heads], 1)


def of_rows(ref, group, at):
    first = group * (HEADS // KV_HEADS)
    heads = range(first, first + HEADS // KV_HEADS)
    return jnp.concatenate([ref[head : head + 1, at] for head in heads], 1)


def columns_of(group, part):
    start = (part * KV_HEADS + group) * HEAD
    return slice(start, start + HEAD)


def mask_bias(tags, query_pos):
    tags = jnp.broadcast_to(tags, (BLOCK, BLOCK)).T
    key_pos = jnp.where(tags >= 0, tags, -tags - 1)
    allowed = (key_pos <= query_pos) & ((tags >= 0) | (key_pos == query_pos))
    bias = jnp.where(allowed, 0.0, negative)
    return jnp.concatenate([bias] * (HEADS // KV_HEADS), 1)


def attend_kernel(
    first_ref, q_ref, kv_ref, pos_ref, tag_ref, out_ref, log_ref, max_ref, sum_ref, acc_ref, kept
):
    blocks = kv_ref.shape[0] // BLOCK
    keep = kept.shape[0] == blocks

    def scores(group, at, rows, bias):
        keys = kv_ref[rows, columns_of(group, 0)]
        return dot(keys, of_group(q_ref, group, at)) + bias

    def query_block(qb, carry):
        at = pl.ds(pl.multiple_of(qb * BLOCK, BLOCK), BLOCK)
        max_ref[...] = jnp.full(max_ref.shape, negative, jnp.float32)
        sum_ref[...] = jnp.zeros(sum_ref.shape, jnp.float32)
        acc_ref[...] = jnp.zeros(acc_ref.shape, jnp.float32)
        limit = first_ref[blocks + qb]

        def find(kb, carry):
            @pl.when(first_ref[kb] <= limit)
            def _():
                rows = pl.ds(pl.multiple_of(kb * BLOCK, BLOCK), BLOCK)
                bias = mask_bias(tag_ref[kb], pos_ref[:, at])
                for group in range(KV_HEADS):
                    found = scores(group, at, rows, bias)
                    if keep:
                        kept[kb, group] = found
                    tops = jnp.max(found.reshape(BLOCK // 8, 8, LANES), 0)
                    max_ref[group] = jnp.maximum(max_ref[group], tops)

            return carry

        lax.fori_loop(0, blocks, find, 0)
        for group in range(KV_HEADS):
            top = jnp.max(max_ref[group], 0, keepdims=True)
            max_ref[group] = jnp.broadcast_to(top, max_ref.shape[1:])

        def gather(kb, carry):
            @pl.when(first_ref[kb] <= limit)
            def _():
                rows = pl.ds(pl.multiple_of(kb * BLOCK, BLOCK), BLOCK)
                bias = None if keep else mask_bias(tag_ref[kb], pos_ref[:, at])
                for group in range(KV_HEADS):
                    found = kept[kb, group] if keep else scores(group, at, rows, bias)
                    weights = jnp.exp(found - max_ref[group, :1])
                    sum_ref[group] += jnp.sum(weights.reshape(BLOCK // 8, 8, LANES), 0)
                    values = kv_ref[rows, columns_of(group, 1)]
                    acc_ref[group] += dot(values, weights.astype(jnp.bfloat16), (0, 0))

            return carry

        lax.fori_loop(0, blocks, gather, 0)
        for group in range(KV_HEADS):
            total = jnp.sum(sum_ref[group], 0, keepdims=True)
            attended = acc_ref[group] / total
            logs = max_ref[group, :1] + jnp.log(total)
            for j in range(HEADS // KV_HEADS):
                head = group * (HEADS // KV_HEADS) + j
                own = slice(j * BLOCK, (j + 1) * BLOCK)
                out_ref[head * HEAD : (head + 1) * HEAD, at] = attended[:, own]
                log_ref[head : head + 1, at] = logs[:, own]
        return carry

    lax.fori_loop(0, q_ref.shape[1] // BLOCK, query_block, 0)


def kernel_params():
    return pltpu.CompilerParams(vmem_limit_bytes=VMEM_BYTES)


def attend(firsts, queries, kv, query_pos, key_tags):
    blocks = kv.shape[0] // BLOCK
    slots = queries.shape[1]
    kept = blocks if blocks <= 16 else 1
    groups = (KV_HEADS, 8, LANES)
    work = 4 * kv.shape[0] * slots * HEADS * HEAD
    return pl.pallas_call(
        attend_kernel,
        out_shape=(
            jax.ShapeDtypeStruct(queries.shape, jnp.float32),
            jax.ShapeDtypeStruct((HEADS + 1, slots), jnp.float32),
        ),
        in_specs=[pl.BlockSpec(memory_space=pltpu.SMEM)] + in_vmem(4),
        out_specs=tuple(in_vmem(2)),
        scratch_shapes=[
            pltpu.VMEM(groups, jnp.float32),
            pltpu.VMEM(groups, jnp.float32),
            pltpu.VMEM((KV_HEADS, HEAD, LANES), jnp.float32),
            pltpu.VMEM((kept, KV_HEADS, BLOCK, LANES), jnp.float32),
        ],
        compiler_params=kernel_params(),
        cost_estimate=pl.CostEstimate(
            flops=work * 8, bytes_accessed=kv.size * 2, transcendentals=work // 256
        ),
    )(firsts, queries, kv, query_pos[None], key_tags.reshape(-1, 1, BLOCK))


def attend_back_kernel(
    first_ref, q_ref, kv_ref, pos_ref, tag_ref, grad_ref, log_ref, delta_ref, *refs
):
    blocks = kv_ref.shape[0] // BLOCK
    cos_ref, sin_ref, out_ref, dkv_ref, acc, dq_ref = refs
    dq_ref[...] = jnp.zeros(dq_ref.shape, dq_ref.dtype)

    def key_block(kb, carry):
        rows = pl.ds(pl.multiple_of(kb * BLOCK, BLOCK), BLOCK)
        acc[...] = jnp.zeros(acc.shape, jnp.float32)

        def query_block(qb, carry):
            @pl.when(first_ref[kb] <= first_ref[blocks + qb])
            def _():
                at = pl.ds(pl.multiple_of(qb * BLOCK, BLOCK), BLOCK)
                bias = mask_bias(tag_ref[kb], pos_ref[:, at])
                for group in range(KV_HEADS):
                    keys = kv_ref[rows, columns_of(group, 0)]
                    values = kv_ref[rows, columns_of(group, 1)]
                    queries = of_group(q_ref, group, at)
                    grads = of_group(grad_ref, group, at)
                    found = dot(keys, queries) + bias
                    probs = jnp.exp(found - of_rows(log_ref, group, at))
                    grad_probs = dot(values, grads)
                    grad_scores = probs * (grad_probs - of_rows(delta_ref, group, at))
                    grad_scores = grad_scores.astype(jnp.bfloat16)
                    acc[group] += dot(grad_scores, queries, (1, 1))
                    acc[KV_HEADS + group] += dot(probs.astype(jnp.bfloat16), grads, (1, 1))
                    grad_q = 0.125 * dot(keys, grad_scores, (0, 0))
                    for j in range(HEADS // KV_HEADS):
                        head = group * (HEADS // KV_HEADS) + j
                        own = slice(head * HEAD, (head + 1) * HEAD)
                        dq_ref[own, at] += grad_q[:, j * BLOCK : (j + 1) * BLOCK]

            return carry

        lax.fori_loop(0, q_ref.shape[1] // BLOCK, query_block, 0)
        dkv_ref[rows, :] = jnp.concatenate(
            [acc[index] for index in range(2 * KV_HEADS)], 1
        ).astype(dkv_ref.dtype)
        return carry

    lax.fori_loop(0, blocks, key_block, 0)
    half_dim = HEAD // 2

    def finish(qb, carry):
        at = pl.ds(pl.multiple_of(qb * BLOCK, BLOCK), BLOCK)
        cos_tab, sin_tab = cos_ref[:, at], sin_ref[:, at]
        for head in range(0, HEADS, 2):
            pair = []
            for start in range(head * HEAD, min(head + 2, HEADS) * HEAD, HEAD):
                low = dq_ref[start : start + half_dim, at]
                high = dq_ref[start + half_dim : start + HEAD, at]
                pair += [low * cos_tab + high * sin_tab, high * cos_tab - low * sin_tab]
            if len(pair) == 2:
                pair += [jnp.zeros_like(part) for part in pair]
            turned = jnp.concatenate(pair, 0).T
            own = slice(head * HEAD, head * HEAD + turned.shape[1])
            out_ref[at, own] = turned.astype(out_ref.dtype)
        return carry

    lax.fori_loop(0, q_ref.shape[1] // BLOCK, finish, 0)


def attend_back(firsts, queries, kv, query_pos, key_tags, grads, log_total, row_delta, tables):
    slots = queries.shape[1]
    work = 10 * kv.shape[0] * slots * HEADS * HEAD
    return pl.pallas_call(
        attend_back_kernel,
        out_shape=(
            jax.ShapeDtypeStruct((slots, -(-HEADS // 2) * 2 * HEAD), jnp.bfloat16),
            jax.ShapeDtypeStruct(kv.shape, jnp.bfloat16),
        ),
        in_specs=[pl.BlockSpec(memory_space=pltpu.SMEM)] + in_vmem(9),
        out_specs=tuple(in_vmem(2)),
        scratch_shapes=[
            pltpu.VMEM((2 * KV_HEADS, BLOCK, HEAD), jnp.float32),
            pltpu.VMEM(queries.shape, jnp.float32),
        ],
        compiler_params=kernel_params(),
        cost_estimate=pl.CostEstimate(
            flops=work * 6, bytes_accessed=kv.size * 4, transcendentals=work // 640
        ),
    )(firsts, queries, kv, query_pos[None], key_tags.reshape(-1, 1, BLOCK), grads, log_total, row_delta, *tables)


def on_device(
    tokens,
    w_query,
    w_key,
    w_value,
    w_out,
    w_gate,
    w_up,
    w_down,
    gain_attn,
    gain_ffn,
    router,
    cotangent,
    positions,
    lengths,
    chosen,
):
    hidden = tokens[0].astype(jnp.float32)
    row_count, width = hidden.shape
    qdim = HEADS * HEAD
    kdim = KV_HEADS * HEAD
    query_pos = positions[0]
    live = query_pos < lengths[0]
    selected = live & (chosen[0] == 1)
    live_mask = live.astype(jnp.float32)[:, None]
    chosen_mask = selected.astype(jnp.float32)[:, None]
    cos_tab, sin_tab = rope_tables(query_pos)
    key_tags = jnp.where(selected, query_pos, -query_pos - 1)
    depth = lax.axis_size("fsdp")
    own_rows = w_query.shape[0]
    w_out_full = lax.all_gather(w_out, "fsdp", axis=0, tiled=True)
    vectors = jnp.stack([gain_attn, gain_ffn, router], 1)
    own_attn = [padded_to(w_query, 1), jnp.concatenate([w_key, w_value, vectors], 1)]
    gathered = gather_rows([padded_to(own, 0) for own in own_attn], depth)
    padded_rows = gathered[0].shape[1]
    w_query = gathered[0].reshape(depth * padded_rows, -1)
    gathered = gathered[1][:, :own_rows].reshape(width, -1)
    w_kv, vectors = gathered[:, : 2 * kdim], gathered[:, 2 * kdim :]
    gain_one, gain_two, router_vec = vectors.T.astype(jnp.float32)
    gating = jax.nn.sigmoid(jnp.sum(hidden * router_vec, -1, keepdims=True))
    grad_y = cotangent[0].astype(jnp.float32) * live_mask
    grad_inc = grad_y * chosen_mask * gating
    grad_ffn = grad_inc.astype(jnp.bfloat16)
    grad_ffn_all = lax.all_gather(grad_ffn, "fsdp", axis=0, tiled=True)

    normed_one, inv_one = norm_forward(hidden, gain_one)
    normed_one = normed_one.astype(jnp.bfloat16)
    spread_one = padded_to(normed_one.reshape(row_count, depth, own_rows), -1)
    spread_one = spread_one.reshape(row_count, -1)
    query_raw = dot(w_query, spread_one, (0, 1))[:qdim]
    queries = rotate_columns(query_raw, cos_tab, sin_tab).astype(jnp.bfloat16) * 0.125
    kv_raw = dot(normed_one, w_kv)
    kv_own = jnp.concatenate([rotate(kv_raw[:, :kdim], cos_tab, sin_tab), kv_raw[:, kdim:]], 1)
    kv_all, tags_all = gather_plane(kv_own.astype(jnp.bfloat16), key_tags)
    first_tags = tags_all[::BLOCK]
    firsts = jnp.concatenate(
        [jnp.where(first_tags >= 0, first_tags, -first_tags - 1), query_pos[BLOCK - 1 :: BLOCK]]
    )
    attended, log_total = attend(firsts, queries, kv_all, query_pos, tags_all)
    attended, grad_ffn_all, w_out_full = lax.optimization_barrier(
        (attended, grad_ffn_all, w_out_full)
    )
    outcome = attended.astype(jnp.bfloat16)
    branch = dot(outcome, w_out_full, (0, 0))
    middle = hidden + branch
    normed_two, inv_two = norm_forward(middle, gain_two)
    normed_two = normed_two.astype(jnp.bfloat16)
    normed_all = lax.all_gather(normed_two, "fsdp", axis=0, tiled=True)
    inner_act, grad_gate_act, grad_up_act, grad_normed_part = ffn_both(
        normed_all, grad_ffn_all, w_gate, w_up, w_down
    )
    grad_normed_two = lax.psum_scatter(
        grad_normed_part, "fsdp", scatter_dimension=0, tiled=True
    ).astype(jnp.float32)
    ffn_part = jnp.dot(inner_act, w_down, preferred_element_type=jnp.float32).astype(jnp.bfloat16)
    grad_wgate = lax.dot_general(
        grad_gate_act, normed_all, across_rows, preferred_element_type=jnp.float32
    )
    grad_wup = lax.dot_general(
        grad_up_act, normed_all, across_rows, preferred_element_type=jnp.float32
    )
    grad_wdown = lax.dot_general(
        inner_act, grad_ffn_all, across_rows, preferred_element_type=jnp.float32
    )
    low = jnp.bfloat16
    grad_normed_two, ffn_part, *grads = lax.optimization_barrier(
        (grad_normed_two, ffn_part, *(g.astype(low) for g in (grad_wgate, grad_wup, grad_wdown)))
    )
    grad_normed_two, row_dot = grad_normed_two[:, :width], grad_normed_two[:, width:]
    totals = tuple(lax.psum(grad, "ctx") for grad in grads)
    grad_middle, grad_gain_two = norm_backward(middle, inv_two, gain_two, grad_normed_two)
    grad_branch = (grad_inc + grad_middle).astype(jnp.bfloat16)
    grad_attended = dot(w_out_full, grad_branch, (1, 1)).astype(jnp.bfloat16)
    spread_out = padded_to(outcome.reshape(depth, own_rows, row_count), 1)
    grad_wout = dot(spread_out.reshape(-1, row_count), padded_to(grad_branch, 1)).astype(low)
    row_delta = jnp.sum(
        (grad_attended.astype(jnp.float32) * attended).reshape(HEADS, HEAD, row_count), 1
    )
    row_delta = jnp.pad(row_delta, ((0, 1), (0, 0)))
    grad_query_raw, grad_kv_all = attend_back(
        firsts,
        queries,
        kv_all,
        query_pos,
        tags_all,
        grad_attended,
        log_total,
        row_delta,
        (cos_tab.T, sin_tab.T),
    )
    grad_kv = scatter_plane(grad_kv_all)
    grad_logit = (jnp.sum(grad_inc * branch, -1, keepdims=True) + row_dot) * (1.0 - gating)
    grad_router = jnp.sum(hidden * grad_logit, 0)
    grad_kv_raw = jnp.concatenate(
        [rotate(grad_kv[:, :kdim], cos_tab, -sin_tab), grad_kv[:, kdim:]], 1
    ).astype(jnp.bfloat16)
    grad_normed_one = dot(grad_query_raw, w_query, (1, 1)).reshape(row_count, depth, -1)
    grad_normed_one = grad_normed_one[..., :own_rows].reshape(row_count, width)
    grad_normed_one = grad_normed_one + dot(grad_kv_raw, w_kv, (1, 1))
    grad_wq = dot(spread_one, grad_query_raw, (0, 0)).astype(low)
    grad_wkv = dot(spread_one, grad_kv_raw, (0, 0)).astype(low)
    grad_hidden_one, grad_gain_one = norm_backward(hidden, inv_one, gain_one, grad_normed_one)
    grad_tokens = (grad_y + grad_logit * router_vec + grad_middle + grad_hidden_one).astype(
        jnp.bfloat16
    )
    vectors = jnp.stack([grad_gain_one, grad_gain_two, grad_router]).reshape(3, depth, own_rows)
    vectors = jnp.pad(vectors.transpose(1, 0, 2).reshape(depth, -1), ((0, 0), (0, -3 * own_rows % 1024)))
    vectors = jnp.pad(vectors.reshape(depth, -1, 1, 128), ((0, 0), (0, 0), (0, 7), (0, 0)))
    layered = [grad.reshape(depth, padded_rows, -1) for grad in (grad_wq, grad_wkv, grad_wout)]
    layered.append(vectors.reshape(depth, -1, 128))
    owned = reduce_rows(layered, 4)
    ffn_out = lax.psum_scatter(ffn_part, "fsdp", scatter_dimension=0, tiled=True)
    *owned, totals, ffn_out = lax.optimization_barrier((*owned, totals, ffn_out))
    increment = branch + ffn_out.astype(jnp.float32)
    block_out = live_mask * (hidden + chosen_mask * gating * increment)
    total_q, total_kv, total_out = (own[:own_rows].astype(jnp.float32) for own in owned[:3])
    total_q, total_out = total_q[:, :qdim], total_out[:, :width]
    total_k, total_v = total_kv[:, :kdim], total_kv[:, kdim:]
    mine = owned[3].reshape(-1, 8, 128)[:, 0].reshape(-1)[: 3 * own_rows].reshape(3, own_rows)
    total_gate, total_up, total_down = (total.astype(jnp.float32) for total in totals)
    return (
        block_out.astype(jnp.bfloat16)[None],
        grad_tokens[None],
        total_q,
        total_k,
        total_v,
        total_out,
        total_gate,
        total_up,
        total_down,
        mine[0],
        mine[1],
        mine[2],
    )


def solution(mesh):
    in_specs = (
        P("fsdp", "ctx", None),
        P("fsdp", None),
        P("fsdp", None),
        P("fsdp", None),
        P("fsdp", None),
        P("fsdp", None),
        P("fsdp", None),
        P("fsdp", None),
        P("fsdp"),
        P("fsdp"),
        P("fsdp"),
        P("fsdp", "ctx", None),
        P("fsdp", "ctx"),
        P("fsdp"),
        P("fsdp", "ctx"),
    )
    out_specs = (
        P("fsdp", "ctx", None),
        P("fsdp", "ctx", None),
        P("fsdp", None),
        P("fsdp", None),
        P("fsdp", None),
        P("fsdp", None),
        P("fsdp", None),
        P("fsdp", None),
        P("fsdp", None),
        P("fsdp"),
        P("fsdp"),
        P("fsdp"),
    )
    return jax.shard_map(
        on_device, mesh=mesh, in_specs=in_specs, out_specs=out_specs, check_vma=False
    )
```

```python
import functools

import jax
import jax.numpy as jnp
from jax import lax
from jax.experimental import pallas as pl
from jax.experimental.pallas import tpu as pltpu
from jax.sharding import PartitionSpec as P

HEADS = 15
KV_HEADS = 5
HEAD = 64


epsilon = 1e-05
negative = -1e30
across_rows = (((0,), (0,)), ((), ()))
across_cols = (((1,), (1,)), ((), ()))


def rope_tables(positions):
    half_dim = HEAD // 2
    frequency = 10000.0 ** (-2.0 * jnp.arange(half_dim, dtype=jnp.float32) / HEAD)
    angles = positions.astype(jnp.float32)[:, None] * frequency[None, :]
    return (jnp.cos(angles), jnp.sin(angles))


def rotate(values, cos_tab, sin_tab):
    slots, width = values.shape
    low, high = jnp.split(values.reshape(slots, width // HEAD, HEAD), 2, -1)
    cos_tab, sin_tab = cos_tab[:, None], sin_tab[:, None]
    turned = [low * cos_tab - high * sin_tab, high * cos_tab + low * sin_tab]
    return jnp.concatenate(turned, -1).reshape(slots, width)


def rotate_columns(values, cos_tab, sin_tab):
    width, slots = values.shape
    low, high = jnp.split(values.reshape(width // HEAD, HEAD, slots), 2, 1)
    cos_tab, sin_tab = cos_tab.T[None], sin_tab.T[None]
    turned = [low * cos_tab - high * sin_tab, high * cos_tab + low * sin_tab]
    return jnp.concatenate(turned, 1).reshape(width, slots)


def norm_forward(values, gain_vec):
    inv_rms = lax.rsqrt(jnp.mean(values * values, -1, keepdims=True) + epsilon)
    return (values * inv_rms * gain_vec, inv_rms)


def norm_backward(values, inv_rms, gain_vec, grad_normed):
    weighted = gain_vec * grad_normed
    grad_gain = jnp.sum(grad_normed * values * inv_rms, 0)
    cubed = inv_rms * inv_rms * inv_rms
    grad_values = inv_rms * weighted - values * cubed * jnp.mean(
        weighted * values, -1, keepdims=True
    )
    return (grad_values, grad_gain)


def padded_to(values, row_dim):
    pads = [(0, 0)] * values.ndim
    pads[row_dim] = (0, -values.shape[row_dim] % 128)
    return jnp.pad(values, pads)


def ffn_both(normed, grad_mixed, gate_rows, up_rows, down_rows):
    gate_proj = lax.dot_general(normed, gate_rows, across_cols, preferred_element_type=jnp.float32)
    up_proj = lax.dot_general(normed, up_rows, across_cols, preferred_element_type=jnp.float32)
    sigma = jax.nn.sigmoid(gate_proj)
    activated = gate_proj * sigma
    inner_act = (activated * up_proj).astype(jnp.bfloat16)
    grad_inner = lax.dot_general(
        grad_mixed, down_rows, across_cols, preferred_element_type=jnp.float32
    )
    grad_gate_act = (grad_inner * up_proj * sigma * (1.0 + gate_proj * (1.0 - sigma))).astype(
        jnp.bfloat16
    )
    grad_up_act = (grad_inner * activated).astype(jnp.bfloat16)
    grad_normed = jnp.dot(grad_gate_act, gate_rows, preferred_element_type=jnp.float32) + jnp.dot(
        grad_up_act, up_rows, preferred_element_type=jnp.float32
    )
    row_dot = jnp.sum(inner_act.astype(jnp.float32) * grad_inner, -1, keepdims=True)
    grad_normed = jnp.concatenate([grad_normed, row_dot], 1).astype(jnp.bfloat16)
    return (inner_act, grad_gate_act, grad_up_act, grad_normed)


CHIPS = 4
SPAN = 2 * CHIPS
VMEM_BYTES = 60 * 1024 * 1024
MESH = pl.DeviceIdType.MESH


def plane_of():
    me = lax.axis_index("ctx")
    core = lax.rem(me, 2)
    chip = me // 2
    return me, core, chip, me + 1 - 2 * core


def chip_at(chip, core, step):
    return 2 * lax.rem(chip + step + CHIPS, CHIPS) + core


def greet(devices):
    barrier = pltpu.get_barrier_semaphore()
    for device in devices:
        pl.semaphore_signal(barrier, inc=1, device_id=device, device_id_type=MESH)
    pl.semaphore_wait(barrier, len(devices))


def send(src, dst, send_sem, recv_sem, device):
    copy = pltpu.make_async_remote_copy(
        src_ref=src,
        dst_ref=dst,
        send_sem=send_sem,
        recv_sem=recv_sem,
        device_id=device,
        device_id_type=MESH,
    )
    copy.start()
    return copy


def comm_params(number):
    return pltpu.CompilerParams(
        collective_id=number, has_side_effects=True, vmem_limit_bytes=VMEM_BYTES
    )


def comm_cost(moved):
    return pl.CostEstimate(flops=0, bytes_accessed=moved * 30, transcendentals=0)


def in_vmem(count):
    return [pl.BlockSpec(memory_space=pltpu.VMEM)] * count


def gather_rows_kernel(depth, count, *refs):
    owns, outs = refs[:count], refs[count : 2 * count]
    z_sems, p_sems, f_sems = refs[2 * count :]
    me, core, chip, partner = plane_of()
    layer = lax.axis_index("fsdp")
    layers = [lax.rem(layer + d, depth) for d in range(1, depth)]
    peers = [chip_at(chip, core, j) for j in range(1, CHIPS)]
    greet([(me, other) for other in layers] + [(peer, layer) for peer in peers + [partner]])
    first, spread, passed = [], [], []
    for a, (own, out) in enumerate(zip(owns, outs)):
        for d, other in enumerate(layers):
            first.append(
                send(
                    own.at[me],
                    out.at[layer, me],
                    z_sems.at[0, a, d],
                    z_sems.at[1, a, d],
                    (me, other),
                )
            )
    for own, out in zip(owns, outs):
        for piece in range(SPAN):
            out[layer, piece] = own[piece]
    for a, out in enumerate(outs):
        for d in range(depth - 1):
            first[a * (depth - 1) + d].wait_recv()
            block = out.at[lax.rem(layer + depth - d - 1, depth), me]
            for j, peer in enumerate(peers):
                spread.append(
                    send(block, block, p_sems.at[0, a, d, j], p_sems.at[1, a, d, j], (peer, layer))
                )
            passed.append(
                send(block, block, f_sems.at[0, a, d, 3], f_sems.at[1, a, d, 3], (partner, layer))
            )
    arrivals = iter(spread)
    for a, out in enumerate(outs):
        for d in range(depth - 1):
            source = lax.rem(layer + depth - d - 1, depth)
            for j in range(CHIPS - 1):
                next(arrivals).wait_recv()
                block = out.at[source, chip_at(chip, core, -j - 1)]
                passed.append(
                    send(
                        block,
                        block,
                        f_sems.at[0, a, d, j],
                        f_sems.at[1, a, d, j],
                        (partner, layer),
                    )
                )
    for copy in first + spread:
        copy.wait_send()
    for copy in passed:
        copy.wait()


def gather_rows(arrays, depth):
    if lax.axis_size("ctx") != SPAN:
        return [lax.all_gather(own, "fsdp", axis=0) for own in arrays]
    count, pieces, outs = len(arrays), [], []
    for own in arrays:
        piece = (own.shape[0] // SPAN, own.shape[1])
        pieces.append(own.reshape(SPAN, *piece))
        outs.append(jax.ShapeDtypeStruct((depth, SPAN, *piece), own.dtype))
    whole = pl.pallas_call(
        functools.partial(gather_rows_kernel, depth, count),
        out_shape=tuple(outs),
        in_specs=in_vmem(count),
        out_specs=tuple(in_vmem(count)),
        scratch_shapes=[
            pltpu.SemaphoreType.DMA((2, count, depth - 1)),
            pltpu.SemaphoreType.DMA((2, count, depth - 1, CHIPS - 1)),
            pltpu.SemaphoreType.DMA((2, count, depth - 1, CHIPS)),
        ],
        compiler_params=comm_params(1),
        cost_estimate=comm_cost(sum(own.size for own in arrays) * 2 * depth),
    )(*pieces)
    return [full.reshape(depth, *own.shape) for full, own in zip(whole, arrays)]


def gather_plane_kernel(kv_ref, tag_ref, kv_out, tag_out, p_sems, f_sems):
    me, core, chip, partner = plane_of()
    layer = lax.axis_index("fsdp")
    peers = [chip_at(chip, core, j) for j in range(1, CHIPS)]
    greet([(peer, layer) for peer in peers + [partner]])
    pairs = ((kv_ref, kv_out), (tag_ref, tag_out))
    spread, passed = [], []
    for j, peer in enumerate(peers):
        for a, (own, out) in enumerate(pairs):
            spread.append(
                send(own, out.at[me], p_sems.at[0, a, j], p_sems.at[1, a, j], (peer, layer))
            )
    for a, (own, out) in enumerate(pairs):
        passed.append(
            send(own, out.at[me], f_sems.at[0, a, 3], f_sems.at[1, a, 3], (partner, layer))
        )
    kv_out[me] = kv_ref[...]
    tag_out[me] = tag_ref[...]
    for j in range(CHIPS - 1):
        for a, (own, out) in enumerate(pairs):
            spread[2 * j + a].wait_recv()
            block = out.at[chip_at(chip, core, -j - 1)]
            passed.append(
                send(block, block, f_sems.at[0, a, j], f_sems.at[1, a, j], (partner, layer))
            )
    for copy in spread:
        copy.wait_send()
    for copy in passed:
        copy.wait()


def gather_plane(kv, tags):
    if lax.axis_size("ctx") != SPAN:
        return tuple(lax.all_gather(part, "ctx", axis=0, tiled=True) for part in (kv, tags))
    rows, columns = kv.shape
    kv_all, tags_all = pl.pallas_call(
        gather_plane_kernel,
        out_shape=(
            jax.ShapeDtypeStruct((SPAN, rows, columns), kv.dtype),
            jax.ShapeDtypeStruct((SPAN, 1, rows), tags.dtype),
        ),
        in_specs=in_vmem(2),
        out_specs=tuple(in_vmem(2)),
        scratch_shapes=[
            pltpu.SemaphoreType.DMA((2, 2, CHIPS - 1)),
            pltpu.SemaphoreType.DMA((2, 2, CHIPS)),
        ],
        compiler_params=comm_params(2),
        cost_estimate=comm_cost(kv.size * 2 * SPAN),
    )(kv, tags[None])
    return kv_all.reshape(SPAN * rows, columns), tags_all.reshape(SPAN * rows)


def added(*parts):
    total = parts[0].astype(jnp.float32)
    for part in parts[1:]:
        total = total + part.astype(jnp.float32)
    return total


def reduce_plane(arrays, h_sems, p_sems):
    me, core, chip, partner = plane_of()
    layer = lax.axis_index("fsdp")
    handed, spread = [], []
    for a, (piece_of, halves, sums, arrived) in enumerate(arrays):
        for j in range(CHIPS):
            slot = (j + 1) % CHIPS
            handed.append(
                send(
                    piece_of(chip_at(chip, 1 - core, slot)),
                    halves.at[slot],
                    h_sems.at[0, a, slot],
                    h_sems.at[1, a, slot],
                    (partner, layer),
                )
            )
    for a, (piece_of, halves, sums, arrived) in enumerate(arrays):
        for j in range(CHIPS):
            slot = (j + 1) % CHIPS
            handed[a * CHIPS + j].wait_recv()
            mine = chip_at(chip, core, slot)

            def add_half(slab, carry, piece=piece_of(mine), halves=halves, sums=sums, slot=slot):
                sums[slot, slab] = added(piece[slab], halves[slot, slab]).astype(sums.dtype)
                return carry

            lax.fori_loop(0, sums.shape[1], add_half, 0)
            if slot:
                spread.append(
                    send(
                        sums.at[slot],
                        arrived.at[slot - 1],
                        p_sems.at[0, a, slot - 1],
                        p_sems.at[1, a, slot - 1],
                        (mine, layer),
                    )
                )
    return handed, spread


def plane_total(sums, arrived, slab):
    return added(sums[0, slab], *(arrived[j, slab] for j in range(CHIPS - 1)))


def plane_scratch(block, dtype):
    return [
        pltpu.VMEM((CHIPS, *block), dtype),
        pltpu.VMEM((CHIPS, *block), dtype),
        pltpu.VMEM((CHIPS - 1, *block), dtype),
    ]


def turned_back(values, cos_tab, sin_tab):
    half_dim, parts = HEAD // 2, []
    for start in range(0, values.shape[1], HEAD):
        low = values[:, start : start + half_dim]
        high = values[:, start + half_dim : start + HEAD]
        parts += [low * cos_tab + high * sin_tab, high * cos_tab - low * sin_tab]
    return jnp.concatenate(parts, 1)


def scatter_plane_kernel(x_ref, cos_ref, sin_ref, out_ref, halves, sums, arrived, h_sems, p_sems):
    me, core, chip, partner = plane_of()
    layer = lax.axis_index("fsdp")
    greet([(chip_at(chip, core, j), layer) for j in range(1, CHIPS)] + [(partner, layer)])
    arrays = [(lambda piece: x_ref.at[piece], halves, sums, arrived)]
    handed, spread = reduce_plane(arrays, h_sems, p_sems)
    for copy in spread:
        copy.wait_recv()

    def add_slab(slab, carry):
        total = plane_total(sums, arrived, slab)
        kdim = KV_HEADS * HEAD
        keys = turned_back(total[:, :kdim], cos_ref[slab], sin_ref[slab])
        out_ref[slab] = jnp.concatenate([keys, total[:, kdim:]], 1).astype(out_ref.dtype)
        return carry

    lax.fori_loop(0, x_ref.shape[1], add_slab, 0)
    for copy in handed + spread:
        copy.wait_send()


def scatter_plane(values, cos_tab, sin_tab):
    if lax.axis_size("ctx") != SPAN:
        own = lax.psum_scatter(values, "ctx", scatter_dimension=0, tiled=True)
        own, kdim = own.astype(jnp.float32), KV_HEADS * HEAD
        keys = turned_back(own[:, :kdim], cos_tab, sin_tab)
        return jnp.concatenate([keys, own[:, kdim:]], 1).astype(values.dtype)
    rows, columns = values.shape
    slabs = 8
    block = (slabs, rows // SPAN // slabs, columns)
    return pl.pallas_call(
        scatter_plane_kernel,
        out_shape=jax.ShapeDtypeStruct(block, values.dtype),
        in_specs=in_vmem(3),
        out_specs=in_vmem(1)[0],
        scratch_shapes=plane_scratch(block, values.dtype)
        + [pltpu.SemaphoreType.DMA((2, 1, CHIPS)), pltpu.SemaphoreType.DMA((2, 1, CHIPS - 1))],
        compiler_params=comm_params(3),
        cost_estimate=comm_cost(values.size * 2),
    )(
        values.reshape(SPAN, *block),
        cos_tab.reshape(*block[:2], -1),
        sin_tab.reshape(*block[:2], -1),
    ).reshape(rows // SPAN, columns)


def reduce_rows_kernel(depth, count, *refs):
    inputs, outs, scratch = refs[:count], refs[count : 2 * count], refs[2 * count : 6 * count]
    h_sems, p_sems, z_sems, g_sems, f_sems = refs[6 * count :]
    me, core, chip, partner = plane_of()
    layer = lax.axis_index("fsdp")
    layers = [lax.rem(layer + d, depth) for d in range(1, depth)]
    peers = [chip_at(chip, core, j) for j in range(1, CHIPS)]
    greet([(me, other) for other in layers] + [(peer, layer) for peer in peers + [partner]])
    arrays, across = [], []
    for a, x_ref in enumerate(inputs):
        halves, sums, arrived, layers_ref = scratch[4 * a : 4 * a + 4]
        arrays.append((lambda piece, x_ref=x_ref: x_ref.at[:, piece], halves, sums, arrived))
        across.append(layers_ref)
    handed, spread = reduce_plane(arrays, h_sems, p_sems)
    moved = []
    for a, (_, _, sums, arrived) in enumerate(arrays):
        for copy in spread[a * (CHIPS - 1) : (a + 1) * (CHIPS - 1)]:
            copy.wait_recv()
        for d in list(range(1, depth)) + [0]:
            target = lax.rem(layer + d, depth)
            across[a][0, d] = plane_total(sums, arrived, target).astype(across[a].dtype)
            if d:
                moved.append(
                    send(
                        across[a].at[0, d],
                        across[a].at[1, d],
                        z_sems.at[0, a, d - 1],
                        z_sems.at[1, a, d - 1],
                        (me, target),
                    )
                )
    given, passed = [], []
    for a, out_ref in enumerate(outs):
        for copy in moved[a * (depth - 1) : (a + 1) * (depth - 1)]:
            copy.wait_recv()
        parts = [across[a][0, 0]] + [across[a][1, d] for d in range(1, depth)]
        out_ref[me] = added(*parts).astype(out_ref.dtype)
        mine = out_ref.at[me]
        for j, peer in enumerate(peers):
            given.append(send(mine, mine, g_sems.at[0, a, j], g_sems.at[1, a, j], (peer, layer)))
        passed.append(send(mine, mine, f_sems.at[0, a, 3], f_sems.at[1, a, 3], (partner, layer)))
    for a, out_ref in enumerate(outs):
        for j in range(CHIPS - 1):
            given[a * (CHIPS - 1) + j].wait_recv()
            block = out_ref.at[chip_at(chip, core, -j - 1)]
            passed.append(
                send(block, block, f_sems.at[0, a, j], f_sems.at[1, a, j], (partner, layer))
            )
    for copy in handed + spread + moved + given:
        copy.wait_send()
    for copy in passed:
        copy.wait()


def reduce_rows(arrays, number):
    if lax.axis_size("ctx") != SPAN:
        return [lax.psum(lax.psum_scatter(v, "fsdp", scatter_dimension=0), "ctx") for v in arrays]
    depth, count = arrays[0].shape[0], len(arrays)
    pieces, outs, scratch = [], [], []
    for values in arrays:
        _, rows, columns = values.shape
        piece = (rows // SPAN, columns)
        pieces.append(values.reshape(depth, SPAN, *piece))
        outs.append(jax.ShapeDtypeStruct((SPAN, *piece), values.dtype))
        scratch += plane_scratch((depth, *piece), values.dtype)
        scratch.append(pltpu.VMEM((2, depth, *piece), values.dtype))
    owned = pl.pallas_call(
        functools.partial(reduce_rows_kernel, depth, count),
        out_shape=tuple(outs),
        in_specs=in_vmem(count),
        out_specs=tuple(in_vmem(count)),
        scratch_shapes=scratch
        + [
            pltpu.SemaphoreType.DMA((2, count, CHIPS)),
            pltpu.SemaphoreType.DMA((2, count, CHIPS - 1)),
            pltpu.SemaphoreType.DMA((2, count, depth - 1)),
            pltpu.SemaphoreType.DMA((2, count, CHIPS - 1)),
            pltpu.SemaphoreType.DMA((2, count, CHIPS)),
        ],
        compiler_params=comm_params(number),
        cost_estimate=comm_cost(sum(values.size for values in arrays) * 2),
    )(*pieces)
    return [own.reshape(values.shape[1:]) for own, values in zip(owned, arrays)]


BLOCK = 128
LANES = (HEADS // KV_HEADS) * BLOCK


def dot(left, right, dims=(1, 0)):
    return lax.dot_general(
        left, right, (((dims[0],), (dims[1],)), ((), ())), preferred_element_type=jnp.float32
    )


def of_group(ref, group, at):
    first = group * (HEADS // KV_HEADS)
    heads = range(first, first + HEADS // KV_HEADS)
    return jnp.concatenate([ref[head * HEAD : (head + 1) * HEAD, at] for head in heads], 1)


def of_rows(ref, group, at):
    first = group * (HEADS // KV_HEADS)
    heads = range(first, first + HEADS // KV_HEADS)
    return jnp.concatenate([ref[head : head + 1, at] for head in heads], 1)


def columns_of(group, part):
    start = (part * KV_HEADS + group) * HEAD
    return slice(start, start + HEAD)


def mask_bias(tags, query_pos):
    tags = jnp.broadcast_to(tags, (BLOCK, BLOCK)).T
    key_pos = jnp.where(tags >= 0, tags, -tags - 1)
    allowed = (key_pos <= query_pos) & ((tags >= 0) | (key_pos == query_pos))
    bias = jnp.where(allowed, 0.0, negative)
    return jnp.concatenate([bias] * (HEADS // KV_HEADS), 1)


def attend_kernel(
    first_ref, q_ref, kv_ref, pos_ref, tag_ref, out_ref, log_ref, max_ref, sum_ref, acc_ref, kept
):
    blocks = kv_ref.shape[0] // BLOCK
    keep = kept.shape[0] == blocks

    def scores(group, at, rows, bias):
        keys = kv_ref[rows, columns_of(group, 0)]
        return dot(keys, of_group(q_ref, group, at)) + bias

    def query_block(qb, carry):
        at = pl.ds(pl.multiple_of(qb * BLOCK, BLOCK), BLOCK)
        max_ref[...] = jnp.full(max_ref.shape, negative, jnp.float32)
        sum_ref[...] = jnp.zeros(sum_ref.shape, jnp.float32)
        acc_ref[...] = jnp.zeros(acc_ref.shape, jnp.float32)
        limit = first_ref[blocks + qb]

        def find(kb, carry):
            @pl.when(first_ref[kb] <= limit)
            def _():
                rows = pl.ds(pl.multiple_of(kb * BLOCK, BLOCK), BLOCK)
                bias = mask_bias(tag_ref[kb], pos_ref[:, at])
                for group in range(KV_HEADS):
                    found = scores(group, at, rows, bias)
                    if keep:
                        kept[kb, group] = found
                    tops = jnp.max(found.reshape(BLOCK // 8, 8, LANES), 0)
                    max_ref[group] = jnp.maximum(max_ref[group], tops)

            return carry

        lax.fori_loop(0, blocks, find, 0)
        for group in range(KV_HEADS):
            top = jnp.max(max_ref[group], 0, keepdims=True)
            max_ref[group] = jnp.broadcast_to(top, max_ref.shape[1:])

        def gather(kb, carry):
            @pl.when(first_ref[kb] <= limit)
            def _():
                rows = pl.ds(pl.multiple_of(kb * BLOCK, BLOCK), BLOCK)
                bias = None if keep else mask_bias(tag_ref[kb], pos_ref[:, at])
                for group in range(KV_HEADS):
                    found = kept[kb, group] if keep else scores(group, at, rows, bias)
                    weights = jnp.exp(found - max_ref[group, :1])
                    sum_ref[group] += jnp.sum(weights.reshape(BLOCK // 8, 8, LANES), 0)
                    values = kv_ref[rows, columns_of(group, 1)]
                    acc_ref[group] += dot(values, weights.astype(jnp.bfloat16), (0, 0))

            return carry

        lax.fori_loop(0, blocks, gather, 0)
        for group in range(KV_HEADS):
            total = jnp.sum(sum_ref[group], 0, keepdims=True)
            attended = acc_ref[group] / total
            logs = max_ref[group, :1] + jnp.log(total)
            for j in range(HEADS // KV_HEADS):
                head = group * (HEADS // KV_HEADS) + j
                own = slice(j * BLOCK, (j + 1) * BLOCK)
                out_ref[head * HEAD : (head + 1) * HEAD, at] = attended[:, own]
                log_ref[head : head + 1, at] = logs[:, own]
        return carry

    lax.fori_loop(0, q_ref.shape[1] // BLOCK, query_block, 0)


def kernel_params():
    return pltpu.CompilerParams(vmem_limit_bytes=VMEM_BYTES)


def attend(firsts, queries, kv, query_pos, key_tags):
    blocks = kv.shape[0] // BLOCK
    slots = queries.shape[1]
    kept = blocks if blocks <= 16 else 1
    groups = (KV_HEADS, 8, LANES)
    work = 4 * kv.shape[0] * slots * HEADS * HEAD
    return pl.pallas_call(
        attend_kernel,
        out_shape=(
            jax.ShapeDtypeStruct(queries.shape, jnp.float32),
            jax.ShapeDtypeStruct((HEADS + 1, slots), jnp.float32),
        ),
        in_specs=[pl.BlockSpec(memory_space=pltpu.SMEM)] + in_vmem(4),
        out_specs=tuple(in_vmem(2)),
        scratch_shapes=[
            pltpu.VMEM(groups, jnp.float32),
            pltpu.VMEM(groups, jnp.float32),
            pltpu.VMEM((KV_HEADS, HEAD, LANES), jnp.float32),
            pltpu.VMEM((kept, KV_HEADS, BLOCK, LANES), jnp.float32),
        ],
        compiler_params=kernel_params(),
        cost_estimate=pl.CostEstimate(
            flops=work * 8, bytes_accessed=kv.size * 2, transcendentals=work // 256
        ),
    )(firsts, queries, kv, query_pos[None], key_tags.reshape(-1, 1, BLOCK))


def attend_back_kernel(
    first_ref, q_ref, kv_ref, pos_ref, tag_ref, grad_ref, log_ref, delta_ref, *refs
):
    blocks = kv_ref.shape[0] // BLOCK
    cos_ref, sin_ref, out_ref, dkv_ref, acc, dq_ref = refs
    dq_ref[...] = jnp.zeros(dq_ref.shape, dq_ref.dtype)

    def key_block(kb, carry):
        rows = pl.ds(pl.multiple_of(kb * BLOCK, BLOCK), BLOCK)
        acc[...] = jnp.zeros(acc.shape, jnp.float32)

        def query_block(qb, carry):
            @pl.when(first_ref[kb] <= first_ref[blocks + qb])
            def _():
                at = pl.ds(pl.multiple_of(qb * BLOCK, BLOCK), BLOCK)
                bias = mask_bias(tag_ref[kb], pos_ref[:, at])
                for group in range(KV_HEADS):
                    keys = kv_ref[rows, columns_of(group, 0)]
                    values = kv_ref[rows, columns_of(group, 1)]
                    queries = of_group(q_ref, group, at)
                    grads = of_group(grad_ref, group, at)
                    found = dot(keys, queries) + bias
                    probs = jnp.exp(found - of_rows(log_ref, group, at))
                    grad_probs = dot(values, grads)
                    grad_scores = probs * (grad_probs - of_rows(delta_ref, group, at))
                    grad_scores = grad_scores.astype(jnp.bfloat16)
                    acc[group] += dot(grad_scores, queries, (1, 1))
                    acc[KV_HEADS + group] += dot(probs.astype(jnp.bfloat16), grads, (1, 1))
                    grad_q = 0.125 * dot(keys, grad_scores, (0, 0))
                    for j in range(HEADS // KV_HEADS):
                        head = group * (HEADS // KV_HEADS) + j
                        own = slice(head * HEAD, (head + 1) * HEAD)
                        dq_ref[own, at] += grad_q[:, j * BLOCK : (j + 1) * BLOCK]

            return carry

        lax.fori_loop(0, q_ref.shape[1] // BLOCK, query_block, 0)
        dkv_ref[rows, :] = jnp.concatenate(
            [acc[index] for index in range(2 * KV_HEADS)], 1
        ).astype(dkv_ref.dtype)
        return carry

    lax.fori_loop(0, blocks, key_block, 0)
    half_dim = HEAD // 2

    def finish(qb, carry):
        at = pl.ds(pl.multiple_of(qb * BLOCK, BLOCK), BLOCK)
        cos_tab, sin_tab = cos_ref[:, at], sin_ref[:, at]
        for head in range(0, HEADS, 2):
            pair = []
            for start in range(head * HEAD, min(head + 2, HEADS) * HEAD, HEAD):
                low = dq_ref[start : start + half_dim, at]
                high = dq_ref[start + half_dim : start + HEAD, at]
                pair += [low * cos_tab + high * sin_tab, high * cos_tab - low * sin_tab]
            if len(pair) == 2:
                pair += [jnp.zeros_like(part) for part in pair]
            turned = jnp.concatenate(pair, 0).T
            own = slice(head * HEAD, head * HEAD + turned.shape[1])
            out_ref[at, own] = turned.astype(out_ref.dtype)
        return carry

    lax.fori_loop(0, q_ref.shape[1] // BLOCK, finish, 0)


def attend_back(firsts, queries, kv, query_pos, key_tags, grads, log_total, row_delta, tables):
    slots = queries.shape[1]
    work = 10 * kv.shape[0] * slots * HEADS * HEAD
    return pl.pallas_call(
        attend_back_kernel,
        out_shape=(
            jax.ShapeDtypeStruct((slots, -(-HEADS // 2) * 2 * HEAD), jnp.bfloat16),
            jax.ShapeDtypeStruct(kv.shape, jnp.bfloat16),
        ),
        in_specs=[pl.BlockSpec(memory_space=pltpu.SMEM)] + in_vmem(9),
        out_specs=tuple(in_vmem(2)),
        scratch_shapes=[
            pltpu.VMEM((2 * KV_HEADS, BLOCK, HEAD), jnp.float32),
            pltpu.VMEM(queries.shape, jnp.float32),
        ],
        compiler_params=kernel_params(),
        cost_estimate=pl.CostEstimate(
            flops=work * 6, bytes_accessed=kv.size * 4, transcendentals=work // 640
        ),
    )(firsts, queries, kv, query_pos[None], key_tags.reshape(-1, 1, BLOCK), grads, log_total, row_delta, *tables)


def on_device(
    tokens,
    w_query,
    w_key,
    w_value,
    w_out,
    w_gate,
    w_up,
    w_down,
    gain_attn,
    gain_ffn,
    router,
    cotangent,
    positions,
    lengths,
    chosen,
):
    hidden = tokens[0].astype(jnp.float32)
    row_count, width = hidden.shape
    qdim = HEADS * HEAD
    kdim = KV_HEADS * HEAD
    query_pos = positions[0]
    live = query_pos < lengths[0]
    selected = live & (chosen[0] == 1)
    live_mask = live.astype(jnp.float32)[:, None]
    chosen_mask = selected.astype(jnp.float32)[:, None]
    cos_tab, sin_tab = rope_tables(query_pos)
    key_tags = jnp.where(selected, query_pos, -query_pos - 1)
    depth = lax.axis_size("fsdp")
    own_rows = w_query.shape[0]
    w_out_full = lax.all_gather(w_out, "fsdp", axis=0, tiled=True)
    vectors = jnp.stack([gain_attn, gain_ffn, router], 1)
    own_attn = [padded_to(w_query, 1), jnp.concatenate([w_key, w_value, vectors], 1)]
    gathered = gather_rows([padded_to(own, 0) for own in own_attn], depth)
    padded_rows = gathered[0].shape[1]
    w_query = gathered[0].reshape(depth * padded_rows, -1)
    gathered = gathered[1][:, :own_rows].reshape(width, -1)
    w_kv, vectors = gathered[:, : 2 * kdim], gathered[:, 2 * kdim :]
    gain_one, gain_two, router_vec = vectors.T.astype(jnp.float32)
    gating = jax.nn.sigmoid(jnp.sum(hidden * router_vec, -1, keepdims=True))
    grad_y = cotangent[0].astype(jnp.float32) * live_mask
    grad_inc = grad_y * chosen_mask * gating
    grad_ffn = grad_inc.astype(jnp.bfloat16)
    grad_ffn_all = lax.all_gather(grad_ffn, "fsdp", axis=0, tiled=True)

    normed_one, inv_one = norm_forward(hidden, gain_one)
    normed_one = normed_one.astype(jnp.bfloat16)
    spread_one = padded_to(normed_one.reshape(row_count, depth, own_rows), -1)
    spread_one = spread_one.reshape(row_count, -1)
    query_raw = dot(w_query, spread_one, (0, 1))[:qdim]
    queries = rotate_columns(query_raw, cos_tab, sin_tab).astype(jnp.bfloat16) * 0.125
    kv_raw = dot(normed_one, w_kv)
    kv_own = jnp.concatenate([rotate(kv_raw[:, :kdim], cos_tab, sin_tab), kv_raw[:, kdim:]], 1)
    kv_all, tags_all = gather_plane(kv_own.astype(jnp.bfloat16), key_tags)
    first_tags = tags_all[::BLOCK]
    firsts = jnp.concatenate(
        [jnp.where(first_tags >= 0, first_tags, -first_tags - 1), query_pos[BLOCK - 1 :: BLOCK]]
    )
    attended, log_total = attend(firsts, queries, kv_all, query_pos, tags_all)
    attended, w_out_full = lax.optimization_barrier((attended, w_out_full))
    outcome = attended.astype(jnp.bfloat16)
    branch = dot(outcome, w_out_full, (0, 0))
    middle = hidden + branch
    normed_two, inv_two = norm_forward(middle, gain_two)
    normed_two = normed_two.astype(jnp.bfloat16)
    normed_two, grad_ffn_all = lax.optimization_barrier((normed_two, grad_ffn_all))
    normed_all = lax.all_gather(normed_two, "fsdp", axis=0, tiled=True)
    inner_act, grad_gate_act, grad_up_act, grad_normed_part = ffn_both(
        normed_all, grad_ffn_all, w_gate, w_up, w_down
    )
    grad_normed_two = lax.psum_scatter(
        grad_normed_part, "fsdp", scatter_dimension=0, tiled=True
    ).astype(jnp.float32)
    ffn_part = jnp.dot(inner_act, w_down, preferred_element_type=jnp.float32).astype(jnp.bfloat16)
    grad_wgate = lax.dot_general(
        grad_gate_act, normed_all, across_rows, preferred_element_type=jnp.float32
    )
    grad_wup = lax.dot_general(
        grad_up_act, normed_all, across_rows, preferred_element_type=jnp.float32
    )
    grad_wdown = lax.dot_general(
        inner_act, grad_ffn_all, across_rows, preferred_element_type=jnp.float32
    )
    low = jnp.bfloat16
    spread_out = padded_to(outcome.reshape(depth, own_rows, row_count), 1)
    grads = [grad.astype(low) for grad in (grad_wgate, grad_wup, grad_wdown)]
    grad_normed_two, ffn_part, spread_out, *grads = lax.optimization_barrier(
        (grad_normed_two, ffn_part, spread_out, *grads)
    )
    grad_normed_two, row_dot = grad_normed_two[:, :width], grad_normed_two[:, width:]
    totals = tuple(lax.psum(grad, "ctx") for grad in grads)
    grad_middle, grad_gain_two = norm_backward(middle, inv_two, gain_two, grad_normed_two)
    grad_branch = (grad_inc + grad_middle).astype(jnp.bfloat16)
    grad_attended = dot(w_out_full, grad_branch, (1, 1)).astype(jnp.bfloat16)
    grad_wout = dot(spread_out.reshape(-1, row_count), padded_to(grad_branch, 1)).astype(low)
    row_delta = jnp.sum(
        (grad_attended.astype(jnp.float32) * attended).reshape(HEADS, HEAD, row_count), 1
    )
    row_delta = jnp.pad(row_delta, ((0, 1), (0, 0)))
    grad_query_raw, grad_kv_all = attend_back(
        firsts,
        queries,
        kv_all,
        query_pos,
        tags_all,
        grad_attended,
        log_total,
        row_delta,
        (cos_tab.T, sin_tab.T),
    )
    grad_kv_raw = scatter_plane(grad_kv_all, cos_tab, sin_tab)
    grad_logit = (jnp.sum(grad_inc * branch, -1, keepdims=True) + row_dot) * (1.0 - gating)
    grad_router = jnp.sum(hidden * grad_logit, 0)
    grad_normed_one = dot(grad_query_raw, w_query, (1, 1)).reshape(row_count, depth, -1)
    grad_normed_one = grad_normed_one[..., :own_rows].reshape(row_count, width)
    grad_normed_one = grad_normed_one + dot(grad_kv_raw, w_kv, (1, 1))
    grad_wq = dot(spread_one, grad_query_raw, (0, 0)).astype(low)
    grad_wkv = dot(spread_one, grad_kv_raw, (0, 0)).astype(low)
    grad_hidden_one, grad_gain_one = norm_backward(hidden, inv_one, gain_one, grad_normed_one)
    grad_tokens = (grad_y + grad_logit * router_vec + grad_middle + grad_hidden_one).astype(
        jnp.bfloat16
    )
    vectors = jnp.stack([grad_gain_one, grad_gain_two, grad_router]).reshape(3, depth, own_rows)
    vectors = jnp.pad(vectors.transpose(1, 0, 2).reshape(depth, -1), ((0, 0), (0, -3 * own_rows % 1024)))
    vectors = jnp.pad(vectors.reshape(depth, -1, 1, 128), ((0, 0), (0, 0), (0, 7), (0, 0)))
    layered = [grad.reshape(depth, padded_rows, -1) for grad in (grad_wout, grad_wq, grad_wkv)]
    layered.append(vectors.reshape(depth, -1, 128))
    owned = reduce_rows(layered, 4)
    ffn_out = lax.psum_scatter(ffn_part, "fsdp", scatter_dimension=0, tiled=True)
    *owned, totals, ffn_out = lax.optimization_barrier((*owned, totals, ffn_out))
    increment = branch + ffn_out.astype(jnp.float32)
    block_out = live_mask * (hidden + chosen_mask * gating * increment)
    total_out, total_q, total_kv = (own[:own_rows].astype(jnp.float32) for own in owned[:3])
    total_q, total_out = total_q[:, :qdim], total_out[:, :width]
    total_k, total_v = total_kv[:, :kdim], total_kv[:, kdim:]
    mine = owned[3].reshape(-1, 8, 128)[:, 0].reshape(-1)[: 3 * own_rows].reshape(3, own_rows)
    total_gate, total_up, total_down = (total.astype(jnp.float32) for total in totals)
    return (
        block_out.astype(jnp.bfloat16)[None],
        grad_tokens[None],
        total_q,
        total_k,
        total_v,
        total_out,
        total_gate,
        total_up,
        total_down,
        mine[0],
        mine[1],
        mine[2],
    )


def solution(mesh):
    in_specs = (
        P("fsdp", "ctx", None),
        P("fsdp", None),
        P("fsdp", None),
        P("fsdp", None),
        P("fsdp", None),
        P("fsdp", None),
        P("fsdp", None),
        P("fsdp", None),
        P("fsdp"),
        P("fsdp"),
        P("fsdp"),
        P("fsdp", "ctx", None),
        P("fsdp", "ctx"),
        P("fsdp"),
        P("fsdp", "ctx"),
    )
    out_specs = (
        P("fsdp", "ctx", None),
        P("fsdp", "ctx", None),
        P("fsdp", None),
        P("fsdp", None),
        P("fsdp", None),
        P("fsdp", None),
        P("fsdp", None),
        P("fsdp", None),
        P("fsdp", None),
        P("fsdp"),
        P("fsdp"),
        P("fsdp"),
    )
    return jax.shard_map(
        on_device, mesh=mesh, in_specs=in_specs, out_specs=out_specs, check_vma=False
    )
```

```python
import functools

import jax
import jax.numpy as jnp
from jax import lax
from jax.experimental import pallas as pl
from jax.experimental.pallas import tpu as pltpu
from jax.sharding import PartitionSpec as P

HEADS = 15
KV_HEADS = 5
HEAD = 64


epsilon = 1e-05
negative = -1e30
across_rows = (((0,), (0,)), ((), ()))
across_cols = (((1,), (1,)), ((), ()))


def rope_tables(positions):
    half_dim = HEAD // 2
    frequency = 10000.0 ** (-2.0 * jnp.arange(half_dim, dtype=jnp.float32) / HEAD)
    angles = positions.astype(jnp.float32)[:, None] * frequency[None, :]
    return (jnp.cos(angles), jnp.sin(angles))


def rotate(values, cos_tab, sin_tab):
    slots, width = values.shape
    low, high = jnp.split(values.reshape(slots, width // HEAD, HEAD), 2, -1)
    cos_tab, sin_tab = cos_tab[:, None], sin_tab[:, None]
    turned = [low * cos_tab - high * sin_tab, high * cos_tab + low * sin_tab]
    return jnp.concatenate(turned, -1).reshape(slots, width)


def rotate_columns(values, cos_tab, sin_tab):
    width, slots = values.shape
    low, high = jnp.split(values.reshape(width // HEAD, HEAD, slots), 2, 1)
    cos_tab, sin_tab = cos_tab.T[None], sin_tab.T[None]
    turned = [low * cos_tab - high * sin_tab, high * cos_tab + low * sin_tab]
    return jnp.concatenate(turned, 1).reshape(width, slots)


def norm_forward(values, gain_vec):
    inv_rms = lax.rsqrt(jnp.mean(values * values, -1, keepdims=True) + epsilon)
    return (values * inv_rms * gain_vec, inv_rms)


def norm_backward(values, inv_rms, gain_vec, grad_normed):
    weighted = gain_vec * grad_normed
    grad_gain = jnp.sum(grad_normed * values * inv_rms, 0)
    cubed = inv_rms * inv_rms * inv_rms
    grad_values = inv_rms * weighted - values * cubed * jnp.mean(
        weighted * values, -1, keepdims=True
    )
    return (grad_values, grad_gain)


def padded_to(values, row_dim):
    pads = [(0, 0)] * values.ndim
    pads[row_dim] = (0, -values.shape[row_dim] % 128)
    return jnp.pad(values, pads)


def ffn_both(normed, grad_mixed, gate_rows, up_rows, down_rows):
    gate_proj = lax.dot_general(normed, gate_rows, across_cols, preferred_element_type=jnp.float32)
    up_proj = lax.dot_general(normed, up_rows, across_cols, preferred_element_type=jnp.float32)
    sigma = jax.nn.sigmoid(gate_proj)
    activated = gate_proj * sigma
    inner_act = (activated * up_proj).astype(jnp.bfloat16)
    grad_inner = lax.dot_general(
        grad_mixed, down_rows, across_cols, preferred_element_type=jnp.float32
    )
    grad_gate_act = (grad_inner * up_proj * sigma * (1.0 + gate_proj * (1.0 - sigma))).astype(
        jnp.bfloat16
    )
    grad_up_act = (grad_inner * activated).astype(jnp.bfloat16)
    grad_normed = jnp.dot(grad_gate_act, gate_rows, preferred_element_type=jnp.float32) + jnp.dot(
        grad_up_act, up_rows, preferred_element_type=jnp.float32
    )
    row_dot = jnp.sum(inner_act.astype(jnp.float32) * grad_inner, -1, keepdims=True)
    grad_normed = jnp.concatenate([grad_normed, row_dot], 1).astype(jnp.bfloat16)
    return (inner_act, grad_gate_act, grad_up_act, grad_normed)


CHIPS = 4
SPAN = 2 * CHIPS
VMEM_BYTES = 60 * 1024 * 1024
MESH = pl.DeviceIdType.MESH


def plane_of():
    me = lax.axis_index("ctx")
    core = lax.rem(me, 2)
    chip = me // 2
    return me, core, chip, me + 1 - 2 * core


def chip_at(chip, core, step):
    return 2 * lax.rem(chip + step + CHIPS, CHIPS) + core


def greet(devices):
    barrier = pltpu.get_barrier_semaphore()
    for device in devices:
        pl.semaphore_signal(barrier, inc=1, device_id=device, device_id_type=MESH)
    pl.semaphore_wait(barrier, len(devices))


def send(src, dst, send_sem, recv_sem, device):
    copy = pltpu.make_async_remote_copy(
        src_ref=src,
        dst_ref=dst,
        send_sem=send_sem,
        recv_sem=recv_sem,
        device_id=device,
        device_id_type=MESH,
    )
    copy.start()
    return copy


def comm_params(number):
    return pltpu.CompilerParams(
        collective_id=number, has_side_effects=True, vmem_limit_bytes=VMEM_BYTES
    )


def comm_cost(moved):
    return pl.CostEstimate(flops=0, bytes_accessed=moved * 30, transcendentals=0)


def in_vmem(count):
    return [pl.BlockSpec(memory_space=pltpu.VMEM)] * count


def gather_rows_kernel(depth, count, *refs):
    owns, outs = refs[:count], refs[count : 2 * count]
    z_sems, p_sems, f_sems = refs[2 * count :]
    me, core, chip, partner = plane_of()
    layer = lax.axis_index("fsdp")
    layers = [lax.rem(layer + d, depth) for d in range(1, depth)]
    peers = [chip_at(chip, core, j) for j in range(1, CHIPS)]
    greet([(me, other) for other in layers] + [(peer, layer) for peer in peers + [partner]])
    first, spread, passed = [], [], []
    for a, (own, out) in enumerate(zip(owns, outs)):
        for d, other in enumerate(layers):
            first.append(
                send(
                    own.at[me],
                    out.at[layer, me],
                    z_sems.at[0, a, d],
                    z_sems.at[1, a, d],
                    (me, other),
                )
            )
    for own, out in zip(owns, outs):
        for piece in range(SPAN):
            out[layer, piece] = own[piece]
    for a, out in enumerate(outs):
        for d in range(depth - 1):
            first[a * (depth - 1) + d].wait_recv()
            block = out.at[lax.rem(layer + depth - d - 1, depth), me]
            for j, peer in enumerate(peers):
                spread.append(
                    send(block, block, p_sems.at[0, a, d, j], p_sems.at[1, a, d, j], (peer, layer))
                )
            passed.append(
                send(block, block, f_sems.at[0, a, d, 3], f_sems.at[1, a, d, 3], (partner, layer))
            )
    arrivals = iter(spread)
    for a, out in enumerate(outs):
        for d in range(depth - 1):
            source = lax.rem(layer + depth - d - 1, depth)
            for j in range(CHIPS - 1):
                next(arrivals).wait_recv()
                block = out.at[source, chip_at(chip, core, -j - 1)]
                passed.append(
                    send(
                        block,
                        block,
                        f_sems.at[0, a, d, j],
                        f_sems.at[1, a, d, j],
                        (partner, layer),
                    )
                )
    for copy in first + spread:
        copy.wait_send()
    for copy in passed:
        copy.wait()


def gather_rows(arrays, depth):
    if lax.axis_size("ctx") != SPAN:
        return [lax.all_gather(own, "fsdp", axis=0) for own in arrays]
    count, pieces, outs = len(arrays), [], []
    for own in arrays:
        piece = (own.shape[0] // SPAN, own.shape[1])
        pieces.append(own.reshape(SPAN, *piece))
        outs.append(jax.ShapeDtypeStruct((depth, SPAN, *piece), own.dtype))
    whole = pl.pallas_call(
        functools.partial(gather_rows_kernel, depth, count),
        out_shape=tuple(outs),
        in_specs=in_vmem(count),
        out_specs=tuple(in_vmem(count)),
        scratch_shapes=[
            pltpu.SemaphoreType.DMA((2, count, depth - 1)),
            pltpu.SemaphoreType.DMA((2, count, depth - 1, CHIPS - 1)),
            pltpu.SemaphoreType.DMA((2, count, depth - 1, CHIPS)),
        ],
        compiler_params=comm_params(1),
        cost_estimate=comm_cost(sum(own.size for own in arrays) * 2 * depth),
    )(*pieces)
    return [full.reshape(depth, *own.shape) for full, own in zip(whole, arrays)]


def gather_plane_kernel(kv_ref, tag_ref, kv_out, tag_out, p_sems, f_sems):
    me, core, chip, partner = plane_of()
    layer = lax.axis_index("fsdp")
    peers = [chip_at(chip, core, j) for j in range(1, CHIPS)]
    greet([(peer, layer) for peer in peers + [partner]])
    pairs = ((kv_ref, kv_out), (tag_ref, tag_out))
    spread, passed = [], []
    for j, peer in enumerate(peers):
        for a, (own, out) in enumerate(pairs):
            spread.append(
                send(own, out.at[me], p_sems.at[0, a, j], p_sems.at[1, a, j], (peer, layer))
            )
    for a, (own, out) in enumerate(pairs):
        passed.append(
            send(own, out.at[me], f_sems.at[0, a, 3], f_sems.at[1, a, 3], (partner, layer))
        )
    kv_out[me] = kv_ref[...]
    tag_out[me] = tag_ref[...]
    for j in range(CHIPS - 1):
        for a, (own, out) in enumerate(pairs):
            spread[2 * j + a].wait_recv()
            block = out.at[chip_at(chip, core, -j - 1)]
            passed.append(
                send(block, block, f_sems.at[0, a, j], f_sems.at[1, a, j], (partner, layer))
            )
    for copy in spread:
        copy.wait_send()
    for copy in passed:
        copy.wait()


def gather_plane(kv, tags):
    if lax.axis_size("ctx") != SPAN:
        return tuple(lax.all_gather(part, "ctx", axis=0, tiled=True) for part in (kv, tags))
    rows, columns = kv.shape
    kv_all, tags_all = pl.pallas_call(
        gather_plane_kernel,
        out_shape=(
            jax.ShapeDtypeStruct((SPAN, rows, columns), kv.dtype),
            jax.ShapeDtypeStruct((SPAN, 1, rows), tags.dtype),
        ),
        in_specs=in_vmem(2),
        out_specs=tuple(in_vmem(2)),
        scratch_shapes=[
            pltpu.SemaphoreType.DMA((2, 2, CHIPS - 1)),
            pltpu.SemaphoreType.DMA((2, 2, CHIPS)),
        ],
        compiler_params=comm_params(2),
        cost_estimate=comm_cost(kv.size * 2 * SPAN),
    )(kv, tags[None])
    return kv_all.reshape(SPAN * rows, columns), tags_all.reshape(SPAN * rows)


def added(*parts):
    total = parts[0].astype(jnp.float32)
    for part in parts[1:]:
        total = total + part.astype(jnp.float32)
    return total


def reduce_plane(arrays, h_sems, p_sems):
    me, core, chip, partner = plane_of()
    layer = lax.axis_index("fsdp")
    handed, spread = [], []
    for a, (piece_of, halves, sums, arrived) in enumerate(arrays):
        for j in range(CHIPS):
            slot = (j + 1) % CHIPS
            handed.append(
                send(
                    piece_of(chip_at(chip, 1 - core, slot)),
                    halves.at[slot],
                    h_sems.at[0, a, slot],
                    h_sems.at[1, a, slot],
                    (partner, layer),
                )
            )
    for a, (piece_of, halves, sums, arrived) in enumerate(arrays):
        for j in range(CHIPS):
            slot = (j + 1) % CHIPS
            handed[a * CHIPS + j].wait_recv()
            mine = chip_at(chip, core, slot)

            def add_half(slab, carry, piece=piece_of(mine), halves=halves, sums=sums, slot=slot):
                sums[slot, slab] = added(piece[slab], halves[slot, slab]).astype(sums.dtype)
                return carry

            lax.fori_loop(0, sums.shape[1], add_half, 0)
            if slot:
                spread.append(
                    send(
                        sums.at[slot],
                        arrived.at[slot - 1],
                        p_sems.at[0, a, slot - 1],
                        p_sems.at[1, a, slot - 1],
                        (mine, layer),
                    )
                )
    return handed, spread


def plane_total(sums, arrived, slab):
    return added(sums[0, slab], *(arrived[j, slab] for j in range(CHIPS - 1)))


def plane_scratch(block, dtype):
    return [
        pltpu.VMEM((CHIPS, *block), dtype),
        pltpu.VMEM((CHIPS, *block), dtype),
        pltpu.VMEM((CHIPS - 1, *block), dtype),
    ]


def turned_back(values, cos_tab, sin_tab):
    half_dim, parts = HEAD // 2, []
    for start in range(0, values.shape[1], HEAD):
        low = values[:, start : start + half_dim]
        high = values[:, start + half_dim : start + HEAD]
        parts += [low * cos_tab + high * sin_tab, high * cos_tab - low * sin_tab]
    return jnp.concatenate(parts, 1)


def scatter_plane_kernel(x_ref, cos_ref, sin_ref, out_ref, halves, sums, arrived, h_sems, p_sems):
    me, core, chip, partner = plane_of()
    layer = lax.axis_index("fsdp")
    greet([(chip_at(chip, core, j), layer) for j in range(1, CHIPS)] + [(partner, layer)])
    arrays = [(lambda piece: x_ref.at[piece], halves, sums, arrived)]
    handed, spread = reduce_plane(arrays, h_sems, p_sems)
    for copy in spread:
        copy.wait_recv()

    def add_slab(slab, carry):
        total = plane_total(sums, arrived, slab)
        kdim = KV_HEADS * HEAD
        keys = turned_back(total[:, :kdim], cos_ref[slab], sin_ref[slab])
        out_ref[slab] = jnp.concatenate([keys, total[:, kdim:]], 1).astype(out_ref.dtype)
        return carry

    lax.fori_loop(0, x_ref.shape[1], add_slab, 0)
    for copy in handed + spread:
        copy.wait_send()


def scatter_plane(values, cos_tab, sin_tab):
    if lax.axis_size("ctx") != SPAN:
        own = lax.psum_scatter(values, "ctx", scatter_dimension=0, tiled=True)
        own, kdim = own.astype(jnp.float32), KV_HEADS * HEAD
        keys = turned_back(own[:, :kdim], cos_tab, sin_tab)
        return jnp.concatenate([keys, own[:, kdim:]], 1).astype(values.dtype)
    rows, columns = values.shape
    slabs = 8
    block = (slabs, rows // SPAN // slabs, columns)
    return pl.pallas_call(
        scatter_plane_kernel,
        out_shape=jax.ShapeDtypeStruct(block, values.dtype),
        in_specs=in_vmem(3),
        out_specs=in_vmem(1)[0],
        scratch_shapes=plane_scratch(block, values.dtype)
        + [pltpu.SemaphoreType.DMA((2, 1, CHIPS)), pltpu.SemaphoreType.DMA((2, 1, CHIPS - 1))],
        compiler_params=comm_params(3),
        cost_estimate=comm_cost(values.size * 2),
    )(
        values.reshape(SPAN, *block),
        cos_tab.reshape(*block[:2], -1),
        sin_tab.reshape(*block[:2], -1),
    ).reshape(rows // SPAN, columns)


def reduce_rows_kernel(depth, count, *refs):
    inputs, outs, scratch = refs[:count], refs[count : 2 * count], refs[2 * count : 6 * count]
    h_sems, p_sems, z_sems, g_sems, f_sems = refs[6 * count :]
    me, core, chip, partner = plane_of()
    layer = lax.axis_index("fsdp")
    layers = [lax.rem(layer + d, depth) for d in range(1, depth)]
    peers = [chip_at(chip, core, j) for j in range(1, CHIPS)]
    greet([(me, other) for other in layers] + [(peer, layer) for peer in peers + [partner]])
    arrays, across = [], []
    for a, x_ref in enumerate(inputs):
        halves, sums, arrived, layers_ref = scratch[4 * a : 4 * a + 4]
        arrays.append((lambda piece, x_ref=x_ref: x_ref.at[:, piece], halves, sums, arrived))
        across.append(layers_ref)
    handed, spread = reduce_plane(arrays, h_sems, p_sems)
    moved = []
    for a, (_, _, sums, arrived) in enumerate(arrays):
        for copy in spread[a * (CHIPS - 1) : (a + 1) * (CHIPS - 1)]:
            copy.wait_recv()
        for d in list(range(1, depth)) + [0]:
            target = lax.rem(layer + d, depth)
            across[a][0, d] = plane_total(sums, arrived, target).astype(across[a].dtype)
            if d:
                moved.append(
                    send(
                        across[a].at[0, d],
                        across[a].at[1, d],
                        z_sems.at[0, a, d - 1],
                        z_sems.at[1, a, d - 1],
                        (me, target),
                    )
                )
    given, passed = [], []
    for a, out_ref in enumerate(outs):
        for copy in moved[a * (depth - 1) : (a + 1) * (depth - 1)]:
            copy.wait_recv()
        parts = [across[a][0, 0]] + [across[a][1, d] for d in range(1, depth)]
        out_ref[me] = added(*parts).astype(out_ref.dtype)
        mine = out_ref.at[me]
        for j, peer in enumerate(peers):
            given.append(send(mine, mine, g_sems.at[0, a, j], g_sems.at[1, a, j], (peer, layer)))
        passed.append(send(mine, mine, f_sems.at[0, a, 3], f_sems.at[1, a, 3], (partner, layer)))
    for a, out_ref in enumerate(outs):
        for j in range(CHIPS - 1):
            given[a * (CHIPS - 1) + j].wait_recv()
            block = out_ref.at[chip_at(chip, core, -j - 1)]
            passed.append(
                send(block, block, f_sems.at[0, a, j], f_sems.at[1, a, j], (partner, layer))
            )
    for copy in handed + spread + moved + given:
        copy.wait_send()
    for copy in passed:
        copy.wait()


def reduce_rows(arrays, number):
    if lax.axis_size("ctx") != SPAN:
        return [lax.psum(lax.psum_scatter(v, "fsdp", scatter_dimension=0), "ctx") for v in arrays]
    depth, count = arrays[0].shape[0], len(arrays)
    pieces, outs, scratch = [], [], []
    for values in arrays:
        _, rows, columns = values.shape
        piece = (rows // SPAN, columns)
        pieces.append(values.reshape(depth, SPAN, *piece))
        outs.append(jax.ShapeDtypeStruct((SPAN, *piece), values.dtype))
        scratch += plane_scratch((depth, *piece), values.dtype)
        scratch.append(pltpu.VMEM((2, depth, *piece), values.dtype))
    owned = pl.pallas_call(
        functools.partial(reduce_rows_kernel, depth, count),
        out_shape=tuple(outs),
        in_specs=in_vmem(count),
        out_specs=tuple(in_vmem(count)),
        scratch_shapes=scratch
        + [
            pltpu.SemaphoreType.DMA((2, count, CHIPS)),
            pltpu.SemaphoreType.DMA((2, count, CHIPS - 1)),
            pltpu.SemaphoreType.DMA((2, count, depth - 1)),
            pltpu.SemaphoreType.DMA((2, count, CHIPS - 1)),
            pltpu.SemaphoreType.DMA((2, count, CHIPS)),
        ],
        compiler_params=comm_params(number),
        cost_estimate=comm_cost(sum(values.size for values in arrays) * 2),
    )(*pieces)
    return [own.reshape(values.shape[1:]) for own, values in zip(owned, arrays)]


BLOCK = 128
LANES = (HEADS // KV_HEADS) * BLOCK


def dot(left, right, dims=(1, 0)):
    return lax.dot_general(
        left, right, (((dims[0],), (dims[1],)), ((), ())), preferred_element_type=jnp.float32
    )


def of_group(ref, group, at):
    first = group * (HEADS // KV_HEADS)
    heads = range(first, first + HEADS // KV_HEADS)
    return jnp.concatenate([ref[head * HEAD : (head + 1) * HEAD, at] for head in heads], 1)


def of_rows(ref, group, at):
    first = group * (HEADS // KV_HEADS)
    heads = range(first, first + HEADS // KV_HEADS)
    return jnp.concatenate([ref[head : head + 1, at] for head in heads], 1)


def columns_of(group, part):
    start = (part * KV_HEADS + group) * HEAD
    return slice(start, start + HEAD)


def mask_bias(tags, query_pos):
    tags = jnp.broadcast_to(tags, (BLOCK, BLOCK)).T
    key_pos = jnp.where(tags >= 0, tags, -tags - 1)
    allowed = (key_pos <= query_pos) & ((tags >= 0) | (key_pos == query_pos))
    bias = jnp.where(allowed, 0.0, negative)
    return jnp.concatenate([bias] * (HEADS // KV_HEADS), 1)


def attend_kernel(
    first_ref, q_ref, kv_ref, pos_ref, tag_ref, out_ref, log_ref, max_ref, sum_ref, acc_ref, kept
):
    blocks = kv_ref.shape[0] // BLOCK
    keep = kept.shape[0] == blocks

    def scores(group, at, rows, bias):
        keys = kv_ref[rows, columns_of(group, 0)]
        return dot(keys, of_group(q_ref, group, at)) + bias

    def query_block(qb, carry):
        at = pl.ds(pl.multiple_of(qb * BLOCK, BLOCK), BLOCK)
        max_ref[...] = jnp.full(max_ref.shape, negative, jnp.float32)
        sum_ref[...] = jnp.zeros(sum_ref.shape, jnp.float32)
        acc_ref[...] = jnp.zeros(acc_ref.shape, jnp.float32)
        limit = first_ref[blocks + qb]

        def find(kb, carry):
            @pl.when(first_ref[kb] <= limit)
            def _():
                rows = pl.ds(pl.multiple_of(kb * BLOCK, BLOCK), BLOCK)
                bias = mask_bias(tag_ref[kb], pos_ref[:, at])
                for group in range(KV_HEADS):
                    found = scores(group, at, rows, bias)
                    if keep:
                        kept[kb, group] = found
                    tops = jnp.max(found.reshape(BLOCK // 8, 8, LANES), 0)
                    max_ref[group] = jnp.maximum(max_ref[group], tops)

            return carry

        lax.fori_loop(0, blocks, find, 0)
        for group in range(KV_HEADS):
            top = jnp.max(max_ref[group], 0, keepdims=True)
            max_ref[group] = jnp.broadcast_to(top, max_ref.shape[1:])

        def gather(kb, carry):
            @pl.when(first_ref[kb] <= limit)
            def _():
                rows = pl.ds(pl.multiple_of(kb * BLOCK, BLOCK), BLOCK)
                bias = None if keep else mask_bias(tag_ref[kb], pos_ref[:, at])
                for group in range(KV_HEADS):
                    found = kept[kb, group] if keep else scores(group, at, rows, bias)
                    weights = jnp.exp(found - max_ref[group, :1])
                    sum_ref[group] += jnp.sum(weights.reshape(BLOCK // 8, 8, LANES), 0)
                    values = kv_ref[rows, columns_of(group, 1)]
                    acc_ref[group] += dot(values, weights.astype(jnp.bfloat16), (0, 0))

            return carry

        lax.fori_loop(0, blocks, gather, 0)
        for group in range(KV_HEADS):
            total = jnp.sum(sum_ref[group], 0, keepdims=True)
            attended = acc_ref[group] / total
            logs = max_ref[group, :1] + jnp.log(total)
            for j in range(HEADS // KV_HEADS):
                head = group * (HEADS // KV_HEADS) + j
                own = slice(j * BLOCK, (j + 1) * BLOCK)
                out_ref[head * HEAD : (head + 1) * HEAD, at] = attended[:, own]
                log_ref[head : head + 1, at] = logs[:, own]
        return carry

    lax.fori_loop(0, q_ref.shape[1] // BLOCK, query_block, 0)


def kernel_params():
    return pltpu.CompilerParams(vmem_limit_bytes=VMEM_BYTES)


def attend(firsts, queries, kv, query_pos, key_tags):
    blocks = kv.shape[0] // BLOCK
    slots = queries.shape[1]
    kept = blocks if blocks <= 16 else 1
    groups = (KV_HEADS, 8, LANES)
    work = 4 * kv.shape[0] * slots * HEADS * HEAD
    return pl.pallas_call(
        attend_kernel,
        out_shape=(
            jax.ShapeDtypeStruct(queries.shape, jnp.float32),
            jax.ShapeDtypeStruct((HEADS + 1, slots), jnp.float32),
        ),
        in_specs=[pl.BlockSpec(memory_space=pltpu.SMEM)] + in_vmem(4),
        out_specs=tuple(in_vmem(2)),
        scratch_shapes=[
            pltpu.VMEM(groups, jnp.float32),
            pltpu.VMEM(groups, jnp.float32),
            pltpu.VMEM((KV_HEADS, HEAD, LANES), jnp.float32),
            pltpu.VMEM((kept, KV_HEADS, BLOCK, LANES), jnp.float32),
        ],
        compiler_params=kernel_params(),
        cost_estimate=pl.CostEstimate(
            flops=work * 8, bytes_accessed=kv.size * 2, transcendentals=work // 256
        ),
    )(firsts, queries, kv, query_pos[None], key_tags.reshape(-1, 1, BLOCK))


def attend_back_kernel(
    first_ref, q_ref, kv_ref, pos_ref, tag_ref, grad_ref, log_ref, delta_ref, *refs
):
    blocks = kv_ref.shape[0] // BLOCK
    cos_ref, sin_ref, out_ref, dkv_ref, acc, dq_ref = refs
    dq_ref[...] = jnp.zeros(dq_ref.shape, dq_ref.dtype)

    def key_block(kb, carry):
        rows = pl.ds(pl.multiple_of(kb * BLOCK, BLOCK), BLOCK)
        acc[...] = jnp.zeros(acc.shape, jnp.float32)

        def query_block(qb, carry):
            @pl.when(first_ref[kb] <= first_ref[blocks + qb])
            def _():
                at = pl.ds(pl.multiple_of(qb * BLOCK, BLOCK), BLOCK)
                bias = mask_bias(tag_ref[kb], pos_ref[:, at])
                for group in range(KV_HEADS):
                    keys = kv_ref[rows, columns_of(group, 0)]
                    values = kv_ref[rows, columns_of(group, 1)]
                    queries = of_group(q_ref, group, at)
                    grads = of_group(grad_ref, group, at)
                    found = dot(keys, queries) + bias
                    probs = jnp.exp(found - of_rows(log_ref, group, at))
                    grad_probs = dot(values, grads)
                    grad_scores = probs * (grad_probs - of_rows(delta_ref, group, at))
                    grad_scores = grad_scores.astype(jnp.bfloat16)
                    acc[group] += dot(grad_scores, queries, (1, 1))
                    acc[KV_HEADS + group] += dot(probs.astype(jnp.bfloat16), grads, (1, 1))
                    grad_q = 0.125 * dot(keys, grad_scores, (0, 0))
                    for j in range(HEADS // KV_HEADS):
                        head = group * (HEADS // KV_HEADS) + j
                        own = slice(head * HEAD, (head + 1) * HEAD)
                        dq_ref[own, at] += grad_q[:, j * BLOCK : (j + 1) * BLOCK]

            return carry

        lax.fori_loop(0, q_ref.shape[1] // BLOCK, query_block, 0)
        dkv_ref[rows, :] = jnp.concatenate(
            [acc[index] for index in range(2 * KV_HEADS)], 1
        ).astype(dkv_ref.dtype)
        return carry

    lax.fori_loop(0, blocks, key_block, 0)
    half_dim = HEAD // 2

    def finish(qb, carry):
        at = pl.ds(pl.multiple_of(qb * BLOCK, BLOCK), BLOCK)
        cos_tab, sin_tab = cos_ref[:, at], sin_ref[:, at]
        for head in range(0, HEADS, 2):
            pair = []
            for start in range(head * HEAD, min(head + 2, HEADS) * HEAD, HEAD):
                low = dq_ref[start : start + half_dim, at]
                high = dq_ref[start + half_dim : start + HEAD, at]
                pair += [low * cos_tab + high * sin_tab, high * cos_tab - low * sin_tab]
            if len(pair) == 2:
                pair += [jnp.zeros_like(part) for part in pair]
            turned = jnp.concatenate(pair, 0).T
            own = slice(head * HEAD, head * HEAD + turned.shape[1])
            out_ref[at, own] = turned.astype(out_ref.dtype)
        return carry

    lax.fori_loop(0, q_ref.shape[1] // BLOCK, finish, 0)


def attend_back(firsts, queries, kv, query_pos, key_tags, grads, log_total, row_delta, tables):
    slots = queries.shape[1]
    work = 10 * kv.shape[0] * slots * HEADS * HEAD
    return pl.pallas_call(
        attend_back_kernel,
        out_shape=(
            jax.ShapeDtypeStruct((slots, -(-HEADS // 2) * 2 * HEAD), jnp.bfloat16),
            jax.ShapeDtypeStruct(kv.shape, jnp.bfloat16),
        ),
        in_specs=[pl.BlockSpec(memory_space=pltpu.SMEM)] + in_vmem(9),
        out_specs=tuple(in_vmem(2)),
        scratch_shapes=[
            pltpu.VMEM((2 * KV_HEADS, BLOCK, HEAD), jnp.float32),
            pltpu.VMEM(queries.shape, jnp.float32),
        ],
        compiler_params=kernel_params(),
        cost_estimate=pl.CostEstimate(
            flops=work * 6, bytes_accessed=kv.size * 4, transcendentals=work // 640
        ),
    )(firsts, queries, kv, query_pos[None], key_tags.reshape(-1, 1, BLOCK), grads, log_total, row_delta, *tables)


def on_device(
    tokens,
    w_query,
    w_key,
    w_value,
    w_out,
    w_gate,
    w_up,
    w_down,
    gain_attn,
    gain_ffn,
    router,
    cotangent,
    positions,
    lengths,
    chosen,
):
    hidden = tokens[0].astype(jnp.float32)
    row_count, width = hidden.shape
    qdim = HEADS * HEAD
    kdim = KV_HEADS * HEAD
    query_pos = positions[0]
    live = query_pos < lengths[0]
    selected = live & (chosen[0] == 1)
    live_mask = live.astype(jnp.float32)[:, None]
    chosen_mask = selected.astype(jnp.float32)[:, None]
    cos_tab, sin_tab = rope_tables(query_pos)
    key_tags = jnp.where(selected, query_pos, -query_pos - 1)
    depth = lax.axis_size("fsdp")
    own_rows = w_query.shape[0]
    w_out_full = lax.all_gather(w_out, "fsdp", axis=0, tiled=True)
    vectors = jnp.stack([gain_attn, gain_ffn, router], 1)
    own_attn = [padded_to(w_query, 1), jnp.concatenate([w_key, w_value, vectors], 1)]
    gathered = gather_rows([padded_to(own, 0) for own in own_attn], depth)
    padded_rows = gathered[0].shape[1]
    w_query = gathered[0].reshape(depth * padded_rows, -1)
    gathered = gathered[1][:, :own_rows].reshape(width, -1)
    w_kv, vectors = gathered[:, : 2 * kdim], gathered[:, 2 * kdim :]
    gain_one, gain_two, router_vec = vectors.T.astype(jnp.float32)
    gating = jax.nn.sigmoid(jnp.sum(hidden * router_vec, -1, keepdims=True))
    grad_y = cotangent[0].astype(jnp.float32) * live_mask
    grad_inc = grad_y * chosen_mask * gating
    grad_ffn = grad_inc.astype(jnp.bfloat16)
    grad_ffn_all = lax.all_gather(grad_ffn, "fsdp", axis=0, tiled=True)

    normed_one, inv_one = norm_forward(hidden, gain_one)
    normed_one = normed_one.astype(jnp.bfloat16)
    spread_one = padded_to(normed_one.reshape(row_count, depth, own_rows), -1)
    spread_one = spread_one.reshape(row_count, -1)
    query_raw = dot(w_query, spread_one, (0, 1))[:qdim]
    queries = rotate_columns(query_raw, cos_tab, sin_tab).astype(jnp.bfloat16) * 0.125
    kv_raw = dot(normed_one, w_kv)
    kv_own = jnp.concatenate([rotate(kv_raw[:, :kdim], cos_tab, sin_tab), kv_raw[:, kdim:]], 1)
    kv_all, tags_all = gather_plane(kv_own.astype(jnp.bfloat16), key_tags)
    first_tags = tags_all[::BLOCK]
    firsts = jnp.concatenate(
        [jnp.where(first_tags >= 0, first_tags, -first_tags - 1), query_pos[BLOCK - 1 :: BLOCK]]
    )
    attended, log_total = attend(firsts, queries, kv_all, query_pos, tags_all)
    attended, w_out_full = lax.optimization_barrier((attended, w_out_full))
    outcome = attended.astype(jnp.bfloat16)
    branch = dot(outcome, w_out_full, (0, 0))
    branch, grad_ffn_all = lax.optimization_barrier((branch, grad_ffn_all))
    middle = hidden + branch
    normed_two, inv_two = norm_forward(middle, gain_two)
    normed_two = normed_two.astype(jnp.bfloat16)
    normed_all = lax.all_gather(normed_two, "fsdp", axis=0, tiled=True)
    inner_act, grad_gate_act, grad_up_act, grad_normed_part = ffn_both(
        normed_all, grad_ffn_all, w_gate, w_up, w_down
    )
    grad_normed_two = lax.psum_scatter(
        grad_normed_part, "fsdp", scatter_dimension=0, tiled=True
    ).astype(jnp.float32)
    ffn_part = jnp.dot(inner_act, w_down, preferred_element_type=jnp.float32).astype(jnp.bfloat16)
    grad_wgate = lax.dot_general(
        grad_gate_act, normed_all, across_rows, preferred_element_type=jnp.float32
    )
    grad_wup = lax.dot_general(
        grad_up_act, normed_all, across_rows, preferred_element_type=jnp.float32
    )
    grad_wdown = lax.dot_general(
        inner_act, grad_ffn_all, across_rows, preferred_element_type=jnp.float32
    )
    low = jnp.bfloat16
    spread_out = padded_to(outcome.reshape(depth, own_rows, row_count), 1)
    grads = [grad.astype(low) for grad in (grad_wgate, grad_wup, grad_wdown)]
    grad_normed_two, ffn_part, spread_out, *grads = lax.optimization_barrier(
        (grad_normed_two, ffn_part, spread_out, *grads)
    )
    grad_normed_two, row_dot = grad_normed_two[:, :width], grad_normed_two[:, width:]
    totals = tuple(lax.psum(grad, "ctx") for grad in grads)
    grad_middle, grad_gain_two = norm_backward(middle, inv_two, gain_two, grad_normed_two)
    grad_branch = (grad_inc + grad_middle).astype(jnp.bfloat16)
    grad_attended = dot(w_out_full, grad_branch, (1, 1)).astype(jnp.bfloat16)
    grad_wout = dot(spread_out.reshape(-1, row_count), padded_to(grad_branch, 1)).astype(low)
    row_delta = jnp.sum(
        (grad_attended.astype(jnp.float32) * attended).reshape(HEADS, HEAD, row_count), 1
    )
    row_delta = jnp.pad(row_delta, ((0, 1), (0, 0)))
    grad_query_raw, grad_kv_all = attend_back(
        firsts,
        queries,
        kv_all,
        query_pos,
        tags_all,
        grad_attended,
        log_total,
        row_delta,
        (cos_tab.T, sin_tab.T),
    )
    grad_kv_raw = scatter_plane(grad_kv_all, cos_tab, sin_tab)
    grad_logit = (jnp.sum(grad_inc * branch, -1, keepdims=True) + row_dot) * (1.0 - gating)
    grad_router = jnp.sum(hidden * grad_logit, 0)
    grad_normed_one = dot(grad_query_raw, w_query, (1, 1)).reshape(row_count, depth, -1)
    grad_normed_one = grad_normed_one[..., :own_rows].reshape(row_count, width)
    grad_normed_one = grad_normed_one + dot(grad_kv_raw, w_kv, (1, 1))
    grad_wq = dot(spread_one, grad_query_raw, (0, 0)).astype(low)
    grad_wkv = dot(spread_one, grad_kv_raw, (0, 0)).astype(low)
    grad_hidden_one, grad_gain_one = norm_backward(hidden, inv_one, gain_one, grad_normed_one)
    grad_tokens = (grad_y + grad_logit * router_vec + grad_middle + grad_hidden_one).astype(
        jnp.bfloat16
    )
    vectors = jnp.stack([grad_gain_one, grad_gain_two, grad_router]).reshape(3, depth, own_rows)
    vectors = jnp.pad(vectors.transpose(1, 0, 2).reshape(depth, -1), ((0, 0), (0, -3 * own_rows % 1024)))
    vectors = jnp.pad(vectors.reshape(depth, -1, 1, 128), ((0, 0), (0, 0), (0, 7), (0, 0)))
    layered = [grad.reshape(depth, padded_rows, -1) for grad in (grad_wout, grad_wq, grad_wkv)]
    layered.append(vectors.reshape(depth, -1, 128))
    owned = reduce_rows(layered, 4)
    ffn_out = lax.psum_scatter(ffn_part, "fsdp", scatter_dimension=0, tiled=True)
    *owned, totals, ffn_out = lax.optimization_barrier((*owned, totals, ffn_out))
    increment = branch + ffn_out.astype(jnp.float32)
    block_out = live_mask * (hidden + chosen_mask * gating * increment)
    total_out, total_q, total_kv = (own[:own_rows].astype(jnp.float32) for own in owned[:3])
    total_q, total_out = total_q[:, :qdim], total_out[:, :width]
    total_k, total_v = total_kv[:, :kdim], total_kv[:, kdim:]
    mine = owned[3].reshape(-1, 8, 128)[:, 0].reshape(-1)[: 3 * own_rows].reshape(3, own_rows)
    total_gate, total_up, total_down = (total.astype(jnp.float32) for total in totals)
    return (
        block_out.astype(jnp.bfloat16)[None],
        grad_tokens[None],
        total_q,
        total_k,
        total_v,
        total_out,
        total_gate,
        total_up,
        total_down,
        mine[0],
        mine[1],
        mine[2],
    )


def solution(mesh):
    in_specs = (
        P("fsdp", "ctx", None),
        P("fsdp", None),
        P("fsdp", None),
        P("fsdp", None),
        P("fsdp", None),
        P("fsdp", None),
        P("fsdp", None),
        P("fsdp", None),
        P("fsdp"),
        P("fsdp"),
        P("fsdp"),
        P("fsdp", "ctx", None),
        P("fsdp", "ctx"),
        P("fsdp"),
        P("fsdp", "ctx"),
    )
    out_specs = (
        P("fsdp", "ctx", None),
        P("fsdp", "ctx", None),
        P("fsdp", None),
        P("fsdp", None),
        P("fsdp", None),
        P("fsdp", None),
        P("fsdp", None),
        P("fsdp", None),
        P("fsdp", None),
        P("fsdp"),
        P("fsdp"),
        P("fsdp"),
    )
    return jax.shard_map(
        on_device, mesh=mesh, in_specs=in_specs, out_specs=out_specs, check_vma=False
    )
```

```python
import functools

import jax
import jax.numpy as jnp
from jax import lax
from jax.experimental import pallas as pl
from jax.experimental.pallas import tpu as pltpu
from jax.sharding import PartitionSpec as P

HEADS = 15
KV_HEADS = 5
HEAD = 64


epsilon = 1e-05
negative = -1e30
across_rows = (((0,), (0,)), ((), ()))
across_cols = (((1,), (1,)), ((), ()))


def rope_tables(positions):
    half_dim = HEAD // 2
    frequency = 10000.0 ** (-2.0 * jnp.arange(half_dim, dtype=jnp.float32) / HEAD)
    angles = positions.astype(jnp.float32)[:, None] * frequency[None, :]
    return (jnp.cos(angles), jnp.sin(angles))


def rotate(values, cos_tab, sin_tab):
    slots, width = values.shape
    low, high = jnp.split(values.reshape(slots, width // HEAD, HEAD), 2, -1)
    cos_tab, sin_tab = cos_tab[:, None], sin_tab[:, None]
    turned = [low * cos_tab - high * sin_tab, high * cos_tab + low * sin_tab]
    return jnp.concatenate(turned, -1).reshape(slots, width)


def rotate_columns(values, cos_tab, sin_tab):
    width, slots = values.shape
    low, high = jnp.split(values.reshape(width // HEAD, HEAD, slots), 2, 1)
    cos_tab, sin_tab = cos_tab.T[None], sin_tab.T[None]
    turned = [low * cos_tab - high * sin_tab, high * cos_tab + low * sin_tab]
    return jnp.concatenate(turned, 1).reshape(width, slots)


def norm_forward(values, gain_vec):
    inv_rms = lax.rsqrt(jnp.mean(values * values, -1, keepdims=True) + epsilon)
    return (values * inv_rms * gain_vec, inv_rms)


def norm_backward(values, inv_rms, gain_vec, grad_normed):
    weighted = gain_vec * grad_normed
    grad_gain = jnp.sum(grad_normed * values * inv_rms, 0)
    cubed = inv_rms * inv_rms * inv_rms
    grad_values = inv_rms * weighted - values * cubed * jnp.mean(
        weighted * values, -1, keepdims=True
    )
    return (grad_values, grad_gain)


def padded_to(values, row_dim):
    pads = [(0, 0)] * values.ndim
    pads[row_dim] = (0, -values.shape[row_dim] % 128)
    return jnp.pad(values, pads)


def ffn_both(normed, grad_mixed, gate_rows, up_rows, down_rows):
    gate_proj = lax.dot_general(normed, gate_rows, across_cols, preferred_element_type=jnp.float32)
    up_proj = lax.dot_general(normed, up_rows, across_cols, preferred_element_type=jnp.float32)
    sigma = jax.nn.sigmoid(gate_proj)
    activated = gate_proj * sigma
    inner_act = (activated * up_proj).astype(jnp.bfloat16)
    grad_inner = lax.dot_general(
        grad_mixed, down_rows, across_cols, preferred_element_type=jnp.float32
    )
    grad_gate_act = (grad_inner * up_proj * sigma * (1.0 + gate_proj * (1.0 - sigma))).astype(
        jnp.bfloat16
    )
    grad_up_act = (grad_inner * activated).astype(jnp.bfloat16)
    grad_normed = jnp.dot(grad_gate_act, gate_rows, preferred_element_type=jnp.float32) + jnp.dot(
        grad_up_act, up_rows, preferred_element_type=jnp.float32
    )
    row_dot = jnp.sum(inner_act.astype(jnp.float32) * grad_inner, -1, keepdims=True)
    grad_normed = jnp.concatenate([grad_normed, row_dot], 1).astype(jnp.bfloat16)
    return (inner_act, grad_gate_act, grad_up_act, grad_normed)


CHIPS = 4
SPAN = 2 * CHIPS
VMEM_BYTES = 60 * 1024 * 1024
MESH = pl.DeviceIdType.MESH


def plane_of():
    me = lax.axis_index("ctx")
    core = lax.rem(me, 2)
    chip = me // 2
    return me, core, chip, me + 1 - 2 * core


def chip_at(chip, core, step):
    return 2 * lax.rem(chip + step + CHIPS, CHIPS) + core


def greet(devices):
    barrier = pltpu.get_barrier_semaphore()
    for device in devices:
        pl.semaphore_signal(barrier, inc=1, device_id=device, device_id_type=MESH)
    pl.semaphore_wait(barrier, len(devices))


def send(src, dst, send_sem, recv_sem, device):
    copy = pltpu.make_async_remote_copy(
        src_ref=src,
        dst_ref=dst,
        send_sem=send_sem,
        recv_sem=recv_sem,
        device_id=device,
        device_id_type=MESH,
    )
    copy.start()
    return copy


def comm_params(number):
    return pltpu.CompilerParams(
        collective_id=number, has_side_effects=True, vmem_limit_bytes=VMEM_BYTES
    )


def comm_cost(moved):
    return pl.CostEstimate(flops=0, bytes_accessed=moved * 30, transcendentals=0)


def in_vmem(count):
    return [pl.BlockSpec(memory_space=pltpu.VMEM)] * count


def gather_rows_kernel(depth, count, *refs):
    owns, outs = refs[:count], refs[count : 2 * count]
    z_sems, p_sems, f_sems = refs[2 * count :]
    me, core, chip, partner = plane_of()
    layer = lax.axis_index("fsdp")
    layers = [lax.rem(layer + d, depth) for d in range(1, depth)]
    peers = [chip_at(chip, core, j) for j in range(1, CHIPS)]
    greet([(me, other) for other in layers] + [(peer, layer) for peer in peers + [partner]])
    first, spread, passed = [], [], []
    for a, (own, out) in enumerate(zip(owns, outs)):
        for d, other in enumerate(layers):
            first.append(
                send(
                    own.at[me],
                    out.at[layer, me],
                    z_sems.at[0, a, d],
                    z_sems.at[1, a, d],
                    (me, other),
                )
            )
    for own, out in zip(owns, outs):
        for piece in range(SPAN):
            out[layer, piece] = own[piece]
    for a, out in enumerate(outs):
        for d in range(depth - 1):
            first[a * (depth - 1) + d].wait_recv()
            block = out.at[lax.rem(layer + depth - d - 1, depth), me]
            for j, peer in enumerate(peers):
                spread.append(
                    send(block, block, p_sems.at[0, a, d, j], p_sems.at[1, a, d, j], (peer, layer))
                )
            passed.append(
                send(block, block, f_sems.at[0, a, d, 3], f_sems.at[1, a, d, 3], (partner, layer))
            )
    arrivals = iter(spread)
    for a, out in enumerate(outs):
        for d in range(depth - 1):
            source = lax.rem(layer + depth - d - 1, depth)
            for j in range(CHIPS - 1):
                next(arrivals).wait_recv()
                block = out.at[source, chip_at(chip, core, -j - 1)]
                passed.append(
                    send(
                        block,
                        block,
                        f_sems.at[0, a, d, j],
                        f_sems.at[1, a, d, j],
                        (partner, layer),
                    )
                )
    for copy in first + spread:
        copy.wait_send()
    for copy in passed:
        copy.wait()


def gather_rows(arrays, depth):
    if lax.axis_size("ctx") != SPAN:
        return [lax.all_gather(own, "fsdp", axis=0) for own in arrays]
    count, pieces, outs = len(arrays), [], []
    for own in arrays:
        piece = (own.shape[0] // SPAN, own.shape[1])
        pieces.append(own.reshape(SPAN, *piece))
        outs.append(jax.ShapeDtypeStruct((depth, SPAN, *piece), own.dtype))
    whole = pl.pallas_call(
        functools.partial(gather_rows_kernel, depth, count),
        out_shape=tuple(outs),
        in_specs=in_vmem(count),
        out_specs=tuple(in_vmem(count)),
        scratch_shapes=[
            pltpu.SemaphoreType.DMA((2, count, depth - 1)),
            pltpu.SemaphoreType.DMA((2, count, depth - 1, CHIPS - 1)),
            pltpu.SemaphoreType.DMA((2, count, depth - 1, CHIPS)),
        ],
        compiler_params=comm_params(1),
        cost_estimate=comm_cost(sum(own.size for own in arrays) * 2 * depth),
    )(*pieces)
    return [full.reshape(depth, *own.shape) for full, own in zip(whole, arrays)]


def gather_plane_kernel(kv_ref, tag_ref, kv_out, tag_out, p_sems, f_sems):
    me, core, chip, partner = plane_of()
    layer = lax.axis_index("fsdp")
    peers = [chip_at(chip, core, j) for j in range(1, CHIPS)]
    greet([(peer, layer) for peer in peers + [partner]])
    pairs = ((kv_ref, kv_out), (tag_ref, tag_out))
    spread, passed = [], []
    for j, peer in enumerate(peers):
        for a, (own, out) in enumerate(pairs):
            spread.append(
                send(own, out.at[me], p_sems.at[0, a, j], p_sems.at[1, a, j], (peer, layer))
            )
    for a, (own, out) in enumerate(pairs):
        passed.append(
            send(own, out.at[me], f_sems.at[0, a, 3], f_sems.at[1, a, 3], (partner, layer))
        )
    kv_out[me] = kv_ref[...]
    tag_out[me] = tag_ref[...]
    for j in range(CHIPS - 1):
        for a, (own, out) in enumerate(pairs):
            spread[2 * j + a].wait_recv()
            block = out.at[chip_at(chip, core, -j - 1)]
            passed.append(
                send(block, block, f_sems.at[0, a, j], f_sems.at[1, a, j], (partner, layer))
            )
    for copy in spread:
        copy.wait_send()
    for copy in passed:
        copy.wait()


def gather_plane(kv, tags):
    if lax.axis_size("ctx") != SPAN:
        return tuple(lax.all_gather(part, "ctx", axis=0, tiled=True) for part in (kv, tags))
    rows, columns = kv.shape
    kv_all, tags_all = pl.pallas_call(
        gather_plane_kernel,
        out_shape=(
            jax.ShapeDtypeStruct((SPAN, rows, columns), kv.dtype),
            jax.ShapeDtypeStruct((SPAN, 1, rows), tags.dtype),
        ),
        in_specs=in_vmem(2),
        out_specs=tuple(in_vmem(2)),
        scratch_shapes=[
            pltpu.SemaphoreType.DMA((2, 2, CHIPS - 1)),
            pltpu.SemaphoreType.DMA((2, 2, CHIPS)),
        ],
        compiler_params=comm_params(2),
        cost_estimate=comm_cost(kv.size * 2 * SPAN),
    )(kv, tags[None])
    return kv_all.reshape(SPAN * rows, columns), tags_all.reshape(SPAN * rows)


def added(*parts):
    total = parts[0].astype(jnp.float32)
    for part in parts[1:]:
        total = total + part.astype(jnp.float32)
    return total


def across_of(chip, core, way):
    along_x, along_y = lax.rem(chip, 2), chip // 2
    along_x = 1 - along_x if way % 2 else along_x
    along_y = 1 - along_y if way // 2 else along_y
    return 2 * (2 * along_y + along_x) + core


def reduce_plane(arrays, h_sems, p_sems):
    me, core, chip, partner = plane_of()
    layer = lax.axis_index("fsdp")
    ways = (3, 1, 2, 0)
    near = (across_of(chip, core, 1), across_of(chip, core, 2))
    handed, started, last = [], [], []
    for a, (piece_of, halves, sums, arrived) in enumerate(arrays):
        for way in ways:
            handed.append(
                send(
                    piece_of(across_of(chip, 1 - core, way)),
                    halves.at[way],
                    h_sems.at[0, a, way],
                    h_sems.at[1, a, way],
                    (partner, layer),
                )
            )
    for a, (piece_of, halves, sums, arrived) in enumerate(arrays):
        middle = sums.shape[1] // 2
        sides = (pl.ds(0, middle), pl.ds(middle, middle))
        copies = {}

        def pass_on(way, side, slot, hop, a=a, sums=sums, arrived=arrived, sides=sides):
            number = 2 * slot + side
            return send(
                sums.at[way, sides[side]],
                arrived.at[slot, sides[side]],
                p_sems.at[0, a, number],
                p_sems.at[1, a, number],
                (near[hop], layer),
            )

        for j, way in enumerate(ways):
            handed[a * CHIPS + j].wait_recv()
            mine = piece_of(across_of(chip, core, way))

            def add_half(slab, carry, mine=mine, halves=halves, sums=sums, way=way):
                sums[way, slab] = added(mine[slab], halves[way, slab]).astype(sums.dtype)
                return carry

            lax.fori_loop(0, sums.shape[1], add_half, 0)
            if way == 3:
                for side in range(2):
                    copies[0, side] = pass_on(3, side, 0, side)
            elif way:
                copies[1, way - 1] = pass_on(way, way - 1, 1, way - 1)
        started.append((copies, pass_on))
    for (copies, pass_on), (_, _, sums, arrived) in zip(started, arrays):
        middle = sums.shape[1] // 2
        for side in range(2):
            copies[0, side].wait_recv()
            way = 2 - side

            def add_opposite(slab, carry, way=way, sums=sums, arrived=arrived):
                total = added(sums[way, slab], arrived[0, slab])
                sums[way, slab] = total.astype(sums.dtype)
                return carry

            lax.fori_loop(side * middle, (side + 1) * middle, add_opposite, 0)
            copies[2, side] = pass_on(way, side, 2, 1 - side)
        last.append([copies[slot, side] for slot in (1, 2) for side in range(2)])
    everything = handed + [copy for copies, _ in started for copy in copies.values()]
    return everything, last


def plane_total(sums, arrived, slab):
    return added(sums[0, slab], arrived[1, slab], arrived[2, slab])


def plane_scratch(block, dtype):
    return [
        pltpu.VMEM((CHIPS, *block), dtype),
        pltpu.VMEM((CHIPS, *block), dtype),
        pltpu.VMEM((CHIPS - 1, *block), dtype),
    ]


def turned_back(values, cos_tab, sin_tab):
    half_dim, parts = HEAD // 2, []
    for start in range(0, values.shape[1], HEAD):
        low = values[:, start : start + half_dim]
        high = values[:, start + half_dim : start + HEAD]
        parts += [low * cos_tab + high * sin_tab, high * cos_tab - low * sin_tab]
    return jnp.concatenate(parts, 1)


def scatter_plane_kernel(x_ref, cos_ref, sin_ref, out_ref, halves, sums, arrived, h_sems, p_sems):
    me, core, chip, partner = plane_of()
    layer = lax.axis_index("fsdp")
    near = [across_of(chip, core, way) for way in (1, 2)]
    greet([(peer, layer) for peer in near + [partner]])
    arrays = [(lambda piece: x_ref.at[piece], halves, sums, arrived)]
    started, last = reduce_plane(arrays, h_sems, p_sems)
    for copy in last[0]:
        copy.wait_recv()

    def add_slab(slab, carry):
        total = plane_total(sums, arrived, slab)
        kdim = KV_HEADS * HEAD
        keys = turned_back(total[:, :kdim], cos_ref[slab], sin_ref[slab])
        out_ref[slab] = jnp.concatenate([keys, total[:, kdim:]], 1).astype(out_ref.dtype)
        return carry

    lax.fori_loop(0, x_ref.shape[1], add_slab, 0)
    for copy in started:
        copy.wait_send()


def scatter_plane(values, cos_tab, sin_tab):
    if lax.axis_size("ctx") != SPAN:
        own = lax.psum_scatter(values, "ctx", scatter_dimension=0, tiled=True)
        own, kdim = own.astype(jnp.float32), KV_HEADS * HEAD
        keys = turned_back(own[:, :kdim], cos_tab, sin_tab)
        return jnp.concatenate([keys, own[:, kdim:]], 1).astype(values.dtype)
    rows, columns = values.shape
    slabs = 8
    block = (slabs, rows // SPAN // slabs, columns)
    return pl.pallas_call(
        scatter_plane_kernel,
        out_shape=jax.ShapeDtypeStruct(block, values.dtype),
        in_specs=in_vmem(3),
        out_specs=in_vmem(1)[0],
        scratch_shapes=plane_scratch(block, values.dtype)
        + [pltpu.SemaphoreType.DMA((2, 1, CHIPS)), pltpu.SemaphoreType.DMA((2, 1, 6))],
        compiler_params=comm_params(3),
        cost_estimate=comm_cost(values.size * 2),
    )(
        values.reshape(SPAN, *block),
        cos_tab.reshape(*block[:2], -1),
        sin_tab.reshape(*block[:2], -1),
    ).reshape(rows // SPAN, columns)


def reduce_rows_kernel(depth, count, *refs):
    inputs, outs, scratch = refs[:count], refs[count : 2 * count], refs[2 * count : 6 * count]
    h_sems, p_sems, z_sems, g_sems, f_sems = refs[6 * count :]
    me, core, chip, partner = plane_of()
    layer = lax.axis_index("fsdp")
    layers = [lax.rem(layer + d, depth) for d in range(1, depth)]
    peers = [chip_at(chip, core, j) for j in range(1, CHIPS)]
    greet([(me, other) for other in layers] + [(peer, layer) for peer in peers + [partner]])
    arrays, across = [], []
    for a, x_ref in enumerate(inputs):
        halves, sums, arrived, layers_ref = scratch[4 * a : 4 * a + 4]
        arrays.append((lambda piece, x_ref=x_ref: x_ref.at[:, piece], halves, sums, arrived))
        across.append(layers_ref)
    started, last = reduce_plane(arrays, h_sems, p_sems)
    moved = []
    for a, (_, _, sums, arrived) in enumerate(arrays):
        for copy in last[a]:
            copy.wait_recv()
        for d in list(range(1, depth)) + [0]:
            target = lax.rem(layer + d, depth)
            across[a][0, d] = plane_total(sums, arrived, target).astype(across[a].dtype)
            if d:
                moved.append(
                    send(
                        across[a].at[0, d],
                        across[a].at[1, d],
                        z_sems.at[0, a, d - 1],
                        z_sems.at[1, a, d - 1],
                        (me, target),
                    )
                )
    given, passed = [], []
    for a, out_ref in enumerate(outs):
        for copy in moved[a * (depth - 1) : (a + 1) * (depth - 1)]:
            copy.wait_recv()
        parts = [across[a][0, 0]] + [across[a][1, d] for d in range(1, depth)]
        out_ref[me] = added(*parts).astype(out_ref.dtype)
        mine = out_ref.at[me]
        for j, peer in enumerate(peers):
            given.append(send(mine, mine, g_sems.at[0, a, j], g_sems.at[1, a, j], (peer, layer)))
        passed.append(send(mine, mine, f_sems.at[0, a, 3], f_sems.at[1, a, 3], (partner, layer)))
    for a, out_ref in enumerate(outs):
        for j in range(CHIPS - 1):
            given[a * (CHIPS - 1) + j].wait_recv()
            block = out_ref.at[chip_at(chip, core, -j - 1)]
            passed.append(
                send(block, block, f_sems.at[0, a, j], f_sems.at[1, a, j], (partner, layer))
            )
    for copy in started + moved + given:
        copy.wait_send()
    for copy in passed:
        copy.wait()


def reduce_rows(arrays, number):
    if lax.axis_size("ctx") != SPAN:
        return [lax.psum(lax.psum_scatter(v, "fsdp", scatter_dimension=0), "ctx") for v in arrays]
    depth, count = arrays[0].shape[0], len(arrays)
    pieces, outs, scratch = [], [], []
    for values in arrays:
        _, rows, columns = values.shape
        piece = (rows // SPAN, columns)
        pieces.append(values.reshape(depth, SPAN, *piece))
        outs.append(jax.ShapeDtypeStruct((SPAN, *piece), values.dtype))
        scratch += plane_scratch((depth, *piece), values.dtype)
        scratch.append(pltpu.VMEM((2, depth, *piece), values.dtype))
    owned = pl.pallas_call(
        functools.partial(reduce_rows_kernel, depth, count),
        out_shape=tuple(outs),
        in_specs=in_vmem(count),
        out_specs=tuple(in_vmem(count)),
        scratch_shapes=scratch
        + [
            pltpu.SemaphoreType.DMA((2, count, CHIPS)),
            pltpu.SemaphoreType.DMA((2, count, 6)),
            pltpu.SemaphoreType.DMA((2, count, depth - 1)),
            pltpu.SemaphoreType.DMA((2, count, CHIPS - 1)),
            pltpu.SemaphoreType.DMA((2, count, CHIPS)),
        ],
        compiler_params=comm_params(number),
        cost_estimate=comm_cost(sum(values.size for values in arrays) * 2),
    )(*pieces)
    return [own.reshape(values.shape[1:]) for own, values in zip(owned, arrays)]


BLOCK = 128
LANES = (HEADS // KV_HEADS) * BLOCK


def dot(left, right, dims=(1, 0)):
    return lax.dot_general(
        left, right, (((dims[0],), (dims[1],)), ((), ())), preferred_element_type=jnp.float32
    )


def of_group(ref, group, at):
    first = group * (HEADS // KV_HEADS)
    heads = range(first, first + HEADS // KV_HEADS)
    return jnp.concatenate([ref[head * HEAD : (head + 1) * HEAD, at] for head in heads], 1)


def of_rows(ref, group, at):
    first = group * (HEADS // KV_HEADS)
    heads = range(first, first + HEADS // KV_HEADS)
    return jnp.concatenate([ref[head : head + 1, at] for head in heads], 1)


def columns_of(group, part):
    start = (part * KV_HEADS + group) * HEAD
    return slice(start, start + HEAD)


def mask_bias(tags, query_pos):
    tags = jnp.broadcast_to(tags, (BLOCK, BLOCK)).T
    key_pos = jnp.where(tags >= 0, tags, -tags - 1)
    allowed = (key_pos <= query_pos) & ((tags >= 0) | (key_pos == query_pos))
    bias = jnp.where(allowed, 0.0, negative)
    return jnp.concatenate([bias] * (HEADS // KV_HEADS), 1)


def attend_kernel(
    first_ref, q_ref, kv_ref, pos_ref, tag_ref, out_ref, log_ref, max_ref, sum_ref, acc_ref, kept
):
    blocks = kv_ref.shape[0] // BLOCK
    keep = kept.shape[0] == blocks

    def scores(group, at, rows, bias):
        keys = kv_ref[rows, columns_of(group, 0)]
        return dot(keys, of_group(q_ref, group, at)) + bias

    def query_block(qb, carry):
        at = pl.ds(pl.multiple_of(qb * BLOCK, BLOCK), BLOCK)
        max_ref[...] = jnp.full(max_ref.shape, negative, jnp.float32)
        sum_ref[...] = jnp.zeros(sum_ref.shape, jnp.float32)
        acc_ref[...] = jnp.zeros(acc_ref.shape, jnp.float32)
        limit = first_ref[blocks + qb]

        def find(kb, carry):
            @pl.when(first_ref[kb] <= limit)
            def _():
                rows = pl.ds(pl.multiple_of(kb * BLOCK, BLOCK), BLOCK)
                bias = mask_bias(tag_ref[kb], pos_ref[:, at])
                for group in range(KV_HEADS):
                    found = scores(group, at, rows, bias)
                    if keep:
                        kept[kb, group] = found
                    tops = jnp.max(found.reshape(BLOCK // 8, 8, LANES), 0)
                    max_ref[group] = jnp.maximum(max_ref[group], tops)

            return carry

        lax.fori_loop(0, blocks, find, 0)
        for group in range(KV_HEADS):
            top = jnp.max(max_ref[group], 0, keepdims=True)
            max_ref[group] = jnp.broadcast_to(top, max_ref.shape[1:])

        def gather(kb, carry):
            @pl.when(first_ref[kb] <= limit)
            def _():
                rows = pl.ds(pl.multiple_of(kb * BLOCK, BLOCK), BLOCK)
                bias = None if keep else mask_bias(tag_ref[kb], pos_ref[:, at])
                for group in range(KV_HEADS):
                    found = kept[kb, group] if keep else scores(group, at, rows, bias)
                    weights = jnp.exp(found - max_ref[group, :1])
                    sum_ref[group] += jnp.sum(weights.reshape(BLOCK // 8, 8, LANES), 0)
                    values = kv_ref[rows, columns_of(group, 1)]
                    acc_ref[group] += dot(values, weights.astype(jnp.bfloat16), (0, 0))

            return carry

        lax.fori_loop(0, blocks, gather, 0)
        for group in range(KV_HEADS):
            total = jnp.sum(sum_ref[group], 0, keepdims=True)
            attended = acc_ref[group] / total
            logs = max_ref[group, :1] + jnp.log(total)
            for j in range(HEADS // KV_HEADS):
                head = group * (HEADS // KV_HEADS) + j
                own = slice(j * BLOCK, (j + 1) * BLOCK)
                out_ref[head * HEAD : (head + 1) * HEAD, at] = attended[:, own]
                log_ref[head : head + 1, at] = logs[:, own]
        return carry

    lax.fori_loop(0, q_ref.shape[1] // BLOCK, query_block, 0)


def kernel_params():
    return pltpu.CompilerParams(vmem_limit_bytes=VMEM_BYTES)


def attend(firsts, queries, kv, query_pos, key_tags):
    blocks = kv.shape[0] // BLOCK
    slots = queries.shape[1]
    kept = blocks if blocks <= 16 else 1
    groups = (KV_HEADS, 8, LANES)
    work = 4 * kv.shape[0] * slots * HEADS * HEAD
    return pl.pallas_call(
        attend_kernel,
        out_shape=(
            jax.ShapeDtypeStruct(queries.shape, jnp.float32),
            jax.ShapeDtypeStruct((HEADS + 1, slots), jnp.float32),
        ),
        in_specs=[pl.BlockSpec(memory_space=pltpu.SMEM)] + in_vmem(4),
        out_specs=tuple(in_vmem(2)),
        scratch_shapes=[
            pltpu.VMEM(groups, jnp.float32),
            pltpu.VMEM(groups, jnp.float32),
            pltpu.VMEM((KV_HEADS, HEAD, LANES), jnp.float32),
            pltpu.VMEM((kept, KV_HEADS, BLOCK, LANES), jnp.float32),
        ],
        compiler_params=kernel_params(),
        cost_estimate=pl.CostEstimate(
            flops=work * 8, bytes_accessed=kv.size * 2, transcendentals=work // 256
        ),
    )(firsts, queries, kv, query_pos[None], key_tags.reshape(-1, 1, BLOCK))


def attend_back_kernel(
    first_ref, q_ref, kv_ref, pos_ref, tag_ref, grad_ref, log_ref, delta_ref, *refs
):
    blocks = kv_ref.shape[0] // BLOCK
    cos_ref, sin_ref, out_ref, dkv_ref, acc, dq_ref = refs
    dq_ref[...] = jnp.zeros(dq_ref.shape, dq_ref.dtype)

    def key_block(kb, carry):
        rows = pl.ds(pl.multiple_of(kb * BLOCK, BLOCK), BLOCK)
        acc[...] = jnp.zeros(acc.shape, jnp.float32)

        def query_block(qb, carry):
            @pl.when(first_ref[kb] <= first_ref[blocks + qb])
            def _():
                at = pl.ds(pl.multiple_of(qb * BLOCK, BLOCK), BLOCK)
                bias = mask_bias(tag_ref[kb], pos_ref[:, at])
                for group in range(KV_HEADS):
                    keys = kv_ref[rows, columns_of(group, 0)]
                    values = kv_ref[rows, columns_of(group, 1)]
                    queries = of_group(q_ref, group, at)
                    grads = of_group(grad_ref, group, at)
                    found = dot(keys, queries) + bias
                    probs = jnp.exp(found - of_rows(log_ref, group, at))
                    grad_probs = dot(values, grads)
                    grad_scores = probs * (grad_probs - of_rows(delta_ref, group, at))
                    grad_scores = grad_scores.astype(jnp.bfloat16)
                    acc[group] += dot(grad_scores, queries, (1, 1))
                    acc[KV_HEADS + group] += dot(probs.astype(jnp.bfloat16), grads, (1, 1))
                    grad_q = 0.125 * dot(keys, grad_scores, (0, 0))
                    for j in range(HEADS // KV_HEADS):
                        head = group * (HEADS // KV_HEADS) + j
                        own = slice(head * HEAD, (head + 1) * HEAD)
                        dq_ref[own, at] += grad_q[:, j * BLOCK : (j + 1) * BLOCK]

            return carry

        lax.fori_loop(0, q_ref.shape[1] // BLOCK, query_block, 0)
        dkv_ref[rows, :] = jnp.concatenate(
            [acc[index] for index in range(2 * KV_HEADS)], 1
        ).astype(dkv_ref.dtype)
        return carry

    lax.fori_loop(0, blocks, key_block, 0)
    half_dim = HEAD // 2

    def finish(qb, carry):
        at = pl.ds(pl.multiple_of(qb * BLOCK, BLOCK), BLOCK)
        cos_tab, sin_tab = cos_ref[:, at], sin_ref[:, at]
        for head in range(0, HEADS, 2):
            pair = []
            for start in range(head * HEAD, min(head + 2, HEADS) * HEAD, HEAD):
                low = dq_ref[start : start + half_dim, at]
                high = dq_ref[start + half_dim : start + HEAD, at]
                pair += [low * cos_tab + high * sin_tab, high * cos_tab - low * sin_tab]
            if len(pair) == 2:
                pair += [jnp.zeros_like(part) for part in pair]
            turned = jnp.concatenate(pair, 0).T
            own = slice(head * HEAD, head * HEAD + turned.shape[1])
            out_ref[at, own] = turned.astype(out_ref.dtype)
        return carry

    lax.fori_loop(0, q_ref.shape[1] // BLOCK, finish, 0)


def attend_back(firsts, queries, kv, query_pos, key_tags, grads, log_total, row_delta, tables):
    slots = queries.shape[1]
    work = 10 * kv.shape[0] * slots * HEADS * HEAD
    return pl.pallas_call(
        attend_back_kernel,
        out_shape=(
            jax.ShapeDtypeStruct((slots, -(-HEADS // 2) * 2 * HEAD), jnp.bfloat16),
            jax.ShapeDtypeStruct(kv.shape, jnp.bfloat16),
        ),
        in_specs=[pl.BlockSpec(memory_space=pltpu.SMEM)] + in_vmem(9),
        out_specs=tuple(in_vmem(2)),
        scratch_shapes=[
            pltpu.VMEM((2 * KV_HEADS, BLOCK, HEAD), jnp.float32),
            pltpu.VMEM(queries.shape, jnp.float32),
        ],
        compiler_params=kernel_params(),
        cost_estimate=pl.CostEstimate(
            flops=work * 6, bytes_accessed=kv.size * 4, transcendentals=work // 640
        ),
    )(firsts, queries, kv, query_pos[None], key_tags.reshape(-1, 1, BLOCK), grads, log_total, row_delta, *tables)


def on_device(
    tokens,
    w_query,
    w_key,
    w_value,
    w_out,
    w_gate,
    w_up,
    w_down,
    gain_attn,
    gain_ffn,
    router,
    cotangent,
    positions,
    lengths,
    chosen,
):
    hidden = tokens[0].astype(jnp.float32)
    row_count, width = hidden.shape
    qdim = HEADS * HEAD
    kdim = KV_HEADS * HEAD
    query_pos = positions[0]
    live = query_pos < lengths[0]
    selected = live & (chosen[0] == 1)
    live_mask = live.astype(jnp.float32)[:, None]
    chosen_mask = selected.astype(jnp.float32)[:, None]
    cos_tab, sin_tab = rope_tables(query_pos)
    key_tags = jnp.where(selected, query_pos, -query_pos - 1)
    depth = lax.axis_size("fsdp")
    own_rows = w_query.shape[0]
    w_out_full = lax.all_gather(w_out, "fsdp", axis=0, tiled=True)
    vectors = jnp.stack([gain_attn, gain_ffn, router], 1)
    own_attn = [padded_to(w_query, 1), jnp.concatenate([w_key, w_value, vectors], 1)]
    gathered = gather_rows([padded_to(own, 0) for own in own_attn], depth)
    padded_rows = gathered[0].shape[1]
    w_query = gathered[0].reshape(depth * padded_rows, -1)
    gathered = gathered[1][:, :own_rows].reshape(width, -1)
    w_kv, vectors = gathered[:, : 2 * kdim], gathered[:, 2 * kdim :]
    gain_one, gain_two, router_vec = vectors.T.astype(jnp.float32)
    gating = jax.nn.sigmoid(jnp.sum(hidden * router_vec, -1, keepdims=True))
    grad_y = cotangent[0].astype(jnp.float32) * live_mask
    grad_inc = grad_y * chosen_mask * gating
    grad_ffn = grad_inc.astype(jnp.bfloat16)
    grad_ffn_all = lax.all_gather(grad_ffn, "fsdp", axis=0, tiled=True)

    normed_one, inv_one = norm_forward(hidden, gain_one)
    normed_one = normed_one.astype(jnp.bfloat16)
    spread_one = padded_to(normed_one.reshape(row_count, depth, own_rows), -1)
    spread_one = spread_one.reshape(row_count, -1)
    query_raw = dot(w_query, spread_one, (0, 1))[:qdim]
    queries = rotate_columns(query_raw, cos_tab, sin_tab).astype(jnp.bfloat16) * 0.125
    kv_raw = dot(normed_one, w_kv)
    kv_own = jnp.concatenate([rotate(kv_raw[:, :kdim], cos_tab, sin_tab), kv_raw[:, kdim:]], 1)
    kv_all, tags_all = gather_plane(kv_own.astype(jnp.bfloat16), key_tags)
    first_tags = tags_all[::BLOCK]
    firsts = jnp.concatenate(
        [jnp.where(first_tags >= 0, first_tags, -first_tags - 1), query_pos[BLOCK - 1 :: BLOCK]]
    )
    attended, log_total = attend(firsts, queries, kv_all, query_pos, tags_all)
    attended, w_out_full = lax.optimization_barrier((attended, w_out_full))
    outcome = attended.astype(jnp.bfloat16)
    branch = dot(outcome, w_out_full, (0, 0))
    branch, grad_ffn_all = lax.optimization_barrier((branch, grad_ffn_all))
    middle = hidden + branch
    normed_two, inv_two = norm_forward(middle, gain_two)
    normed_two = normed_two.astype(jnp.bfloat16)
    normed_all = lax.all_gather(normed_two, "fsdp", axis=0, tiled=True)
    inner_act, grad_gate_act, grad_up_act, grad_normed_part = ffn_both(
        normed_all, grad_ffn_all, w_gate, w_up, w_down
    )
    grad_normed_two = lax.psum_scatter(
        grad_normed_part, "fsdp", scatter_dimension=0, tiled=True
    ).astype(jnp.float32)
    ffn_part = jnp.dot(inner_act, w_down, preferred_element_type=jnp.float32).astype(jnp.bfloat16)
    grad_wgate = lax.dot_general(
        grad_gate_act, normed_all, across_rows, preferred_element_type=jnp.float32
    )
    grad_wup = lax.dot_general(
        grad_up_act, normed_all, across_rows, preferred_element_type=jnp.float32
    )
    grad_wdown = lax.dot_general(
        inner_act, grad_ffn_all, across_rows, preferred_element_type=jnp.float32
    )
    low = jnp.bfloat16
    spread_out = padded_to(outcome.reshape(depth, own_rows, row_count), 1)
    grads = [grad.astype(low) for grad in (grad_wgate, grad_wup, grad_wdown)]
    grad_normed_two, ffn_part, spread_out, *grads = lax.optimization_barrier(
        (grad_normed_two, ffn_part, spread_out, *grads)
    )
    grad_normed_two, row_dot = grad_normed_two[:, :width], grad_normed_two[:, width:]
    totals = tuple(lax.psum(grad, "ctx") for grad in grads)
    grad_middle, grad_gain_two = norm_backward(middle, inv_two, gain_two, grad_normed_two)
    grad_branch = (grad_inc + grad_middle).astype(jnp.bfloat16)
    grad_attended = dot(w_out_full, grad_branch, (1, 1)).astype(jnp.bfloat16)
    grad_wout = dot(spread_out.reshape(-1, row_count), padded_to(grad_branch, 1)).astype(low)
    row_delta = jnp.sum(
        (grad_attended.astype(jnp.float32) * attended).reshape(HEADS, HEAD, row_count), 1
    )
    row_delta = jnp.pad(row_delta, ((0, 1), (0, 0)))
    grad_query_raw, grad_kv_all = attend_back(
        firsts,
        queries,
        kv_all,
        query_pos,
        tags_all,
        grad_attended,
        log_total,
        row_delta,
        (cos_tab.T, sin_tab.T),
    )
    grad_kv_raw = scatter_plane(grad_kv_all, cos_tab, sin_tab)
    grad_logit = (jnp.sum(grad_inc * branch, -1, keepdims=True) + row_dot) * (1.0 - gating)
    grad_router = jnp.sum(hidden * grad_logit, 0)
    grad_normed_one = dot(grad_query_raw, w_query, (1, 1)).reshape(row_count, depth, -1)
    grad_normed_one = grad_normed_one[..., :own_rows].reshape(row_count, width)
    grad_normed_one = grad_normed_one + dot(grad_kv_raw, w_kv, (1, 1))
    grad_wq = dot(spread_one, grad_query_raw, (0, 0)).astype(low)
    grad_wkv = dot(spread_one, grad_kv_raw, (0, 0)).astype(low)
    grad_hidden_one, grad_gain_one = norm_backward(hidden, inv_one, gain_one, grad_normed_one)
    grad_tokens = (grad_y + grad_logit * router_vec + grad_middle + grad_hidden_one).astype(
        jnp.bfloat16
    )
    vectors = jnp.stack([grad_gain_one, grad_gain_two, grad_router]).reshape(3, depth, own_rows)
    vectors = jnp.pad(vectors.transpose(1, 0, 2).reshape(depth, -1), ((0, 0), (0, -3 * own_rows % 1024)))
    vectors = jnp.pad(vectors.reshape(depth, -1, 1, 128), ((0, 0), (0, 0), (0, 7), (0, 0)))
    layered = [grad.reshape(depth, padded_rows, -1) for grad in (grad_wout, grad_wq, grad_wkv)]
    layered.append(vectors.reshape(depth, -1, 128))
    owned = reduce_rows(layered, 4)
    ffn_out = lax.psum_scatter(ffn_part, "fsdp", scatter_dimension=0, tiled=True)
    *owned, totals = lax.optimization_barrier((*owned, totals))
    total_out, total_q, total_kv = (own[:own_rows].astype(jnp.float32) for own in owned[:3])
    total_q, total_out = total_q[:, :qdim], total_out[:, :width]
    total_k, total_v = total_kv[:, :kdim], total_kv[:, kdim:]
    mine = owned[3].reshape(-1, 8, 128)[:, 0].reshape(-1)[: 3 * own_rows].reshape(3, own_rows)
    totals = [total.astype(jnp.float32) for total in totals]
    ffn_out, *totals = lax.optimization_barrier((ffn_out, *totals))
    total_gate, total_up, total_down = totals
    increment = branch + ffn_out.astype(jnp.float32)
    block_out = live_mask * (hidden + chosen_mask * gating * increment)
    return (
        block_out.astype(jnp.bfloat16)[None],
        grad_tokens[None],
        total_q,
        total_k,
        total_v,
        total_out,
        total_gate,
        total_up,
        total_down,
        mine[0],
        mine[1],
        mine[2],
    )


def solution(mesh):
    in_specs = (
        P("fsdp", "ctx", None),
        P("fsdp", None),
        P("fsdp", None),
        P("fsdp", None),
        P("fsdp", None),
        P("fsdp", None),
        P("fsdp", None),
        P("fsdp", None),
        P("fsdp"),
        P("fsdp"),
        P("fsdp"),
        P("fsdp", "ctx", None),
        P("fsdp", "ctx"),
        P("fsdp"),
        P("fsdp", "ctx"),
    )
    out_specs = (
        P("fsdp", "ctx", None),
        P("fsdp", "ctx", None),
        P("fsdp", None),
        P("fsdp", None),
        P("fsdp", None),
        P("fsdp", None),
        P("fsdp", None),
        P("fsdp", None),
        P("fsdp", None),
        P("fsdp"),
        P("fsdp"),
        P("fsdp"),
    )
    return jax.shard_map(
        on_device, mesh=mesh, in_specs=in_specs, out_specs=out_specs, check_vma=False
    )
```

```python
import functools

import jax
import jax.numpy as jnp
from jax import lax
from jax.experimental import pallas as pl
from jax.experimental.pallas import tpu as pltpu
from jax.sharding import PartitionSpec as P

HEADS = 15
KV_HEADS = 5
HEAD = 64


epsilon = 1e-05
negative = -1e30
across_rows = (((0,), (0,)), ((), ()))
across_cols = (((1,), (1,)), ((), ()))


def rope_tables(positions):
    half_dim = HEAD // 2
    frequency = 10000.0 ** (-2.0 * jnp.arange(half_dim, dtype=jnp.float32) / HEAD)
    angles = positions.astype(jnp.float32)[:, None] * frequency[None, :]
    return (jnp.cos(angles), jnp.sin(angles))


def rotate(values, cos_tab, sin_tab):
    slots, width = values.shape
    low, high = jnp.split(values.reshape(slots, width // HEAD, HEAD), 2, -1)
    cos_tab, sin_tab = cos_tab[:, None], sin_tab[:, None]
    turned = [low * cos_tab - high * sin_tab, high * cos_tab + low * sin_tab]
    return jnp.concatenate(turned, -1).reshape(slots, width)


def rotate_columns(values, cos_tab, sin_tab):
    width, slots = values.shape
    low, high = jnp.split(values.reshape(width // HEAD, HEAD, slots), 2, 1)
    cos_tab, sin_tab = cos_tab.T[None], sin_tab.T[None]
    turned = [low * cos_tab - high * sin_tab, high * cos_tab + low * sin_tab]
    return jnp.concatenate(turned, 1).reshape(width, slots)


def norm_forward(values, gain_vec):
    inv_rms = lax.rsqrt(jnp.mean(values * values, -1, keepdims=True) + epsilon)
    return (values * inv_rms * gain_vec, inv_rms)


def norm_backward(values, inv_rms, gain_vec, grad_normed):
    weighted = gain_vec * grad_normed
    grad_gain = jnp.sum(grad_normed * values * inv_rms, 0)
    cubed = inv_rms * inv_rms * inv_rms
    grad_values = inv_rms * weighted - values * cubed * jnp.mean(
        weighted * values, -1, keepdims=True
    )
    return (grad_values, grad_gain)


def padded_to(values, row_dim):
    pads = [(0, 0)] * values.ndim
    pads[row_dim] = (0, -values.shape[row_dim] % 128)
    return jnp.pad(values, pads)


def ffn_both(normed, grad_mixed, gate_rows, up_rows, down_rows):
    gate_proj = lax.dot_general(normed, gate_rows, across_cols, preferred_element_type=jnp.float32)
    up_proj = lax.dot_general(normed, up_rows, across_cols, preferred_element_type=jnp.float32)
    sigma = jax.nn.sigmoid(gate_proj)
    activated = gate_proj * sigma
    inner_act = (activated * up_proj).astype(jnp.bfloat16)
    grad_inner = lax.dot_general(
        grad_mixed, down_rows, across_cols, preferred_element_type=jnp.float32
    )
    grad_gate_act = (grad_inner * up_proj * sigma * (1.0 + gate_proj * (1.0 - sigma))).astype(
        jnp.bfloat16
    )
    grad_up_act = (grad_inner * activated).astype(jnp.bfloat16)
    grad_normed = jnp.dot(grad_gate_act, gate_rows, preferred_element_type=jnp.float32) + jnp.dot(
        grad_up_act, up_rows, preferred_element_type=jnp.float32
    )
    row_dot = jnp.sum(inner_act.astype(jnp.float32) * grad_inner, -1, keepdims=True)
    grad_normed = jnp.concatenate([grad_normed, row_dot], 1).astype(jnp.bfloat16)
    return (inner_act, grad_gate_act, grad_up_act, grad_normed)


CHIPS = 4
SPAN = 2 * CHIPS
VMEM_BYTES = 60 * 1024 * 1024
MESH = pl.DeviceIdType.MESH


def plane_of():
    me = lax.axis_index("ctx")
    core = lax.rem(me, 2)
    chip = me // 2
    return me, core, chip, me + 1 - 2 * core


def chip_at(chip, core, step):
    return 2 * lax.rem(chip + step + CHIPS, CHIPS) + core


def greet(devices):
    barrier = pltpu.get_barrier_semaphore()
    for device in devices:
        pl.semaphore_signal(barrier, inc=1, device_id=device, device_id_type=MESH)
    pl.semaphore_wait(barrier, len(devices))


def send(src, dst, send_sem, recv_sem, device):
    copy = pltpu.make_async_remote_copy(
        src_ref=src,
        dst_ref=dst,
        send_sem=send_sem,
        recv_sem=recv_sem,
        device_id=device,
        device_id_type=MESH,
    )
    copy.start()
    return copy


def comm_params(number):
    return pltpu.CompilerParams(
        collective_id=number, has_side_effects=True, vmem_limit_bytes=VMEM_BYTES
    )


def comm_cost(moved):
    return pl.CostEstimate(flops=0, bytes_accessed=moved * 30, transcendentals=0)


def in_vmem(count):
    return [pl.BlockSpec(memory_space=pltpu.VMEM)] * count


def gather_rows_kernel(depth, count, *refs):
    owns, outs = refs[:count], refs[count : 2 * count]
    z_sems, p_sems, f_sems = refs[2 * count :]
    me, core, chip, partner = plane_of()
    layer = lax.axis_index("fsdp")
    layers = [lax.rem(layer + d, depth) for d in range(1, depth)]
    peers = [chip_at(chip, core, j) for j in range(1, CHIPS)]
    greet([(me, other) for other in layers] + [(peer, layer) for peer in peers + [partner]])
    first, spread, passed = [], [], []
    for a, (own, out) in enumerate(zip(owns, outs)):
        for d, other in enumerate(layers):
            first.append(
                send(
                    own.at[me],
                    out.at[layer, me],
                    z_sems.at[0, a, d],
                    z_sems.at[1, a, d],
                    (me, other),
                )
            )
    for own, out in zip(owns, outs):
        for piece in range(SPAN):
            out[layer, piece] = own[piece]
    for a, out in enumerate(outs):
        for d in range(depth - 1):
            first[a * (depth - 1) + d].wait_recv()
            block = out.at[lax.rem(layer + depth - d - 1, depth), me]
            for j, peer in enumerate(peers):
                spread.append(
                    send(block, block, p_sems.at[0, a, d, j], p_sems.at[1, a, d, j], (peer, layer))
                )
            passed.append(
                send(block, block, f_sems.at[0, a, d, 3], f_sems.at[1, a, d, 3], (partner, layer))
            )
    arrivals = iter(spread)
    for a, out in enumerate(outs):
        for d in range(depth - 1):
            source = lax.rem(layer + depth - d - 1, depth)
            for j in range(CHIPS - 1):
                next(arrivals).wait_recv()
                block = out.at[source, chip_at(chip, core, -j - 1)]
                passed.append(
                    send(
                        block,
                        block,
                        f_sems.at[0, a, d, j],
                        f_sems.at[1, a, d, j],
                        (partner, layer),
                    )
                )
    for copy in first + spread:
        copy.wait_send()
    for copy in passed:
        copy.wait()


def gather_rows(arrays, depth):
    if lax.axis_size("ctx") != SPAN:
        return [lax.all_gather(own, "fsdp", axis=0) for own in arrays]
    count, pieces, outs = len(arrays), [], []
    for own in arrays:
        piece = (own.shape[0] // SPAN, own.shape[1])
        pieces.append(own.reshape(SPAN, *piece))
        outs.append(jax.ShapeDtypeStruct((depth, SPAN, *piece), own.dtype))
    whole = pl.pallas_call(
        functools.partial(gather_rows_kernel, depth, count),
        out_shape=tuple(outs),
        in_specs=in_vmem(count),
        out_specs=tuple(in_vmem(count)),
        scratch_shapes=[
            pltpu.SemaphoreType.DMA((2, count, depth - 1)),
            pltpu.SemaphoreType.DMA((2, count, depth - 1, CHIPS - 1)),
            pltpu.SemaphoreType.DMA((2, count, depth - 1, CHIPS)),
        ],
        compiler_params=comm_params(1),
        cost_estimate=comm_cost(sum(own.size for own in arrays) * 2 * depth),
    )(*pieces)
    return [full.reshape(depth, *own.shape) for full, own in zip(whole, arrays)]


def gather_plane_kernel(kv_ref, tag_ref, kv_out, tag_out, p_sems, f_sems):
    me, core, chip, partner = plane_of()
    layer = lax.axis_index("fsdp")
    peers = [chip_at(chip, core, j) for j in range(1, CHIPS)]
    greet([(peer, layer) for peer in peers + [partner]])
    pairs = ((kv_ref, kv_out), (tag_ref, tag_out))
    spread, passed = [], []
    for j, peer in enumerate(peers):
        for a, (own, out) in enumerate(pairs):
            spread.append(
                send(own, out.at[me], p_sems.at[0, a, j], p_sems.at[1, a, j], (peer, layer))
            )
    for a, (own, out) in enumerate(pairs):
        passed.append(
            send(own, out.at[me], f_sems.at[0, a, 3], f_sems.at[1, a, 3], (partner, layer))
        )
    kv_out[me] = kv_ref[...]
    tag_out[me] = tag_ref[...]
    for j in range(CHIPS - 1):
        for a, (own, out) in enumerate(pairs):
            spread[2 * j + a].wait_recv()
            block = out.at[chip_at(chip, core, -j - 1)]
            passed.append(
                send(block, block, f_sems.at[0, a, j], f_sems.at[1, a, j], (partner, layer))
            )
    for copy in spread:
        copy.wait_send()
    for copy in passed:
        copy.wait()


def gather_plane(kv, tags):
    if lax.axis_size("ctx") != SPAN:
        return tuple(lax.all_gather(part, "ctx", axis=0, tiled=True) for part in (kv, tags))
    rows, columns = kv.shape
    kv_all, tags_all = pl.pallas_call(
        gather_plane_kernel,
        out_shape=(
            jax.ShapeDtypeStruct((SPAN, rows, columns), kv.dtype),
            jax.ShapeDtypeStruct((SPAN, 1, rows), tags.dtype),
        ),
        in_specs=in_vmem(2),
        out_specs=tuple(in_vmem(2)),
        scratch_shapes=[
            pltpu.SemaphoreType.DMA((2, 2, CHIPS - 1)),
            pltpu.SemaphoreType.DMA((2, 2, CHIPS)),
        ],
        compiler_params=comm_params(2),
        cost_estimate=comm_cost(kv.size * 2 * SPAN),
    )(kv, tags[None])
    return kv_all.reshape(SPAN * rows, columns), tags_all.reshape(SPAN * rows)


def added(*parts):
    total = parts[0].astype(jnp.float32)
    for part in parts[1:]:
        total = total + part.astype(jnp.float32)
    return total


def across_of(chip, core, way):
    along_x, along_y = lax.rem(chip, 2), chip // 2
    along_x = 1 - along_x if way % 2 else along_x
    along_y = 1 - along_y if way // 2 else along_y
    return 2 * (2 * along_y + along_x) + core


def reduce_plane(arrays, h_sems, p_sems):
    me, core, chip, partner = plane_of()
    layer = lax.axis_index("fsdp")
    ways = (3, 1, 2, 0)
    near = (across_of(chip, core, 1), across_of(chip, core, 2))
    handed, started = [], []
    for a, (piece_of, halves, sums, arrived) in enumerate(arrays):
        for way in ways:
            handed.append(
                send(
                    piece_of(across_of(chip, 1 - core, way)),
                    halves.at[way],
                    h_sems.at[0, a, way],
                    h_sems.at[1, a, way],
                    (partner, layer),
                )
            )
    for a, (piece_of, halves, sums, arrived) in enumerate(arrays):
        middle = sums.shape[1] // 2
        sides = (pl.ds(0, middle), pl.ds(middle, middle))
        copies = {}

        def pass_on(way, side, slot, hop, a=a, sums=sums, arrived=arrived, sides=sides):
            number = 2 * slot + side
            return send(
                sums.at[way, sides[side]],
                arrived.at[slot, sides[side]],
                p_sems.at[0, a, number],
                p_sems.at[1, a, number],
                (near[hop], layer),
            )

        for j, way in enumerate(ways):
            handed[a * CHIPS + j].wait_recv()
            mine = piece_of(across_of(chip, core, way))

            def add_half(slab, carry, mine=mine, halves=halves, sums=sums, way=way):
                sums[way, slab] = added(mine[slab], halves[way, slab]).astype(sums.dtype)
                return carry

            lax.fori_loop(0, sums.shape[1], add_half, 0)
            if way == 3:
                for side in range(2):
                    copies[0, side] = pass_on(3, side, 0, side)
            elif way:
                copies[1, way - 1] = pass_on(way, way - 1, 1, way - 1)
        started.append((copies, pass_on))

    def second_hop(a):
        (copies, pass_on), (_, _, sums, arrived) = started[a], arrays[a]
        middle = sums.shape[1] // 2
        for side in range(2):
            copies[0, side].wait_recv()
            way = 2 - side

            def add_opposite(slab, carry, way=way, sums=sums, arrived=arrived):
                total = added(sums[way, slab], arrived[0, slab])
                sums[way, slab] = total.astype(sums.dtype)
                return carry

            lax.fori_loop(side * middle, (side + 1) * middle, add_opposite, 0)
            copies[2, side] = pass_on(way, side, 2, 1 - side)
        handed.extend(copies.values())
        return [copies[slot, side] for slot in (1, 2) for side in range(2)]

    return handed, second_hop


def plane_total(sums, arrived, slab):
    return added(sums[0, slab], arrived[1, slab], arrived[2, slab])


def plane_scratch(block, dtype):
    return [
        pltpu.VMEM((CHIPS, *block), dtype),
        pltpu.VMEM((CHIPS, *block), dtype),
        pltpu.VMEM((CHIPS - 1, *block), dtype),
    ]


def turned_back(values, cos_tab, sin_tab):
    half_dim, parts = HEAD // 2, []
    for start in range(0, values.shape[1], HEAD):
        low = values[:, start : start + half_dim]
        high = values[:, start + half_dim : start + HEAD]
        parts += [low * cos_tab + high * sin_tab, high * cos_tab - low * sin_tab]
    return jnp.concatenate(parts, 1)


def scatter_plane_kernel(x_ref, cos_ref, sin_ref, out_ref, halves, sums, arrived, h_sems, p_sems):
    me, core, chip, partner = plane_of()
    layer = lax.axis_index("fsdp")
    near = [across_of(chip, core, way) for way in (1, 2)]
    greet([(peer, layer) for peer in near + [partner]])
    arrays = [(lambda piece: x_ref.at[piece], halves, sums, arrived)]
    started, second_hop = reduce_plane(arrays, h_sems, p_sems)
    for copy in second_hop(0):
        copy.wait_recv()

    def add_slab(slab, carry):
        total = plane_total(sums, arrived, slab)
        kdim = KV_HEADS * HEAD
        keys = turned_back(total[:, :kdim], cos_ref[slab], sin_ref[slab])
        out_ref[slab] = jnp.concatenate([keys, total[:, kdim:]], 1).astype(out_ref.dtype)
        return carry

    lax.fori_loop(0, x_ref.shape[1], add_slab, 0)
    for copy in started:
        copy.wait_send()


def scatter_plane(values, cos_tab, sin_tab):
    if lax.axis_size("ctx") != SPAN:
        own = lax.psum_scatter(values, "ctx", scatter_dimension=0, tiled=True)
        own, kdim = own.astype(jnp.float32), KV_HEADS * HEAD
        keys = turned_back(own[:, :kdim], cos_tab, sin_tab)
        return jnp.concatenate([keys, own[:, kdim:]], 1).astype(values.dtype)
    rows, columns = values.shape
    slabs = 8
    block = (slabs, rows // SPAN // slabs, columns)
    return pl.pallas_call(
        scatter_plane_kernel,
        out_shape=jax.ShapeDtypeStruct(block, values.dtype),
        in_specs=in_vmem(3),
        out_specs=in_vmem(1)[0],
        scratch_shapes=plane_scratch(block, values.dtype)
        + [pltpu.SemaphoreType.DMA((2, 1, CHIPS)), pltpu.SemaphoreType.DMA((2, 1, 6))],
        compiler_params=comm_params(3),
        cost_estimate=comm_cost(values.size * 2),
    )(
        values.reshape(SPAN, *block),
        cos_tab.reshape(*block[:2], -1),
        sin_tab.reshape(*block[:2], -1),
    ).reshape(rows // SPAN, columns)


def reduce_rows_kernel(depth, count, *refs):
    inputs, outs, scratch = refs[:count], refs[count : 2 * count], refs[2 * count : 6 * count]
    h_sems, p_sems, z_sems, g_sems, f_sems = refs[6 * count :]
    me, core, chip, partner = plane_of()
    layer = lax.axis_index("fsdp")
    layers = [lax.rem(layer + d, depth) for d in range(1, depth)]
    peers = [chip_at(chip, core, j) for j in range(1, CHIPS)]
    greet([(me, other) for other in layers] + [(peer, layer) for peer in peers + [partner]])
    arrays, across = [], []
    for a, x_ref in enumerate(inputs):
        halves, sums, arrived, layers_ref = scratch[4 * a : 4 * a + 4]
        arrays.append((lambda piece, x_ref=x_ref: x_ref.at[:, piece], halves, sums, arrived))
        across.append(layers_ref)
    started, second_hop = reduce_plane(arrays, h_sems, p_sems)
    last, moved, given, passed = [], [], [], []

    def over_layers(a):
        _, _, sums, arrived = arrays[a]
        for copy in last[a]:
            copy.wait_recv()
        for d in list(range(1, depth)) + [0]:
            target = lax.rem(layer + d, depth)
            across[a][0, d] = plane_total(sums, arrived, target).astype(across[a].dtype)
            if d:
                moved.append(
                    send(
                        across[a].at[0, d],
                        across[a].at[1, d],
                        z_sems.at[0, a, d - 1],
                        z_sems.at[1, a, d - 1],
                        (me, target),
                    )
                )

    def hand_out(a):
        out_ref = outs[a]
        for copy in moved[a * (depth - 1) : (a + 1) * (depth - 1)]:
            copy.wait_recv()
        parts = [across[a][0, 0]] + [across[a][1, d] for d in range(1, depth)]
        out_ref[me] = added(*parts).astype(out_ref.dtype)
        mine = out_ref.at[me]
        for j, peer in enumerate(peers):
            given.append(send(mine, mine, g_sems.at[0, a, j], g_sems.at[1, a, j], (peer, layer)))
        passed.append(send(mine, mine, f_sems.at[0, a, 3], f_sems.at[1, a, 3], (partner, layer)))

    for step in range(count + 2):
        if step < count:
            last.append(second_hop(step))
        if 0 < step <= count:
            over_layers(step - 1)
        if step > 1:
            hand_out(step - 2)
    for a, out_ref in enumerate(outs):
        for j in range(CHIPS - 1):
            given[a * (CHIPS - 1) + j].wait_recv()
            block = out_ref.at[chip_at(chip, core, -j - 1)]
            passed.append(
                send(block, block, f_sems.at[0, a, j], f_sems.at[1, a, j], (partner, layer))
            )
    for copy in started + moved + given:
        copy.wait_send()
    for copy in passed:
        copy.wait()


def reduce_rows(arrays, number):
    if lax.axis_size("ctx") != SPAN:
        return [lax.psum(lax.psum_scatter(v, "fsdp", scatter_dimension=0), "ctx") for v in arrays]
    depth, count = arrays[0].shape[0], len(arrays)
    pieces, outs, scratch = [], [], []
    for values in arrays:
        _, rows, columns = values.shape
        piece = (rows // SPAN, columns)
        pieces.append(values.reshape(depth, SPAN, *piece))
        outs.append(jax.ShapeDtypeStruct((SPAN, *piece), values.dtype))
        scratch += plane_scratch((depth, *piece), values.dtype)
        scratch.append(pltpu.VMEM((2, depth, *piece), values.dtype))
    owned = pl.pallas_call(
        functools.partial(reduce_rows_kernel, depth, count),
        out_shape=tuple(outs),
        in_specs=in_vmem(count),
        out_specs=tuple(in_vmem(count)),
        scratch_shapes=scratch
        + [
            pltpu.SemaphoreType.DMA((2, count, CHIPS)),
            pltpu.SemaphoreType.DMA((2, count, 6)),
            pltpu.SemaphoreType.DMA((2, count, depth - 1)),
            pltpu.SemaphoreType.DMA((2, count, CHIPS - 1)),
            pltpu.SemaphoreType.DMA((2, count, CHIPS)),
        ],
        compiler_params=comm_params(number),
        cost_estimate=comm_cost(sum(values.size for values in arrays) * 2),
    )(*pieces)
    return [own.reshape(values.shape[1:]) for own, values in zip(owned, arrays)]


BLOCK = 128
LANES = (HEADS // KV_HEADS) * BLOCK


def dot(left, right, dims=(1, 0)):
    return lax.dot_general(
        left, right, (((dims[0],), (dims[1],)), ((), ())), preferred_element_type=jnp.float32
    )


def of_group(ref, group, at):
    first = group * (HEADS // KV_HEADS)
    heads = range(first, first + HEADS // KV_HEADS)
    return jnp.concatenate([ref[head * HEAD : (head + 1) * HEAD, at] for head in heads], 1)


def of_rows(ref, group, at):
    first = group * (HEADS // KV_HEADS)
    heads = range(first, first + HEADS // KV_HEADS)
    return jnp.concatenate([ref[head : head + 1, at] for head in heads], 1)


def columns_of(group, part):
    start = (part * KV_HEADS + group) * HEAD
    return slice(start, start + HEAD)


def mask_bias(tags, query_pos):
    tags = jnp.broadcast_to(tags, (BLOCK, BLOCK)).T
    key_pos = jnp.where(tags >= 0, tags, -tags - 1)
    allowed = (key_pos <= query_pos) & ((tags >= 0) | (key_pos == query_pos))
    bias = jnp.where(allowed, 0.0, negative)
    return jnp.concatenate([bias] * (HEADS // KV_HEADS), 1)


def attend_kernel(
    first_ref, q_ref, kv_ref, pos_ref, tag_ref, out_ref, log_ref, max_ref, sum_ref, acc_ref, kept
):
    blocks = kv_ref.shape[0] // BLOCK
    keep = kept.shape[0] == blocks

    def scores(group, at, rows, bias):
        keys = kv_ref[rows, columns_of(group, 0)]
        return dot(keys, of_group(q_ref, group, at)) + bias

    def query_block(qb, carry):
        at = pl.ds(pl.multiple_of(qb * BLOCK, BLOCK), BLOCK)
        max_ref[...] = jnp.full(max_ref.shape, negative, jnp.float32)
        sum_ref[...] = jnp.zeros(sum_ref.shape, jnp.float32)
        acc_ref[...] = jnp.zeros(acc_ref.shape, jnp.float32)
        limit = first_ref[blocks + qb]

        def find(kb, carry):
            @pl.when(first_ref[kb] <= limit)
            def _():
                rows = pl.ds(pl.multiple_of(kb * BLOCK, BLOCK), BLOCK)
                bias = mask_bias(tag_ref[kb], pos_ref[:, at])
                for group in range(KV_HEADS):
                    found = scores(group, at, rows, bias)
                    if keep:
                        kept[kb, group] = found
                    tops = jnp.max(found.reshape(BLOCK // 8, 8, LANES), 0)
                    max_ref[group] = jnp.maximum(max_ref[group], tops)

            return carry

        lax.fori_loop(0, blocks, find, 0)
        for group in range(KV_HEADS):
            top = jnp.max(max_ref[group], 0, keepdims=True)
            max_ref[group] = jnp.broadcast_to(top, max_ref.shape[1:])

        def gather(kb, carry):
            @pl.when(first_ref[kb] <= limit)
            def _():
                rows = pl.ds(pl.multiple_of(kb * BLOCK, BLOCK), BLOCK)
                bias = None if keep else mask_bias(tag_ref[kb], pos_ref[:, at])
                for group in range(KV_HEADS):
                    found = kept[kb, group] if keep else scores(group, at, rows, bias)
                    weights = jnp.exp(found - max_ref[group, :1])
                    sum_ref[group] += jnp.sum(weights.reshape(BLOCK // 8, 8, LANES), 0)
                    values = kv_ref[rows, columns_of(group, 1)]
                    acc_ref[group] += dot(values, weights.astype(jnp.bfloat16), (0, 0))

            return carry

        lax.fori_loop(0, blocks, gather, 0)
        for group in range(KV_HEADS):
            total = jnp.sum(sum_ref[group], 0, keepdims=True)
            attended = acc_ref[group] / total
            logs = max_ref[group, :1] + jnp.log(total)
            for j in range(HEADS // KV_HEADS):
                head = group * (HEADS // KV_HEADS) + j
                own = slice(j * BLOCK, (j + 1) * BLOCK)
                out_ref[head * HEAD : (head + 1) * HEAD, at] = attended[:, own]
                log_ref[head : head + 1, at] = logs[:, own]
        return carry

    lax.fori_loop(0, q_ref.shape[1] // BLOCK, query_block, 0)


def kernel_params():
    return pltpu.CompilerParams(vmem_limit_bytes=VMEM_BYTES)


def attend(firsts, queries, kv, query_pos, key_tags):
    blocks = kv.shape[0] // BLOCK
    slots = queries.shape[1]
    kept = blocks if blocks <= 16 else 1
    groups = (KV_HEADS, 8, LANES)
    work = 4 * kv.shape[0] * slots * HEADS * HEAD
    return pl.pallas_call(
        attend_kernel,
        out_shape=(
            jax.ShapeDtypeStruct(queries.shape, jnp.float32),
            jax.ShapeDtypeStruct((HEADS + 1, slots), jnp.float32),
        ),
        in_specs=[pl.BlockSpec(memory_space=pltpu.SMEM)] + in_vmem(4),
        out_specs=tuple(in_vmem(2)),
        scratch_shapes=[
            pltpu.VMEM(groups, jnp.float32),
            pltpu.VMEM(groups, jnp.float32),
            pltpu.VMEM((KV_HEADS, HEAD, LANES), jnp.float32),
            pltpu.VMEM((kept, KV_HEADS, BLOCK, LANES), jnp.float32),
        ],
        compiler_params=kernel_params(),
        cost_estimate=pl.CostEstimate(
            flops=work * 8, bytes_accessed=kv.size * 2, transcendentals=work // 256
        ),
    )(firsts, queries, kv, query_pos[None], key_tags.reshape(-1, 1, BLOCK))


def attend_back_kernel(
    first_ref, q_ref, kv_ref, pos_ref, tag_ref, grad_ref, log_ref, delta_ref, *refs
):
    blocks = kv_ref.shape[0] // BLOCK
    cos_ref, sin_ref, out_ref, dkv_ref, acc, dq_ref = refs
    dq_ref[...] = jnp.zeros(dq_ref.shape, dq_ref.dtype)

    def key_block(kb, carry):
        rows = pl.ds(pl.multiple_of(kb * BLOCK, BLOCK), BLOCK)
        acc[...] = jnp.zeros(acc.shape, jnp.float32)

        def query_block(qb, carry):
            @pl.when(first_ref[kb] <= first_ref[blocks + qb])
            def _():
                at = pl.ds(pl.multiple_of(qb * BLOCK, BLOCK), BLOCK)
                bias = mask_bias(tag_ref[kb], pos_ref[:, at])
                for group in range(KV_HEADS):
                    keys = kv_ref[rows, columns_of(group, 0)]
                    values = kv_ref[rows, columns_of(group, 1)]
                    queries = of_group(q_ref, group, at)
                    grads = of_group(grad_ref, group, at)
                    found = dot(keys, queries) + bias
                    probs = jnp.exp(found - of_rows(log_ref, group, at))
                    grad_probs = dot(values, grads)
                    grad_scores = probs * (grad_probs - of_rows(delta_ref, group, at))
                    grad_scores = grad_scores.astype(jnp.bfloat16)
                    acc[group] += dot(grad_scores, queries, (1, 1))
                    acc[KV_HEADS + group] += dot(probs.astype(jnp.bfloat16), grads, (1, 1))
                    grad_q = 0.125 * dot(keys, grad_scores, (0, 0))
                    for j in range(HEADS // KV_HEADS):
                        head = group * (HEADS // KV_HEADS) + j
                        own = slice(head * HEAD, (head + 1) * HEAD)
                        dq_ref[own, at] += grad_q[:, j * BLOCK : (j + 1) * BLOCK]

            return carry

        lax.fori_loop(0, q_ref.shape[1] // BLOCK, query_block, 0)
        dkv_ref[rows, :] = jnp.concatenate(
            [acc[index] for index in range(2 * KV_HEADS)], 1
        ).astype(dkv_ref.dtype)
        return carry

    lax.fori_loop(0, blocks, key_block, 0)
    half_dim = HEAD // 2

    def finish(qb, carry):
        at = pl.ds(pl.multiple_of(qb * BLOCK, BLOCK), BLOCK)
        cos_tab, sin_tab = cos_ref[:, at], sin_ref[:, at]
        for head in range(0, HEADS, 2):
            pair = []
            for start in range(head * HEAD, min(head + 2, HEADS) * HEAD, HEAD):
                low = dq_ref[start : start + half_dim, at]
                high = dq_ref[start + half_dim : start + HEAD, at]
                pair += [low * cos_tab + high * sin_tab, high * cos_tab - low * sin_tab]
            if len(pair) == 2:
                pair += [jnp.zeros_like(part) for part in pair]
            turned = jnp.concatenate(pair, 0).T
            own = slice(head * HEAD, head * HEAD + turned.shape[1])
            out_ref[at, own] = turned.astype(out_ref.dtype)
        return carry

    lax.fori_loop(0, q_ref.shape[1] // BLOCK, finish, 0)


def attend_back(firsts, queries, kv, query_pos, key_tags, grads, log_total, row_delta, tables):
    slots = queries.shape[1]
    work = 10 * kv.shape[0] * slots * HEADS * HEAD
    return pl.pallas_call(
        attend_back_kernel,
        out_shape=(
            jax.ShapeDtypeStruct((slots, -(-HEADS // 2) * 2 * HEAD), jnp.bfloat16),
            jax.ShapeDtypeStruct(kv.shape, jnp.bfloat16),
        ),
        in_specs=[pl.BlockSpec(memory_space=pltpu.SMEM)] + in_vmem(9),
        out_specs=tuple(in_vmem(2)),
        scratch_shapes=[
            pltpu.VMEM((2 * KV_HEADS, BLOCK, HEAD), jnp.float32),
            pltpu.VMEM(queries.shape, jnp.float32),
        ],
        compiler_params=kernel_params(),
        cost_estimate=pl.CostEstimate(
            flops=work * 6, bytes_accessed=kv.size * 4, transcendentals=work // 640
        ),
    )(firsts, queries, kv, query_pos[None], key_tags.reshape(-1, 1, BLOCK), grads, log_total, row_delta, *tables)


def on_device(
    tokens,
    w_query,
    w_key,
    w_value,
    w_out,
    w_gate,
    w_up,
    w_down,
    gain_attn,
    gain_ffn,
    router,
    cotangent,
    positions,
    lengths,
    chosen,
):
    hidden = tokens[0].astype(jnp.float32)
    row_count, width = hidden.shape
    qdim = HEADS * HEAD
    kdim = KV_HEADS * HEAD
    query_pos = positions[0]
    live = query_pos < lengths[0]
    selected = live & (chosen[0] == 1)
    live_mask = live.astype(jnp.float32)[:, None]
    chosen_mask = selected.astype(jnp.float32)[:, None]
    cos_tab, sin_tab = rope_tables(query_pos)
    key_tags = jnp.where(selected, query_pos, -query_pos - 1)
    depth = lax.axis_size("fsdp")
    own_rows = w_query.shape[0]
    w_out_full = lax.all_gather(w_out, "fsdp", axis=0, tiled=True)
    vectors = jnp.stack([gain_attn, gain_ffn, router], 1)
    own_attn = [padded_to(w_query, 1), jnp.concatenate([w_key, w_value, vectors], 1)]
    gathered = gather_rows([padded_to(own, 0) for own in own_attn], depth)
    padded_rows = gathered[0].shape[1]
    w_query = gathered[0].reshape(depth * padded_rows, -1)
    gathered = gathered[1][:, :own_rows].reshape(width, -1)
    w_kv, vectors = gathered[:, : 2 * kdim], gathered[:, 2 * kdim :]
    gain_one, gain_two, router_vec = vectors.T.astype(jnp.float32)
    gating = jax.nn.sigmoid(jnp.sum(hidden * router_vec, -1, keepdims=True))
    grad_y = cotangent[0].astype(jnp.float32) * live_mask
    grad_inc = grad_y * chosen_mask * gating
    grad_ffn = grad_inc.astype(jnp.bfloat16)
    grad_ffn_all = lax.all_gather(grad_ffn, "fsdp", axis=0, tiled=True)

    normed_one, inv_one = norm_forward(hidden, gain_one)
    normed_one = normed_one.astype(jnp.bfloat16)
    spread_one = padded_to(normed_one.reshape(row_count, depth, own_rows), -1)
    spread_one = spread_one.reshape(row_count, -1)
    query_raw = dot(w_query, spread_one, (0, 1))[:qdim]
    queries = rotate_columns(query_raw, cos_tab, sin_tab).astype(jnp.bfloat16) * 0.125
    kv_raw = dot(normed_one, w_kv)
    kv_own = jnp.concatenate([rotate(kv_raw[:, :kdim], cos_tab, sin_tab), kv_raw[:, kdim:]], 1)
    kv_all, tags_all = gather_plane(kv_own.astype(jnp.bfloat16), key_tags)
    first_tags = tags_all[::BLOCK]
    firsts = jnp.concatenate(
        [jnp.where(first_tags >= 0, first_tags, -first_tags - 1), query_pos[BLOCK - 1 :: BLOCK]]
    )
    attended, log_total = attend(firsts, queries, kv_all, query_pos, tags_all)
    attended, w_out_full = lax.optimization_barrier((attended, w_out_full))
    outcome = attended.astype(jnp.bfloat16)
    branch = dot(outcome, w_out_full, (0, 0))
    branch, grad_ffn_all = lax.optimization_barrier((branch, grad_ffn_all))
    middle = hidden + branch
    normed_two, inv_two = norm_forward(middle, gain_two)
    normed_two = normed_two.astype(jnp.bfloat16)
    normed_all = lax.all_gather(normed_two, "fsdp", axis=0, tiled=True)
    inner_act, grad_gate_act, grad_up_act, grad_normed_part = ffn_both(
        normed_all, grad_ffn_all, w_gate, w_up, w_down
    )
    grad_normed_two = lax.psum_scatter(
        grad_normed_part, "fsdp", scatter_dimension=0, tiled=True
    ).astype(jnp.float32)
    ffn_part = jnp.dot(inner_act, w_down, preferred_element_type=jnp.float32).astype(jnp.bfloat16)
    grad_wgate = lax.dot_general(
        grad_gate_act, normed_all, across_rows, preferred_element_type=jnp.float32
    )
    grad_wup = lax.dot_general(
        grad_up_act, normed_all, across_rows, preferred_element_type=jnp.float32
    )
    grad_wdown = lax.dot_general(
        inner_act, grad_ffn_all, across_rows, preferred_element_type=jnp.float32
    )
    low = jnp.bfloat16
    spread_out = padded_to(outcome.reshape(depth, own_rows, row_count), 1)
    grads = [grad.astype(low) for grad in (grad_wgate, grad_wup, grad_wdown)]
    grad_normed_two, ffn_part, spread_out, *grads = lax.optimization_barrier(
        (grad_normed_two, ffn_part, spread_out, *grads)
    )
    grad_normed_two, row_dot = grad_normed_two[:, :width], grad_normed_two[:, width:]
    totals = tuple(lax.psum(grad, "ctx") for grad in grads)
    grad_middle, grad_gain_two = norm_backward(middle, inv_two, gain_two, grad_normed_two)
    grad_branch = (grad_inc + grad_middle).astype(jnp.bfloat16)
    grad_attended = dot(w_out_full, grad_branch, (1, 1)).astype(jnp.bfloat16)
    grad_wout = dot(spread_out.reshape(-1, row_count), padded_to(grad_branch, 1)).astype(low)
    row_delta = jnp.sum(
        (grad_attended.astype(jnp.float32) * attended).reshape(HEADS, HEAD, row_count), 1
    )
    row_delta = jnp.pad(row_delta, ((0, 1), (0, 0)))
    grad_query_raw, grad_kv_all = attend_back(
        firsts,
        queries,
        kv_all,
        query_pos,
        tags_all,
        grad_attended,
        log_total,
        row_delta,
        (cos_tab.T, sin_tab.T),
    )
    grad_kv_raw = scatter_plane(grad_kv_all, cos_tab, sin_tab)
    grad_logit = (jnp.sum(grad_inc * branch, -1, keepdims=True) + row_dot) * (1.0 - gating)
    grad_router = jnp.sum(hidden * grad_logit, 0)
    grad_normed_one = dot(grad_query_raw, w_query, (1, 1)).reshape(row_count, depth, -1)
    grad_normed_one = grad_normed_one[..., :own_rows].reshape(row_count, width)
    grad_normed_one = grad_normed_one + dot(grad_kv_raw, w_kv, (1, 1))
    grad_wq = dot(spread_one, grad_query_raw, (0, 0)).astype(low)
    grad_wkv = dot(spread_one, grad_kv_raw, (0, 0)).astype(low)
    grad_hidden_one, grad_gain_one = norm_backward(hidden, inv_one, gain_one, grad_normed_one)
    grad_tokens = (grad_y + grad_logit * router_vec + grad_middle + grad_hidden_one).astype(
        jnp.bfloat16
    )
    vectors = jnp.stack([grad_gain_one, grad_gain_two, grad_router]).reshape(3, depth, own_rows)
    vectors = jnp.pad(vectors.transpose(1, 0, 2).reshape(depth, -1), ((0, 0), (0, -3 * own_rows % 1024)))
    vectors = jnp.pad(vectors.reshape(depth, -1, 1, 128), ((0, 0), (0, 0), (0, 7), (0, 0)))
    layered = [grad.reshape(depth, padded_rows, -1) for grad in (grad_wout, grad_wq, grad_wkv)]
    layered.insert(0, vectors.reshape(depth, -1, 128))
    owned = reduce_rows(layered, 4)
    ffn_out = lax.psum_scatter(ffn_part, "fsdp", scatter_dimension=0, tiled=True)
    *owned, totals = lax.optimization_barrier((*owned, totals))
    total_out, total_q, total_kv = (own[:own_rows].astype(jnp.float32) for own in owned[1:])
    total_q, total_out = total_q[:, :qdim], total_out[:, :width]
    total_k, total_v = total_kv[:, :kdim], total_kv[:, kdim:]
    mine = owned[0].reshape(-1, 8, 128)[:, 0].reshape(-1)[: 3 * own_rows].reshape(3, own_rows)
    totals = [total.astype(jnp.float32) for total in totals]
    ffn_out, *totals = lax.optimization_barrier((ffn_out, *totals))
    total_gate, total_up, total_down = totals
    increment = branch + ffn_out.astype(jnp.float32)
    block_out = live_mask * (hidden + chosen_mask * gating * increment)
    return (
        block_out.astype(jnp.bfloat16)[None],
        grad_tokens[None],
        total_q,
        total_k,
        total_v,
        total_out,
        total_gate,
        total_up,
        total_down,
        mine[0],
        mine[1],
        mine[2],
    )


def solution(mesh):
    in_specs = (
        P("fsdp", "ctx", None),
        P("fsdp", None),
        P("fsdp", None),
        P("fsdp", None),
        P("fsdp", None),
        P("fsdp", None),
        P("fsdp", None),
        P("fsdp", None),
        P("fsdp"),
        P("fsdp"),
        P("fsdp"),
        P("fsdp", "ctx", None),
        P("fsdp", "ctx"),
        P("fsdp"),
        P("fsdp", "ctx"),
    )
    out_specs = (
        P("fsdp", "ctx", None),
        P("fsdp", "ctx", None),
        P("fsdp", None),
        P("fsdp", None),
        P("fsdp", None),
        P("fsdp", None),
        P("fsdp", None),
        P("fsdp", None),
        P("fsdp", None),
        P("fsdp"),
        P("fsdp"),
        P("fsdp"),
    )
    return jax.shard_map(
        on_device, mesh=mesh, in_specs=in_specs, out_specs=out_specs, check_vma=False
    )
```

```python
import functools

import jax
import jax.numpy as jnp
from jax import lax
from jax.experimental import pallas as pl
from jax.experimental.pallas import tpu as pltpu
from jax.sharding import PartitionSpec as P

HEADS = 15
KV_HEADS = 5
HEAD = 64


epsilon = 1e-05
negative = -1e30
across_rows = (((0,), (0,)), ((), ()))
across_cols = (((1,), (1,)), ((), ()))


def rope_tables(positions):
    half_dim = HEAD // 2
    frequency = 10000.0 ** (-2.0 * jnp.arange(half_dim, dtype=jnp.float32) / HEAD)
    angles = positions.astype(jnp.float32)[:, None] * frequency[None, :]
    return (jnp.cos(angles), jnp.sin(angles))


def rotate(values, cos_tab, sin_tab):
    slots, width = values.shape
    low, high = jnp.split(values.reshape(slots, width // HEAD, HEAD), 2, -1)
    cos_tab, sin_tab = cos_tab[:, None], sin_tab[:, None]
    turned = [low * cos_tab - high * sin_tab, high * cos_tab + low * sin_tab]
    return jnp.concatenate(turned, -1).reshape(slots, width)


def rotate_columns(values, cos_tab, sin_tab):
    width, slots = values.shape
    low, high = jnp.split(values.reshape(width // HEAD, HEAD, slots), 2, 1)
    cos_tab, sin_tab = cos_tab.T[None], sin_tab.T[None]
    turned = [low * cos_tab - high * sin_tab, high * cos_tab + low * sin_tab]
    return jnp.concatenate(turned, 1).reshape(width, slots)


def norm_forward(values, gain_vec):
    inv_rms = lax.rsqrt(jnp.mean(values * values, -1, keepdims=True) + epsilon)
    return (values * inv_rms * gain_vec, inv_rms)


def norm_backward(values, inv_rms, gain_vec, grad_normed):
    weighted = gain_vec * grad_normed
    grad_gain = jnp.sum(grad_normed * values * inv_rms, 0)
    cubed = inv_rms * inv_rms * inv_rms
    grad_values = inv_rms * weighted - values * cubed * jnp.mean(
        weighted * values, -1, keepdims=True
    )
    return (grad_values, grad_gain)


def padded_to(values, row_dim):
    pads = [(0, 0)] * values.ndim
    pads[row_dim] = (0, -values.shape[row_dim] % 128)
    return jnp.pad(values, pads)


def ffn_both(normed, grad_mixed, gate_rows, up_rows, down_rows):
    gate_proj = lax.dot_general(normed, gate_rows, across_cols, preferred_element_type=jnp.float32)
    up_proj = lax.dot_general(normed, up_rows, across_cols, preferred_element_type=jnp.float32)
    sigma = jax.nn.sigmoid(gate_proj)
    activated = gate_proj * sigma
    inner_act = (activated * up_proj).astype(jnp.bfloat16)
    grad_inner = lax.dot_general(
        grad_mixed, down_rows, across_cols, preferred_element_type=jnp.float32
    )
    grad_gate_act = (grad_inner * up_proj * sigma * (1.0 + gate_proj * (1.0 - sigma))).astype(
        jnp.bfloat16
    )
    grad_up_act = (grad_inner * activated).astype(jnp.bfloat16)
    grad_normed = jnp.dot(grad_gate_act, gate_rows, preferred_element_type=jnp.float32) + jnp.dot(
        grad_up_act, up_rows, preferred_element_type=jnp.float32
    )
    row_dot = jnp.sum(inner_act.astype(jnp.float32) * grad_inner, -1, keepdims=True)
    grad_normed = jnp.concatenate([grad_normed, row_dot], 1).astype(jnp.bfloat16)
    return (inner_act, grad_gate_act, grad_up_act, grad_normed)


CHIPS = 4
SPAN = 2 * CHIPS
VMEM_BYTES = 60 * 1024 * 1024
MESH = pl.DeviceIdType.MESH


def plane_of():
    me = lax.axis_index("ctx")
    core = lax.rem(me, 2)
    chip = me // 2
    return me, core, chip, me + 1 - 2 * core


def chip_at(chip, core, step):
    return 2 * lax.rem(chip + step + CHIPS, CHIPS) + core


def greet(devices):
    barrier = pltpu.get_barrier_semaphore()
    for device in devices:
        pl.semaphore_signal(barrier, inc=1, device_id=device, device_id_type=MESH)
    pl.semaphore_wait(barrier, len(devices))


def send(src, dst, send_sem, recv_sem, device):
    copy = pltpu.make_async_remote_copy(
        src_ref=src,
        dst_ref=dst,
        send_sem=send_sem,
        recv_sem=recv_sem,
        device_id=device,
        device_id_type=MESH,
    )
    copy.start()
    return copy


def comm_params(number):
    return pltpu.CompilerParams(
        collective_id=number, has_side_effects=True, vmem_limit_bytes=VMEM_BYTES
    )


def comm_cost(moved):
    return pl.CostEstimate(flops=0, bytes_accessed=moved * 30, transcendentals=0)


def in_vmem(count):
    return [pl.BlockSpec(memory_space=pltpu.VMEM)] * count


def gather_rows_kernel(depth, count, *refs):
    owns, outs = refs[:count], refs[count : 2 * count]
    z_sems, p_sems, f_sems = refs[2 * count :]
    me, core, chip, partner = plane_of()
    layer = lax.axis_index("fsdp")
    layers = [lax.rem(layer + d, depth) for d in range(1, depth)]
    peers = [chip_at(chip, core, j) for j in range(1, CHIPS)]
    greet([(me, other) for other in layers] + [(peer, layer) for peer in peers + [partner]])
    first, spread, passed = [], [], []
    for a, (own, out) in enumerate(zip(owns, outs)):
        for d, other in enumerate(layers):
            first.append(
                send(
                    own.at[me],
                    out.at[layer, me],
                    z_sems.at[0, a, d],
                    z_sems.at[1, a, d],
                    (me, other),
                )
            )
    for own, out in zip(owns, outs):
        for piece in range(SPAN):
            out[layer, piece] = own[piece]
    for a, out in enumerate(outs):
        for d in range(depth - 1):
            first[a * (depth - 1) + d].wait_recv()
            block = out.at[lax.rem(layer + depth - d - 1, depth), me]
            for j, peer in enumerate(peers):
                spread.append(
                    send(block, block, p_sems.at[0, a, d, j], p_sems.at[1, a, d, j], (peer, layer))
                )
            passed.append(
                send(block, block, f_sems.at[0, a, d, 3], f_sems.at[1, a, d, 3], (partner, layer))
            )
    arrivals = iter(spread)
    for a, out in enumerate(outs):
        for d in range(depth - 1):
            source = lax.rem(layer + depth - d - 1, depth)
            for j in range(CHIPS - 1):
                next(arrivals).wait_recv()
                block = out.at[source, chip_at(chip, core, -j - 1)]
                passed.append(
                    send(
                        block,
                        block,
                        f_sems.at[0, a, d, j],
                        f_sems.at[1, a, d, j],
                        (partner, layer),
                    )
                )
    for copy in first + spread:
        copy.wait_send()
    for copy in passed:
        copy.wait()


def gather_rows(arrays, depth):
    if lax.axis_size("ctx") != SPAN:
        return [lax.all_gather(own, "fsdp", axis=0) for own in arrays]
    count, pieces, outs = len(arrays), [], []
    for own in arrays:
        piece = (own.shape[0] // SPAN, own.shape[1])
        pieces.append(own.reshape(SPAN, *piece))
        outs.append(jax.ShapeDtypeStruct((depth, SPAN, *piece), own.dtype))
    whole = pl.pallas_call(
        functools.partial(gather_rows_kernel, depth, count),
        out_shape=tuple(outs),
        in_specs=in_vmem(count),
        out_specs=tuple(in_vmem(count)),
        scratch_shapes=[
            pltpu.SemaphoreType.DMA((2, count, depth - 1)),
            pltpu.SemaphoreType.DMA((2, count, depth - 1, CHIPS - 1)),
            pltpu.SemaphoreType.DMA((2, count, depth - 1, CHIPS)),
        ],
        compiler_params=comm_params(1),
        cost_estimate=comm_cost(sum(own.size for own in arrays) * 2 * depth),
    )(*pieces)
    return [full.reshape(depth, *own.shape) for full, own in zip(whole, arrays)]


def gather_plane_kernel(kv_ref, tag_ref, kv_out, tag_out, p_sems, f_sems):
    me, core, chip, partner = plane_of()
    layer = lax.axis_index("fsdp")
    peers = [chip_at(chip, core, j) for j in range(1, CHIPS)]
    greet([(peer, layer) for peer in peers + [partner]])
    pairs = ((kv_ref, kv_out), (tag_ref, tag_out))
    spread, passed = [], []
    for j, peer in enumerate(peers):
        for a, (own, out) in enumerate(pairs):
            spread.append(
                send(own, out.at[me], p_sems.at[0, a, j], p_sems.at[1, a, j], (peer, layer))
            )
    for a, (own, out) in enumerate(pairs):
        passed.append(
            send(own, out.at[me], f_sems.at[0, a, 3], f_sems.at[1, a, 3], (partner, layer))
        )
    kv_out[me] = kv_ref[...]
    tag_out[me] = tag_ref[...]
    for j in range(CHIPS - 1):
        for a, (own, out) in enumerate(pairs):
            spread[2 * j + a].wait_recv()
            block = out.at[chip_at(chip, core, -j - 1)]
            passed.append(
                send(block, block, f_sems.at[0, a, j], f_sems.at[1, a, j], (partner, layer))
            )
    for copy in spread:
        copy.wait_send()
    for copy in passed:
        copy.wait()


def gather_plane(kv, tags):
    if lax.axis_size("ctx") != SPAN:
        return tuple(lax.all_gather(part, "ctx", axis=0, tiled=True) for part in (kv, tags))
    rows, columns = kv.shape
    kv_all, tags_all = pl.pallas_call(
        gather_plane_kernel,
        out_shape=(
            jax.ShapeDtypeStruct((SPAN, rows, columns), kv.dtype),
            jax.ShapeDtypeStruct((SPAN, 1, rows), tags.dtype),
        ),
        in_specs=in_vmem(2),
        out_specs=tuple(in_vmem(2)),
        scratch_shapes=[
            pltpu.SemaphoreType.DMA((2, 2, CHIPS - 1)),
            pltpu.SemaphoreType.DMA((2, 2, CHIPS)),
        ],
        compiler_params=comm_params(2),
        cost_estimate=comm_cost(kv.size * 2 * SPAN),
    )(kv, tags[None])
    return kv_all.reshape(SPAN * rows, columns), tags_all.reshape(SPAN * rows)


def added(*parts):
    total = parts[0].astype(jnp.float32)
    for part in parts[1:]:
        total = total + part.astype(jnp.float32)
    return total


def across_of(chip, core, way):
    along_x, along_y = lax.rem(chip, 2), chip // 2
    along_x = 1 - along_x if way % 2 else along_x
    along_y = 1 - along_y if way // 2 else along_y
    return 2 * (2 * along_y + along_x) + core


def reduce_plane(arrays, h_sems, p_sems):
    me, core, chip, partner = plane_of()
    layer = lax.axis_index("fsdp")
    ways = (3, 1, 2, 0)
    near = (across_of(chip, core, 1), across_of(chip, core, 2))
    handed, started = [], []
    for a, (piece_of, halves, sums, arrived) in enumerate(arrays):
        for way in ways:
            handed.append(
                send(
                    piece_of(across_of(chip, 1 - core, way)),
                    halves.at[way],
                    h_sems.at[0, a, way],
                    h_sems.at[1, a, way],
                    (partner, layer),
                )
            )
    for a, (piece_of, halves, sums, arrived) in enumerate(arrays):
        middle = sums.shape[1] // 2
        sides = (pl.ds(0, middle), pl.ds(middle, middle))
        copies = {}

        def pass_on(way, side, slot, hop, a=a, sums=sums, arrived=arrived, sides=sides):
            number = 2 * slot + side
            return send(
                sums.at[way, sides[side]],
                arrived.at[slot, sides[side]],
                p_sems.at[0, a, number],
                p_sems.at[1, a, number],
                (near[hop], layer),
            )

        for j, way in enumerate(ways):
            handed[a * CHIPS + j].wait_recv()
            mine = piece_of(across_of(chip, core, way))

            def add_half(slab, carry, mine=mine, halves=halves, sums=sums, way=way):
                sums[way, slab] = added(mine[slab], halves[way, slab]).astype(sums.dtype)
                return carry

            lax.fori_loop(0, sums.shape[1], add_half, 0)
            if way == 3:
                for side in range(2):
                    copies[0, side] = pass_on(3, side, 0, side)
            elif way:
                copies[1, way - 1] = pass_on(way, way - 1, 1, way - 1)
        started.append((copies, pass_on))

    def second_hop(a):
        (copies, pass_on), (_, _, sums, arrived) = started[a], arrays[a]
        middle = sums.shape[1] // 2
        for side in range(2):
            copies[0, side].wait_recv()
            way = 2 - side

            def add_opposite(slab, carry, way=way, sums=sums, arrived=arrived):
                total = added(sums[way, slab], arrived[0, slab])
                sums[way, slab] = total.astype(sums.dtype)
                return carry

            lax.fori_loop(side * middle, (side + 1) * middle, add_opposite, 0)
            copies[2, side] = pass_on(way, side, 2, 1 - side)
        handed.extend(copies.values())
        return [copies[slot, side] for slot in (1, 2) for side in range(2)]

    return handed, second_hop


def plane_total(sums, arrived, slab):
    return added(sums[0, slab], arrived[1, slab], arrived[2, slab])


def plane_scratch(block, dtype):
    return [
        pltpu.VMEM((CHIPS, *block), dtype),
        pltpu.VMEM((CHIPS, *block), dtype),
        pltpu.VMEM((CHIPS - 1, *block), dtype),
    ]


def turned_back(values, cos_tab, sin_tab):
    half_dim, parts = HEAD // 2, []
    for start in range(0, values.shape[1], HEAD):
        low = values[:, start : start + half_dim]
        high = values[:, start + half_dim : start + HEAD]
        parts += [low * cos_tab + high * sin_tab, high * cos_tab - low * sin_tab]
    return jnp.concatenate(parts, 1)


def reduce_rows_kernel(depth, count, extra, *refs):
    sizes = (count, 3 * extra, count, extra, 4 * count, 3 * extra, 5)
    ends = [sum(sizes[: index + 1]) for index in range(len(sizes))]
    inputs, kv_in, outs, kv_out, scratch, kv_scratch, sems = (
        refs[end - size : end] for size, end in zip(sizes, ends)
    )
    h_sems, p_sems, z_sems, g_sems, f_sems = sems
    me, core, chip, partner = plane_of()
    layer = lax.axis_index("fsdp")
    layers = [lax.rem(layer + d, depth) for d in range(1, depth)]
    peers = [chip_at(chip, core, j) for j in range(1, CHIPS)]
    greet([(me, other) for other in layers] + [(peer, layer) for peer in peers + [partner]])
    arrays, across = [], []
    if extra:
        arrays.append((lambda piece: kv_in[0].at[piece], *kv_scratch))
    for a, x_ref in enumerate(inputs):
        halves, sums, arrived, layers_ref = scratch[4 * a : 4 * a + 4]
        arrays.append((lambda piece, x_ref=x_ref: x_ref.at[:, piece], halves, sums, arrived))
        across.append(layers_ref)
    started, second_hop = reduce_plane(arrays, h_sems, p_sems)
    last, moved, given, passed = [], [], [], []

    def finish_kv():
        _, _, sums, arrived = arrays[0]
        for copy in last[0]:
            copy.wait_recv()

        def add_slab(slab, carry):
            total = plane_total(sums, arrived, slab)
            kdim = KV_HEADS * HEAD
            keys = turned_back(total[:, :kdim], kv_in[1][slab], kv_in[2][slab])
            both = jnp.concatenate([keys, total[:, kdim:]], 1)
            kv_out[0][slab] = both.astype(kv_out[0].dtype)
            return carry

        lax.fori_loop(0, sums.shape[1], add_slab, 0)

    def over_layers(a):
        _, _, sums, arrived = arrays[a + extra]
        for copy in last[a + extra]:
            copy.wait_recv()
        for d in list(range(1, depth)) + [0]:
            target = lax.rem(layer + d, depth)
            across[a][0, d] = plane_total(sums, arrived, target).astype(across[a].dtype)
            if d:
                moved.append(
                    send(
                        across[a].at[0, d],
                        across[a].at[1, d],
                        z_sems.at[0, a, d - 1],
                        z_sems.at[1, a, d - 1],
                        (me, target),
                    )
                )

    def hand_out(a):
        out_ref = outs[a]
        for copy in moved[a * (depth - 1) : (a + 1) * (depth - 1)]:
            copy.wait_recv()
        parts = [across[a][0, 0]] + [across[a][1, d] for d in range(1, depth)]
        out_ref[me] = added(*parts).astype(out_ref.dtype)
        mine = out_ref.at[me]
        for j, peer in enumerate(peers):
            given.append(send(mine, mine, g_sems.at[0, a, j], g_sems.at[1, a, j], (peer, layer)))
        passed.append(send(mine, mine, f_sems.at[0, a, 3], f_sems.at[1, a, 3], (partner, layer)))

    for step in range(count + extra + 2):
        if step < count + extra:
            last.append(second_hop(step))
        if 0 <= step - 1 - extra < count:
            over_layers(step - 1 - extra)
        if extra and step == 1:
            finish_kv()
        if 0 <= step - 2 - extra:
            hand_out(step - 2 - extra)
    for a, out_ref in enumerate(outs):
        for j in range(CHIPS - 1):
            given[a * (CHIPS - 1) + j].wait_recv()
            block = out_ref.at[chip_at(chip, core, -j - 1)]
            passed.append(
                send(block, block, f_sems.at[0, a, j], f_sems.at[1, a, j], (partner, layer))
            )
    for copy in started + moved + given:
        copy.wait_send()
    for copy in passed:
        copy.wait()


def reduce_rows(arrays, number, kv=None):
    if lax.axis_size("ctx") != SPAN:
        own = [lax.psum(lax.psum_scatter(v, "fsdp", scatter_dimension=0), "ctx") for v in arrays]
        if kv is None:
            return own
        total = lax.psum_scatter(kv[0], "ctx", scatter_dimension=0, tiled=True)
        total, kdim = total.astype(jnp.float32), KV_HEADS * HEAD
        keys = turned_back(total[:, :kdim], *kv[1:])
        return own + [jnp.concatenate([keys, total[:, kdim:]], 1).astype(kv[0].dtype)]
    depth, count, extra = arrays[0].shape[0], len(arrays), int(kv is not None)
    pieces, outs, scratch, shapes = [], [], [], []
    for values in arrays:
        _, rows, columns = values.shape
        piece = (rows // SPAN, columns)
        pieces.append(values.reshape(depth, SPAN, *piece))
        outs.append(jax.ShapeDtypeStruct((SPAN, *piece), values.dtype))
        scratch += plane_scratch((depth, *piece), values.dtype)
        scratch.append(pltpu.VMEM((2, depth, *piece), values.dtype))
        shapes.append(values.shape[1:])
    moved = sum(values.size for values in arrays) * 2
    if extra:
        rows, columns = kv[0].shape
        slabs = 8
        block = (slabs, rows // SPAN // slabs, columns)
        pieces.append(kv[0].reshape(SPAN, *block))
        pieces += [table.reshape(*block[:2], -1) for table in kv[1:]]
        outs.append(jax.ShapeDtypeStruct(block, kv[0].dtype))
        scratch += plane_scratch(block, kv[0].dtype)
        shapes.append((rows // SPAN, columns))
        moved += kv[0].size * 2
    owned = pl.pallas_call(
        functools.partial(reduce_rows_kernel, depth, count, extra),
        out_shape=tuple(outs),
        in_specs=in_vmem(len(pieces)),
        out_specs=tuple(in_vmem(len(outs))),
        scratch_shapes=scratch
        + [
            pltpu.SemaphoreType.DMA((2, count + extra, CHIPS)),
            pltpu.SemaphoreType.DMA((2, count + extra, 6)),
            pltpu.SemaphoreType.DMA((2, count, depth - 1)),
            pltpu.SemaphoreType.DMA((2, count, CHIPS - 1)),
            pltpu.SemaphoreType.DMA((2, count, CHIPS)),
        ],
        compiler_params=comm_params(number),
        cost_estimate=comm_cost(moved),
    )(*pieces)
    return [own.reshape(shape) for own, shape in zip(owned, shapes)]


BLOCK = 128
LANES = (HEADS // KV_HEADS) * BLOCK


def dot(left, right, dims=(1, 0)):
    return lax.dot_general(
        left, right, (((dims[0],), (dims[1],)), ((), ())), preferred_element_type=jnp.float32
    )


def of_group(ref, group, at):
    first = group * (HEADS // KV_HEADS)
    heads = range(first, first + HEADS // KV_HEADS)
    return jnp.concatenate([ref[head * HEAD : (head + 1) * HEAD, at] for head in heads], 1)


def of_rows(ref, group, at):
    first = group * (HEADS // KV_HEADS)
    heads = range(first, first + HEADS // KV_HEADS)
    return jnp.concatenate([ref[head : head + 1, at] for head in heads], 1)


def columns_of(group, part):
    start = (part * KV_HEADS + group) * HEAD
    return slice(start, start + HEAD)


def mask_bias(tags, query_pos):
    tags = jnp.broadcast_to(tags, (BLOCK, BLOCK)).T
    key_pos = jnp.where(tags >= 0, tags, -tags - 1)
    allowed = (key_pos <= query_pos) & ((tags >= 0) | (key_pos == query_pos))
    bias = jnp.where(allowed, 0.0, negative)
    return jnp.concatenate([bias] * (HEADS // KV_HEADS), 1)


def attend_kernel(
    first_ref, q_ref, kv_ref, pos_ref, tag_ref, out_ref, log_ref, max_ref, sum_ref, acc_ref, kept
):
    blocks = kv_ref.shape[0] // BLOCK
    keep = kept.shape[0] == blocks

    def scores(group, at, rows, bias):
        keys = kv_ref[rows, columns_of(group, 0)]
        return dot(keys, of_group(q_ref, group, at)) + bias

    def query_block(qb, carry):
        at = pl.ds(pl.multiple_of(qb * BLOCK, BLOCK), BLOCK)
        max_ref[...] = jnp.full(max_ref.shape, negative, jnp.float32)
        sum_ref[...] = jnp.zeros(sum_ref.shape, jnp.float32)
        acc_ref[...] = jnp.zeros(acc_ref.shape, jnp.float32)
        limit = first_ref[blocks + qb]

        def find(kb, carry):
            @pl.when(first_ref[kb] <= limit)
            def _():
                rows = pl.ds(pl.multiple_of(kb * BLOCK, BLOCK), BLOCK)
                bias = mask_bias(tag_ref[kb], pos_ref[:, at])
                for group in range(KV_HEADS):
                    found = scores(group, at, rows, bias)
                    if keep:
                        kept[kb, group] = found
                    tops = jnp.max(found.reshape(BLOCK // 8, 8, LANES), 0)
                    max_ref[group] = jnp.maximum(max_ref[group], tops)

            return carry

        lax.fori_loop(0, blocks, find, 0)
        for group in range(KV_HEADS):
            top = jnp.max(max_ref[group], 0, keepdims=True)
            max_ref[group] = jnp.broadcast_to(top, max_ref.shape[1:])

        def gather(kb, carry):
            @pl.when(first_ref[kb] <= limit)
            def _():
                rows = pl.ds(pl.multiple_of(kb * BLOCK, BLOCK), BLOCK)
                bias = None if keep else mask_bias(tag_ref[kb], pos_ref[:, at])
                for group in range(KV_HEADS):
                    found = kept[kb, group] if keep else scores(group, at, rows, bias)
                    weights = jnp.exp(found - max_ref[group, :1])
                    sum_ref[group] += jnp.sum(weights.reshape(BLOCK // 8, 8, LANES), 0)
                    values = kv_ref[rows, columns_of(group, 1)]
                    acc_ref[group] += dot(values, weights.astype(jnp.bfloat16), (0, 0))

            return carry

        lax.fori_loop(0, blocks, gather, 0)
        for group in range(KV_HEADS):
            total = jnp.sum(sum_ref[group], 0, keepdims=True)
            attended = acc_ref[group] / total
            logs = max_ref[group, :1] + jnp.log(total)
            for j in range(HEADS // KV_HEADS):
                head = group * (HEADS // KV_HEADS) + j
                own = slice(j * BLOCK, (j + 1) * BLOCK)
                out_ref[head * HEAD : (head + 1) * HEAD, at] = attended[:, own]
                log_ref[head : head + 1, at] = logs[:, own]
        return carry

    lax.fori_loop(0, q_ref.shape[1] // BLOCK, query_block, 0)


def kernel_params():
    return pltpu.CompilerParams(vmem_limit_bytes=VMEM_BYTES)


def attend(firsts, queries, kv, query_pos, key_tags):
    blocks = kv.shape[0] // BLOCK
    slots = queries.shape[1]
    kept = blocks if blocks <= 16 else 1
    groups = (KV_HEADS, 8, LANES)
    work = 4 * kv.shape[0] * slots * HEADS * HEAD
    return pl.pallas_call(
        attend_kernel,
        out_shape=(
            jax.ShapeDtypeStruct(queries.shape, jnp.float32),
            jax.ShapeDtypeStruct((HEADS + 1, slots), jnp.float32),
        ),
        in_specs=[pl.BlockSpec(memory_space=pltpu.SMEM)] + in_vmem(4),
        out_specs=tuple(in_vmem(2)),
        scratch_shapes=[
            pltpu.VMEM(groups, jnp.float32),
            pltpu.VMEM(groups, jnp.float32),
            pltpu.VMEM((KV_HEADS, HEAD, LANES), jnp.float32),
            pltpu.VMEM((kept, KV_HEADS, BLOCK, LANES), jnp.float32),
        ],
        compiler_params=kernel_params(),
        cost_estimate=pl.CostEstimate(
            flops=work * 8, bytes_accessed=kv.size * 2, transcendentals=work // 256
        ),
    )(firsts, queries, kv, query_pos[None], key_tags.reshape(-1, 1, BLOCK))


def attend_back_kernel(
    first_ref, q_ref, kv_ref, pos_ref, tag_ref, grad_ref, log_ref, delta_ref, *refs
):
    blocks = kv_ref.shape[0] // BLOCK
    cos_ref, sin_ref, out_ref, dkv_ref, acc, dq_ref = refs
    dq_ref[...] = jnp.zeros(dq_ref.shape, dq_ref.dtype)

    def key_block(kb, carry):
        rows = pl.ds(pl.multiple_of(kb * BLOCK, BLOCK), BLOCK)
        acc[...] = jnp.zeros(acc.shape, jnp.float32)

        def query_block(qb, carry):
            @pl.when(first_ref[kb] <= first_ref[blocks + qb])
            def _():
                at = pl.ds(pl.multiple_of(qb * BLOCK, BLOCK), BLOCK)
                bias = mask_bias(tag_ref[kb], pos_ref[:, at])
                for group in range(KV_HEADS):
                    keys = kv_ref[rows, columns_of(group, 0)]
                    values = kv_ref[rows, columns_of(group, 1)]
                    queries = of_group(q_ref, group, at)
                    grads = of_group(grad_ref, group, at)
                    found = dot(keys, queries) + bias
                    probs = jnp.exp(found - of_rows(log_ref, group, at))
                    grad_probs = dot(values, grads)
                    grad_scores = probs * (grad_probs - of_rows(delta_ref, group, at))
                    grad_scores = grad_scores.astype(jnp.bfloat16)
                    acc[group] += dot(grad_scores, queries, (1, 1))
                    acc[KV_HEADS + group] += dot(probs.astype(jnp.bfloat16), grads, (1, 1))
                    grad_q = 0.125 * dot(keys, grad_scores, (0, 0))
                    for j in range(HEADS // KV_HEADS):
                        head = group * (HEADS // KV_HEADS) + j
                        own = slice(head * HEAD, (head + 1) * HEAD)
                        dq_ref[own, at] += grad_q[:, j * BLOCK : (j + 1) * BLOCK]

            return carry

        lax.fori_loop(0, q_ref.shape[1] // BLOCK, query_block, 0)
        dkv_ref[rows, :] = jnp.concatenate(
            [acc[index] for index in range(2 * KV_HEADS)], 1
        ).astype(dkv_ref.dtype)
        return carry

    lax.fori_loop(0, blocks, key_block, 0)
    half_dim = HEAD // 2

    def finish(qb, carry):
        at = pl.ds(pl.multiple_of(qb * BLOCK, BLOCK), BLOCK)
        cos_tab, sin_tab = cos_ref[:, at], sin_ref[:, at]
        for head in range(0, HEADS, 2):
            pair = []
            for start in range(head * HEAD, min(head + 2, HEADS) * HEAD, HEAD):
                low = dq_ref[start : start + half_dim, at]
                high = dq_ref[start + half_dim : start + HEAD, at]
                pair += [low * cos_tab + high * sin_tab, high * cos_tab - low * sin_tab]
            if len(pair) == 2:
                pair += [jnp.zeros_like(part) for part in pair]
            turned = jnp.concatenate(pair, 0).T
            own = slice(head * HEAD, head * HEAD + turned.shape[1])
            out_ref[at, own] = turned.astype(out_ref.dtype)
        return carry

    lax.fori_loop(0, q_ref.shape[1] // BLOCK, finish, 0)


def attend_back(firsts, queries, kv, query_pos, key_tags, grads, log_total, row_delta, tables):
    slots = queries.shape[1]
    work = 10 * kv.shape[0] * slots * HEADS * HEAD
    return pl.pallas_call(
        attend_back_kernel,
        out_shape=(
            jax.ShapeDtypeStruct((slots, -(-HEADS // 2) * 2 * HEAD), jnp.bfloat16),
            jax.ShapeDtypeStruct(kv.shape, jnp.bfloat16),
        ),
        in_specs=[pl.BlockSpec(memory_space=pltpu.SMEM)] + in_vmem(9),
        out_specs=tuple(in_vmem(2)),
        scratch_shapes=[
            pltpu.VMEM((2 * KV_HEADS, BLOCK, HEAD), jnp.float32),
            pltpu.VMEM(queries.shape, jnp.float32),
        ],
        compiler_params=kernel_params(),
        cost_estimate=pl.CostEstimate(
            flops=work * 6, bytes_accessed=kv.size * 4, transcendentals=work // 640
        ),
    )(firsts, queries, kv, query_pos[None], key_tags.reshape(-1, 1, BLOCK), grads, log_total, row_delta, *tables)


def on_device(
    tokens,
    w_query,
    w_key,
    w_value,
    w_out,
    w_gate,
    w_up,
    w_down,
    gain_attn,
    gain_ffn,
    router,
    cotangent,
    positions,
    lengths,
    chosen,
):
    hidden = tokens[0].astype(jnp.float32)
    row_count, width = hidden.shape
    qdim = HEADS * HEAD
    kdim = KV_HEADS * HEAD
    query_pos = positions[0]
    live = query_pos < lengths[0]
    selected = live & (chosen[0] == 1)
    live_mask = live.astype(jnp.float32)[:, None]
    chosen_mask = selected.astype(jnp.float32)[:, None]
    cos_tab, sin_tab = rope_tables(query_pos)
    key_tags = jnp.where(selected, query_pos, -query_pos - 1)
    depth = lax.axis_size("fsdp")
    own_rows = w_query.shape[0]
    w_out_full = lax.all_gather(w_out, "fsdp", axis=0, tiled=True)
    vectors = jnp.stack([gain_attn, gain_ffn, router], 1)
    own_attn = [padded_to(w_query, 1), jnp.concatenate([w_key, w_value, vectors], 1)]
    gathered = gather_rows([padded_to(own, 0) for own in own_attn], depth)
    padded_rows = gathered[0].shape[1]
    w_query = gathered[0].reshape(depth * padded_rows, -1)
    gathered = gathered[1][:, :own_rows].reshape(width, -1)
    w_kv, vectors = gathered[:, : 2 * kdim], gathered[:, 2 * kdim :]
    gain_one, gain_two, router_vec = vectors.T.astype(jnp.float32)
    gating = jax.nn.sigmoid(jnp.sum(hidden * router_vec, -1, keepdims=True))
    grad_y = cotangent[0].astype(jnp.float32) * live_mask
    grad_inc = grad_y * chosen_mask * gating
    grad_ffn = grad_inc.astype(jnp.bfloat16)
    grad_ffn_all = lax.all_gather(grad_ffn, "fsdp", axis=0, tiled=True)

    normed_one, inv_one = norm_forward(hidden, gain_one)
    normed_one = normed_one.astype(jnp.bfloat16)
    spread_one = padded_to(normed_one.reshape(row_count, depth, own_rows), -1)
    spread_one = spread_one.reshape(row_count, -1)
    query_raw = dot(w_query, spread_one, (0, 1))[:qdim]
    queries = rotate_columns(query_raw, cos_tab, sin_tab).astype(jnp.bfloat16) * 0.125
    kv_raw = dot(normed_one, w_kv)
    kv_own = jnp.concatenate([rotate(kv_raw[:, :kdim], cos_tab, sin_tab), kv_raw[:, kdim:]], 1)
    kv_all, tags_all = gather_plane(kv_own.astype(jnp.bfloat16), key_tags)
    first_tags = tags_all[::BLOCK]
    firsts = jnp.concatenate(
        [jnp.where(first_tags >= 0, first_tags, -first_tags - 1), query_pos[BLOCK - 1 :: BLOCK]]
    )
    attended, log_total = attend(firsts, queries, kv_all, query_pos, tags_all)
    attended, w_out_full = lax.optimization_barrier((attended, w_out_full))
    outcome = attended.astype(jnp.bfloat16)
    branch = dot(outcome, w_out_full, (0, 0))
    branch, grad_ffn_all = lax.optimization_barrier((branch, grad_ffn_all))
    middle = hidden + branch
    normed_two, inv_two = norm_forward(middle, gain_two)
    normed_two = normed_two.astype(jnp.bfloat16)
    normed_all = lax.all_gather(normed_two, "fsdp", axis=0, tiled=True)
    inner_act, grad_gate_act, grad_up_act, grad_normed_part = ffn_both(
        normed_all, grad_ffn_all, w_gate, w_up, w_down
    )
    grad_normed_two = lax.psum_scatter(
        grad_normed_part, "fsdp", scatter_dimension=0, tiled=True
    ).astype(jnp.float32)
    ffn_part = jnp.dot(inner_act, w_down, preferred_element_type=jnp.float32).astype(jnp.bfloat16)
    grad_wgate = lax.dot_general(
        grad_gate_act, normed_all, across_rows, preferred_element_type=jnp.float32
    )
    grad_wup = lax.dot_general(
        grad_up_act, normed_all, across_rows, preferred_element_type=jnp.float32
    )
    grad_wdown = lax.dot_general(
        inner_act, grad_ffn_all, across_rows, preferred_element_type=jnp.float32
    )
    low = jnp.bfloat16
    spread_out = padded_to(outcome.reshape(depth, own_rows, row_count), 1)
    grads = [grad.astype(low) for grad in (grad_wgate, grad_wup, grad_wdown)]
    grad_normed_two, ffn_part, spread_out, *grads = lax.optimization_barrier(
        (grad_normed_two, ffn_part, spread_out, *grads)
    )
    grad_normed_two, row_dot = grad_normed_two[:, :width], grad_normed_two[:, width:]
    totals = tuple(lax.psum(grad, "ctx") for grad in grads)
    grad_middle, grad_gain_two = norm_backward(middle, inv_two, gain_two, grad_normed_two)
    grad_branch = (grad_inc + grad_middle).astype(jnp.bfloat16)
    grad_attended = dot(w_out_full, grad_branch, (1, 1)).astype(jnp.bfloat16)
    grad_wout = dot(spread_out.reshape(-1, row_count), padded_to(grad_branch, 1)).astype(low)
    row_delta = jnp.sum(
        (grad_attended.astype(jnp.float32) * attended).reshape(HEADS, HEAD, row_count), 1
    )
    row_delta = jnp.pad(row_delta, ((0, 1), (0, 0)))
    grad_query_raw, grad_kv_all = attend_back(
        firsts,
        queries,
        kv_all,
        query_pos,
        tags_all,
        grad_attended,
        log_total,
        row_delta,
        (cos_tab.T, sin_tab.T),
    )
    own_out, grad_kv_raw = reduce_rows(
        [grad_wout.reshape(depth, padded_rows, -1)], 3, (grad_kv_all, cos_tab, sin_tab)
    )
    grad_logit = (jnp.sum(grad_inc * branch, -1, keepdims=True) + row_dot) * (1.0 - gating)
    grad_router = jnp.sum(hidden * grad_logit, 0)
    grad_normed_one = dot(grad_query_raw, w_query, (1, 1)).reshape(row_count, depth, -1)
    grad_normed_one = grad_normed_one[..., :own_rows].reshape(row_count, width)
    grad_normed_one = grad_normed_one + dot(grad_kv_raw, w_kv, (1, 1))
    grad_wq = dot(spread_one, grad_query_raw, (0, 0)).astype(low)
    grad_wkv = dot(spread_one, grad_kv_raw, (0, 0)).astype(low)
    grad_hidden_one, grad_gain_one = norm_backward(hidden, inv_one, gain_one, grad_normed_one)
    grad_tokens = (grad_y + grad_logit * router_vec + grad_middle + grad_hidden_one).astype(
        jnp.bfloat16
    )
    vectors = jnp.stack([grad_gain_one, grad_gain_two, grad_router]).reshape(3, depth, own_rows)
    vectors = jnp.pad(vectors.transpose(1, 0, 2).reshape(depth, -1), ((0, 0), (0, -3 * own_rows % 1024)))
    vectors = jnp.pad(vectors.reshape(depth, -1, 1, 128), ((0, 0), (0, 0), (0, 7), (0, 0)))
    layered = [grad.reshape(depth, padded_rows, -1) for grad in (grad_wq, grad_wkv)]
    layered.insert(0, vectors.reshape(depth, -1, 128))
    owned = reduce_rows(layered, 4)
    ffn_out = lax.psum_scatter(ffn_part, "fsdp", scatter_dimension=0, tiled=True)
    *owned, totals = lax.optimization_barrier((*owned, totals))
    owned.append(own_out)
    total_q, total_kv, total_out = (own[:own_rows].astype(jnp.float32) for own in owned[1:])
    total_q, total_out = total_q[:, :qdim], total_out[:, :width]
    total_k, total_v = total_kv[:, :kdim], total_kv[:, kdim:]
    mine = owned[0].reshape(-1, 8, 128)[:, 0].reshape(-1)[: 3 * own_rows].reshape(3, own_rows)
    totals = [total.astype(jnp.float32) for total in totals]
    ffn_out, *totals = lax.optimization_barrier((ffn_out, *totals))
    total_gate, total_up, total_down = totals
    increment = branch + ffn_out.astype(jnp.float32)
    block_out = live_mask * (hidden + chosen_mask * gating * increment)
    return (
        block_out.astype(jnp.bfloat16)[None],
        grad_tokens[None],
        total_q,
        total_k,
        total_v,
        total_out,
        total_gate,
        total_up,
        total_down,
        mine[0],
        mine[1],
        mine[2],
    )


def solution(mesh):
    in_specs = (
        P("fsdp", "ctx", None),
        P("fsdp", None),
        P("fsdp", None),
        P("fsdp", None),
        P("fsdp", None),
        P("fsdp", None),
        P("fsdp", None),
        P("fsdp", None),
        P("fsdp"),
        P("fsdp"),
        P("fsdp"),
        P("fsdp", "ctx", None),
        P("fsdp", "ctx"),
        P("fsdp"),
        P("fsdp", "ctx"),
    )
    out_specs = (
        P("fsdp", "ctx", None),
        P("fsdp", "ctx", None),
        P("fsdp", None),
        P("fsdp", None),
        P("fsdp", None),
        P("fsdp", None),
        P("fsdp", None),
        P("fsdp", None),
        P("fsdp", None),
        P("fsdp"),
        P("fsdp"),
        P("fsdp"),
    )
    return jax.shard_map(
        on_device, mesh=mesh, in_specs=in_specs, out_specs=out_specs, check_vma=False
    )
```

```python
import functools

import jax
import jax.numpy as jnp
from jax import lax
from jax.experimental import pallas as pl
from jax.experimental.pallas import tpu as pltpu
from jax.sharding import PartitionSpec as P

HEADS = 15
KV_HEADS = 5
HEAD = 64


epsilon = 1e-05
negative = -1e30
across_rows = (((0,), (0,)), ((), ()))
across_cols = (((1,), (1,)), ((), ()))


def rope_tables(positions):
    half_dim = HEAD // 2
    frequency = 10000.0 ** (-2.0 * jnp.arange(half_dim, dtype=jnp.float32) / HEAD)
    angles = positions.astype(jnp.float32)[:, None] * frequency[None, :]
    return (jnp.cos(angles), jnp.sin(angles))


def rotate(values, cos_tab, sin_tab):
    slots, width = values.shape
    low, high = jnp.split(values.reshape(slots, width // HEAD, HEAD), 2, -1)
    cos_tab, sin_tab = cos_tab[:, None], sin_tab[:, None]
    turned = [low * cos_tab - high * sin_tab, high * cos_tab + low * sin_tab]
    return jnp.concatenate(turned, -1).reshape(slots, width)


def rotate_columns(values, cos_tab, sin_tab):
    width, slots = values.shape
    low, high = jnp.split(values.reshape(width // HEAD, HEAD, slots), 2, 1)
    cos_tab, sin_tab = cos_tab.T[None], sin_tab.T[None]
    turned = [low * cos_tab - high * sin_tab, high * cos_tab + low * sin_tab]
    return jnp.concatenate(turned, 1).reshape(width, slots)


def norm_forward(values, gain_vec):
    inv_rms = lax.rsqrt(jnp.mean(values * values, -1, keepdims=True) + epsilon)
    return (values * inv_rms * gain_vec, inv_rms)


def norm_backward(values, inv_rms, gain_vec, grad_normed):
    weighted = gain_vec * grad_normed
    grad_gain = jnp.sum(grad_normed * values * inv_rms, 0)
    cubed = inv_rms * inv_rms * inv_rms
    grad_values = inv_rms * weighted - values * cubed * jnp.mean(
        weighted * values, -1, keepdims=True
    )
    return (grad_values, grad_gain)


def padded_to(values, row_dim):
    pads = [(0, 0)] * values.ndim
    pads[row_dim] = (0, -values.shape[row_dim] % 128)
    return jnp.pad(values, pads)


def ffn_both(normed, grad_mixed, gate_rows, up_rows, down_rows):
    gate_proj = lax.dot_general(normed, gate_rows, across_cols, preferred_element_type=jnp.float32)
    up_proj = lax.dot_general(normed, up_rows, across_cols, preferred_element_type=jnp.float32)
    sigma = jax.nn.sigmoid(gate_proj)
    activated = gate_proj * sigma
    inner_act = (activated * up_proj).astype(jnp.bfloat16)
    grad_inner = lax.dot_general(
        grad_mixed, down_rows, across_cols, preferred_element_type=jnp.float32
    )
    grad_gate_act = (grad_inner * up_proj * sigma * (1.0 + gate_proj * (1.0 - sigma))).astype(
        jnp.bfloat16
    )
    grad_up_act = (grad_inner * activated).astype(jnp.bfloat16)
    grad_normed = jnp.dot(grad_gate_act, gate_rows, preferred_element_type=jnp.float32) + jnp.dot(
        grad_up_act, up_rows, preferred_element_type=jnp.float32
    )
    row_dot = jnp.sum(inner_act.astype(jnp.float32) * grad_inner, -1, keepdims=True)
    grad_normed = jnp.concatenate([grad_normed, row_dot], 1).astype(jnp.bfloat16)
    return (inner_act, grad_gate_act, grad_up_act, grad_normed)


CHIPS = 4
SPAN = 2 * CHIPS
VMEM_BYTES = 60 * 1024 * 1024
MESH = pl.DeviceIdType.MESH


def plane_of():
    me = lax.axis_index("ctx")
    core = lax.rem(me, 2)
    chip = me // 2
    return me, core, chip, me + 1 - 2 * core


def chip_at(chip, core, step):
    return 2 * lax.rem(chip + step + CHIPS, CHIPS) + core


def greet(devices):
    barrier = pltpu.get_barrier_semaphore()
    for device in devices:
        pl.semaphore_signal(barrier, inc=1, device_id=device, device_id_type=MESH)
    pl.semaphore_wait(barrier, len(devices))


def send(src, dst, send_sem, recv_sem, device):
    copy = pltpu.make_async_remote_copy(
        src_ref=src,
        dst_ref=dst,
        send_sem=send_sem,
        recv_sem=recv_sem,
        device_id=device,
        device_id_type=MESH,
    )
    copy.start()
    return copy


def comm_params(number):
    return pltpu.CompilerParams(
        collective_id=number, has_side_effects=True, vmem_limit_bytes=VMEM_BYTES
    )


def comm_cost(moved):
    return pl.CostEstimate(flops=0, bytes_accessed=moved * 30, transcendentals=0)


def in_vmem(count):
    return [pl.BlockSpec(memory_space=pltpu.VMEM)] * count


def gather_rows_kernel(depth, count, *refs):
    owns, outs = refs[:count], refs[count : 2 * count]
    z_sems, p_sems, f_sems = refs[2 * count :]
    me, core, chip, partner = plane_of()
    layer = lax.axis_index("fsdp")
    layers = [lax.rem(layer + d, depth) for d in range(1, depth)]
    peers = [chip_at(chip, core, j) for j in range(1, CHIPS)]
    greet([(me, other) for other in layers] + [(peer, layer) for peer in peers + [partner]])
    first, spread, passed = [], [], []
    for a, (own, out) in enumerate(zip(owns, outs)):
        for d, other in enumerate(layers):
            first.append(
                send(
                    own.at[me],
                    out.at[layer, me],
                    z_sems.at[0, a, d],
                    z_sems.at[1, a, d],
                    (me, other),
                )
            )
    for own, out in zip(owns, outs):
        for piece in range(SPAN):
            out[layer, piece] = own[piece]
    for a, out in enumerate(outs):
        for d in range(depth - 1):
            first[a * (depth - 1) + d].wait_recv()
            block = out.at[lax.rem(layer + depth - d - 1, depth), me]
            for j, peer in enumerate(peers):
                spread.append(
                    send(block, block, p_sems.at[0, a, d, j], p_sems.at[1, a, d, j], (peer, layer))
                )
            passed.append(
                send(block, block, f_sems.at[0, a, d, 3], f_sems.at[1, a, d, 3], (partner, layer))
            )
    arrivals = iter(spread)
    for a, out in enumerate(outs):
        for d in range(depth - 1):
            source = lax.rem(layer + depth - d - 1, depth)
            for j in range(CHIPS - 1):
                next(arrivals).wait_recv()
                block = out.at[source, chip_at(chip, core, -j - 1)]
                passed.append(
                    send(
                        block,
                        block,
                        f_sems.at[0, a, d, j],
                        f_sems.at[1, a, d, j],
                        (partner, layer),
                    )
                )
    for copy in first + spread:
        copy.wait_send()
    for copy in passed:
        copy.wait()


def gather_rows(arrays, depth):
    if lax.axis_size("ctx") != SPAN:
        return [lax.all_gather(own, "fsdp", axis=0) for own in arrays]
    count, pieces, outs = len(arrays), [], []
    for own in arrays:
        piece = (own.shape[0] // SPAN, own.shape[1])
        pieces.append(own.reshape(SPAN, *piece))
        outs.append(jax.ShapeDtypeStruct((depth, SPAN, *piece), own.dtype))
    whole = pl.pallas_call(
        functools.partial(gather_rows_kernel, depth, count),
        out_shape=tuple(outs),
        in_specs=in_vmem(count),
        out_specs=tuple(in_vmem(count)),
        scratch_shapes=[
            pltpu.SemaphoreType.DMA((2, count, depth - 1)),
            pltpu.SemaphoreType.DMA((2, count, depth - 1, CHIPS - 1)),
            pltpu.SemaphoreType.DMA((2, count, depth - 1, CHIPS)),
        ],
        compiler_params=comm_params(1),
        cost_estimate=comm_cost(sum(own.size for own in arrays) * 2 * depth),
    )(*pieces)
    return [full.reshape(depth, *own.shape) for full, own in zip(whole, arrays)]


def gather_plane_kernel(kv_ref, tag_ref, kv_out, tag_out, p_sems, f_sems):
    me, core, chip, partner = plane_of()
    layer = lax.axis_index("fsdp")
    peers = [chip_at(chip, core, j) for j in range(1, CHIPS)]
    greet([(peer, layer) for peer in peers + [partner]])
    pairs = ((kv_ref, kv_out), (tag_ref, tag_out))
    spread, passed = [], []
    for j, peer in enumerate(peers):
        for a, (own, out) in enumerate(pairs):
            spread.append(
                send(own, out.at[me], p_sems.at[0, a, j], p_sems.at[1, a, j], (peer, layer))
            )
    for a, (own, out) in enumerate(pairs):
        passed.append(
            send(own, out.at[me], f_sems.at[0, a, 3], f_sems.at[1, a, 3], (partner, layer))
        )
    kv_out[me] = kv_ref[...]
    tag_out[me] = tag_ref[...]
    for j in range(CHIPS - 1):
        for a, (own, out) in enumerate(pairs):
            spread[2 * j + a].wait_recv()
            block = out.at[chip_at(chip, core, -j - 1)]
            passed.append(
                send(block, block, f_sems.at[0, a, j], f_sems.at[1, a, j], (partner, layer))
            )
    for copy in spread:
        copy.wait_send()
    for copy in passed:
        copy.wait()


def gather_plane(kv, tags):
    if lax.axis_size("ctx") != SPAN:
        return tuple(lax.all_gather(part, "ctx", axis=0, tiled=True) for part in (kv, tags))
    rows, columns = kv.shape
    kv_all, tags_all = pl.pallas_call(
        gather_plane_kernel,
        out_shape=(
            jax.ShapeDtypeStruct((SPAN, rows, columns), kv.dtype),
            jax.ShapeDtypeStruct((SPAN, 1, rows), tags.dtype),
        ),
        in_specs=in_vmem(2),
        out_specs=tuple(in_vmem(2)),
        scratch_shapes=[
            pltpu.SemaphoreType.DMA((2, 2, CHIPS - 1)),
            pltpu.SemaphoreType.DMA((2, 2, CHIPS)),
        ],
        compiler_params=comm_params(2),
        cost_estimate=comm_cost(kv.size * 2 * SPAN),
    )(kv, tags[None])
    return kv_all.reshape(SPAN * rows, columns), tags_all.reshape(SPAN * rows)


def added(*parts):
    total = parts[0].astype(jnp.float32)
    for part in parts[1:]:
        total = total + part.astype(jnp.float32)
    return total


def across_of(chip, core, way):
    along_x, along_y = lax.rem(chip, 2), chip // 2
    along_x = 1 - along_x if way % 2 else along_x
    along_y = 1 - along_y if way // 2 else along_y
    return 2 * (2 * along_y + along_x) + core


def reduce_plane(arrays, h_sems, p_sems):
    me, core, chip, partner = plane_of()
    layer = lax.axis_index("fsdp")
    ways = (3, 1, 2, 0)
    near = (across_of(chip, core, 1), across_of(chip, core, 2))
    handed, started, last = [], [], []
    for a, (piece_of, halves, sums, arrived) in enumerate(arrays):
        for way in ways:
            handed.append(
                send(
                    piece_of(across_of(chip, 1 - core, way)),
                    halves.at[way],
                    h_sems.at[0, a, way],
                    h_sems.at[1, a, way],
                    (partner, layer),
                )
            )
    for a, (piece_of, halves, sums, arrived) in enumerate(arrays):
        middle = sums.shape[1] // 2
        sides = (pl.ds(0, middle), pl.ds(middle, middle))
        copies = {}

        def pass_on(way, side, slot, hop, a=a, sums=sums, arrived=arrived, sides=sides):
            number = 2 * slot + side
            return send(
                sums.at[way, sides[side]],
                arrived.at[slot, sides[side]],
                p_sems.at[0, a, number],
                p_sems.at[1, a, number],
                (near[hop], layer),
            )

        for j, way in enumerate(ways):
            handed[a * CHIPS + j].wait_recv()
            mine = piece_of(across_of(chip, core, way))

            def add_half(slab, carry, mine=mine, halves=halves, sums=sums, way=way):
                sums[way, slab] = added(mine[slab], halves[way, slab]).astype(sums.dtype)
                return carry

            lax.fori_loop(0, sums.shape[1], add_half, 0)
            if way == 3:
                for side in range(2):
                    copies[0, side] = pass_on(3, side, 0, side)
            elif way:
                copies[1, way - 1] = pass_on(way, way - 1, 1, way - 1)
        started.append((copies, pass_on))
    for (copies, pass_on), (_, _, sums, arrived) in zip(started, arrays):
        middle = sums.shape[1] // 2
        for side in range(2):
            copies[0, side].wait_recv()
            way = 2 - side

            def add_opposite(slab, carry, way=way, sums=sums, arrived=arrived):
                total = added(sums[way, slab], arrived[0, slab])
                sums[way, slab] = total.astype(sums.dtype)
                return carry

            lax.fori_loop(side * middle, (side + 1) * middle, add_opposite, 0)
            copies[2, side] = pass_on(way, side, 2, 1 - side)
        last.append([copies[slot, side] for slot in (1, 2) for side in range(2)])
    everything = handed + [copy for copies, _ in started for copy in copies.values()]
    return everything, last


def plane_total(sums, arrived, slab):
    return added(sums[0, slab], arrived[1, slab], arrived[2, slab])


def plane_scratch(block, dtype):
    return [
        pltpu.VMEM((CHIPS, *block), dtype),
        pltpu.VMEM((CHIPS, *block), dtype),
        pltpu.VMEM((CHIPS - 1, *block), dtype),
    ]


def turned_back(values, cos_tab, sin_tab):
    half_dim, parts = HEAD // 2, []
    for start in range(0, values.shape[1], HEAD):
        low = values[:, start : start + half_dim]
        high = values[:, start + half_dim : start + HEAD]
        parts += [low * cos_tab + high * sin_tab, high * cos_tab - low * sin_tab]
    return jnp.concatenate(parts, 1)


def scatter_plane_kernel(x_ref, cos_ref, sin_ref, out_ref, halves, sums, arrived, h_sems, p_sems):
    me, core, chip, partner = plane_of()
    layer = lax.axis_index("fsdp")
    near = [across_of(chip, core, way) for way in (1, 2)]
    greet([(peer, layer) for peer in near + [partner]])
    arrays = [(lambda piece: x_ref.at[piece], halves, sums, arrived)]
    started, last = reduce_plane(arrays, h_sems, p_sems)
    for copy in last[0]:
        copy.wait_recv()

    def add_slab(slab, carry):
        total = plane_total(sums, arrived, slab)
        kdim = KV_HEADS * HEAD
        keys = turned_back(total[:, :kdim], cos_ref[slab], sin_ref[slab])
        out_ref[slab] = jnp.concatenate([keys, total[:, kdim:]], 1).astype(out_ref.dtype)
        return carry

    lax.fori_loop(0, x_ref.shape[1], add_slab, 0)
    for copy in started:
        copy.wait_send()


def scatter_plane(values, cos_tab, sin_tab):
    if lax.axis_size("ctx") != SPAN:
        own = lax.psum_scatter(values, "ctx", scatter_dimension=0, tiled=True)
        own, kdim = own.astype(jnp.float32), KV_HEADS * HEAD
        keys = turned_back(own[:, :kdim], cos_tab, sin_tab)
        return jnp.concatenate([keys, own[:, kdim:]], 1).astype(values.dtype)
    rows, columns = values.shape
    slabs = 8
    block = (slabs, rows // SPAN // slabs, columns)
    return pl.pallas_call(
        scatter_plane_kernel,
        out_shape=jax.ShapeDtypeStruct(block, values.dtype),
        in_specs=in_vmem(3),
        out_specs=in_vmem(1)[0],
        scratch_shapes=plane_scratch(block, values.dtype)
        + [pltpu.SemaphoreType.DMA((2, 1, CHIPS)), pltpu.SemaphoreType.DMA((2, 1, 6))],
        compiler_params=comm_params(3),
        cost_estimate=comm_cost(values.size * 2),
    )(
        values.reshape(SPAN, *block),
        cos_tab.reshape(*block[:2], -1),
        sin_tab.reshape(*block[:2], -1),
    ).reshape(rows // SPAN, columns)


def reduce_direct(arrays, h_sems, p_sems):
    me, core, chip, partner = plane_of()
    layer = lax.axis_index("fsdp")
    handed, spread = [], []
    for a, (piece_of, halves, sums, arrived) in enumerate(arrays):
        for j in range(CHIPS):
            slot = (j + 1) % CHIPS
            handed.append(
                send(
                    piece_of(chip_at(chip, 1 - core, slot)),
                    halves.at[slot],
                    h_sems.at[0, a, slot],
                    h_sems.at[1, a, slot],
                    (partner, layer),
                )
            )
    for a, (piece_of, halves, sums, arrived) in enumerate(arrays):
        for j in range(CHIPS):
            slot = (j + 1) % CHIPS
            handed[a * CHIPS + j].wait_recv()
            mine = chip_at(chip, core, slot)

            def add_half(slab, carry, piece=piece_of(mine), halves=halves, sums=sums, slot=slot):
                sums[slot, slab] = added(piece[slab], halves[slot, slab]).astype(sums.dtype)
                return carry

            lax.fori_loop(0, sums.shape[1], add_half, 0)
            if slot:
                spread.append(
                    send(
                        sums.at[slot],
                        arrived.at[slot - 1],
                        p_sems.at[0, a, slot - 1],
                        p_sems.at[1, a, slot - 1],
                        (mine, layer),
                    )
                )
    return handed, spread


def direct_total(sums, arrived, slab):
    return added(sums[0, slab], *(arrived[j, slab] for j in range(CHIPS - 1)))


def reduce_rows_kernel(depth, count, *refs):
    inputs, outs, scratch = refs[:count], refs[count : 2 * count], refs[2 * count : 6 * count]
    h_sems, p_sems, z_sems, g_sems, f_sems = refs[6 * count :]
    me, core, chip, partner = plane_of()
    layer = lax.axis_index("fsdp")
    layers = [lax.rem(layer + d, depth) for d in range(1, depth)]
    peers = [chip_at(chip, core, j) for j in range(1, CHIPS)]
    greet([(me, other) for other in layers] + [(peer, layer) for peer in peers + [partner]])
    arrays, across = [], []
    for a, x_ref in enumerate(inputs):
        halves, sums, arrived, layers_ref = scratch[4 * a : 4 * a + 4]
        arrays.append((lambda piece, x_ref=x_ref: x_ref.at[:, piece], halves, sums, arrived))
        across.append(layers_ref)
    handed, spread = reduce_direct(arrays, h_sems, p_sems)
    moved = []
    for a, (_, _, sums, arrived) in enumerate(arrays):
        for copy in spread[a * (CHIPS - 1) : (a + 1) * (CHIPS - 1)]:
            copy.wait_recv()
        for d in list(range(1, depth)) + [0]:
            target = lax.rem(layer + d, depth)
            across[a][0, d] = direct_total(sums, arrived, target).astype(across[a].dtype)
            if d:
                moved.append(
                    send(
                        across[a].at[0, d],
                        across[a].at[1, d],
                        z_sems.at[0, a, d - 1],
                        z_sems.at[1, a, d - 1],
                        (me, target),
                    )
                )
    given, passed = [], []
    for a, out_ref in enumerate(outs):
        for copy in moved[a * (depth - 1) : (a + 1) * (depth - 1)]:
            copy.wait_recv()
        parts = [across[a][0, 0]] + [across[a][1, d] for d in range(1, depth)]
        out_ref[me] = added(*parts).astype(out_ref.dtype)
        mine = out_ref.at[me]
        for j, peer in enumerate(peers):
            given.append(send(mine, mine, g_sems.at[0, a, j], g_sems.at[1, a, j], (peer, layer)))
        passed.append(send(mine, mine, f_sems.at[0, a, 3], f_sems.at[1, a, 3], (partner, layer)))
    for a, out_ref in enumerate(outs):
        for j in range(CHIPS - 1):
            given[a * (CHIPS - 1) + j].wait_recv()
            block = out_ref.at[chip_at(chip, core, -j - 1)]
            passed.append(
                send(block, block, f_sems.at[0, a, j], f_sems.at[1, a, j], (partner, layer))
            )
    for copy in handed + spread + moved + given:
        copy.wait_send()
    for copy in passed:
        copy.wait()


def reduce_rows(arrays, number):
    if lax.axis_size("ctx") != SPAN:
        return [lax.psum(lax.psum_scatter(v, "fsdp", scatter_dimension=0), "ctx") for v in arrays]
    depth, count = arrays[0].shape[0], len(arrays)
    pieces, outs, scratch = [], [], []
    for values in arrays:
        _, rows, columns = values.shape
        piece = (rows // SPAN, columns)
        pieces.append(values.reshape(depth, SPAN, *piece))
        outs.append(jax.ShapeDtypeStruct((SPAN, *piece), values.dtype))
        scratch += plane_scratch((depth, *piece), values.dtype)
        scratch.append(pltpu.VMEM((2, depth, *piece), values.dtype))
    owned = pl.pallas_call(
        functools.partial(reduce_rows_kernel, depth, count),
        out_shape=tuple(outs),
        in_specs=in_vmem(count),
        out_specs=tuple(in_vmem(count)),
        scratch_shapes=scratch
        + [
            pltpu.SemaphoreType.DMA((2, count, CHIPS)),
            pltpu.SemaphoreType.DMA((2, count, CHIPS - 1)),
            pltpu.SemaphoreType.DMA((2, count, depth - 1)),
            pltpu.SemaphoreType.DMA((2, count, CHIPS - 1)),
            pltpu.SemaphoreType.DMA((2, count, CHIPS)),
        ],
        compiler_params=comm_params(number),
        cost_estimate=comm_cost(sum(values.size for values in arrays) * 2),
    )(*pieces)
    return [own.reshape(values.shape[1:]) for own, values in zip(owned, arrays)]


BLOCK = 128
LANES = (HEADS // KV_HEADS) * BLOCK


def dot(left, right, dims=(1, 0)):
    return lax.dot_general(
        left, right, (((dims[0],), (dims[1],)), ((), ())), preferred_element_type=jnp.float32
    )


def of_group(ref, group, at):
    first = group * (HEADS // KV_HEADS)
    heads = range(first, first + HEADS // KV_HEADS)
    return jnp.concatenate([ref[head * HEAD : (head + 1) * HEAD, at] for head in heads], 1)


def of_rows(ref, group, at):
    first = group * (HEADS // KV_HEADS)
    heads = range(first, first + HEADS // KV_HEADS)
    return jnp.concatenate([ref[head : head + 1, at] for head in heads], 1)


def columns_of(group, part):
    start = (part * KV_HEADS + group) * HEAD
    return slice(start, start + HEAD)


def mask_bias(tags, query_pos):
    tags = jnp.broadcast_to(tags, (BLOCK, BLOCK)).T
    key_pos = jnp.where(tags >= 0, tags, -tags - 1)
    allowed = (key_pos <= query_pos) & ((tags >= 0) | (key_pos == query_pos))
    bias = jnp.where(allowed, 0.0, negative)
    return jnp.concatenate([bias] * (HEADS // KV_HEADS), 1)


def attend_kernel(
    first_ref, q_ref, kv_ref, pos_ref, tag_ref, out_ref, log_ref, max_ref, sum_ref, acc_ref, kept
):
    blocks = kv_ref.shape[0] // BLOCK
    keep = kept.shape[0] == blocks

    def scores(group, at, rows, bias):
        keys = kv_ref[rows, columns_of(group, 0)]
        return dot(keys, of_group(q_ref, group, at)) + bias

    def query_block(qb, carry):
        at = pl.ds(pl.multiple_of(qb * BLOCK, BLOCK), BLOCK)
        max_ref[...] = jnp.full(max_ref.shape, negative, jnp.float32)
        sum_ref[...] = jnp.zeros(sum_ref.shape, jnp.float32)
        acc_ref[...] = jnp.zeros(acc_ref.shape, jnp.float32)
        limit = first_ref[blocks + qb]

        def find(kb, carry):
            @pl.when(first_ref[kb] <= limit)
            def _():
                rows = pl.ds(pl.multiple_of(kb * BLOCK, BLOCK), BLOCK)
                bias = mask_bias(tag_ref[kb], pos_ref[:, at])
                for group in range(KV_HEADS):
                    found = scores(group, at, rows, bias)
                    if keep:
                        kept[kb, group] = found
                    tops = jnp.max(found.reshape(BLOCK // 8, 8, LANES), 0)
                    max_ref[group] = jnp.maximum(max_ref[group], tops)

            return carry

        lax.fori_loop(0, blocks, find, 0)
        for group in range(KV_HEADS):
            top = jnp.max(max_ref[group], 0, keepdims=True)
            max_ref[group] = jnp.broadcast_to(top, max_ref.shape[1:])

        def gather(kb, carry):
            @pl.when(first_ref[kb] <= limit)
            def _():
                rows = pl.ds(pl.multiple_of(kb * BLOCK, BLOCK), BLOCK)
                bias = None if keep else mask_bias(tag_ref[kb], pos_ref[:, at])
                for group in range(KV_HEADS):
                    found = kept[kb, group] if keep else scores(group, at, rows, bias)
                    weights = jnp.exp(found - max_ref[group, :1])
                    sum_ref[group] += jnp.sum(weights.reshape(BLOCK // 8, 8, LANES), 0)
                    values = kv_ref[rows, columns_of(group, 1)]
                    acc_ref[group] += dot(values, weights.astype(jnp.bfloat16), (0, 0))

            return carry

        lax.fori_loop(0, blocks, gather, 0)
        for group in range(KV_HEADS):
            total = jnp.sum(sum_ref[group], 0, keepdims=True)
            attended = acc_ref[group] / total
            logs = max_ref[group, :1] + jnp.log(total)
            for j in range(HEADS // KV_HEADS):
                head = group * (HEADS // KV_HEADS) + j
                own = slice(j * BLOCK, (j + 1) * BLOCK)
                out_ref[head * HEAD : (head + 1) * HEAD, at] = attended[:, own]
                log_ref[head : head + 1, at] = logs[:, own]
        return carry

    lax.fori_loop(0, q_ref.shape[1] // BLOCK, query_block, 0)


def kernel_params():
    return pltpu.CompilerParams(vmem_limit_bytes=VMEM_BYTES)


def attend(firsts, queries, kv, query_pos, key_tags):
    blocks = kv.shape[0] // BLOCK
    slots = queries.shape[1]
    kept = blocks if blocks <= 16 else 1
    groups = (KV_HEADS, 8, LANES)
    work = 4 * kv.shape[0] * slots * HEADS * HEAD
    return pl.pallas_call(
        attend_kernel,
        out_shape=(
            jax.ShapeDtypeStruct(queries.shape, jnp.float32),
            jax.ShapeDtypeStruct((HEADS + 1, slots), jnp.float32),
        ),
        in_specs=[pl.BlockSpec(memory_space=pltpu.SMEM)] + in_vmem(4),
        out_specs=tuple(in_vmem(2)),
        scratch_shapes=[
            pltpu.VMEM(groups, jnp.float32),
            pltpu.VMEM(groups, jnp.float32),
            pltpu.VMEM((KV_HEADS, HEAD, LANES), jnp.float32),
            pltpu.VMEM((kept, KV_HEADS, BLOCK, LANES), jnp.float32),
        ],
        compiler_params=kernel_params(),
        cost_estimate=pl.CostEstimate(
            flops=work * 8, bytes_accessed=kv.size * 2, transcendentals=work // 256
        ),
    )(firsts, queries, kv, query_pos[None], key_tags.reshape(-1, 1, BLOCK))


def attend_back_kernel(
    first_ref, q_ref, kv_ref, pos_ref, tag_ref, grad_ref, log_ref, delta_ref, *refs
):
    blocks = kv_ref.shape[0] // BLOCK
    cos_ref, sin_ref, out_ref, dkv_ref, acc, dq_ref = refs
    dq_ref[...] = jnp.zeros(dq_ref.shape, dq_ref.dtype)

    def key_block(kb, carry):
        rows = pl.ds(pl.multiple_of(kb * BLOCK, BLOCK), BLOCK)
        acc[...] = jnp.zeros(acc.shape, jnp.float32)

        def query_block(qb, carry):
            @pl.when(first_ref[kb] <= first_ref[blocks + qb])
            def _():
                at = pl.ds(pl.multiple_of(qb * BLOCK, BLOCK), BLOCK)
                bias = mask_bias(tag_ref[kb], pos_ref[:, at])
                for group in range(KV_HEADS):
                    keys = kv_ref[rows, columns_of(group, 0)]
                    values = kv_ref[rows, columns_of(group, 1)]
                    queries = of_group(q_ref, group, at)
                    grads = of_group(grad_ref, group, at)
                    found = dot(keys, queries) + bias
                    probs = jnp.exp(found - of_rows(log_ref, group, at))
                    grad_probs = dot(values, grads)
                    grad_scores = probs * (grad_probs - of_rows(delta_ref, group, at))
                    grad_scores = grad_scores.astype(jnp.bfloat16)
                    acc[group] += dot(grad_scores, queries, (1, 1))
                    acc[KV_HEADS + group] += dot(probs.astype(jnp.bfloat16), grads, (1, 1))
                    grad_q = 0.125 * dot(keys, grad_scores, (0, 0))
                    for j in range(HEADS // KV_HEADS):
                        head = group * (HEADS // KV_HEADS) + j
                        own = slice(head * HEAD, (head + 1) * HEAD)
                        dq_ref[own, at] += grad_q[:, j * BLOCK : (j + 1) * BLOCK]

            return carry

        lax.fori_loop(0, q_ref.shape[1] // BLOCK, query_block, 0)
        dkv_ref[rows, :] = jnp.concatenate(
            [acc[index] for index in range(2 * KV_HEADS)], 1
        ).astype(dkv_ref.dtype)
        return carry

    lax.fori_loop(0, blocks, key_block, 0)
    half_dim = HEAD // 2

    def finish(qb, carry):
        at = pl.ds(pl.multiple_of(qb * BLOCK, BLOCK), BLOCK)
        cos_tab, sin_tab = cos_ref[:, at], sin_ref[:, at]
        for head in range(0, HEADS, 2):
            pair = []
            for start in range(head * HEAD, min(head + 2, HEADS) * HEAD, HEAD):
                low = dq_ref[start : start + half_dim, at]
                high = dq_ref[start + half_dim : start + HEAD, at]
                pair += [low * cos_tab + high * sin_tab, high * cos_tab - low * sin_tab]
            if len(pair) == 2:
                pair += [jnp.zeros_like(part) for part in pair]
            turned = jnp.concatenate(pair, 0).T
            own = slice(head * HEAD, head * HEAD + turned.shape[1])
            out_ref[at, own] = turned.astype(out_ref.dtype)
        return carry

    lax.fori_loop(0, q_ref.shape[1] // BLOCK, finish, 0)


def attend_back(firsts, queries, kv, query_pos, key_tags, grads, log_total, row_delta, tables):
    slots = queries.shape[1]
    work = 10 * kv.shape[0] * slots * HEADS * HEAD
    return pl.pallas_call(
        attend_back_kernel,
        out_shape=(
            jax.ShapeDtypeStruct((slots, -(-HEADS // 2) * 2 * HEAD), jnp.bfloat16),
            jax.ShapeDtypeStruct(kv.shape, jnp.bfloat16),
        ),
        in_specs=[pl.BlockSpec(memory_space=pltpu.SMEM)] + in_vmem(9),
        out_specs=tuple(in_vmem(2)),
        scratch_shapes=[
            pltpu.VMEM((2 * KV_HEADS, BLOCK, HEAD), jnp.float32),
            pltpu.VMEM(queries.shape, jnp.float32),
        ],
        compiler_params=kernel_params(),
        cost_estimate=pl.CostEstimate(
            flops=work * 6, bytes_accessed=kv.size * 4, transcendentals=work // 640
        ),
    )(firsts, queries, kv, query_pos[None], key_tags.reshape(-1, 1, BLOCK), grads, log_total, row_delta, *tables)


def on_device(
    tokens,
    w_query,
    w_key,
    w_value,
    w_out,
    w_gate,
    w_up,
    w_down,
    gain_attn,
    gain_ffn,
    router,
    cotangent,
    positions,
    lengths,
    chosen,
):
    hidden = tokens[0].astype(jnp.float32)
    row_count, width = hidden.shape
    qdim = HEADS * HEAD
    kdim = KV_HEADS * HEAD
    query_pos = positions[0]
    live = query_pos < lengths[0]
    selected = live & (chosen[0] == 1)
    live_mask = live.astype(jnp.float32)[:, None]
    chosen_mask = selected.astype(jnp.float32)[:, None]
    cos_tab, sin_tab = rope_tables(query_pos)
    key_tags = jnp.where(selected, query_pos, -query_pos - 1)
    depth = lax.axis_size("fsdp")
    own_rows = w_query.shape[0]
    w_out_full = lax.all_gather(w_out, "fsdp", axis=0, tiled=True)
    vectors = jnp.stack([gain_attn, gain_ffn, router], 1)
    own_attn = [padded_to(w_query, 1), jnp.concatenate([w_key, w_value, vectors], 1)]
    gathered = gather_rows([padded_to(own, 0) for own in own_attn], depth)
    padded_rows = gathered[0].shape[1]
    w_query = gathered[0].reshape(depth * padded_rows, -1)
    gathered = gathered[1][:, :own_rows].reshape(width, -1)
    w_kv, vectors = gathered[:, : 2 * kdim], gathered[:, 2 * kdim :]
    gain_one, gain_two, router_vec = vectors.T.astype(jnp.float32)
    gating = jax.nn.sigmoid(jnp.sum(hidden * router_vec, -1, keepdims=True))
    grad_y = cotangent[0].astype(jnp.float32) * live_mask
    grad_inc = grad_y * chosen_mask * gating
    grad_ffn = grad_inc.astype(jnp.bfloat16)
    grad_ffn_all = lax.all_gather(grad_ffn, "fsdp", axis=0, tiled=True)

    normed_one, inv_one = norm_forward(hidden, gain_one)
    normed_one = normed_one.astype(jnp.bfloat16)
    spread_one = padded_to(normed_one.reshape(row_count, depth, own_rows), -1)
    spread_one = spread_one.reshape(row_count, -1)
    query_raw = dot(w_query, spread_one, (0, 1))[:qdim]
    queries = rotate_columns(query_raw, cos_tab, sin_tab).astype(jnp.bfloat16) * 0.125
    kv_raw = dot(normed_one, w_kv)
    kv_own = jnp.concatenate([rotate(kv_raw[:, :kdim], cos_tab, sin_tab), kv_raw[:, kdim:]], 1)
    kv_all, tags_all = gather_plane(kv_own.astype(jnp.bfloat16), key_tags)
    first_tags = tags_all[::BLOCK]
    firsts = jnp.concatenate(
        [jnp.where(first_tags >= 0, first_tags, -first_tags - 1), query_pos[BLOCK - 1 :: BLOCK]]
    )
    attended, log_total = attend(firsts, queries, kv_all, query_pos, tags_all)
    attended, w_out_full = lax.optimization_barrier((attended, w_out_full))
    outcome = attended.astype(jnp.bfloat16)
    branch = dot(outcome, w_out_full, (0, 0))
    branch, grad_ffn_all = lax.optimization_barrier((branch, grad_ffn_all))
    middle = hidden + branch
    normed_two, inv_two = norm_forward(middle, gain_two)
    normed_two = normed_two.astype(jnp.bfloat16)
    normed_all = lax.all_gather(normed_two, "fsdp", axis=0, tiled=True)
    inner_act, grad_gate_act, grad_up_act, grad_normed_part = ffn_both(
        normed_all, grad_ffn_all, w_gate, w_up, w_down
    )
    grad_normed_two = lax.psum_scatter(
        grad_normed_part, "fsdp", scatter_dimension=0, tiled=True
    ).astype(jnp.float32)
    ffn_part = jnp.dot(inner_act, w_down, preferred_element_type=jnp.float32).astype(jnp.bfloat16)
    grad_wgate = lax.dot_general(
        grad_gate_act, normed_all, across_rows, preferred_element_type=jnp.float32
    )
    grad_wup = lax.dot_general(
        grad_up_act, normed_all, across_rows, preferred_element_type=jnp.float32
    )
    grad_wdown = lax.dot_general(
        inner_act, grad_ffn_all, across_rows, preferred_element_type=jnp.float32
    )
    low = jnp.bfloat16
    spread_out = padded_to(outcome.reshape(depth, own_rows, row_count), 1)
    grads = [grad.astype(low) for grad in (grad_wgate, grad_wup, grad_wdown)]
    grad_normed_two, ffn_part, spread_out, *grads = lax.optimization_barrier(
        (grad_normed_two, ffn_part, spread_out, *grads)
    )
    grad_normed_two, row_dot = grad_normed_two[:, :width], grad_normed_two[:, width:]
    totals = tuple(lax.psum(grad, "ctx") for grad in grads)
    grad_middle, grad_gain_two = norm_backward(middle, inv_two, gain_two, grad_normed_two)
    grad_branch = (grad_inc + grad_middle).astype(jnp.bfloat16)
    grad_attended = dot(w_out_full, grad_branch, (1, 1)).astype(jnp.bfloat16)
    grad_wout = dot(spread_out.reshape(-1, row_count), padded_to(grad_branch, 1)).astype(low)
    row_delta = jnp.sum(
        (grad_attended.astype(jnp.float32) * attended).reshape(HEADS, HEAD, row_count), 1
    )
    row_delta = jnp.pad(row_delta, ((0, 1), (0, 0)))
    grad_query_raw, grad_kv_all = attend_back(
        firsts,
        queries,
        kv_all,
        query_pos,
        tags_all,
        grad_attended,
        log_total,
        row_delta,
        (cos_tab.T, sin_tab.T),
    )
    grad_kv_raw = scatter_plane(grad_kv_all, cos_tab, sin_tab)
    grad_logit = (jnp.sum(grad_inc * branch, -1, keepdims=True) + row_dot) * (1.0 - gating)
    grad_router = jnp.sum(hidden * grad_logit, 0)
    grad_normed_one = dot(grad_query_raw, w_query, (1, 1)).reshape(row_count, depth, -1)
    grad_normed_one = grad_normed_one[..., :own_rows].reshape(row_count, width)
    grad_normed_one = grad_normed_one + dot(grad_kv_raw, w_kv, (1, 1))
    grad_wq = dot(spread_one, grad_query_raw, (0, 0)).astype(low)
    grad_wkv = dot(spread_one, grad_kv_raw, (0, 0)).astype(low)
    grad_hidden_one, grad_gain_one = norm_backward(hidden, inv_one, gain_one, grad_normed_one)
    grad_tokens = (grad_y + grad_logit * router_vec + grad_middle + grad_hidden_one).astype(
        jnp.bfloat16
    )
    vectors = jnp.stack([grad_gain_one, grad_gain_two, grad_router]).reshape(3, depth, own_rows)
    vectors = jnp.pad(vectors.transpose(1, 0, 2).reshape(depth, -1), ((0, 0), (0, -3 * own_rows % 1024)))
    vectors = jnp.pad(vectors.reshape(depth, -1, 1, 128), ((0, 0), (0, 0), (0, 7), (0, 0)))
    layered = [grad.reshape(depth, padded_rows, -1) for grad in (grad_wout, grad_wq, grad_wkv)]
    layered.append(vectors.reshape(depth, -1, 128))
    owned = reduce_rows(layered, 4)
    ffn_out = lax.psum_scatter(ffn_part, "fsdp", scatter_dimension=0, tiled=True)
    *owned, totals = lax.optimization_barrier((*owned, totals))
    total_out, total_q, total_kv = (own[:own_rows].astype(jnp.float32) for own in owned[:3])
    total_q, total_out = total_q[:, :qdim], total_out[:, :width]
    total_k, total_v = total_kv[:, :kdim], total_kv[:, kdim:]
    mine = owned[3].reshape(-1, 8, 128)[:, 0].reshape(-1)[: 3 * own_rows].reshape(3, own_rows)
    totals = [total.astype(jnp.float32) for total in totals]
    ffn_out, *totals = lax.optimization_barrier((ffn_out, *totals))
    total_gate, total_up, total_down = totals
    increment = branch + ffn_out.astype(jnp.float32)
    block_out = live_mask * (hidden + chosen_mask * gating * increment)
    return (
        block_out.astype(jnp.bfloat16)[None],
        grad_tokens[None],
        total_q,
        total_k,
        total_v,
        total_out,
        total_gate,
        total_up,
        total_down,
        mine[0],
        mine[1],
        mine[2],
    )


def solution(mesh):
    in_specs = (
        P("fsdp", "ctx", None),
        P("fsdp", None),
        P("fsdp", None),
        P("fsdp", None),
        P("fsdp", None),
        P("fsdp", None),
        P("fsdp", None),
        P("fsdp", None),
        P("fsdp"),
        P("fsdp"),
        P("fsdp"),
        P("fsdp", "ctx", None),
        P("fsdp", "ctx"),
        P("fsdp"),
        P("fsdp", "ctx"),
    )
    out_specs = (
        P("fsdp", "ctx", None),
        P("fsdp", "ctx", None),
        P("fsdp", None),
        P("fsdp", None),
        P("fsdp", None),
        P("fsdp", None),
        P("fsdp", None),
        P("fsdp", None),
        P("fsdp", None),
        P("fsdp"),
        P("fsdp"),
        P("fsdp"),
    )
    return jax.shard_map(
        on_device, mesh=mesh, in_specs=in_specs, out_specs=out_specs, check_vma=False
    )
```

```python
import functools

import jax
import jax.numpy as jnp
from jax import lax
from jax.experimental import pallas as pl
from jax.experimental.pallas import tpu as pltpu
from jax.sharding import PartitionSpec as P

HEADS = 15
KV_HEADS = 5
HEAD = 64


epsilon = 1e-05
negative = -1e30
across_rows = (((0,), (0,)), ((), ()))
across_cols = (((1,), (1,)), ((), ()))


def rope_tables(positions):
    half_dim = HEAD // 2
    frequency = 10000.0 ** (-2.0 * jnp.arange(half_dim, dtype=jnp.float32) / HEAD)
    angles = positions.astype(jnp.float32)[:, None] * frequency[None, :]
    return (jnp.cos(angles), jnp.sin(angles))


def rotate(values, cos_tab, sin_tab):
    slots, width = values.shape
    low, high = jnp.split(values.reshape(slots, width // HEAD, HEAD), 2, -1)
    cos_tab, sin_tab = cos_tab[:, None], sin_tab[:, None]
    turned = [low * cos_tab - high * sin_tab, high * cos_tab + low * sin_tab]
    return jnp.concatenate(turned, -1).reshape(slots, width)


def rotate_columns(values, cos_tab, sin_tab):
    width, slots = values.shape
    low, high = jnp.split(values.reshape(width // HEAD, HEAD, slots), 2, 1)
    cos_tab, sin_tab = cos_tab.T[None], sin_tab.T[None]
    turned = [low * cos_tab - high * sin_tab, high * cos_tab + low * sin_tab]
    return jnp.concatenate(turned, 1).reshape(width, slots)


def norm_forward(values, gain_vec):
    inv_rms = lax.rsqrt(jnp.mean(values * values, -1, keepdims=True) + epsilon)
    return (values * inv_rms * gain_vec, inv_rms)


def norm_backward(values, inv_rms, gain_vec, grad_normed):
    weighted = gain_vec * grad_normed
    grad_gain = jnp.sum(grad_normed * values * inv_rms, 0)
    cubed = inv_rms * inv_rms * inv_rms
    grad_values = inv_rms * weighted - values * cubed * jnp.mean(
        weighted * values, -1, keepdims=True
    )
    return (grad_values, grad_gain)


def padded_to(values, row_dim):
    pads = [(0, 0)] * values.ndim
    pads[row_dim] = (0, -values.shape[row_dim] % 128)
    return jnp.pad(values, pads)


def ffn_both(normed, grad_mixed, gate_rows, up_rows, down_rows):
    gate_proj = lax.dot_general(normed, gate_rows, across_cols, preferred_element_type=jnp.float32)
    up_proj = lax.dot_general(normed, up_rows, across_cols, preferred_element_type=jnp.float32)
    sigma = jax.nn.sigmoid(gate_proj)
    activated = gate_proj * sigma
    inner_act = (activated * up_proj).astype(jnp.bfloat16)
    grad_inner = lax.dot_general(
        grad_mixed, down_rows, across_cols, preferred_element_type=jnp.float32
    )
    grad_gate_act = (grad_inner * up_proj * sigma * (1.0 + gate_proj * (1.0 - sigma))).astype(
        jnp.bfloat16
    )
    grad_up_act = (grad_inner * activated).astype(jnp.bfloat16)
    grad_normed = jnp.dot(grad_gate_act, gate_rows, preferred_element_type=jnp.float32) + jnp.dot(
        grad_up_act, up_rows, preferred_element_type=jnp.float32
    )
    row_dot = jnp.sum(inner_act.astype(jnp.float32) * grad_inner, -1, keepdims=True)
    grad_normed = jnp.concatenate([grad_normed, row_dot], 1).astype(jnp.bfloat16)
    return (inner_act, grad_gate_act, grad_up_act, grad_normed)


CHIPS = 4
SPAN = 2 * CHIPS
VMEM_BYTES = 60 * 1024 * 1024
MESH = pl.DeviceIdType.MESH


def plane_of():
    me = lax.axis_index("ctx")
    core = lax.rem(me, 2)
    chip = me // 2
    return me, core, chip, me + 1 - 2 * core


def chip_at(chip, core, step):
    return 2 * lax.rem(chip + step + CHIPS, CHIPS) + core


def greet(devices):
    barrier = pltpu.get_barrier_semaphore()
    for device in devices:
        pl.semaphore_signal(barrier, inc=1, device_id=device, device_id_type=MESH)
    pl.semaphore_wait(barrier, len(devices))


def send(src, dst, send_sem, recv_sem, device):
    copy = pltpu.make_async_remote_copy(
        src_ref=src,
        dst_ref=dst,
        send_sem=send_sem,
        recv_sem=recv_sem,
        device_id=device,
        device_id_type=MESH,
    )
    copy.start()
    return copy


def comm_params(number):
    return pltpu.CompilerParams(
        collective_id=number, has_side_effects=True, vmem_limit_bytes=VMEM_BYTES
    )


def comm_cost(moved):
    return pl.CostEstimate(flops=0, bytes_accessed=moved * 30, transcendentals=0)


def in_vmem(count):
    return [pl.BlockSpec(memory_space=pltpu.VMEM)] * count


def gather_rows_kernel(depth, count, *refs):
    owns, outs = refs[:count], refs[count : 2 * count]
    z_sems, p_sems, f_sems = refs[2 * count :]
    me, core, chip, partner = plane_of()
    layer = lax.axis_index("fsdp")
    layers = [lax.rem(layer + d, depth) for d in range(1, depth)]
    peers = [chip_at(chip, core, j) for j in range(1, CHIPS)]
    greet([(me, other) for other in layers] + [(peer, layer) for peer in peers + [partner]])
    first, spread, passed = [], [], []
    for a, (own, out) in enumerate(zip(owns, outs)):
        for d, other in enumerate(layers):
            first.append(
                send(
                    own.at[me],
                    out.at[layer, me],
                    z_sems.at[0, a, d],
                    z_sems.at[1, a, d],
                    (me, other),
                )
            )
    for own, out in zip(owns, outs):
        for piece in range(SPAN):
            out[layer, piece] = own[piece]
    for a, out in enumerate(outs):
        for d in range(depth - 1):
            first[a * (depth - 1) + d].wait_recv()
            block = out.at[lax.rem(layer + depth - d - 1, depth), me]
            for j, peer in enumerate(peers):
                spread.append(
                    send(block, block, p_sems.at[0, a, d, j], p_sems.at[1, a, d, j], (peer, layer))
                )
            passed.append(
                send(block, block, f_sems.at[0, a, d, 3], f_sems.at[1, a, d, 3], (partner, layer))
            )
    arrivals = iter(spread)
    for a, out in enumerate(outs):
        for d in range(depth - 1):
            source = lax.rem(layer + depth - d - 1, depth)
            for j in range(CHIPS - 1):
                next(arrivals).wait_recv()
                block = out.at[source, chip_at(chip, core, -j - 1)]
                passed.append(
                    send(
                        block,
                        block,
                        f_sems.at[0, a, d, j],
                        f_sems.at[1, a, d, j],
                        (partner, layer),
                    )
                )
    for copy in first + spread:
        copy.wait_send()
    for copy in passed:
        copy.wait()


def gather_rows(arrays, depth):
    if lax.axis_size("ctx") != SPAN:
        return [lax.all_gather(own, "fsdp", axis=0) for own in arrays]
    count, pieces, outs = len(arrays), [], []
    for own in arrays:
        piece = (own.shape[0] // SPAN, own.shape[1])
        pieces.append(own.reshape(SPAN, *piece))
        outs.append(jax.ShapeDtypeStruct((depth, SPAN, *piece), own.dtype))
    whole = pl.pallas_call(
        functools.partial(gather_rows_kernel, depth, count),
        out_shape=tuple(outs),
        in_specs=in_vmem(count),
        out_specs=tuple(in_vmem(count)),
        scratch_shapes=[
            pltpu.SemaphoreType.DMA((2, count, depth - 1)),
            pltpu.SemaphoreType.DMA((2, count, depth - 1, CHIPS - 1)),
            pltpu.SemaphoreType.DMA((2, count, depth - 1, CHIPS)),
        ],
        compiler_params=comm_params(1),
        cost_estimate=comm_cost(sum(own.size for own in arrays) * 2 * depth),
    )(*pieces)
    return [full.reshape(depth, *own.shape) for full, own in zip(whole, arrays)]


def gather_plane_kernel(kv_ref, tag_ref, kv_out, tag_out, p_sems, f_sems):
    me, core, chip, partner = plane_of()
    layer = lax.axis_index("fsdp")
    peers = [chip_at(chip, core, j) for j in range(1, CHIPS)]
    greet([(peer, layer) for peer in peers + [partner]])
    pairs = ((kv_ref, kv_out), (tag_ref, tag_out))
    spread, passed = [], []
    for j, peer in enumerate(peers):
        for a, (own, out) in enumerate(pairs):
            spread.append(
                send(own, out.at[me], p_sems.at[0, a, j], p_sems.at[1, a, j], (peer, layer))
            )
    for a, (own, out) in enumerate(pairs):
        passed.append(
            send(own, out.at[me], f_sems.at[0, a, 3], f_sems.at[1, a, 3], (partner, layer))
        )
    kv_out[me] = kv_ref[...]
    tag_out[me] = tag_ref[...]
    for j in range(CHIPS - 1):
        for a, (own, out) in enumerate(pairs):
            spread[2 * j + a].wait_recv()
            block = out.at[chip_at(chip, core, -j - 1)]
            passed.append(
                send(block, block, f_sems.at[0, a, j], f_sems.at[1, a, j], (partner, layer))
            )
    for copy in spread:
        copy.wait_send()
    for copy in passed:
        copy.wait()


def gather_plane(kv, tags):
    if lax.axis_size("ctx") != SPAN:
        return tuple(lax.all_gather(part, "ctx", axis=0, tiled=True) for part in (kv, tags))
    rows, columns = kv.shape
    kv_all, tags_all = pl.pallas_call(
        gather_plane_kernel,
        out_shape=(
            jax.ShapeDtypeStruct((SPAN, rows, columns), kv.dtype),
            jax.ShapeDtypeStruct((SPAN, 1, rows), tags.dtype),
        ),
        in_specs=in_vmem(2),
        out_specs=tuple(in_vmem(2)),
        scratch_shapes=[
            pltpu.SemaphoreType.DMA((2, 2, CHIPS - 1)),
            pltpu.SemaphoreType.DMA((2, 2, CHIPS)),
        ],
        compiler_params=comm_params(2),
        cost_estimate=comm_cost(kv.size * 2 * SPAN),
    )(kv, tags[None])
    return kv_all.reshape(SPAN * rows, columns), tags_all.reshape(SPAN * rows)


def added(*parts):
    total = parts[0].astype(jnp.float32)
    for part in parts[1:]:
        total = total + part.astype(jnp.float32)
    return total


def across_of(chip, core, way):
    along_x, along_y = lax.rem(chip, 2), chip // 2
    along_x = 1 - along_x if way % 2 else along_x
    along_y = 1 - along_y if way // 2 else along_y
    return 2 * (2 * along_y + along_x) + core


def reduce_plane(arrays, h_sems, p_sems):
    me, core, chip, partner = plane_of()
    layer = lax.axis_index("fsdp")
    ways = (3, 1, 2, 0)
    near = (across_of(chip, core, 1), across_of(chip, core, 2))
    handed, started, last = [], [], []
    for a, (piece_of, halves, sums, arrived) in enumerate(arrays):
        for way in ways:
            handed.append(
                send(
                    piece_of(across_of(chip, 1 - core, way)),
                    halves.at[way],
                    h_sems.at[0, a, way],
                    h_sems.at[1, a, way],
                    (partner, layer),
                )
            )
    for a, (piece_of, halves, sums, arrived) in enumerate(arrays):
        middle = sums.shape[1] // 2
        sides = (pl.ds(0, middle), pl.ds(middle, middle))
        copies = {}

        def pass_on(way, side, slot, hop, a=a, sums=sums, arrived=arrived, sides=sides):
            number = 2 * slot + side
            return send(
                sums.at[way, sides[side]],
                arrived.at[slot, sides[side]],
                p_sems.at[0, a, number],
                p_sems.at[1, a, number],
                (near[hop], layer),
            )

        for j, way in enumerate(ways):
            handed[a * CHIPS + j].wait_recv()
            mine = piece_of(across_of(chip, core, way))

            def add_half(slab, carry, mine=mine, halves=halves, sums=sums, way=way):
                sums[way, slab] = added(mine[slab], halves[way, slab]).astype(sums.dtype)
                return carry

            lax.fori_loop(0, sums.shape[1], add_half, 0)
            if way == 3:
                for side in range(2):
                    copies[0, side] = pass_on(3, side, 0, side)
            elif way:
                copies[1, way - 1] = pass_on(way, way - 1, 1, way - 1)
        started.append((copies, pass_on))
    for (copies, pass_on), (_, _, sums, arrived) in zip(started, arrays):
        middle = sums.shape[1] // 2
        for side in range(2):
            copies[0, side].wait_recv()
            way = 2 - side

            def add_opposite(slab, carry, way=way, sums=sums, arrived=arrived):
                total = added(sums[way, slab], arrived[0, slab])
                sums[way, slab] = total.astype(sums.dtype)
                return carry

            lax.fori_loop(side * middle, (side + 1) * middle, add_opposite, 0)
            copies[2, side] = pass_on(way, side, 2, 1 - side)
        last.append([copies[slot, side] for slot in (1, 2) for side in range(2)])
    everything = handed + [copy for copies, _ in started for copy in copies.values()]
    return everything, last


def plane_total(sums, arrived, slab):
    return added(sums[0, slab], arrived[1, slab], arrived[2, slab])


def plane_scratch(block, dtype):
    return [
        pltpu.VMEM((CHIPS, *block), dtype),
        pltpu.VMEM((CHIPS, *block), dtype),
        pltpu.VMEM((CHIPS - 1, *block), dtype),
    ]


def turned_back(values, cos_tab, sin_tab):
    half_dim, parts = HEAD // 2, []
    for start in range(0, values.shape[1], HEAD):
        low = values[:, start : start + half_dim]
        high = values[:, start + half_dim : start + HEAD]
        parts += [low * cos_tab + high * sin_tab, high * cos_tab - low * sin_tab]
    return jnp.concatenate(parts, 1)


def scatter_plane_kernel(x_ref, cos_ref, sin_ref, out_ref, halves, sums, arrived, h_sems, p_sems):
    me, core, chip, partner = plane_of()
    layer = lax.axis_index("fsdp")
    near = [across_of(chip, core, way) for way in (1, 2)]
    greet([(peer, layer) for peer in near + [partner]])
    arrays = [(lambda piece: x_ref.at[piece], halves, sums, arrived)]
    started, last = reduce_plane(arrays, h_sems, p_sems)
    for copy in last[0]:
        copy.wait_recv()

    def add_slab(slab, carry):
        total = plane_total(sums, arrived, slab)
        kdim = KV_HEADS * HEAD
        keys = turned_back(total[:, :kdim], cos_ref[slab], sin_ref[slab])
        out_ref[slab] = jnp.concatenate([keys, total[:, kdim:]], 1).astype(out_ref.dtype)
        return carry

    lax.fori_loop(0, x_ref.shape[1], add_slab, 0)
    for copy in started:
        copy.wait_send()


def scatter_plane(values, cos_tab, sin_tab):
    if lax.axis_size("ctx") != SPAN:
        own = lax.psum_scatter(values, "ctx", scatter_dimension=0, tiled=True)
        own, kdim = own.astype(jnp.float32), KV_HEADS * HEAD
        keys = turned_back(own[:, :kdim], cos_tab, sin_tab)
        return jnp.concatenate([keys, own[:, kdim:]], 1).astype(values.dtype)
    rows, columns = values.shape
    slabs = 8
    block = (slabs, rows // SPAN // slabs, columns)
    return pl.pallas_call(
        scatter_plane_kernel,
        out_shape=jax.ShapeDtypeStruct(block, values.dtype),
        in_specs=in_vmem(3),
        out_specs=in_vmem(1)[0],
        scratch_shapes=plane_scratch(block, values.dtype)
        + [pltpu.SemaphoreType.DMA((2, 1, CHIPS)), pltpu.SemaphoreType.DMA((2, 1, 6))],
        compiler_params=comm_params(3),
        cost_estimate=comm_cost(values.size * 2),
    )(
        values.reshape(SPAN, *block),
        cos_tab.reshape(*block[:2], -1),
        sin_tab.reshape(*block[:2], -1),
    ).reshape(rows // SPAN, columns)


def reduce_direct(arrays, h_sems, p_sems):
    me, core, chip, partner = plane_of()
    layer = lax.axis_index("fsdp")
    handed, spread = [], []
    for a, (piece_of, halves, sums, arrived) in enumerate(arrays):
        for j in range(CHIPS):
            slot = (j + 1) % CHIPS
            handed.append(
                send(
                    piece_of(chip_at(chip, 1 - core, slot)),
                    halves.at[slot],
                    h_sems.at[0, a, slot],
                    h_sems.at[1, a, slot],
                    (partner, layer),
                )
            )
    for a, (piece_of, halves, sums, arrived) in enumerate(arrays):
        for j in range(CHIPS):
            slot = (j + 1) % CHIPS
            handed[a * CHIPS + j].wait_recv()
            mine = chip_at(chip, core, slot)

            def add_half(slab, carry, piece=piece_of(mine), halves=halves, sums=sums, slot=slot):
                sums[slot, slab] = added(piece[slab], halves[slot, slab]).astype(sums.dtype)
                return carry

            lax.fori_loop(0, sums.shape[1], add_half, 0)
            if slot:
                spread.append(
                    send(
                        sums.at[slot],
                        arrived.at[slot - 1],
                        p_sems.at[0, a, slot - 1],
                        p_sems.at[1, a, slot - 1],
                        (mine, layer),
                    )
                )
    return handed, spread


def direct_total(sums, arrived, slab):
    return added(sums[0, slab], *(arrived[j, slab] for j in range(CHIPS - 1)))


def reduce_rows_kernel(depth, count, *refs):
    inputs, outs, scratch = refs[:count], refs[count : 2 * count], refs[2 * count : 6 * count]
    h_sems, p_sems, z_sems, g_sems, f_sems = refs[6 * count :]
    me, core, chip, partner = plane_of()
    layer = lax.axis_index("fsdp")
    layers = [lax.rem(layer + d, depth) for d in range(1, depth)]
    peers = [chip_at(chip, core, j) for j in range(1, CHIPS)]
    greet([(me, other) for other in layers] + [(peer, layer) for peer in peers + [partner]])
    arrays, across = [], []
    for a, x_ref in enumerate(inputs):
        halves, sums, arrived, layers_ref = scratch[4 * a : 4 * a + 4]
        arrays.append((lambda piece, x_ref=x_ref: x_ref.at[:, piece], halves, sums, arrived))
        across.append(layers_ref)
    handed, spread = reduce_direct(arrays, h_sems, p_sems)
    moved = []
    for a, (_, _, sums, arrived) in enumerate(arrays):
        for copy in spread[a * (CHIPS - 1) : (a + 1) * (CHIPS - 1)]:
            copy.wait_recv()
        for d in list(range(1, depth)) + [0]:
            target = lax.rem(layer + d, depth)
            across[a][0, d] = direct_total(sums, arrived, target).astype(across[a].dtype)
            if d:
                moved.append(
                    send(
                        across[a].at[0, d],
                        across[a].at[1, d],
                        z_sems.at[0, a, d - 1],
                        z_sems.at[1, a, d - 1],
                        (me, target),
                    )
                )
    given, passed = [], []
    for a, out_ref in enumerate(outs):
        for copy in moved[a * (depth - 1) : (a + 1) * (depth - 1)]:
            copy.wait_recv()
        parts = [across[a][0, 0]] + [across[a][1, d] for d in range(1, depth)]
        out_ref[me] = added(*parts).astype(out_ref.dtype)
        mine = out_ref.at[me]
        for j, peer in enumerate(peers):
            given.append(send(mine, mine, g_sems.at[0, a, j], g_sems.at[1, a, j], (peer, layer)))
        passed.append(send(mine, mine, f_sems.at[0, a, 3], f_sems.at[1, a, 3], (partner, layer)))
    for a, out_ref in enumerate(outs):
        for j in range(CHIPS - 1):
            given[a * (CHIPS - 1) + j].wait_recv()
            block = out_ref.at[chip_at(chip, core, -j - 1)]
            passed.append(
                send(block, block, f_sems.at[0, a, j], f_sems.at[1, a, j], (partner, layer))
            )
    for copy in handed + spread + moved + given:
        copy.wait_send()
    for copy in passed:
        copy.wait()


def reduce_rows(arrays, number):
    if lax.axis_size("ctx") != SPAN:
        return [lax.psum(lax.psum_scatter(v, "fsdp", scatter_dimension=0), "ctx") for v in arrays]
    depth, count = arrays[0].shape[0], len(arrays)
    pieces, outs, scratch = [], [], []
    for values in arrays:
        _, rows, columns = values.shape
        piece = (rows // SPAN, columns)
        pieces.append(values.reshape(depth, SPAN, *piece))
        outs.append(jax.ShapeDtypeStruct((SPAN, *piece), values.dtype))
        scratch += plane_scratch((depth, *piece), values.dtype)
        scratch.append(pltpu.VMEM((2, depth, *piece), values.dtype))
    owned = pl.pallas_call(
        functools.partial(reduce_rows_kernel, depth, count),
        out_shape=tuple(outs),
        in_specs=in_vmem(count),
        out_specs=tuple(in_vmem(count)),
        scratch_shapes=scratch
        + [
            pltpu.SemaphoreType.DMA((2, count, CHIPS)),
            pltpu.SemaphoreType.DMA((2, count, CHIPS - 1)),
            pltpu.SemaphoreType.DMA((2, count, depth - 1)),
            pltpu.SemaphoreType.DMA((2, count, CHIPS - 1)),
            pltpu.SemaphoreType.DMA((2, count, CHIPS)),
        ],
        compiler_params=comm_params(number),
        cost_estimate=comm_cost(sum(values.size for values in arrays) * 2),
    )(*pieces)
    return [own.reshape(values.shape[1:]) for own, values in zip(owned, arrays)]


BLOCK = 128
LANES = (HEADS // KV_HEADS) * BLOCK


def dot(left, right, dims=(1, 0)):
    return lax.dot_general(
        left, right, (((dims[0],), (dims[1],)), ((), ())), preferred_element_type=jnp.float32
    )


def of_group(ref, group, at):
    first = group * (HEADS // KV_HEADS)
    heads = range(first, first + HEADS // KV_HEADS)
    return jnp.concatenate([ref[head * HEAD : (head + 1) * HEAD, at] for head in heads], 1)


def of_rows(ref, group, at):
    first = group * (HEADS // KV_HEADS)
    heads = range(first, first + HEADS // KV_HEADS)
    return jnp.concatenate([ref[head : head + 1, at] for head in heads], 1)


def columns_of(group, part):
    start = (part * KV_HEADS + group) * HEAD
    return slice(start, start + HEAD)


def mask_bias(tags, query_pos):
    tags = jnp.broadcast_to(tags, (BLOCK, BLOCK)).T
    key_pos = jnp.where(tags >= 0, tags, -tags - 1)
    allowed = (key_pos <= query_pos) & ((tags >= 0) | (key_pos == query_pos))
    bias = jnp.where(allowed, 0.0, negative)
    return jnp.concatenate([bias] * (HEADS // KV_HEADS), 1)


def attend_kernel(
    first_ref, q_ref, kv_ref, pos_ref, tag_ref, out_ref, log_ref, max_ref, sum_ref, acc_ref, kept
):
    blocks = kv_ref.shape[0] // BLOCK
    keep = kept.shape[0] == blocks

    def scores(group, at, rows, bias):
        keys = kv_ref[rows, columns_of(group, 0)]
        return dot(keys, of_group(q_ref, group, at)) + bias

    def query_block(qb, carry):
        at = pl.ds(pl.multiple_of(qb * BLOCK, BLOCK), BLOCK)
        max_ref[...] = jnp.full(max_ref.shape, negative, jnp.float32)
        sum_ref[...] = jnp.zeros(sum_ref.shape, jnp.float32)
        acc_ref[...] = jnp.zeros(acc_ref.shape, jnp.float32)
        limit = first_ref[blocks + qb]

        def find(kb, carry):
            @pl.when(first_ref[kb] <= limit)
            def _():
                rows = pl.ds(pl.multiple_of(kb * BLOCK, BLOCK), BLOCK)
                bias = mask_bias(tag_ref[kb], pos_ref[:, at])
                for group in range(KV_HEADS):
                    found = scores(group, at, rows, bias)
                    if keep:
                        kept[kb, group] = found
                    tops = jnp.max(found.reshape(BLOCK // 8, 8, LANES), 0)
                    max_ref[group] = jnp.maximum(max_ref[group], tops)

            return carry

        lax.fori_loop(0, blocks, find, 0)
        for group in range(KV_HEADS):
            top = jnp.max(max_ref[group], 0, keepdims=True)
            max_ref[group] = jnp.broadcast_to(top, max_ref.shape[1:])

        def gather(kb, carry):
            @pl.when(first_ref[kb] <= limit)
            def _():
                rows = pl.ds(pl.multiple_of(kb * BLOCK, BLOCK), BLOCK)
                bias = None if keep else mask_bias(tag_ref[kb], pos_ref[:, at])
                for group in range(KV_HEADS):
                    found = kept[kb, group] if keep else scores(group, at, rows, bias)
                    weights = jnp.exp(found - max_ref[group, :1])
                    sum_ref[group] += jnp.sum(weights.reshape(BLOCK // 8, 8, LANES), 0)
                    values = kv_ref[rows, columns_of(group, 1)]
                    acc_ref[group] += dot(values, weights.astype(jnp.bfloat16), (0, 0))

            return carry

        lax.fori_loop(0, blocks, gather, 0)
        for group in range(KV_HEADS):
            total = jnp.sum(sum_ref[group], 0, keepdims=True)
            attended = acc_ref[group] / total
            logs = max_ref[group, :1] + jnp.log(total)
            for j in range(HEADS // KV_HEADS):
                head = group * (HEADS // KV_HEADS) + j
                own = slice(j * BLOCK, (j + 1) * BLOCK)
                out_ref[head * HEAD : (head + 1) * HEAD, at] = attended[:, own]
                log_ref[head : head + 1, at] = logs[:, own]
        return carry

    lax.fori_loop(0, q_ref.shape[1] // BLOCK, query_block, 0)


def kernel_params():
    return pltpu.CompilerParams(vmem_limit_bytes=VMEM_BYTES)


def attend(firsts, queries, kv, query_pos, key_tags):
    blocks = kv.shape[0] // BLOCK
    slots = queries.shape[1]
    kept = blocks if blocks <= 16 else 1
    groups = (KV_HEADS, 8, LANES)
    work = 4 * kv.shape[0] * slots * HEADS * HEAD
    return pl.pallas_call(
        attend_kernel,
        out_shape=(
            jax.ShapeDtypeStruct(queries.shape, jnp.float32),
            jax.ShapeDtypeStruct((HEADS + 1, slots), jnp.float32),
        ),
        in_specs=[pl.BlockSpec(memory_space=pltpu.SMEM)] + in_vmem(4),
        out_specs=tuple(in_vmem(2)),
        scratch_shapes=[
            pltpu.VMEM(groups, jnp.float32),
            pltpu.VMEM(groups, jnp.float32),
            pltpu.VMEM((KV_HEADS, HEAD, LANES), jnp.float32),
            pltpu.VMEM((kept, KV_HEADS, BLOCK, LANES), jnp.float32),
        ],
        compiler_params=kernel_params(),
        cost_estimate=pl.CostEstimate(
            flops=work * 8, bytes_accessed=kv.size * 2, transcendentals=work // 256
        ),
    )(firsts, queries, kv, query_pos[None], key_tags.reshape(-1, 1, BLOCK))


def attend_back_kernel(
    first_ref, q_ref, kv_ref, pos_ref, tag_ref, grad_ref, log_ref, delta_ref, *refs
):
    blocks = kv_ref.shape[0] // BLOCK
    cos_ref, sin_ref, out_ref, dkv_ref, acc, dq_ref = refs
    dq_ref[...] = jnp.zeros(dq_ref.shape, dq_ref.dtype)

    def key_block(kb, carry):
        rows = pl.ds(pl.multiple_of(kb * BLOCK, BLOCK), BLOCK)
        acc[...] = jnp.zeros(acc.shape, jnp.float32)

        def query_block(qb, carry):
            @pl.when(first_ref[kb] <= first_ref[blocks + qb])
            def _():
                at = pl.ds(pl.multiple_of(qb * BLOCK, BLOCK), BLOCK)
                bias = mask_bias(tag_ref[kb], pos_ref[:, at])
                for group in range(KV_HEADS):
                    keys = kv_ref[rows, columns_of(group, 0)]
                    values = kv_ref[rows, columns_of(group, 1)]
                    queries = of_group(q_ref, group, at)
                    grads = of_group(grad_ref, group, at)
                    found = dot(keys, queries) + bias
                    probs = jnp.exp(found - of_rows(log_ref, group, at))
                    grad_probs = dot(values, grads)
                    grad_scores = probs * (grad_probs - of_rows(delta_ref, group, at))
                    grad_scores = grad_scores.astype(jnp.bfloat16)
                    acc[group] += dot(grad_scores, queries, (1, 1))
                    acc[KV_HEADS + group] += dot(probs.astype(jnp.bfloat16), grads, (1, 1))
                    grad_q = 0.125 * dot(keys, grad_scores, (0, 0))
                    for j in range(HEADS // KV_HEADS):
                        head = group * (HEADS // KV_HEADS) + j
                        own = slice(head * HEAD, (head + 1) * HEAD)
                        dq_ref[own, at] += grad_q[:, j * BLOCK : (j + 1) * BLOCK]

            return carry

        lax.fori_loop(0, q_ref.shape[1] // BLOCK, query_block, 0)
        dkv_ref[rows, :] = jnp.concatenate(
            [acc[index] for index in range(2 * KV_HEADS)], 1
        ).astype(dkv_ref.dtype)
        return carry

    lax.fori_loop(0, blocks, key_block, 0)
    half_dim = HEAD // 2

    def finish(qb, carry):
        at = pl.ds(pl.multiple_of(qb * BLOCK, BLOCK), BLOCK)
        cos_tab, sin_tab = cos_ref[:, at], sin_ref[:, at]
        for head in range(0, HEADS, 2):
            pair = []
            for start in range(head * HEAD, min(head + 2, HEADS) * HEAD, HEAD):
                low = dq_ref[start : start + half_dim, at]
                high = dq_ref[start + half_dim : start + HEAD, at]
                pair += [low * cos_tab + high * sin_tab, high * cos_tab - low * sin_tab]
            if len(pair) == 2:
                pair += [jnp.zeros_like(part) for part in pair]
            turned = jnp.concatenate(pair, 0).T
            own = slice(head * HEAD, head * HEAD + turned.shape[1])
            out_ref[at, own] = turned.astype(out_ref.dtype)
        return carry

    lax.fori_loop(0, q_ref.shape[1] // BLOCK, finish, 0)


def attend_back(firsts, queries, kv, query_pos, key_tags, grads, log_total, row_delta, tables):
    slots = queries.shape[1]
    work = 10 * kv.shape[0] * slots * HEADS * HEAD
    return pl.pallas_call(
        attend_back_kernel,
        out_shape=(
            jax.ShapeDtypeStruct((slots, -(-HEADS // 2) * 2 * HEAD), jnp.bfloat16),
            jax.ShapeDtypeStruct(kv.shape, jnp.bfloat16),
        ),
        in_specs=[pl.BlockSpec(memory_space=pltpu.SMEM)] + in_vmem(9),
        out_specs=tuple(in_vmem(2)),
        scratch_shapes=[
            pltpu.VMEM((2 * KV_HEADS, BLOCK, HEAD), jnp.float32),
            pltpu.VMEM(queries.shape, jnp.float32),
        ],
        compiler_params=kernel_params(),
        cost_estimate=pl.CostEstimate(
            flops=work * 6, bytes_accessed=kv.size * 4, transcendentals=work // 640
        ),
    )(firsts, queries, kv, query_pos[None], key_tags.reshape(-1, 1, BLOCK), grads, log_total, row_delta, *tables)


def on_device(
    tokens,
    w_query,
    w_key,
    w_value,
    w_out,
    w_gate,
    w_up,
    w_down,
    gain_attn,
    gain_ffn,
    router,
    cotangent,
    positions,
    lengths,
    chosen,
):
    hidden = tokens[0].astype(jnp.float32)
    row_count, width = hidden.shape
    qdim = HEADS * HEAD
    kdim = KV_HEADS * HEAD
    query_pos = positions[0]
    live = query_pos < lengths[0]
    selected = live & (chosen[0] == 1)
    live_mask = live.astype(jnp.float32)[:, None]
    chosen_mask = selected.astype(jnp.float32)[:, None]
    cos_tab, sin_tab = rope_tables(query_pos)
    key_tags = jnp.where(selected, query_pos, -query_pos - 1)
    depth = lax.axis_size("fsdp")
    own_rows = w_query.shape[0]
    w_out_full = lax.all_gather(w_out, "fsdp", axis=0, tiled=True)
    vectors = jnp.stack([gain_attn, gain_ffn, router], 1)
    own_attn = [padded_to(w_query, 1), jnp.concatenate([w_key, w_value, vectors], 1)]
    gathered = gather_rows([padded_to(own, 0) for own in own_attn], depth)
    padded_rows = gathered[0].shape[1]
    w_query = gathered[0].reshape(depth * padded_rows, -1)
    gathered = gathered[1][:, :own_rows].reshape(width, -1)
    w_kv, vectors = gathered[:, : 2 * kdim], gathered[:, 2 * kdim :]
    gain_one, gain_two, router_vec = vectors.T.astype(jnp.float32)
    gating = jax.nn.sigmoid(jnp.sum(hidden * router_vec, -1, keepdims=True))
    grad_y = cotangent[0].astype(jnp.float32) * live_mask
    grad_inc = grad_y * chosen_mask * gating
    grad_ffn = grad_inc.astype(jnp.bfloat16)
    grad_ffn_all = lax.all_gather(grad_ffn, "fsdp", axis=0, tiled=True)

    normed_one, inv_one = norm_forward(hidden, gain_one)
    normed_one = normed_one.astype(jnp.bfloat16)
    spread_one = padded_to(normed_one.reshape(row_count, depth, own_rows), -1)
    spread_one = spread_one.reshape(row_count, -1)
    query_raw = dot(w_query, spread_one, (0, 1))[:qdim]
    queries = rotate_columns(query_raw, cos_tab, sin_tab).astype(jnp.bfloat16) * 0.125
    kv_raw = dot(normed_one, w_kv)
    kv_own = jnp.concatenate([rotate(kv_raw[:, :kdim], cos_tab, sin_tab), kv_raw[:, kdim:]], 1)
    kv_all, tags_all = gather_plane(kv_own.astype(jnp.bfloat16), key_tags)
    first_tags = tags_all[::BLOCK]
    firsts = jnp.concatenate(
        [jnp.where(first_tags >= 0, first_tags, -first_tags - 1), query_pos[BLOCK - 1 :: BLOCK]]
    )
    attended, log_total = attend(firsts, queries, kv_all, query_pos, tags_all)
    attended, w_out_full = lax.optimization_barrier((attended, w_out_full))
    outcome = attended.astype(jnp.bfloat16)
    branch = dot(outcome, w_out_full, (0, 0))
    branch, grad_ffn_all = lax.optimization_barrier((branch, grad_ffn_all))
    middle = hidden + branch
    normed_two, inv_two = norm_forward(middle, gain_two)
    normed_two = normed_two.astype(jnp.bfloat16)
    normed_all = lax.all_gather(normed_two, "fsdp", axis=0, tiled=True)
    inner_act, grad_gate_act, grad_up_act, grad_normed_part = ffn_both(
        normed_all, grad_ffn_all, w_gate, w_up, w_down
    )
    grad_normed_two = lax.psum_scatter(
        grad_normed_part, "fsdp", scatter_dimension=0, tiled=True
    ).astype(jnp.float32)
    ffn_part = jnp.dot(inner_act, w_down, preferred_element_type=jnp.float32).astype(jnp.bfloat16)
    grad_wgate = lax.dot_general(
        grad_gate_act, normed_all, across_rows, preferred_element_type=jnp.float32
    )
    grad_wup = lax.dot_general(
        grad_up_act, normed_all, across_rows, preferred_element_type=jnp.float32
    )
    grad_wdown = lax.dot_general(
        inner_act, grad_ffn_all, across_rows, preferred_element_type=jnp.float32
    )
    low = jnp.bfloat16
    spread_out = padded_to(outcome.reshape(depth, own_rows, row_count), 1)
    grads = [grad.astype(low) for grad in (grad_wgate, grad_wup, grad_wdown)]
    grad_normed_two, ffn_part, spread_out, *grads = lax.optimization_barrier(
        (grad_normed_two, ffn_part, spread_out, *grads)
    )
    grad_normed_two, row_dot = grad_normed_two[:, :width], grad_normed_two[:, width:]
    totals = tuple(lax.psum(grad, "ctx") for grad in grads)
    grad_middle, grad_gain_two = norm_backward(middle, inv_two, gain_two, grad_normed_two)
    grad_branch = (grad_inc + grad_middle).astype(jnp.bfloat16)
    grad_attended = dot(w_out_full, grad_branch, (1, 1)).astype(jnp.bfloat16)
    grad_wout = dot(spread_out.reshape(-1, row_count), padded_to(grad_branch, 1)).astype(low)
    row_delta = jnp.sum(
        (grad_attended.astype(jnp.float32) * attended).reshape(HEADS, HEAD, row_count), 1
    )
    row_delta = jnp.pad(row_delta, ((0, 1), (0, 0)))
    grad_query_raw, grad_kv_all = attend_back(
        firsts,
        queries,
        kv_all,
        query_pos,
        tags_all,
        grad_attended,
        log_total,
        row_delta,
        (cos_tab.T, sin_tab.T),
    )
    grad_kv_raw = scatter_plane(grad_kv_all, cos_tab, sin_tab)
    grad_logit = (jnp.sum(grad_inc * branch, -1, keepdims=True) + row_dot) * (1.0 - gating)
    grad_router = jnp.sum(hidden * grad_logit, 0)
    grad_normed_one = dot(grad_query_raw, w_query, (1, 1)).reshape(row_count, depth, -1)
    grad_normed_one = grad_normed_one[..., :own_rows].reshape(row_count, width)
    grad_normed_one = grad_normed_one + dot(grad_kv_raw, w_kv, (1, 1))
    grad_wq = dot(spread_one, grad_query_raw, (0, 0)).astype(low)
    grad_wkv = dot(spread_one, grad_kv_raw, (0, 0)).astype(low)
    grad_hidden_one, grad_gain_one = norm_backward(hidden, inv_one, gain_one, grad_normed_one)
    grad_tokens = (grad_y + grad_logit * router_vec + grad_middle + grad_hidden_one).astype(
        jnp.bfloat16
    )
    vectors = jnp.stack([grad_gain_one, grad_gain_two, grad_router]).reshape(3, depth, own_rows)
    vectors = jnp.pad(vectors.transpose(1, 0, 2).reshape(depth, -1), ((0, 0), (0, -3 * own_rows % 1024)))
    vectors = jnp.pad(vectors.reshape(depth, -1, 1, 128), ((0, 0), (0, 0), (0, 7), (0, 0)))
    layered = [grad.reshape(depth, padded_rows, -1) for grad in (grad_wout, grad_wq, grad_wkv)]
    layered.insert(0, vectors.reshape(depth, -1, 128))
    owned = reduce_rows(layered, 4)
    ffn_out = lax.psum_scatter(ffn_part, "fsdp", scatter_dimension=0, tiled=True)
    *owned, totals = lax.optimization_barrier((*owned, totals))
    total_out, total_q, total_kv = (own[:own_rows].astype(jnp.float32) for own in owned[1:])
    total_q, total_out = total_q[:, :qdim], total_out[:, :width]
    total_k, total_v = total_kv[:, :kdim], total_kv[:, kdim:]
    mine = owned[0].reshape(-1, 8, 128)[:, 0].reshape(-1)[: 3 * own_rows].reshape(3, own_rows)
    totals = [total.astype(jnp.float32) for total in totals]
    ffn_out, *totals = lax.optimization_barrier((ffn_out, *totals))
    total_gate, total_up, total_down = totals
    increment = branch + ffn_out.astype(jnp.float32)
    block_out = live_mask * (hidden + chosen_mask * gating * increment)
    return (
        block_out.astype(jnp.bfloat16)[None],
        grad_tokens[None],
        total_q,
        total_k,
        total_v,
        total_out,
        total_gate,
        total_up,
        total_down,
        mine[0],
        mine[1],
        mine[2],
    )


def solution(mesh):
    in_specs = (
        P("fsdp", "ctx", None),
        P("fsdp", None),
        P("fsdp", None),
        P("fsdp", None),
        P("fsdp", None),
        P("fsdp", None),
        P("fsdp", None),
        P("fsdp", None),
        P("fsdp"),
        P("fsdp"),
        P("fsdp"),
        P("fsdp", "ctx", None),
        P("fsdp", "ctx"),
        P("fsdp"),
        P("fsdp", "ctx"),
    )
    out_specs = (
        P("fsdp", "ctx", None),
        P("fsdp", "ctx", None),
        P("fsdp", None),
        P("fsdp", None),
        P("fsdp", None),
        P("fsdp", None),
        P("fsdp", None),
        P("fsdp", None),
        P("fsdp", None),
        P("fsdp"),
        P("fsdp"),
        P("fsdp"),
    )
    return jax.shard_map(
        on_device, mesh=mesh, in_specs=in_specs, out_specs=out_specs, check_vma=False
    )
```
